16 devices in a mesh: dp: 2 (over y, z), tp: 8 (over x, core).
Axes of the slice: x: 4, y: 2, z: 1, core: 2. Of those that a mesh axis runs over, the one named last changes fastest.
The devices are a block of a 4x4x8 slice.
Arguments:
- x_in: bfloat16 [32, 512, 1024], P('dp', 'tp'), parts along dimension 0
- grad_y: bfloat16 [32, 512, 1024], P('dp', 'tp'), parts along dimension 0
- pad_mask: int32 [32, 512], P('dp'), parts along dimension 0
- ln1_gain: float32 [1024], replicated
- ln1_bias: float32 [1024], replicated
- w_qkv: bfloat16 [3, 1024, 16, 64], P(None, None, 'tp')
- b_qkv: float32 [3, 16, 64], P(None, 'tp')
- w_out: bfloat16 [16, 64, 1024], P('tp')
- b_out: float32 [1024], replicated
- ln2_gain: float32 [1024], replicated
- ln2_bias: float32 [1024], replicated
- w_up: bfloat16 [1024, 4096], P(None, 'tp')
- b_up: float32 [4096], P('tp')
- w_down: bfloat16 [4096, 1024], P('tp')
- b_down: float32 [1024], replicated
Outputs:
- output 1: bfloat16 [32, 512, 1024], P('dp', 'tp'), parts along dimension 0
- output 2: bfloat16 [32, 512, 1024], P('dp', 'tp'), parts along dimension 0
- output 3: float32 [2048], P('dp'), parts along dimension 0
- output 4: float32 [2048], P('dp'), parts along dimension 0
- output 5: float32 [6, 1024, 16, 64], P('dp', None, 'tp'), parts along dimension 0
- output 6: float32 [6, 16, 64], P('dp', 'tp'), parts along dimension 0
- output 7: float32 [32, 64, 1024], P(('dp', 'tp')), parts along dimension 0
- output 8: float32 [2048], P('dp'), parts along dimension 0
- output 9: float32 [2048], P('dp'), parts along dimension 0
- output 10: float32 [2048], P('dp'), parts along dimension 0
- output 11: float32 [2048, 4096], P('dp', 'tp'), parts along dimension 0
- output 12: float32 [8192], P(('dp', 'tp')), parts along dimension 0
- output 13: float32 [8192, 1024], P(('dp', 'tp')), parts along dimension 0
- output 14: float32 [2048], P('dp'), parts along dimension 0
There are 2 independent parts. The reference program is written for one: setup_inputs(seed, part) draws one part's arguments, and reference() takes and returns one part's arrays. A program takes and returns all parts, laid end to end along the dimension named above; an argument that names none is the same for every part.
All inputs are finite; a program needn't handle non-finite values.
Results may differ from the reference program's by a relative error of at most 0.0122089.
Values are sent between devices in bfloat16 or wider.
A program may use at most 768 MiB of HBM per device.

```python
import jax
import jax.numpy as jnp
from jax import lax

BATCH_SEQS = 16
SEQ_LEN = 512
MODEL_DIM = 1024
NUM_HEADS = 16
HEAD_DIM = 64
FFN_DIM = 4096
HALF_DIM = HEAD_DIM // 2
TOKENS = BATCH_SEQS * SEQ_LEN
LN_EPS = 1e-5
ROPE_BASE = 10000.0
INV_SQRT2 = 0.7071067811865476
INV_SQRT_2PI = 0.3989422804014327
NEG_LARGE = -1e30


def setup_inputs(seed: int = 0, part: int = 0) -> dict:
    root_key = jax.random.key(seed)
    shared_key, data_key = jax.random.split(root_key)
    weight_keys = jax.random.split(shared_key, 12)
    part_key = jax.random.fold_in(data_key, part)
    data_keys = jax.random.split(part_key, 4)
    tok_shape = (BATCH_SEQS, SEQ_LEN, MODEL_DIM)
    row_scale = 0.5 + jax.random.uniform(data_keys[0], (BATCH_SEQS, SEQ_LEN, 1), jnp.float32)
    x_in = (jax.random.normal(data_keys[1], tok_shape, jnp.float32) * row_scale).astype(jnp.bfloat16)
    grad_y = jax.random.normal(data_keys[2], tok_shape, jnp.float32).astype(jnp.bfloat16)
    lengths = jax.random.randint(data_keys[3], (BATCH_SEQS,), SEQ_LEN // 8, SEQ_LEN + 1)
    pad_mask = (jnp.arange(SEQ_LEN)[None, :] < lengths[:, None]).astype(jnp.int32)
    qkv_gain = jnp.array([1.5, 1.5, 1.0], jnp.float32)[:, None, None, None]
    w_qkv = jax.random.normal(weight_keys[0], (3, MODEL_DIM, NUM_HEADS, HEAD_DIM), jnp.float32) * qkv_gain * MODEL_DIM ** -0.5
    w_out = jax.random.normal(weight_keys[1], (NUM_HEADS, HEAD_DIM, MODEL_DIM), jnp.float32) * MODEL_DIM ** -0.5
    w_up = jax.random.normal(weight_keys[2], (MODEL_DIM, FFN_DIM), jnp.float32) * MODEL_DIM ** -0.5
    w_down = jax.random.normal(weight_keys[3], (FFN_DIM, MODEL_DIM), jnp.float32) * FFN_DIM ** -0.5
    return {
        'x_in': x_in,
        'grad_y': grad_y,
        'pad_mask': pad_mask,
        'ln1_gain': 1.0 + 0.2 * jax.random.normal(weight_keys[4], (MODEL_DIM,), jnp.float32),
        'ln1_bias': 0.2 * jax.random.normal(weight_keys[5], (MODEL_DIM,), jnp.float32),
        'w_qkv': w_qkv.astype(jnp.bfloat16),
        'b_qkv': 0.5 * jax.random.normal(weight_keys[6], (3, NUM_HEADS, HEAD_DIM), jnp.float32),
        'w_out': w_out.astype(jnp.bfloat16),
        'b_out': 0.3 * jax.random.normal(weight_keys[7], (MODEL_DIM,), jnp.float32),
        'ln2_gain': 1.0 + 0.2 * jax.random.normal(weight_keys[8], (MODEL_DIM,), jnp.float32),
        'ln2_bias': 0.2 * jax.random.normal(weight_keys[9], (MODEL_DIM,), jnp.float32),
        'w_up': w_up.astype(jnp.bfloat16),
        'b_up': 0.5 * jax.random.normal(weight_keys[10], (FFN_DIM,), jnp.float32),
        'w_down': w_down.astype(jnp.bfloat16),
        'b_down': 0.3 * jax.random.normal(weight_keys[11], (MODEL_DIM,), jnp.float32),
    }


def layer_norm(values, ln_gain, ln_bias):
    centered = values - jnp.mean(values, axis=-1, keepdims=True)
    inv_std = lax.rsqrt(jnp.mean(centered * centered, axis=-1, keepdims=True) + LN_EPS)
    x_hat = centered * inv_std
    return x_hat * ln_gain + ln_bias, x_hat, inv_std


def layer_norm_grad(d_out, x_hat, inv_std, ln_gain):
    d_hat = d_out * ln_gain
    return inv_std * (d_hat - jnp.mean(d_hat, axis=-1, keepdims=True) - x_hat * jnp.mean(d_hat * x_hat, axis=-1, keepdims=True))


def rope_tables():
    inv_freq = ROPE_BASE ** (-2.0 * jnp.arange(HALF_DIM, dtype=jnp.float32) / HEAD_DIM)
    angles = jnp.arange(SEQ_LEN, dtype=jnp.float32)[:, None] * inv_freq[None, :]
    angles = jnp.concatenate([angles, angles], axis=-1)
    return jnp.cos(angles)[:, None, :], jnp.sin(angles)[:, None, :]


def rotate(tensor, cos_tab, sin_tab):
    swapped = jnp.concatenate([-tensor[..., HALF_DIM:], tensor[..., :HALF_DIM]], axis=-1)
    return tensor * cos_tab + swapped * sin_tab


def rotate_back(grad_in, cos_tab, sin_tab):
    scaled = grad_in * sin_tab
    swapped = jnp.concatenate([scaled[..., HALF_DIM:], -scaled[..., :HALF_DIM]], axis=-1)
    return grad_in * cos_tab + swapped


def attention_probs(q_seq, k_seq, key_ok):
    scores = jnp.einsum('qhk,shk->hqs', q_seq.astype(jnp.float32), k_seq.astype(jnp.float32))
    return jax.nn.softmax(jnp.where(key_ok[None, None, :], scores, NEG_LARGE), axis=-1)


def seq_attention(operands):
    q_seq, k_seq, v_seq, key_ok = operands
    probs_low = attention_probs(q_seq, k_seq, key_ok).astype(jnp.bfloat16)
    return jnp.einsum('hqs,shk->qhk', probs_low.astype(jnp.float32), v_seq.astype(jnp.float32)).astype(jnp.bfloat16)


def seq_attention_grad(operands):
    q_seq, k_seq, v_seq, key_ok, d_out = operands
    attn_probs = attention_probs(q_seq, k_seq, key_ok)
    probs_low = attn_probs.astype(jnp.bfloat16).astype(jnp.float32)
    d_out_f = d_out.astype(jnp.float32)
    d_value = jnp.einsum('hqs,qhk->shk', probs_low, d_out_f)
    d_probs = jnp.einsum('qhk,shk->hqs', d_out_f, v_seq.astype(jnp.float32))
    d_scores = attn_probs * (d_probs - jnp.sum(d_probs * attn_probs, axis=-1, keepdims=True))
    d_scores_low = d_scores.astype(jnp.bfloat16).astype(jnp.float32)
    d_query = jnp.einsum('hqs,shk->qhk', d_scores_low, k_seq.astype(jnp.float32))
    d_key = jnp.einsum('hqs,qhk->shk', d_scores_low, q_seq.astype(jnp.float32))
    return d_query, d_key, d_value


def reference(x_in, grad_y, pad_mask, ln1_gain, ln1_bias, w_qkv, b_qkv, w_out, b_out, ln2_gain, ln2_bias, w_up, b_up, w_down, b_down):
    q_scale = HEAD_DIM ** -0.5
    cos_tab, sin_tab = rope_tables()
    key_ok = pad_mask > 0
    x_f = x_in.astype(jnp.float32)
    h1_f, x_hat1, inv_std1 = layer_norm(x_f, ln1_gain, ln1_bias)
    h1_b = h1_f.astype(jnp.bfloat16)
    qkv_all = jnp.einsum('bsd,idhk->ibshk', h1_b.astype(jnp.float32), w_qkv.astype(jnp.float32)) + b_qkv[:, None, None]
    q_rot = rotate(qkv_all[0] * q_scale, cos_tab, sin_tab).astype(jnp.bfloat16)
    k_rot = rotate(qkv_all[1], cos_tab, sin_tab).astype(jnp.bfloat16)
    v_heads = qkv_all[2].astype(jnp.bfloat16)
    attn_o = lax.map(seq_attention, (q_rot, k_rot, v_heads, key_ok))
    attn_sum = jnp.einsum('bshk,hkd->bsd', attn_o.astype(jnp.float32), w_out.astype(jnp.float32)) + b_out
    x1_f = (x_f + attn_sum).astype(jnp.bfloat16).astype(jnp.float32)
    h2_f, x_hat2, inv_std2 = layer_norm(x1_f, ln2_gain, ln2_bias)
    h2_flat = h2_f.astype(jnp.bfloat16).reshape(TOKENS, MODEL_DIM)
    pre_act = jnp.dot(h2_flat, w_up, preferred_element_type=jnp.float32) + b_up
    erf_term = lax.erf(pre_act * INV_SQRT2)
    act_b = (0.5 * pre_act * (1.0 + erf_term)).astype(jnp.bfloat16)
    gelu_slope = 0.5 * (1.0 + erf_term) + pre_act * jnp.exp(-0.5 * pre_act * pre_act) * INV_SQRT_2PI
    mlp_sum = jnp.dot(act_b, w_down, preferred_element_type=jnp.float32) + b_down
    y_out = (x1_f + mlp_sum.reshape(x_f.shape)).astype(jnp.bfloat16)
    dy_flat = grad_y.reshape(TOKENS, MODEL_DIM)
    dy_f = grad_y.astype(jnp.float32)
    grad_b_down = jnp.sum(dy_f, axis=(0, 1))
    grad_w_down = jnp.dot(act_b.T, dy_flat, preferred_element_type=jnp.float32)
    d_act = jnp.dot(dy_flat, w_down.T, preferred_element_type=jnp.float32)
    d_pre = d_act * gelu_slope
    grad_b_up = jnp.sum(d_pre, axis=0)
    d_pre_b = d_pre.astype(jnp.bfloat16)
    grad_w_up = jnp.dot(h2_flat.T, d_pre_b, preferred_element_type=jnp.float32)
    d_h2 = jnp.dot(d_pre_b, w_up.T, preferred_element_type=jnp.float32).reshape(x_f.shape)
    grad_ln2_gain = jnp.sum(d_h2 * x_hat2, axis=(0, 1))
    grad_ln2_bias = jnp.sum(d_h2, axis=(0, 1))
    d_x1 = dy_f + layer_norm_grad(d_h2, x_hat2, inv_std2, ln2_gain)
    grad_b_out = jnp.sum(d_x1, axis=(0, 1))
    d_x1_b = d_x1.astype(jnp.bfloat16).astype(jnp.float32)
    grad_w_out = jnp.einsum('bshk,bsd->hkd', attn_o.astype(jnp.float32), d_x1_b)
    d_attn_o = jnp.einsum('bsd,hkd->bshk', d_x1_b, w_out.astype(jnp.float32)).astype(jnp.bfloat16)
    d_query, d_key, d_value = lax.map(seq_attention_grad, (q_rot, k_rot, v_heads, key_ok, d_attn_o))
    d_qkv = jnp.stack([rotate_back(d_query, cos_tab, sin_tab) * q_scale, rotate_back(d_key, cos_tab, sin_tab), d_value])
    grad_b_qkv = jnp.sum(d_qkv, axis=(1, 2))
    d_qkv_b = d_qkv.astype(jnp.bfloat16).astype(jnp.float32)
    grad_w_qkv = jnp.einsum('bsd,ibshk->idhk', h1_b.astype(jnp.float32), d_qkv_b)
    d_h1 = jnp.einsum('ibshk,idhk->bsd', d_qkv_b, w_qkv.astype(jnp.float32))
    grad_ln1_gain = jnp.sum(d_h1 * x_hat1, axis=(0, 1))
    grad_ln1_bias = jnp.sum(d_h1, axis=(0, 1))
    grad_x = (d_x1 + layer_norm_grad(d_h1, x_hat1, inv_std1, ln1_gain)).astype(jnp.bfloat16)
    return (y_out, grad_x, grad_ln1_gain, grad_ln1_bias, grad_w_qkv, grad_b_qkv, grad_w_out, grad_b_out, grad_ln2_gain, grad_ln2_bias, grad_w_up, grad_b_up, grad_w_down, grad_b_down)
```

```python
import jax
import jax.numpy as jnp
from jax import lax
from jax.sharding import PartitionSpec as P

LN_EPS = 1e-5
ROPE_BASE = 10000.0
INV_SQRT2 = 0.7071067811865476
INV_SQRT_2PI = 0.3989422804014327
NEG_LARGE = -1e30
F32 = jnp.float32
BF16 = jnp.bfloat16


def layer_norm(values, ln_gain, ln_bias):
    centered = values - jnp.mean(values, axis=-1, keepdims=True)
    inv_std = lax.rsqrt(jnp.mean(centered * centered, axis=-1, keepdims=True) + LN_EPS)
    x_hat = centered * inv_std
    return x_hat * ln_gain + ln_bias, x_hat, inv_std


def layer_norm_grad(d_out, x_hat, inv_std, ln_gain):
    d_hat = d_out * ln_gain
    return inv_std * (d_hat - jnp.mean(d_hat, axis=-1, keepdims=True) - x_hat * jnp.mean(d_hat * x_hat, axis=-1, keepdims=True))


def rope_tables(seq_len, head_dim):
    half_dim = head_dim // 2
    inv_freq = ROPE_BASE ** (-2.0 * jnp.arange(half_dim, dtype=F32) / head_dim)
    angles = jnp.arange(seq_len, dtype=F32)[:, None] * inv_freq[None, :]
    angles = jnp.concatenate([angles, angles], axis=-1)
    return jnp.cos(angles)[:, None, :], jnp.sin(angles)[:, None, :]


def rotate(tensor, cos_tab, sin_tab):
    half_dim = tensor.shape[-1] // 2
    swapped = jnp.concatenate([-tensor[..., half_dim:], tensor[..., :half_dim]], axis=-1)
    return tensor * cos_tab + swapped * sin_tab


def rotate_back(grad_in, cos_tab, sin_tab):
    half_dim = grad_in.shape[-1] // 2
    scaled = grad_in * sin_tab
    swapped = jnp.concatenate([scaled[..., half_dim:], -scaled[..., :half_dim]], axis=-1)
    return grad_in * cos_tab + swapped


def dot(spec, a, b):
    return jnp.einsum(spec, a, b, preferred_element_type=F32)


def solution(mesh):
    n_tp = mesh.shape['tp']
    act_spec = P('dp', 'tp', None)
    rep_vec = P(None)
    part_vec = P('dp')
    in_specs = (act_spec, act_spec, P('dp', None), rep_vec, rep_vec, P(None, None, 'tp', None), P(None, 'tp', None),
                P('tp', None, None), rep_vec, rep_vec, rep_vec, P(None, 'tp'), P('tp'), P('tp', None), rep_vec)
    out_specs = (act_spec, act_spec, part_vec, part_vec, P('dp', None, 'tp', None), P('dp', 'tp', None),
                 P(('dp', 'tp'), None, None), part_vec, part_vec, part_vec, P('dp', 'tp'), P(('dp', 'tp')),
                 P(('dp', 'tp'), None), part_vec)

    def device_step(x_in, grad_y, pad_mask, ln1_gain, ln1_bias, w_qkv, b_qkv, w_out, b_out, ln2_gain, ln2_bias, w_up, b_up, w_down, b_down):
        batch, shard_len, dim = x_in.shape
        seq_len = pad_mask.shape[1]
        _, _, heads, head_dim = w_qkv.shape
        seqs = batch // n_tp
        ffn = w_up.shape[1]
        tok = seqs * seq_len
        me = lax.axis_index('tp')
        q_scale = head_dim ** -0.5

        def to_seq(t):
            return lax.all_to_all(t, 'tp', split_axis=0, concat_axis=1, tiled=True)

        def to_pos(t):
            return lax.all_to_all(t, 'tp', split_axis=1, concat_axis=0, tiled=True)

        def gather(t):
            return lax.all_gather(t, 'tp', axis=0, tiled=False)

        x_seq = to_seq(x_in)
        w_q3 = gather(w_qkv.transpose(0, 2, 3, 1).reshape(3, heads * head_dim, dim))
        small = gather(jnp.concatenate([b_qkv.reshape(-1), b_up]))
        b_qkv_all = small[:, :3 * heads * head_dim].reshape(n_tp, 3, 1, heads * head_dim)
        b_up_all = small[:, 3 * heads * head_dim:].reshape(-1)
        w_o = gather(w_out.reshape(heads * head_dim, dim)).reshape(-1, dim)
        w_u = gather(w_up)
        dy = to_seq(grad_y).reshape(tok, dim)
        w_d = gather(w_down).reshape(-1, dim)
        mask = lax.dynamic_slice_in_dim(pad_mask, me * seqs, seqs, 0)
        key_ok = (mask > 0)[None, :, None, None, :]
        cos_tab, sin_tab = rope_tables(seq_len, head_dim)

        x_f = x_seq.reshape(tok, dim).astype(F32)
        h1_f, x_hat1, inv_std1 = layer_norm(x_f, ln1_gain, ln1_bias)
        h1 = h1_f.astype(BF16)
        qkv = dot('td,gind->igtn', h1, w_q3) + b_qkv_all.swapaxes(0, 1)
        qkv = qkv.reshape(3, n_tp, seqs, seq_len, heads, head_dim)
        q_rot = rotate(qkv[0] * q_scale, cos_tab, sin_tab).astype(BF16)
        k_rot = rotate(qkv[1], cos_tab, sin_tab).astype(BF16)
        v_heads = qkv[2].astype(BF16)
        scores = dot('gbqhk,gbshk->gbhqs', q_rot, k_rot)
        probs = jax.nn.softmax(jnp.where(key_ok, scores, NEG_LARGE), axis=-1)
        probs_low = probs.astype(BF16)
        attn_o = dot('gbhqs,gbshk->bqghk', probs_low, v_heads).astype(BF16).reshape(tok, -1)
        x1_f = (x_f + (dot('tn,nd->td', attn_o, w_o) + b_out)).astype(BF16).astype(F32)
        h2_f, x_hat2, inv_std2 = layer_norm(x1_f, ln2_gain, ln2_bias)
        h2 = h2_f.astype(BF16)
        pre_act = dot('td,gdf->tgf', h2, w_u).reshape(tok, -1) + b_up_all
        erf_term = lax.erf(pre_act * INV_SQRT2)
        act_b = (0.5 * pre_act * (1.0 + erf_term)).astype(BF16)
        gelu_slope = 0.5 * (1.0 + erf_term) + pre_act * jnp.exp(-0.5 * pre_act * pre_act) * INV_SQRT_2PI

        def scatter(t):
            return lax.psum_scatter(t, 'tp', scatter_dimension=0, tiled=True)

        grad_w_down = scatter(dot('tf,td->fd', act_b, dy))
        d_pre = dot('td,fd->tf', dy, w_d) * gelu_slope
        d_pre_b = d_pre.astype(BF16).reshape(tok, n_tp, ffn)
        grad_w_up = scatter(dot('td,tgf->gdf', h2, d_pre_b).reshape(n_tp * dim, ffn))
        mlp_sum = dot('tf,fd->td', act_b, w_d)
        y_out = to_pos((x1_f + (mlp_sum + b_down)).astype(BF16).reshape(seqs, seq_len, dim))
        d_h2 = dot('tgf,gdf->td', d_pre_b, w_u)
        dy_f = dy.astype(F32)
        d_x1 = dy_f + layer_norm_grad(d_h2, x_hat2, inv_std2, ln2_gain)
        d_x1_b = d_x1.astype(BF16)
        grad_w_out = scatter(dot('tn,td->nd', attn_o, d_x1_b))
        d_o = dot('td,nd->tn', d_x1_b, w_o).astype(BF16).reshape(seqs, seq_len, n_tp, heads, head_dim)
        d_value = dot('gbhqs,bqghk->gbshk', probs_low, d_o)
        d_probs = dot('bqghk,gbshk->gbhqs', d_o, v_heads)
        d_scores = (probs * (d_probs - jnp.sum(d_probs * probs, axis=-1, keepdims=True))).astype(BF16)
        d_query = dot('gbhqs,gbshk->gbqhk', d_scores, k_rot)
        d_key = dot('gbhqs,gbqhk->gbshk', d_scores, q_rot)
        d_qkv = jnp.stack([rotate_back(d_query, cos_tab, sin_tab) * q_scale, rotate_back(d_key, cos_tab, sin_tab), d_value])
        d_qkv_b = d_qkv.astype(BF16).reshape(3, n_tp, tok, heads * head_dim)
        grad_w_qkv = scatter(dot('igtn,td->gind', d_qkv_b, h1).reshape(n_tp * 3 * heads * head_dim, dim))
        d_h1 = dot('igtn,gind->td', d_qkv_b, w_q3)
        grad_x = to_pos((d_x1 + layer_norm_grad(d_h1, x_hat1, inv_std1, ln1_gain)).astype(BF16).reshape(seqs, seq_len, dim))
        vec = jnp.concatenate([
            jnp.sum(d_h1 * x_hat1, axis=0), jnp.sum(d_h1, axis=0), jnp.sum(d_x1, axis=0),
            jnp.sum(d_h2 * x_hat2, axis=0), jnp.sum(d_h2, axis=0), jnp.sum(dy_f, axis=0)])
        part = jnp.concatenate([
            jnp.sum(d_qkv, axis=(2, 3)).swapaxes(0, 1).reshape(n_tp, -1),
            jnp.sum(d_pre, axis=0).reshape(n_tp, -1)], axis=1)
        total = lax.psum(jnp.concatenate([vec, part.reshape(-1)]), 'tp')
        vec = total[:6 * dim].reshape(6, dim)
        part = lax.dynamic_slice_in_dim(total[6 * dim:].reshape(n_tp, -1), me, 1, 0)[0]
        grad_b_qkv = part[:3 * heads * head_dim].reshape(3, heads, head_dim)
        grad_b_up = part[3 * heads * head_dim:]
        return (y_out, grad_x, vec[0], vec[1], grad_w_qkv.reshape(3, heads, head_dim, dim).transpose(0, 3, 1, 2), grad_b_qkv,
                grad_w_out.reshape(heads, head_dim, dim), vec[2], vec[3], vec[4], grad_w_up, grad_b_up, grad_w_down, vec[5])

    return jax.shard_map(device_step, mesh=mesh, in_specs=in_specs, out_specs=out_specs, check_vma=False)
```

```python
import functools

import jax
import jax.numpy as jnp
from jax import lax
from jax.experimental import pallas as pl
from jax.experimental.pallas import tpu as pltpu
from jax.sharding import PartitionSpec as P


LN_EPS = 1e-5
ROPE_BASE = 10000.0
INV_SQRT2 = 0.7071067811865476
INV_SQRT_2PI = 0.3989422804014327
NEG_LARGE = -1e30
F32 = jnp.float32
BF16 = jnp.bfloat16
MESH = pl.DeviceIdType.MESH
VMEM_LIMIT = 56 * 1024 * 1024
NN = (((1,), (0,)), ((), ()))
NT = (((1,), (1,)), ((), ()))
TN = (((0,), (0,)), ((), ()))


def mm(a, b, dims):
    return lax.dot_general(a, b, dims, preferred_element_type=F32)


def ln_stats(v):
    centered = v - jnp.mean(v, axis=-1, keepdims=True)
    inv_std = lax.rsqrt(jnp.mean(centered * centered, axis=-1, keepdims=True) + LN_EPS)
    return centered * inv_std, inv_std


def ln_grad(d_out, x_hat, inv_std, gain):
    d_hat = d_out * gain
    return inv_std * (d_hat - jnp.mean(d_hat, axis=-1, keepdims=True) - x_hat * jnp.mean(d_hat * x_hat, axis=-1, keepdims=True))


def low_half(shape, head_dim):
    lane = lax.broadcasted_iota(jnp.int32, shape, 1)
    return (lane % head_dim) < (head_dim // 2)


def swap_halves(t, head_dim):
    half = head_dim // 2
    width = t.shape[-1]
    return jnp.where(low_half(t.shape, head_dim), pltpu.roll(t, width - half, 1), pltpu.roll(t, half, 1))


def call(body, out_shape, grid, in_specs, out_specs, flops, nbytes, scratch=(), trans=0):
    return pl.pallas_call(
        body, out_shape=out_shape, grid=grid, in_specs=in_specs, out_specs=out_specs, scratch_shapes=scratch,
        compiler_params=pltpu.CompilerParams(dimension_semantics=('arbitrary',) * len(grid), vmem_limit_bytes=VMEM_LIMIT),
        cost_estimate=pl.CostEstimate(flops=flops, bytes_accessed=nbytes, transcendentals=trans))


def rep(shape):
    return pl.BlockSpec(shape, lambda *_: (0,) * len(shape))


def entry(x_in, small, n_tp):
    def body(x_src, b_src, x_out, b_out, x_send, x_recv, b_send, b_recv, own):
        me = lax.axis_index('tp')
        barrier = pltpu.get_barrier_semaphore()
        for j in range(1, n_tp):
            pl.semaphore_signal(barrier, inc=1, device_id={'tp': lax.rem(me + j, n_tp)}, device_id_type=MESH)
        pl.semaphore_wait(barrier, n_tp - 1)
        copies = []
        for j in range(1, n_tp):
            peer = lax.rem(me + j, n_tp)
            copies.append(pltpu.make_async_remote_copy(
                src_ref=b_src, dst_ref=b_out.at[me], send_sem=b_send.at[j], recv_sem=b_recv.at[j],
                device_id={'tp': peer}, device_id_type=MESH))
        for j in range(1, n_tp):
            peer = lax.rem(me + j, n_tp)
            copies.append(pltpu.make_async_remote_copy(
                src_ref=x_src.at[peer], dst_ref=x_out.at[me], send_sem=x_send.at[j], recv_sem=x_recv.at[j],
                device_id={'tp': peer}, device_id_type=MESH))
        for c in copies:
            c.start()
        mine = pltpu.make_async_copy(x_src.at[me], x_out.at[me], own)
        mine.start()
        b_out[me] = b_src[...]
        mine.wait()
        for c in copies:
            c.wait()

    sem = pltpu.SemaphoreType.DMA((n_tp,))
    return pl.pallas_call(
        body, out_shape=(jax.ShapeDtypeStruct(x_in.shape, x_in.dtype), jax.ShapeDtypeStruct((n_tp,) + small.shape, small.dtype)),
        in_specs=[pl.BlockSpec(memory_space=pl.ANY), pl.BlockSpec(memory_space=pltpu.VMEM)],
        out_specs=(pl.BlockSpec(memory_space=pl.ANY), pl.BlockSpec(memory_space=pltpu.VMEM)),
        scratch_shapes=[sem, sem, sem, sem, pltpu.SemaphoreType.DMA], name='entry',
        compiler_params=pltpu.CompilerParams(collective_id=0, has_side_effects=True, vmem_limit_bytes=VMEM_LIMIT),
        cost_estimate=pl.CostEstimate(flops=20_000_000_000, bytes_accessed=1 << 22, transcendentals=0))(x_in, small)


def qkv_body(hd, chunk, x_ref, w_ref, b_ref, cos_ref, sin_ref, gain_ref, bias_ref, h1_ref, q_ref, k_ref, v_ref):
    tok = x_ref.shape[0]
    width = q_ref.shape[2]

    @pl.when(pl.program_id(0) == 0)
    def _():
        @pl.loop(0, tok // 128)
        def _(i):
            rows = pl.ds(pl.multiple_of(i * 128, 128), 128)
            x_hat, _ = ln_stats(x_ref[rows, :].astype(F32))
            h1_ref[rows, :] = (x_hat * gain_ref[...] + bias_ref[...]).astype(BF16)

    @pl.loop(0, tok // chunk)
    def _(i):
        rows = pl.ds(pl.multiple_of(i * chunk, chunk), chunk)
        t = mm(h1_ref[rows, :], w_ref[0], NT) + b_ref[0]
        cos, sin = cos_ref[rows, :], sin_ref[rows, :]
        tq = t[:, :width] * (hd ** -0.5)
        tk = t[:, width:2 * width]
        q_ref[0, rows, :] = (tq * cos + swap_halves(tq, hd) * sin).astype(BF16)
        k_ref[0, rows, :] = (tk * cos + swap_halves(tk, hd) * sin).astype(BF16)
        v_ref[0, rows, :] = t[:, 2 * width:].astype(BF16)


def attn_fwd_body(hd, qc, len_ref, q_ref, k_ref, v_ref, o_ref, m_ref, l_ref):
    n_src, _, p_len, width = q_ref.shape[1:]
    seq = n_src * p_len
    heads = width // hd
    key_ok = lax.broadcasted_iota(jnp.int32, (seq, 1), 0) < len_ref[pl.program_id(1)]
    k = k_ref[...].reshape(seq, width)
    v_t = v_ref[...].reshape(seq, width).T
    lane = lax.broadcasted_iota(jnp.int32, (qc, width), 1)
    srcs = qc // p_len
    for c in range(seq // qc):
        q = q_ref[0, c * srcs:(c + 1) * srcs, 0].reshape(qc, width)
        outs = []
        for h in range(heads):
            q_h = jnp.where(lane // hd == h, q, jnp.zeros_like(q))
            s = jnp.where(key_ok, mm(k, q_h, NT), NEG_LARGE)
            m = jnp.max(s, axis=0, keepdims=True)
            e = jnp.exp(s - m)
            r = 1.0 / jnp.sum(e, axis=0, keepdims=True)
            p = (e * r).astype(BF16)
            outs.append(mm(v_t[h * hd:(h + 1) * hd], p, NN))
            m_ref[0, 0, h:h + 1, c * qc:(c + 1) * qc] = m
            l_ref[0, 0, h:h + 1, c * qc:(c + 1) * qc] = r
        o = jnp.concatenate(outs, axis=0).T.astype(BF16)
        o_ref[c * srcs:(c + 1) * srcs, 0] = o.reshape(srcs, p_len, width)


def attn_bwd_body(hd, qc, len_ref, q_ref, k_ref, v_ref, do_ref, m_ref, l_ref, cos_ref, sin_ref, d_ref, bsum_ref, dk_acc, dv_acc, dq_acc):
    n_src, _, p_len, width = q_ref.shape[1:]
    seq = n_src * p_len
    heads = width // hd
    key_ok = lax.broadcasted_iota(jnp.int32, (seq, 1), 0) < len_ref[pl.program_id(1)]
    k = k_ref[...].reshape(seq, width)
    v = v_ref[...].reshape(seq, width)
    k_t = k.T
    lane = lax.broadcasted_iota(jnp.int32, (qc, width), 1)
    srcs = qc // p_len
    for c in range(seq // qc):
        q = q_ref[0, c * srcs:(c + 1) * srcs, 0].reshape(qc, width)
        d_o = do_ref[c * srcs:(c + 1) * srcs, 0].reshape(qc, width)
        dk = jnp.zeros((seq, width), F32)
        dv = jnp.zeros((seq, width), F32)
        dqs = []
        for h in range(heads):
            mine = lane // hd == h
            q_h = jnp.where(mine, q, jnp.zeros_like(q))
            do_h = jnp.where(mine, d_o, jnp.zeros_like(d_o))
            cols = slice(c * qc, (c + 1) * qc)
            s = jnp.where(key_ok, mm(k, q_h, NT), NEG_LARGE)
            p = jnp.exp(s - m_ref[0, 0, h:h + 1, cols]) * l_ref[0, 0, h:h + 1, cols]
            dv += mm(p.astype(BF16), do_h, NN)
            dp = mm(v, do_h, NT)
            ds = (p * (dp - jnp.sum(dp * p, axis=0, keepdims=True))).astype(BF16)
            dk += mm(ds, q_h, NN)
            dqs.append(mm(k_t[h * hd:(h + 1) * hd], ds, NN))
        dq_acc[c * qc:(c + 1) * qc, :] = jnp.concatenate(dqs, axis=0).T
        if c == 0:
            dk_acc[...] = dk
            dv_acc[...] = dv
        else:
            dk_acc[...] += dk
            dv_acc[...] += dv
    cos, sin = cos_ref[...], sin_ref[...]
    dq, dk, dv = dq_acc[...], dk_acc[...], dv_acc[...]
    dtq = (dq * cos - swap_halves(dq, hd) * sin) * (hd ** -0.5)
    dtk = dk * cos - swap_halves(dk, hd) * sin
    for i, t in enumerate((dtq, dtk, dv)):
        d_ref[0, :, 0, :, i * width:(i + 1) * width] = t.astype(BF16).reshape(n_src, p_len, width)
        bsum_ref[0, 0, i:i + 1, :] = jnp.sum(t, axis=0, keepdims=True)


def proj_body(x_ref, o_ref, w_ref, bo_ref, gain_ref, bias_ref, x1_ref, h2_ref):
    w = w_ref[...].reshape(-1, w_ref.shape[2])
    x1 = (x_ref[...].astype(F32) + (mm(o_ref[...], w, NN) + bo_ref[...])).astype(BF16)
    x1_ref[...] = x1
    x_hat, _ = ln_stats(x1.astype(F32))
    h2_ref[...] = (x_hat * gain_ref[...] + bias_ref[...]).astype(BF16)


def up_body(chunk, h2_ref, w_ref, b_ref, dy_ref, act_ref, slope_ref, gw_ref):
    @pl.loop(0, h2_ref.shape[0] // chunk)
    def _(i):
        rows = pl.ds(pl.multiple_of(i * chunk, chunk), chunk)
        pre = mm(h2_ref[rows, :], w_ref[0], NN) + b_ref[0]
        erf_term = lax.erf(pre * INV_SQRT2)
        act_ref[rows, :] = (0.5 * pre * (1.0 + erf_term)).astype(BF16)
        slope_ref[rows, :] = 0.5 * (1.0 + erf_term) + pre * jnp.exp(-0.5 * pre * pre) * INV_SQRT_2PI

    gw_ref[0] = mm(act_ref[...], dy_ref[...], TN)


def dpre_body(chunk, dy_ref, w_ref, slope_ref, h2_ref, dpre_ref, gw_ref, gb_ref):
    gb_ref[...] = jnp.zeros_like(gb_ref)

    @pl.loop(0, dy_ref.shape[0] // chunk)
    def _(i):
        rows = pl.ds(pl.multiple_of(i * chunk, chunk), chunk)
        d_pre = mm(dy_ref[rows, :], w_ref[0], NT) * slope_ref[rows, :]
        gb_ref[0] += jnp.sum(d_pre, axis=0, keepdims=True)
        dpre_ref[rows, :] = d_pre.astype(BF16)

    gw_ref[0] = mm(h2_ref[...], dpre_ref[...], TN)


def down_body(chunk, act_ref, wd_ref, dpre_ref, wu_ref, x1_ref, dy_ref, wo_ref, bd_ref, gain_ref,
              y_ref, dx1_ref, dx1b_ref, do_ref, sums_ref, y_acc, dh_acc):
    g = pl.program_id(0)
    y_new = mm(act_ref[...], wd_ref[0], NN)
    dh_new = mm(dpre_ref[...], wu_ref[0], NT)

    @pl.when(g == 0)
    def _():
        y_acc[...] = y_new
        dh_acc[...] = dh_new

    @pl.when(g > 0)
    def _():
        y_acc[...] += y_new
        dh_acc[...] += dh_new

    @pl.when(g == pl.num_programs(0) - 1)
    def _():
        sums_ref[...] = jnp.zeros_like(sums_ref)

        @pl.loop(0, y_acc.shape[0] // chunk)
        def _(i):
            rows = pl.ds(pl.multiple_of(i * chunk, chunk), chunk)
            x1 = x1_ref[rows, :].astype(F32)
            dy = dy_ref[rows, :].astype(F32)
            dh = dh_acc[rows, :]
            y_ref[rows, :] = (x1 + (y_acc[rows, :] + bd_ref[...])).astype(BF16)
            x_hat, inv_std = ln_stats(x1)
            d_x1 = dy + ln_grad(dh, x_hat, inv_std, gain_ref[...])
            dx1_ref[rows, :] = d_x1
            low = d_x1.astype(BF16)
            dx1b_ref[rows, :] = low
            do_ref[rows, :] = mm(low, wo_ref[...].reshape(-1, wo_ref.shape[2]), NT).astype(BF16)
            for n, t in enumerate((d_x1, dh * x_hat, dh, dy)):
                sums_ref[n:n + 1, :] += jnp.sum(t, axis=0, keepdims=True)


def final_body(n_tp, chunk, d_ref, w_ref, h1_ref, o_ref, dx1b_ref, dx1_ref, x_ref, gain_ref, sums_ref, bsum_ref, gb_ref,
               gx_ref, gw_ref, dh_acc, vec):
    s = pl.program_id(0)
    n3 = d_ref.shape[2]
    width = o_ref.shape[1]
    n_b = bsum_ref.shape[2]

    @pl.when(s == 0)
    def _():
        dh_acc[...] = mm(d_ref[0], w_ref[0], NN)

    @pl.when(jnp.logical_and(s > 0, s < n_tp))
    def _():
        dh_acc[...] += mm(d_ref[0], w_ref[0], NN)

    @pl.when(s == n_tp - 1)
    def _():
        vec[...] = jnp.zeros_like(vec)
        vec[2:6, :] = sums_ref[0:4, :]

        @pl.loop(0, dh_acc.shape[0] // chunk)
        def _(i):
            rows = pl.ds(pl.multiple_of(i * chunk, chunk), chunk)
            x_hat, inv_std = ln_stats(x_ref[rows, :].astype(F32))
            dh = dh_acc[rows, :]
            gx_ref[rows, :] = (dx1_ref[rows, :] + ln_grad(dh, x_hat, inv_std, gain_ref[...])).astype(BF16)
            vec[0:1, :] += jnp.sum(dh * x_hat, axis=0, keepdims=True)
            vec[1:2, :] += jnp.sum(dh, axis=0, keepdims=True)

    @pl.when(s >= n_tp)
    def _():
        gw_ref[0, 0:n3, :] = mm(d_ref[0], h1_ref[...], TN)
        gw_ref[0, n3:n3 + width, :] = mm(o_ref[...], dx1b_ref[...], TN)
        gw_ref[0, n3 + width:, :] = vec[...]
        gw_ref[0, n3 + width + 6:n3 + width + 7, 0:n_b] = bsum_ref[0]
        gw_ref[0, n3 + width + 6:n3 + width + 7, n_b:n_b + gb_ref.shape[2]] = gb_ref[0]


def rope_tables(seq_len, head_dim):
    half_dim = head_dim // 2
    inv_freq = ROPE_BASE ** (-2.0 * jnp.arange(half_dim, dtype=F32) / head_dim)
    angles = jnp.arange(seq_len, dtype=F32)[:, None] * inv_freq[None, :]
    cos, sin = jnp.cos(angles), jnp.sin(angles)
    return jnp.concatenate([cos, cos], axis=-1), jnp.concatenate([-sin, sin], axis=-1)


def solution(mesh):
    n_tp = mesh.shape['tp']
    act_spec = P('dp', 'tp', None)
    rep_vec = P(None)
    part_vec = P('dp')
    in_specs = (act_spec, act_spec, P('dp', None), rep_vec, rep_vec, P(None, None, 'tp', None), P(None, 'tp', None),
                P('tp', None, None), rep_vec, rep_vec, rep_vec, P(None, 'tp'), P('tp'), P('tp', None), rep_vec)
    out_specs = (act_spec, act_spec, part_vec, part_vec, P('dp', None, 'tp', None), P('dp', 'tp', None),
                 P(('dp', 'tp'), None, None), part_vec, part_vec, part_vec, P('dp', 'tp'), P(('dp', 'tp')),
                 P(('dp', 'tp'), None), part_vec)

    def device_step(x_in, grad_y, pad_mask, ln1_gain, ln1_bias, w_qkv, b_qkv, w_out, b_out, ln2_gain, ln2_bias, w_up, b_up, w_down, b_down):
        batch, p_len, dim = x_in.shape
        seq_len = pad_mask.shape[1]
        _, _, heads, hd = w_qkv.shape
        seqs = batch // n_tp
        ffn = w_up.shape[1]
        width = heads * hd
        n3 = 3 * width
        tok = seqs * seq_len
        me = lax.axis_index('tp')
        sds = jax.ShapeDtypeStruct

        def exchange(t):
            return lax.all_to_all(t, 'tp', split_axis=0, concat_axis=0, tiled=True)

        w_att = jnp.concatenate([w_qkv.transpose(0, 2, 3, 1).reshape(n3, dim), w_out.reshape(width, dim)], axis=0)
        w_att = lax.all_gather(w_att, 'tp', axis=0, tiled=False)
        pad = -(n3 + ffn) % 1024
        small = jnp.concatenate([b_qkv.reshape(-1), b_up, jnp.zeros((pad,), F32)]).reshape(-1, 128)
        x, small = entry(x_in.reshape(n_tp, seqs * p_len, dim), small, n_tp)
        x = x.reshape(tok, dim)
        small = small.reshape(n_tp, 1, -1)
        b_att, b_ffn = small[:, :, :n3], small[:, :, n3:n3 + ffn]
        w_u = lax.all_gather(w_up, 'tp', axis=0, tiled=False)
        x, grad_y = lax.optimization_barrier((x, grad_y))
        dy = exchange(grad_y).reshape(tok, dim)
        w_d = lax.all_gather(w_down, 'tp', axis=0, tiled=False)
        lens = jnp.sum((lax.dynamic_slice_in_dim(pad_mask, me * seqs, seqs, 0) > 0).astype(jnp.int32), axis=1)
        cos, sin = rope_tables(seq_len, hd)
        cos, sin = jnp.tile(cos, (1, heads)), jnp.tile(sin, (1, heads))

        def by_token(t):
            return jnp.broadcast_to(t.reshape(n_tp, 1, p_len, width), (n_tp, seqs, p_len, width)).reshape(tok, width)

        row = lambda t: t.reshape(1, dim)
        full = rep((tok, dim))
        vec = rep((1, dim))
        per_head = pl.BlockSpec((1, tok, width), lambda g: (g, 0, 0))
        w_spec = pl.BlockSpec((1, n3, dim), lambda g: (g, 0, 0))
        h1, q, k, v = call(
            functools.partial(qkv_body, hd, 256),
            (sds((tok, dim), BF16),) + (sds((n_tp, tok, width), BF16),) * 3, (n_tp,),
            [full, w_spec, pl.BlockSpec((1, 1, n3), lambda g: (g, 0, 0)), rep((tok, width)), rep((tok, width)), vec, vec],
            (full, per_head, per_head, per_head), 2 * tok * dim * n3 * n_tp, 2 * (tok * dim * 5 + n_tp * n3 * dim),
        )(x, w_att, b_att, by_token(cos), by_token(sin), row(ln1_gain), row(ln1_bias))

        five = (n_tp, n_tp, seqs, p_len, width)
        q5, k5, v5 = (t.reshape(five) for t in (q, k, v))
        head_blk = pl.BlockSpec((1, n_tp, 1, p_len, width), lambda g, b, *_: (g, 0, b, 0, 0))
        o_blk = pl.BlockSpec((n_tp, 1, p_len, width), lambda g, b, *_: (0, b, 0, g))
        stat_blk = pl.BlockSpec((1, 1, heads, seq_len), lambda g, b, *_: (g, b, 0, 0))
        stat = sds((n_tp, seqs, heads, seq_len), F32)
        att_flops = n_tp * seqs * heads * seq_len * seq_len * hd * 2
        o, m_stat, l_stat = pl.pallas_call(
            functools.partial(attn_fwd_body, hd, 256), name='attn_fwd',
            out_shape=(sds((n_tp, seqs, p_len, n_tp * width), BF16), stat, stat),
            grid_spec=pltpu.PrefetchScalarGridSpec(
                num_scalar_prefetch=1, grid=(n_tp, seqs), in_specs=[head_blk] * 3, out_specs=(o_blk, stat_blk, stat_blk)),
            compiler_params=pltpu.CompilerParams(dimension_semantics=('arbitrary', 'arbitrary'), vmem_limit_bytes=VMEM_LIMIT),
            cost_estimate=pl.CostEstimate(flops=8 * att_flops, bytes_accessed=8 * tok * dim, transcendentals=att_flops // 128),
        )(lens, q5, k5, v5)
        o = o.reshape(tok, n_tp * width)

        rows = pl.BlockSpec((256, dim), lambda i: (i, 0))
        wo_spec = pl.BlockSpec((n_tp, width, dim), lambda *_: (0, n3 // width, 0))
        x1, h2 = call(proj_body, (sds((tok, dim), BF16),) * 2, (tok // 256,), [rows, rows, wo_spec, vec, vec, vec], (rows, rows),
                      2 * tok * dim * dim, 8 * tok * dim)(x, o, w_att, row(b_out), row(ln2_gain), row(ln2_bias))

        cols = pl.BlockSpec((tok, ffn), lambda g: (0, g))
        wu_spec = pl.BlockSpec((1, dim, ffn), lambda g: (g, 0, 0))
        wd_spec = pl.BlockSpec((1, ffn, dim), lambda g: (g, 0, 0))
        b_spec = pl.BlockSpec((1, 1, ffn), lambda g: (g, 0, 0))
        mlp_flops = 2 * tok * dim * ffn * n_tp
        act, slope, gw_down = call(
            functools.partial(up_body, 512), (sds((tok, n_tp * ffn), BF16), sds((tok, n_tp * ffn), F32), sds((n_tp, ffn, dim), F32)), (n_tp,),
            [full, wu_spec, b_spec, full], (cols, cols, wd_spec), 2 * mlp_flops, 60 << 20)(h2, w_u, b_ffn, dy)
        scatter = lambda t: lax.psum_scatter(t.reshape(-1, t.shape[-1]), 'tp', scatter_dimension=0, tiled=True)
        grad_w_down = scatter(gw_down)
        d_pre, gw_up, gb_up = call(
            functools.partial(dpre_body, 512), (sds((tok, n_tp * ffn), BF16), sds((n_tp, dim, ffn), F32), sds((n_tp, 1, ffn), F32)), (n_tp,),
            [full, wd_spec, cols, full], (cols, wu_spec, b_spec), 2 * mlp_flops, 60 << 20)(dy, w_d, slope, h2)
        grad_w_up = scatter(gw_up)
        y, d_x1, d_x1b, d_o, sums = call(
            functools.partial(down_body, 256),
            (sds((tok, dim), BF16), sds((tok, dim), F32), sds((tok, dim), BF16), sds((tok, n_tp * width), BF16), sds((8, dim), F32)), (n_tp,),
            [cols, wd_spec, cols, wu_spec, full, full, wo_spec, vec, vec],
            (full, full, full, full, rep((8, dim))), 2 * mlp_flops, 60 << 20,
            scratch=[pltpu.VMEM((tok, dim), F32), pltpu.VMEM((tok, dim), F32)],
        )(act, w_d, d_pre, w_u, x1, dy, w_att, row(b_down), row(ln2_gain))
        y_out = exchange(y.reshape(batch, p_len, dim))

        d_qkv, bsum = pl.pallas_call(
            functools.partial(attn_bwd_body, hd, 256), name='attn_bwd',
            out_shape=(sds((n_tp, n_tp, seqs, p_len, n3), BF16), sds((n_tp, seqs, 3, width), F32)),
            grid_spec=pltpu.PrefetchScalarGridSpec(
                num_scalar_prefetch=1, grid=(n_tp, seqs),
                in_specs=[head_blk] * 3 + [o_blk, stat_blk, stat_blk, rep((seq_len, width)), rep((seq_len, width))],
                out_specs=(pl.BlockSpec((1, n_tp, 1, p_len, n3), lambda g, b, *_: (g, 0, b, 0, 0)),
                           pl.BlockSpec((1, 1, 3, width), lambda g, b, *_: (g, b, 0, 0))),
                scratch_shapes=[pltpu.VMEM((seq_len, width), F32)] * 3),
            compiler_params=pltpu.CompilerParams(dimension_semantics=('arbitrary', 'arbitrary'), vmem_limit_bytes=VMEM_LIMIT),
            cost_estimate=pl.CostEstimate(flops=20 * att_flops, bytes_accessed=16 * tok * dim, transcendentals=att_flops // 128),
        )(lens, q5, k5, v5, d_o.reshape(n_tp, seqs, p_len, n_tp * width), m_stat, l_stat, cos, sin)

        y_out, d_qkv = lax.optimization_barrier((y_out, d_qkv))
        first = lambda s: (jnp.minimum(s, n_tp - 1), 0, 0)
        second = lambda s: jnp.maximum(s - n_tp, 0)
        n_rows = n3 + width + 8
        grad_x, gw_att = call(
            functools.partial(final_body, n_tp, 256), (sds((tok, dim), BF16), sds((n_tp, n_rows, dim), F32)), (2 * n_tp,),
            [pl.BlockSpec((1, tok, n3), lambda s: (lax.rem(s, n_tp), 0, 0)), pl.BlockSpec((1, n3, dim), first), full,
             pl.BlockSpec((tok, width), lambda s: (0, second(s))), full, full, full, vec, rep((8, dim)),
             pl.BlockSpec((1, 1, n3), lambda s: (second(s), 0, 0)), pl.BlockSpec((1, 1, ffn), lambda s: (second(s), 0, 0))],
            (full, pl.BlockSpec((1, n_rows, dim), lambda s: (second(s), 0, 0))), 2 * tok * dim * (2 * n3 + width) * n_tp, 40 << 20,
            scratch=[pltpu.VMEM((tok, dim), F32), pltpu.VMEM((8, dim), F32)],
        )(d_qkv.reshape(n_tp, tok, n3), w_att, h1, o, d_x1b, d_x1, x, row(ln1_gain), sums,
          jnp.sum(bsum, axis=1).reshape(n_tp, 1, n3), gb_up)
        grad_x = exchange(grad_x.reshape(batch, p_len, dim))
        tail = scatter(gw_att)
        grad_w_qkv = tail[:n3].reshape(3, heads, hd, dim).transpose(0, 3, 1, 2)
        grad_w_out = tail[n3:n3 + width].reshape(heads, hd, dim)
        vecs = tail[n3 + width:]
        grad_b_qkv = vecs[6, :n3].reshape(3, heads, hd)
        grad_b_up = vecs[6, n3:n3 + ffn]
        return (y_out, grad_x, vecs[0], vecs[1], grad_w_qkv, grad_b_qkv, grad_w_out, vecs[2], vecs[3], vecs[4], grad_w_up,
                grad_b_up, grad_w_down, vecs[5])

    return jax.shard_map(device_step, mesh=mesh, in_specs=in_specs, out_specs=out_specs, check_vma=False)
```

```python
import functools

import jax
import jax.numpy as jnp
from jax import lax
from jax.experimental import pallas as pl
from jax.experimental.pallas import tpu as pltpu
from jax.sharding import PartitionSpec as P

LN_EPS = 1e-5
ROPE_BASE = 10000.0
INV_SQRT2 = 0.7071067811865476
INV_SQRT_2PI = 0.3989422804014327
NEG_LARGE = -1e30
F32 = jnp.float32
BF16 = jnp.bfloat16
VMEM_LIMIT = 66_500_000
LANES = 128
NN = (((1,), (0,)), ((), ()))
NT = (((1,), (1,)), ((), ()))
TN = (((0,), (0,)), ((), ()))
ANY = pl.BlockSpec(memory_space=pl.ANY)


def mm(a, b, dims):
    return lax.dot_general(a, b, dims, preferred_element_type=F32)


def ln_stats(v):
    centered = v - jnp.mean(v, axis=-1, keepdims=True)
    inv_std = lax.rsqrt(jnp.mean(centered * centered, axis=-1, keepdims=True) + LN_EPS)
    return centered * inv_std, inv_std


def ln_grad(d_out, x_hat, inv_std, gain):
    d_hat = d_out * gain
    return inv_std * (d_hat - jnp.mean(d_hat, axis=-1, keepdims=True) - x_hat * jnp.mean(d_hat * x_hat, axis=-1, keepdims=True))


def col_sum(t):
    return jnp.sum(t, axis=0, keepdims=True)


def swap_halves(t, head_dim):
    half = head_dim // 2
    lane = lax.broadcasted_iota(jnp.int32, t.shape, t.ndim - 1)
    return jnp.where(lane % head_dim < half, pltpu.roll(t, t.shape[-1] - half, t.ndim - 1), pltpu.roll(t, half, t.ndim - 1))


def span(i, n):
    return pl.ds(pl.multiple_of(i * n, n), n)


def loop_rows(total, n, body):
    @pl.loop(0, total // n)
    def _(i):
        body(span(i, n))


class Net:
    def __init__(self, n_tp, send, recv, local):
        self.n_tp, self.send, self.recv, self.local = n_tp, send, recv, local
        self.copies, self.count, self.n_local = {}, 0, 0

    def peer(self, chip, core):
        me = lax.axis_index('tp')
        at = lax.rem(me + 2 * chip, self.n_tp) if chip else me
        return at + 1 - 2 * lax.rem(at, 2) if core else at

    def add(self, name, src, dst, chip, core=0):
        n = self.count
        self.count += 1

        def make():
            return pltpu.make_async_remote_copy(
                src_ref=src(), dst_ref=dst(), send_sem=self.send.at[n], recv_sem=self.recv.at[n],
                device_id={'tp': self.peer(chip, core)}, device_id_type=pl.DeviceIdType.MESH)

        self.copies.setdefault(name, []).append(make)

    def add_local(self, name, src, dst):
        n = self.n_local
        self.n_local += 1
        self.copies.setdefault(name, []).append(lambda: pltpu.make_async_copy(src(), dst(), self.local.at[n]))

    def start(self, *names):
        for name in names:
            for make in self.copies[name]:
                make().start()

    def got(self, *names):
        for name in names:
            for make in self.copies[name]:
                make().wait_recv()

    def sent(self, *names):
        for name in names:
            for make in self.copies[name]:
                make().wait_send()

    def done(self, *names):
        for name in names:
            for make in self.copies[name]:
                make().wait()

    def gather(self, name, own, buf):
        rows = own.shape[0]
        top, bot, whole = pl.ds(0, rows // 2), pl.ds(rows // 2, rows // 2), pl.ds(0, rows)

        def put(stage, src, slot, part, chip, core=0):
            take = (lambda: own.at[part]) if src is None else (lambda: buf.at[src, part])
            self.add(name + stage, take, lambda: buf.at[slot, part], chip, core)

        put('_a', None, 6, top, 1)
        put('_a', None, 2, bot, 3)
        put('_b', None, 6, bot, 1)
        put('_b', None, 2, top, 3)
        put('_b', None, 1, whole, 0, 1)
        put('_relay', 6, 4, top, 1)
        put('_relay', 2, 4, bot, 3)
        put('_fwd', 6, 7, whole, 0, 1)
        put('_fwd', 2, 3, whole, 0, 1)
        put('_last', 4, 5, whole, 0, 1)

    def exchange(self, name, src, dst, rows):
        me = lax.axis_index('tp')
        for core in range(2):
            for chip in (1, 3, 2, 0):
                if chip + core:
                    self.add(name, lambda c=chip, k=core: src.at[span(self.peer(c, k), rows)], lambda: dst.at[span(me, rows)], chip, core)
        self.add_local(name + '_own', lambda: src.at[span(me, rows)], lambda: dst.at[span(me, rows)])

    def scatter(self, name, p, got, summed, out):
        half = p.shape[1] // 2
        top, bot = pl.ds(0, half), pl.ds(half, half)
        self.add(name + '_relay', lambda: p.at[2, top], lambda: got.at[0], 1)
        self.add(name + '_relay', lambda: p.at[2, bot], lambda: got.at[1], 3)
        self.add(name + '_next', lambda: p.at[1, bot], lambda: out.at[0, bot], 1)
        self.add(name + '_prev', lambda: p.at[3, top], lambda: out.at[1, top], 3)
        self.add(name + '_sum', lambda: summed.at[0], lambda: out.at[0, top], 1)
        self.add(name + '_sum', lambda: summed.at[1], lambda: out.at[1, bot], 3)


def solution(mesh):
    n_tp = mesh.shape['tp']
    n_chips = n_tp // 2
    act_spec = P('dp', 'tp', None)
    rep_vec = P(None)
    part_vec = P('dp')
    in_specs = (act_spec, act_spec, P('dp', None), rep_vec, rep_vec, P(None, None, 'tp', None), P(None, 'tp', None),
                P('tp', None, None), rep_vec, rep_vec, rep_vec, P(None, 'tp'), P('tp'), P('tp', None), rep_vec)
    out_specs = (act_spec, act_spec, part_vec, part_vec, P('dp', None, 'tp', None), P('dp', 'tp', None),
                 P(('dp', 'tp'), None, None), part_vec, part_vec, part_vec, P('dp', 'tp'), P(('dp', 'tp')),
                 P(('dp', 'tp'), None), part_vec)

    def device_step(x_in, grad_y, pad_mask, ln1_gain, ln1_bias, w_qkv, b_qkv, w_out, b_out, ln2_gain, ln2_bias, w_up, b_up, w_down, b_down):
        batch, p_len, dim = x_in.shape
        seq = pad_mask.shape[1]
        _, _, heads, hd = w_qkv.shape
        seqs = batch // n_tp
        ffn = w_up.shape[1]
        width = heads * hd
        n3 = 3 * width
        tok = seqs * seq
        chunk = seqs * p_len
        qc = seq // 2
        q_scale = hd ** -0.5
        sds = jax.ShapeDtypeStruct
        n_tile = n3 + width
        n_rows = n_tile + 16
        half = dim // 2

        def kernel(x_ref, dy_ref, mask_ref, wq_ref, bq_ref, wo_ref, wu_ref, bu_ref, wd_ref, vecs_ref, freq_ref,
                   y_out, gx_out, g_att, g_up, g_down, g_vec,
                   wq, wu, wd, q_hbm, k_hbm, v_hbm, act_hbm, slope_hbm, p_dn, p_up, p_at, got_dn, got_up, got_at,
                   sum_dn, sum_up, sum_at, r_dn, r_up, r_at,
                   x, h1, dy, o4, x1, h2, wo, dx1b, do4, acc, acc2, p_rcv, p_snd, t_got, t_own, d4, dq_acc, dk_acc, dv_acc,
                   cos_t, sin_t, ok, m_st, l_st, b_att, b_ffn, b_all, u_all, gb, vec, vec_all, dpre,
                   send, recv, local, pair_send, pair_recv, pair_ready):
            net = Net(n_tp, send, recv, local)
            me = lax.axis_index('tp')
            gain1, bias1, bias_o, gain2, bias2, bias_d = (vecs_ref[i:i + 1, :] for i in range(6))

            net.gather('wq', wq_ref, wq)
            net.gather('wo', wo_ref, wo)
            net.gather('wu', wu_ref, wu)
            net.gather('wd', wd_ref, wd)
            net.exchange('x', x_ref, x, chunk)
            net.exchange('dy', dy_ref, dy, chunk)
            net.exchange('y', x1, y_out, chunk)
            net.exchange('gx', h1, gx_out, chunk)
            for chip in range(n_chips):
                for core in range(2):
                    if chip + core:
                        slot = 2 * (-chip % n_chips) + core
                        net.add('bias', lambda: bq_ref, lambda n=slot: b_all.at[n], chip, core)
                        net.add('bias', lambda: bu_ref, lambda n=slot: u_all.at[n], chip, core)
                        net.add('vec', lambda: vec, lambda n=slot: vec_all.at[n], chip, core)
            net.scatter('dn', p_dn, got_dn, sum_dn, r_dn)
            net.scatter('up', p_up, got_up, sum_up, r_up)
            net.scatter('at', p_at, got_at, sum_at, r_at)
            for name, ref, tmp, buf in (('wq', wq_ref, lambda: h2.at[pl.ds(0, n3)], wq), ('wu', wu_ref, lambda: x1.at[:, pl.ds(0, ffn)], wu),
                                        ('wd', wd_ref, lambda: dx1b.at[pl.ds(0, ffn)], wd)):
                net.add_local('load', lambda r=ref: r, tmp)
                net.add_local('store', tmp, lambda b=buf: b.at[0])
            net.add_local('own', lambda: wo_ref, lambda: wo.at[0])
            net.add_local('own', lambda: bq_ref, lambda: b_all.at[0])
            net.add_local('own', lambda: bu_ref, lambda: u_all.at[0])
            parts = {'dn': (p_dn, got_dn, sum_dn, n_tile), 'up': (p_up, got_up, sum_up, n_tile), 'at': (p_at, got_at, sum_at, n_rows)}
            for name, (p, got, summed, rows) in parts.items():
                h = rows // 2
                for i, (j, lo) in enumerate(((1, 0), (3, h))):
                    net.add_local(name + '_load', lambda g=got, i=i: g.at[i], lambda i=i, h=h: t_got.at[i, pl.ds(0, h)])
                    net.add_local(name + '_load', lambda p=p, j=j, lo=lo, h=h: p.at[j, pl.ds(lo, h)], lambda i=i, h=h: t_own.at[i, pl.ds(0, h)])
                    net.add_local(name + '_store', lambda i=i, h=h: t_own.at[i, pl.ds(0, h)], lambda s=summed, i=i: s.at[i])

            def add_relayed(name):
                h = parts[name][3] // 2
                net.done(name + '_load')

                def body(rows):
                    for i in range(2):
                        t_own[i, rows] += t_got[i, rows]

                loop_rows(h, 8, body)
                net.start(name + '_store')

            def hooks(step, table):
                for at, act in table.items():
                    @pl.when(step == at)
                    def _(act=act):
                        act()

            tile_order = (2, 1, 3, 0)

            def place(i):
                return jnp.where(i == 0, 2, jnp.where(i == 1, 1, jnp.where(i == 2, 3, 0)))

            def order(s):
                return 2 * place(lax.rem(s, n_chips)) + 1 - lax.div(s, n_chips)

            def pair(s, name, tile, rows):
                n = n_chips
                base = n * list(parts).index(name)
                p = parts[name][0]

                def copy(i):
                    return pltpu.make_async_remote_copy(
                        src_ref=p_snd.at[lax.rem(i, 2), pl.ds(0, rows)], dst_ref=p_rcv.at[i, pl.ds(0, rows)],
                        send_sem=pair_send.at[base + i], recv_sem=pair_recv.at[base + i],
                        device_id={'tp': net.peer(0, 1)}, device_id_type=pl.DeviceIdType.MESH)

                @pl.when(jnp.logical_and(s >= 1, s <= n))
                def _():
                    copy(s - 1).start()

                @pl.when(jnp.logical_and(s >= 2, s < n))
                def _():
                    copy(s - 2).wait_send()

                @pl.when(s < n)
                def _():
                    tile(lambda at, v: p_snd.__setitem__((lax.rem(s, 2),) + at, v))

                @pl.when(s >= n)
                def _():
                    copy(s - n).wait_recv()
                    tile(lambda at, v: p_rcv.__setitem__((s - n,) + at, v + p_rcv[(s - n,) + at]))
                    store(name, s - n, place(s - n), rows).start()

                @pl.when(s == 2 * n - 1)
                def _():
                    copy(n - 2).wait_send()
                    copy(n - 1).wait_send()

            def store(name, i, chip, rows):
                p = parts[name][0]
                return pltpu.make_async_copy(p_rcv.at[i, pl.ds(0, rows)], p.at[chip], pair_send.at[3 * n_chips + i])

            def stored(name, i):
                store(name, i, tile_order[i], parts[name][3]).wait()

            def pair_begin(first):
                if not first:
                    pl.semaphore_signal(pair_ready, inc=1, device_id={'tp': net.peer(0, 1)}, device_id_type=pl.DeviceIdType.MESH)
                    pl.semaphore_wait(pair_ready, 1)

            barrier = pltpu.get_barrier_semaphore()
            for chip in range(n_chips):
                for core in range(2):
                    if chip + core:
                        pl.semaphore_signal(barrier, inc=1, device_id={'tp': net.peer(chip, core)}, device_id_type=pl.DeviceIdType.MESH)
            pl.semaphore_wait(barrier, n_tp - 1)
            net.start('wq_a', 'wq_b', 'bias', 'x', 'load', 'own', 'x_own', 'dy_own')
            angle = lax.broadcasted_iota(jnp.int32, (seq, width), 0).astype(F32) * freq_ref[0:1, :]
            cos_t[...] = jnp.cos(angle)
            sin_t[...] = jnp.sin(angle) * freq_ref[1:2, :]
            for b in range(seqs):
                row = mask_ref[pl.ds(me * seqs + b, 1), :].astype(F32)
                ok[b] = jnp.broadcast_to(row, (LANES, seq)).T
            net.done('load')
            net.start('store')
            net.got('wq_a')
            net.start('wq_relay', 'wo_a', 'wo_b', 'wu_a', 'wu_b')
            net.got('wq_b')
            net.start('wq_fwd')
            net.done('own', 'x_own', 'dy_own')
            net.got('bias')
            for n in range(n_tp):
                b = b_all[n]
                b_att[n] = jnp.concatenate([b[i // heads, i % heads:i % heads + 1, :] for i in range(3 * heads)], axis=1)
                b_ffn[n] = u_all[n]
            net.got('x')

            def ln1(rows):
                x_hat, _ = ln_stats(x[rows, :].astype(F32))
                h1[rows, :] = (x_hat * gain1 + bias1).astype(BF16)

            loop_rows(tok, chunk, ln1)
            net.done('store')
            net.got('wq_relay')
            net.start('wq_last')
            net.got('wq_fwd', 'wq_last')

            def qkv_step(ps, w, q_ref, k_ref, v_ref):
                s = ps.index[0]
                hooks(s, {2: lambda: (net.got('wo_a'), net.start('wo_relay', 'dy')), 7: lambda: (net.got('wu_a'), net.start('wu_relay'))})
                n_src = tok // chunk // 2

                @pl.loop(0, 2)
                def _(i):
                    rows = span(i, tok // 2)
                    t = mm(h1[rows, :], w[0], NT) + b_att[s]
                    cos, sin = (t_ref[span(i, seq // 2), :].reshape(n_src, 1, p_len, width) for t_ref in (cos_t, sin_t))

                    def rope(v):
                        out = v.reshape(n_src, seqs, p_len, width) * cos + swap_halves(v, hd).reshape(n_src, seqs, p_len, width) * sin
                        return out.astype(BF16)

                    src = span(i, n_src)
                    q_ref[0, src] = rope(t[:, :width] * q_scale)
                    k_ref[0, src] = rope(t[:, width:2 * width])
                    v_ref[0, src] = t[:, 2 * width:].reshape(n_src, seqs, p_len, width).astype(BF16)

            slot3 = lambda rows, cols, f=lambda s: s: pl.BlockSpec((1, rows, cols), lambda s: (f(s), 0, 0))
            pipe = functools.partial(pltpu.emit_pipeline, _explicit_indices=True)
            pipe(qkv_step, grid=(n_tp,), in_specs=[slot3(n3, dim)], out_specs=[pl.BlockSpec((1, n_tp, seqs, p_len, width), lambda s: (s, 0, 0, 0, 0))] * 3)(
                wq, q_hbm, k_hbm, v_hbm)

            srcs = qc // p_len
            lane = lax.broadcasted_iota(jnp.int32, (qc, width), 1)

            def attn_step(ps, q_ref, k_ref, v_ref):
                g, b = ps.index
                hooks(g * seqs + b, {
                    0: lambda: (net.got('wo_b'), net.start('wo_fwd')), 1: lambda: (net.got('wo_relay'), net.start('wo_last')),
                    3: lambda: (net.got('wu_b'), net.start('wu_fwd')), 5: lambda: net.start('wd_a', 'wd_b'),
                    12: lambda: (net.got('wu_relay'), net.start('wu_last'))})
                bad = ok[b][:, 0:1] <= 0
                k = k_ref[0, :, 0].reshape(seq, width)
                v_t = v_ref[0, :, 0].reshape(seq, width).T
                for c in range(seq // qc):
                    src = slice(c * srcs, (c + 1) * srcs)
                    cols = slice(c * qc, (c + 1) * qc)
                    q = q_ref[0, src, 0].reshape(qc, width)
                    outs = []
                    for h in range(heads):
                        s = jnp.where(bad, NEG_LARGE, mm(k, jnp.where(lane // hd == h, q, jnp.zeros_like(q)), NT))
                        m = jnp.max(s, axis=0, keepdims=True)
                        e = jnp.exp(s - m)
                        r = 1.0 / col_sum(e)
                        outs.append(mm(v_t[h * hd:(h + 1) * hd], (e * r).astype(BF16), NN))
                        m_st[g, b, h:h + 1, cols] = m
                        l_st[g, b, h:h + 1, cols] = r
                    o4[src, b, :, span(g, width)] = jnp.concatenate(outs, axis=0).T.astype(BF16).reshape(srcs, p_len, width)

            head_blk = pl.BlockSpec((1, n_tp, 1, p_len, width), lambda g, b: (g, 0, b, 0, 0))
            pipe(attn_step, grid=(n_tp, seqs), in_specs=[head_blk] * 3)(q_hbm, k_hbm, v_hbm)

            net.got('wo_fwd', 'wo_last')

            @pl.loop(0, tok // (2 * chunk))
            def _(i):
                rows = span(i, 2 * chunk)
                o = o4[pl.ds(2 * i, 2)].reshape(2 * chunk, n_tp * width)
                low = (x[rows, :].astype(F32) + (mm(o, wo[...].reshape(n_tp * width, dim), NN) + bias_o)).astype(BF16)
                x1[rows, :] = low
                x_hat, _ = ln_stats(low.astype(F32))
                h2[rows, :] = (x_hat * gain2 + bias2).astype(BF16)

            net.got('wu_fwd', 'wu_last', 'dy')

            def up_step(ps, w, act_ref, slope_ref):
                s = ps.index[0]
                hooks(s, {0: lambda: (net.got('wd_a'), net.start('wd_relay')), 2: lambda: (net.got('wd_b'), net.start('wd_fwd')),
                          5: lambda: (net.got('wd_relay'), net.start('wd_last'), stored('dn', 0), net.start('dn_relay')),
                          6: lambda: (stored('dn', 1), net.start('dn_next')), 7: lambda: (stored('dn', 2), net.start('dn_prev'))})

                def gelu(rows):
                    pre = mm(h2[rows, :], w[0], NN) + b_ffn[order(s)]
                    erf_term = lax.erf(pre * INV_SQRT2)
                    act_ref[rows, :] = (0.5 * pre * (1.0 + erf_term)).astype(BF16)
                    slope_ref[rows, :] = 0.5 * (1.0 + erf_term) + pre * jnp.exp(-0.5 * pre * pre) * INV_SQRT_2PI

                loop_rows(tok, half, gelu)

                def tile(put):
                    put((pl.ds(0, ffn),), mm(act_ref[...], dy[...], TN))

                pair(s, 'dn', tile, n_tile)

            cols = pl.BlockSpec((tok, ffn), lambda s: (0, order(s)))
            wu_spec, wd_spec = slot3(dim, ffn, order), slot3(ffn, dim, order)
            pair_begin(True)
            pipe(up_step, grid=(n_tp,), in_specs=[wu_spec], out_specs=[cols, cols])(wu, act_hbm, slope_hbm)

            net.got('wd_fwd', 'wd_last')
            stored('dn', 3)
            pair_begin(False)

            def mlp_step(ps, wd_s, wu_s, act_ref, slope_ref):
                s = ps.index[0]
                hooks(s, {2: lambda: (net.got('dn_relay'), net.start('dn_load')), 3: lambda: add_relayed('dn'),
                          4: lambda: (net.done('dn_store'), net.start('dn_sum')),
                          5: lambda: (stored('up', 0), net.start('up_relay')), 6: lambda: (stored('up', 1), net.start('up_next')),
                          7: lambda: (stored('up', 2), net.start('up_prev'))})

                @pl.when(s == 0)
                def _():
                    acc[...] = jnp.zeros_like(acc)
                    acc2[...] = jnp.zeros_like(acc2)

                gb[order(s)] = jnp.zeros_like(gb[0])

                def rows_step(rows):
                    d_pre = mm(dy[rows, :], wd_s[0], NT) * slope_ref[rows, :]
                    gb[order(s)] += col_sum(d_pre)
                    low = d_pre.astype(BF16)
                    dpre[rows, :] = low
                    acc[rows, :] += mm(act_ref[rows, :], wd_s[0], NN)
                    acc2[rows, :] += mm(low, wu_s[0], NT)

                loop_rows(tok, half, rows_step)

                def tile(put):
                    for i in range(2):
                        part = pl.ds(i * half, half)
                        put((pl.ds(0, ffn), part), mm(h2[:, part], dpre[...], TN))

                pair(s, 'up', tile, n_tile)

            pipe(mlp_step, grid=(n_tp,), in_specs=[wd_spec, wu_spec, cols, cols])(wd, wu, act_hbm, slope_hbm)
            vec[...] = jnp.zeros_like(vec)

            @pl.loop(0, tok // (2 * chunk))
            def _(i):
                rows = span(i, 2 * chunk)
                x1_f, dy_f, dh = x1[rows, :].astype(F32), dy[rows, :].astype(F32), acc2[rows, :]
                x1[rows, :] = (x1_f + (acc[rows, :] + bias_d)).astype(BF16)
                x_hat, inv_std = ln_stats(x1_f)
                d_x1 = dy_f + ln_grad(dh, x_hat, inv_std, gain2)
                acc2[rows, :] = d_x1
                low = d_x1.astype(BF16)
                dx1b[rows, :] = low
                d_o = mm(low, wo[...].reshape(n_tp * width, dim), NT).astype(BF16)
                do4[pl.ds(2 * i, 2)] = d_o.reshape(2, seqs, p_len, n_tp * width)
                for n, t in enumerate((d_x1, dh * x_hat, dh, dy_f)):
                    vec[2 + n:3 + n, :] += col_sum(t)

            stored('up', 3)
            pair_begin(False)

            def bwd_step(ps, q_ref, k_ref, v_ref, w):
                step = ps.index[0]
                g = order(step)
                hooks(step, {0: lambda: net.start('y', 'y_own'), 1: lambda: (net.got('up_relay'), net.start('up_load')),
                             2: lambda: add_relayed('up'), 3: lambda: (net.done('up_store'), net.start('up_sum')),
                             5: lambda: (stored('at', 0), net.start('at_relay')), 6: lambda: (stored('at', 1), net.start('at_next')),
                             7: lambda: (stored('at', 2), net.start('at_prev'))})
                b_sum = jnp.zeros((1, n3), F32)
                for b in range(seqs):
                    bad = ok[b][:, 0:1] <= 0
                    k = k_ref[0, :, b].reshape(seq, width)
                    v = v_ref[0, :, b].reshape(seq, width)
                    k_t = k.T
                    for c in range(seq // qc):
                        src = slice(c * srcs, (c + 1) * srcs)
                        at = slice(c * qc, (c + 1) * qc)
                        q = q_ref[0, src, b].reshape(qc, width)
                        d_o = do4[src, b, :, span(g, width)].reshape(qc, width)
                        dk = jnp.zeros((seq, width), F32)
                        dv = jnp.zeros((seq, width), F32)
                        dqs = []
                        for h in range(heads):
                            mine = lane // hd == h
                            q_h = jnp.where(mine, q, jnp.zeros_like(q))
                            do_h = jnp.where(mine, d_o, jnp.zeros_like(d_o))
                            s = jnp.where(bad, NEG_LARGE, mm(k, q_h, NT))
                            p = jnp.exp(s - m_st[g, b, h:h + 1, at]) * l_st[g, b, h:h + 1, at]
                            dv += mm(p.astype(BF16), do_h, NN)
                            dp = mm(v, do_h, NT)
                            ds = (p * (dp - col_sum(dp * p))).astype(BF16)
                            dk += mm(ds, q_h, NN)
                            dqs.append(mm(k_t[h * hd:(h + 1) * hd], ds, NN))
                        dq_acc[at, :] = jnp.concatenate(dqs, axis=0).T
                        dk_acc[...] = dk if c == 0 else dk_acc[...] + dk
                        dv_acc[...] = dv if c == 0 else dv_acc[...] + dv
                    cos, sin = cos_t[...], sin_t[...]
                    dq, dk, dv = dq_acc[...], dk_acc[...], dv_acc[...]
                    dq = (dq * cos - swap_halves(dq, hd) * sin) * q_scale
                    dk = dk * cos - swap_halves(dk, hd) * sin
                    for i, t in enumerate((dq, dk, dv)):
                        d4[:, b, :, i * width:(i + 1) * width] = t.astype(BF16).reshape(n_tp, p_len, width)
                    b_sum += jnp.concatenate([col_sum(t) for t in (dq, dk, dv)], axis=1)

                @pl.when(step == 0)
                def _():
                    acc[...] = jnp.zeros_like(acc)

                @pl.loop(0, 2)
                def _(i):
                    acc[span(i, half), :] += mm(d4[pl.ds(n_chips * i, n_chips)].reshape(half, n3), w[0], NN)

                def tile(put):
                    put((pl.ds(0, n3),), mm(d4[...].reshape(tok, n3), h1[...], TN))
                    put((pl.ds(n3, width),), mm(o4[:, :, :, span(g, width)].reshape(tok, width), dx1b[...], TN))
                    rest = jnp.zeros((1, dim - n3 - ffn), F32)
                    line = jnp.concatenate([b_sum, gb[g], rest], axis=1)
                    put((pl.ds(n_tile, 16),), jnp.broadcast_to(line, (16, dim)))

                pair(step, 'at', tile, n_rows)

            slot_blk = pl.BlockSpec((1, n_tp, seqs, p_len, width), lambda s: (order(s), 0, 0, 0, 0))
            pipe(bwd_step, grid=(n_tp,), in_specs=[slot_blk] * 3 + [slot3(n3, dim, order)])(
                q_hbm, k_hbm, v_hbm, wq)

            def ln1_bwd(rows):
                x_hat, inv_std = ln_stats(x[rows, :].astype(F32))
                dh = acc[rows, :]
                h1[rows, :] = (acc2[rows, :] + ln_grad(dh, x_hat, inv_std, gain1)).astype(BF16)
                vec[0:1, :] += col_sum(dh * x_hat)
                vec[1:2, :] += col_sum(dh)

            loop_rows(tok, 2 * chunk, ln1_bwd)
            stored('at', 3)
            net.start('gx', 'gx_own', 'vec')
            net.got('at_relay')
            net.start('at_load')
            add_relayed('at')
            net.done('at_store')
            net.start('at_sum')

            def total(p, r, out, n, blocks):
                def body(_, a, b, o_ref):
                    o_ref[...] = a[0] + b[0] + b[1]

                grid, a, b, o = blocks
                pipe(body, grid=grid, in_specs=[a, b], out_specs=[o])(p, r, out)

            def by_rows(n):
                return (2,), pl.BlockSpec((1, n, dim), lambda i: (0, i, 0)), pl.BlockSpec((2, n, dim), lambda i: (0, i, 0)), pl.BlockSpec((n, dim), lambda i: (i, 0))

            net.got('dn_next', 'dn_prev', 'dn_sum')
            total(p_dn, r_dn, g_down, n_tile, by_rows(n_tile // 2))
            net.got('up_next', 'up_prev', 'up_sum')
            total(p_up, r_up, g_up, n_tile, (
                (2,), pl.BlockSpec((1, n_tile, half), lambda i: (0, 0, i)), pl.BlockSpec((2, n_tile, half), lambda i: (0, 0, i)),
                pl.BlockSpec((n_tile, half), lambda i: (i, 0))))
            net.got('vec')
            summed = vec[...]
            for n in range(1, n_tp):
                summed += vec_all[n]
            g_vec[...] = summed
            net.got('at_next', 'at_prev', 'at_sum')
            total(p_at, r_at, g_att, n_rows, by_rows(n_rows // 2))
            net.got('gx', 'y')
            net.done('y_own', 'gx_own')
            for name in net.copies:
                if name not in ('load', 'store', 'own') and not name.endswith(('_own', '_load', '_store')):
                    net.sent(name)

        big = (tok, dim)
        shapes = lambda *dims, dtype=F32: sds(dims, dtype)
        halves = lambda rows: shapes(2, rows // 2, dim)
        flat = lambda t: t.reshape(tok, dim)
        inv_freq = ROPE_BASE ** (-2.0 * jnp.arange(hd // 2, dtype=F32) / hd)
        sign = jnp.concatenate([-jnp.ones_like(inv_freq), jnp.ones_like(inv_freq)])
        freq = jnp.stack([jnp.tile(inv_freq, 2 * heads), jnp.tile(sign, heads)])
        vectors = jnp.stack([ln1_gain, ln1_bias, b_out, ln2_gain, ln2_bias, b_down])
        vmem = pl.BlockSpec(memory_space=pltpu.VMEM)
        sem = lambda n: pltpu.SemaphoreType.DMA((n,))
        outs = pl.pallas_call(
            kernel, name='layer',
            out_shape=(sds(big, BF16), sds(big, BF16), shapes(n_rows, dim), shapes(dim, ffn), shapes(ffn, dim), shapes(8, dim),
                       shapes(n_tp, n3, dim, dtype=BF16), shapes(n_tp, dim, ffn, dtype=BF16), shapes(n_tp, ffn, dim, dtype=BF16))
            + (shapes(n_tp, n_tp, seqs, p_len, width, dtype=BF16),) * 3 + (shapes(tok, n_tp * ffn, dtype=BF16), shapes(tok, n_tp * ffn))
            + tuple(shapes(n_chips, n, dim) for n in (n_tile, n_tile, n_rows)) + tuple(halves(n) for n in (n_tile, n_tile, n_rows)) * 2
            + tuple(shapes(2, n, dim) for n in (n_tile, n_tile, n_rows)),
            in_specs=[ANY, ANY, vmem, ANY, ANY, ANY, ANY, ANY, ANY, vmem, vmem], out_specs=(ANY,) * 5 + (vmem,) + (ANY,) * 20,
            scratch_shapes=[pltpu.VMEM(big, BF16)] * 3 + [pltpu.VMEM((n_tp, seqs, p_len, n_tp * width), BF16)]
            + [pltpu.VMEM(big, BF16)] * 2 + [pltpu.VMEM((n_tp, width, dim), BF16), pltpu.VMEM(big, BF16),
                                             pltpu.VMEM((n_tp, seqs, p_len, n_tp * width), BF16)]
            + [pltpu.VMEM(big, F32)] * 2 + [pltpu.VMEM((n_chips, n_rows, dim), F32), pltpu.VMEM((2, n_rows, dim), F32)]
            + [pltpu.VMEM((2, n_rows // 2, dim), F32)] * 2 + [pltpu.VMEM((n_tp, seqs, p_len, n3), BF16)]
            + [pltpu.VMEM((seq, width), F32)] * 5 + [pltpu.VMEM((seqs, seq, LANES), F32)]
            + [pltpu.VMEM((n_tp, seqs, heads, seq), F32)] * 2
            + [pltpu.VMEM((n_tp, 1, n3), F32), pltpu.VMEM((n_tp, 1, ffn), F32), pltpu.VMEM((n_tp,) + b_qkv.shape, F32)]
            + [pltpu.VMEM((n_tp, 1, ffn), F32)] * 2 + [pltpu.VMEM((8, dim), F32), pltpu.VMEM((n_tp, 8, dim), F32), pltpu.VMEM((tok, ffn), BF16)]
            + [sem(128), sem(128), sem(64), sem(4 * n_chips), sem(3 * n_chips), pltpu.SemaphoreType.REGULAR],
            compiler_params=pltpu.CompilerParams(collective_id=0, has_side_effects=True, vmem_limit_bytes=VMEM_LIMIT),
        )(flat(x_in), flat(grad_y), pad_mask, w_qkv.transpose(0, 2, 3, 1).reshape(n3, dim), b_qkv, w_out.reshape(width, dim),
          w_up, b_up.reshape(1, ffn), w_down, vectors, freq)
        y_out, grad_x, att, grad_w_up, grad_w_down, vec = outs[:6]
        grad_w_qkv = att[:n3].reshape(3, heads, hd, dim).transpose(0, 3, 1, 2)
        grad_w_out = att[n3:n_tile].reshape(heads, hd, dim)
        grad_b_qkv = att[n_tile, :n3].reshape(3, heads, hd)
        grad_b_up = att[n_tile, n3:n3 + ffn]
        return (y_out.reshape(x_in.shape), grad_x.reshape(x_in.shape), vec[0], vec[1], grad_w_qkv, grad_b_qkv, grad_w_out,
                vec[2], vec[3], vec[4], grad_w_up, grad_b_up, grad_w_down, vec[5])

    return jax.shard_map(device_step, mesh=mesh, in_specs=in_specs, out_specs=out_specs, check_vma=False)
```

```python
import functools

import jax
import jax.numpy as jnp
import numpy as np
from jax import lax
from jax.experimental import pallas as pl
from jax.experimental.pallas import tpu as pltpu
from jax.sharding import PartitionSpec as P

LN_EPS = 1e-5
ROPE_BASE = 10000.0
INV_SQRT2 = 0.7071067811865476
INV_SQRT_2PI = 0.3989422804014327
NEG_LARGE = -1e30
F32 = jnp.float32
BF16 = jnp.bfloat16
VMEM_LIMIT = 66_500_000
LANES = 128
NN = (((1,), (0,)), ((), ()))
NT = (((1,), (1,)), ((), ()))
TN = (((0,), (0,)), ((), ()))
ANY = pl.BlockSpec(memory_space=pl.ANY)


def mm(a, b, dims):
    return lax.dot_general(a, b, dims, preferred_element_type=F32)


def ln_stats(v):
    centered = v - jnp.mean(v, axis=-1, keepdims=True)
    inv_std = lax.rsqrt(jnp.mean(centered * centered, axis=-1, keepdims=True) + LN_EPS)
    return centered * inv_std, inv_std


def ln_grad(d_out, x_hat, inv_std, gain):
    d_hat = d_out * gain
    return inv_std * (d_hat - jnp.mean(d_hat, axis=-1, keepdims=True) - x_hat * jnp.mean(d_hat * x_hat, axis=-1, keepdims=True))


def col_sum(t):
    return jnp.sum(t, axis=0, keepdims=True)


def swap_halves(t, head_dim):
    half = head_dim // 2
    lane = lax.broadcasted_iota(jnp.int32, t.shape, t.ndim - 1)
    return jnp.where(lane % head_dim < half, pltpu.roll(t, t.shape[-1] - half, t.ndim - 1), pltpu.roll(t, half, t.ndim - 1))


def span(i, n):
    return pl.ds(pl.multiple_of(i * n, n), n)


def loop_rows(total, n, body):
    @pl.loop(0, total // n)
    def _(i):
        body(span(i, n))


class Net:
    def __init__(self, n_tp, send, recv, local):
        self.n_tp, self.send, self.recv, self.local = n_tp, send, recv, local
        self.copies, self.count, self.n_local = {}, 0, 0

    def peer(self, chip, core):
        me = lax.axis_index('tp')
        at = lax.rem(me + 2 * chip, self.n_tp) if chip else me
        return at + 1 - 2 * lax.rem(at, 2) if core else at

    def add(self, name, src, dst, chip, core=0):
        n = self.count
        self.count += 1

        def make():
            return pltpu.make_async_remote_copy(
                src_ref=src(), dst_ref=dst(), send_sem=self.send.at[n], recv_sem=self.recv.at[n],
                device_id={'tp': self.peer(chip, core)}, device_id_type=pl.DeviceIdType.MESH)

        self.copies.setdefault(name, []).append(make)

    def add_local(self, name, src, dst):
        n = self.n_local
        self.n_local += 1
        self.copies.setdefault(name, []).append(lambda: pltpu.make_async_copy(src(), dst(), self.local.at[n]))

    def start(self, *names):
        for name in names:
            for make in self.copies[name]:
                make().start()

    def got(self, *names):
        for name in names:
            with jax.named_scope('got_' + name):
                for make in self.copies[name]:
                    make().wait_recv()

    def sent(self, *names):
        for name in names:
            for make in self.copies[name]:
                make().wait_send()

    def done(self, *names):
        for name in names:
            with jax.named_scope('done_' + name):
                for make in self.copies[name]:
                    make().wait()

    def gather(self, name, own, buf):
        rows = own.shape[0]
        top, bot, whole = pl.ds(0, rows // 2), pl.ds(rows // 2, rows // 2), pl.ds(0, rows)

        def put(stage, src, slot, part, chip, core=0):
            take = (lambda: own.at[part]) if src is None else (lambda: buf.at[src, part])
            self.add(name + stage, take, lambda: buf.at[slot, part], chip, core)

        put('_a', None, 6, top, 1)
        put('_a', None, 2, bot, 3)
        put('_b', None, 6, bot, 1)
        put('_b', None, 2, top, 3)
        put('_b', None, 1, whole, 0, 1)
        put('_relay', 6, 4, top, 1)
        put('_relay', 2, 4, bot, 3)
        put('_fwd', 6, 7, whole, 0, 1)
        put('_fwd', 2, 3, whole, 0, 1)
        put('_last', 4, 5, whole, 0, 1)

    def exchange(self, name, src, dst, rows):
        me = lax.axis_index('tp')
        for core in range(2):
            for chip in (1, 3, 2, 0):
                if chip + core:
                    self.add(name, lambda c=chip, k=core: src.at[span(self.peer(c, k), rows)], lambda: dst.at[span(me, rows)], chip, core)
        self.add_local(name + '_own', lambda: src.at[span(me, rows)], lambda: dst.at[span(me, rows)])

    def scatter(self, name, p, got, summed, early, last):
        half = p.shape[1] // 2
        top, bot = pl.ds(0, half), pl.ds(half, half)
        self.add(name + '_relay', lambda: p.at[2, top], lambda: got.at[0], 1)
        self.add(name + '_relay', lambda: p.at[2, bot], lambda: got.at[1], 3)
        self.add(name + '_next', lambda: p.at[1, bot], lambda: early.at[bot], 1)
        self.add(name + '_prev', lambda: p.at[3, top], lambda: early.at[top], 3)
        self.add(name + '_sum', lambda: summed.at[0], lambda: last.at[top], 1)
        self.add(name + '_sum', lambda: summed.at[1], lambda: last.at[bot], 3)


def solution(mesh):
    n_tp = mesh.shape['tp']
    n_chips = n_tp // 2
    act_spec = P('dp', 'tp', None)
    rep_vec = P(None)
    part_vec = P('dp')
    in_specs = (act_spec, act_spec, P('dp', None), rep_vec, rep_vec, P(None, None, 'tp', None), P(None, 'tp', None),
                P('tp', None, None), rep_vec, rep_vec, rep_vec, P(None, 'tp'), P('tp'), P('tp', None), rep_vec)
    out_specs = (act_spec, act_spec, part_vec, part_vec, P('dp', None, 'tp', None), P('dp', 'tp', None),
                 P(('dp', 'tp'), None, None), part_vec, part_vec, part_vec, P('dp', 'tp'), P(('dp', 'tp')),
                 P(('dp', 'tp'), None), part_vec)

    def device_step(x_in, grad_y, pad_mask, ln1_gain, ln1_bias, w_qkv, b_qkv, w_out, b_out, ln2_gain, ln2_bias, w_up, b_up, w_down, b_down):
        batch, p_len, dim = x_in.shape
        seq = pad_mask.shape[1]
        _, _, heads, hd = w_qkv.shape
        seqs = batch // n_tp
        ffn = w_up.shape[1]
        width = heads * hd
        n3 = 3 * width
        tok = seqs * seq
        chunk = seqs * p_len
        qc = seq // 2
        q_scale = hd ** -0.5
        sds = jax.ShapeDtypeStruct
        n_tile = n3 + width
        half = dim // 2

        def kernel(*refs):
            it = iter(refs)
            take = lambda n: [next(it) for _ in range(n)]
            (x_ref, dy_ref, wq_ref, bq_ref, wo_ref, wu_ref, bu_ref, wd_ref), plain = take(8), take(8)
            y_out, gx_out, g_up, g_down, g_at, g_vec, g_b, wq, wu, wd, q_hbm, k_hbm, v_hbm, act_hbm, slope_hbm = take(15)
            parts = {name: take(5) for name in ('dn', 'up', 'at')}
            x, h1, dy, x1, h2, dx1b, o4, do4, wo, acc, acc2, p_rcv, p_snd, t_got, t_own, d4 = take(16)
            dq_acc, dk_acc, dv_acc, cos_t, sin_t, ok, m_st, l_st, b_att, b_ffn, u_all, gb, b_all, b8, b_in, vec, v_in, v_sum, v_all, dpre = take(20)
            here = take(8)
            send, recv, local, pair_send, pair_recv, pair_ready = take(6)
            net = Net(n_tp, send, recv, local)
            me = lax.axis_index('tp')
            mask_ref, gain1, bias1, bias_o, gain2, bias_d, bias2, freq_ref = here

            net.gather('wq', wq_ref, wq)
            net.gather('wo', wo_ref, wo)
            net.gather('wu', wu_ref, wu)
            net.gather('wd', wd_ref, wd)
            net.exchange('x', x_ref, x, chunk)
            net.exchange('dy', dy_ref, dy, chunk)
            net.exchange('y', x1, y_out, chunk)
            net.exchange('gx', h1, gx_out, chunk)
            for chip in range(n_chips):
                for core in range(2):
                    if chip + core:
                        slot = 2 * (-chip % n_chips) + core
                        net.add('bias', lambda: bq_ref, lambda n=slot: b_all.at[n], chip, core)
                        net.add('bias', lambda: bu_ref, lambda n=slot: u_all.at[n], chip, core)
                        own = 2 * chip + core
                        net.add('b8', lambda n=own: b8.at[n], lambda n=slot: b_in.at[n], chip, core)
                        net.add('vec', lambda c=chip, k=core: vec.at[:, span(net.peer(c, k), LANES)], lambda n=slot: v_in.at[n], chip, core)
                        net.add('v_sum', lambda: v_sum, lambda: v_all.at[:, span(me, LANES)], chip, core)
            for src, dst in zip(plain, here):
                net.add_local('own', lambda r=src: r, lambda r=dst: r)
            net.add_local('write', lambda: v_all, lambda: g_vec)
            net.add_local('write', lambda: b8.at[0], lambda: g_b)
            for name, ref, tmp, buf in (('wq', wq_ref, lambda: h2.at[pl.ds(0, n3)], wq), ('wu', wu_ref, lambda: x1.at[:, pl.ds(0, ffn)], wu),
                                        ('wd', wd_ref, lambda: dx1b.at[pl.ds(0, ffn)], wd)):
                net.add_local('load', lambda r=ref: r, tmp)
                net.add_local('store', tmp, lambda b=buf: b.at[0])
            net.add_local('own', lambda: wo_ref, lambda: wo.at[0])
            net.add_local('own', lambda: bq_ref, lambda: b_all.at[0])
            net.add_local('own', lambda: bu_ref, lambda: u_all.at[0])
            t_half = n_tile // 2
            for name, (p, got, summed, early, last) in parts.items():
                net.scatter(name, p, got, summed, early, last)
                for i in range(2):
                    net.add_local(name + '_load', lambda g=got, i=i: g.at[i], lambda i=i: t_got.at[i])
                    net.add_local(name + '_load', lambda p=p, i=i: p.at[1 + 2 * i, pl.ds(i * t_half, t_half)], lambda i=i: t_own.at[i])
                    net.add_local(name + '_store', lambda i=i: t_own.at[i], lambda s=summed, i=i: s.at[i])

            def add_relayed(name):
                net.done(name + '_load')

                def body(rows):
                    for i in range(2):
                        t_own[i, rows] += t_got[i, rows]

                loop_rows(t_half, 8, body)
                net.start(name + '_store')

            def hooks(step, table):
                for at, act in table.items():
                    @pl.when(step == at)
                    def _(act=act):
                        act()

            tile_order = (2, 1, 3, 0)

            def place(i):
                return jnp.where(i == 0, 2, jnp.where(i == 1, 1, jnp.where(i == 2, 3, 0)))

            def order(s):
                return 2 * place(lax.rem(s, n_chips)) + 1 - lax.div(s, n_chips)

            def pair(s, name, tile):
                n = n_chips
                base = n * list(parts).index(name)

                def copy(i):
                    return pltpu.make_async_remote_copy(
                        src_ref=p_snd.at[lax.rem(i, 2)], dst_ref=p_rcv.at[i],
                        send_sem=pair_send.at[base + i], recv_sem=pair_recv.at[base + i],
                        device_id={'tp': net.peer(0, 1)}, device_id_type=pl.DeviceIdType.MESH)

                @pl.when(jnp.logical_and(s >= 1, s <= n))
                def _():
                    copy(s - 1).start()

                @pl.when(jnp.logical_and(s >= 2, s < n))
                def _():
                    copy(s - 2).wait_send()

                @pl.when(s < n)
                def _():
                    tile(lambda at, v: p_snd.__setitem__((lax.rem(s, 2),) + at, v))

                @pl.when(s >= n)
                def _():
                    copy(s - n).wait_recv()
                    tile(lambda at, v: p_rcv.__setitem__((s - n,) + at, v + p_rcv[(s - n,) + at]))
                    store(name, s - n, place(s - n)).start()

                @pl.when(s == 2 * n - 1)
                def _():
                    copy(n - 2).wait_send()
                    copy(n - 1).wait_send()

            def store(name, i, chip):
                return pltpu.make_async_copy(p_rcv.at[i], parts[name][0].at[chip], pair_send.at[3 * n_chips + i])

            def stored(name, i):
                store(name, i, tile_order[i]).wait()

            def pair_begin(first):
                if not first:
                    pl.semaphore_signal(pair_ready, inc=1, device_id={'tp': net.peer(0, 1)}, device_id_type=pl.DeviceIdType.MESH)
                    pl.semaphore_wait(pair_ready, 1)

            barrier = pltpu.get_barrier_semaphore()
            for chip in range(n_chips):
                for core in range(2):
                    if chip + core:
                        pl.semaphore_signal(barrier, inc=1, device_id={'tp': net.peer(chip, core)}, device_id_type=pl.DeviceIdType.MESH)
            pl.semaphore_wait(barrier, n_tp - 1)
            net.start('wq_a', 'wq_b', 'bias', 'x', 'own', 'load', 'x_own', 'dy_own')
            net.done('own')
            angle = lax.broadcasted_iota(jnp.int32, (seq, width), 0).astype(F32) * freq_ref[0:1, :]
            cos_t[...] = jnp.cos(angle)
            sin_t[...] = jnp.sin(angle) * freq_ref[1:2, :]
            for b in range(seqs):
                row = mask_ref[pl.ds(me * seqs + b, 1), :].astype(F32)
                ok[b] = jnp.broadcast_to(row, (LANES, seq)).T
            net.done('load')
            net.start('store')
            net.got('wq_a')
            net.start('wq_relay', 'wo_a', 'wo_b')
            net.got('wq_b')
            net.start('wq_fwd')
            net.done('x_own', 'dy_own')
            net.got('bias')
            for n in range(n_tp):
                b = b_all[n]
                b_att[n] = jnp.concatenate([b[i // heads, i % heads:i % heads + 1, :] for i in range(3 * heads)], axis=1)
                b_ffn[n] = u_all[n]
            net.got('x')

            def ln1(rows):
                x_hat, _ = ln_stats(x[rows, :].astype(F32))
                h1[rows, :] = (x_hat * gain1[...] + bias1[...]).astype(BF16)

            loop_rows(tok, chunk, ln1)
            net.done('store')
            net.got('wq_relay')
            net.start('wq_last')
            net.got('wq_fwd', 'wq_last')

            def qkv_step(ps, w, q_ref, k_ref, v_ref):
                s = ps.index[0]
                hooks(s, {1: lambda: (net.got('wo_a'), net.start('wo_relay', 'wu_a', 'wu_b')), 3: lambda: (net.got('wo_b'), net.start('wo_fwd')),
                          5: lambda: (net.got('wo_relay'), net.start('wo_last'))})
                n_src = tok // chunk // 2

                @pl.loop(0, 2)
                def _(i):
                    rows = span(i, tok // 2)
                    t = mm(h1[rows, :], w[0], NT) + b_att[s]
                    cos, sin = (t_ref[span(i, seq // 2), :].reshape(n_src, 1, p_len, width) for t_ref in (cos_t, sin_t))

                    def rope(v):
                        out = v.reshape(n_src, seqs, p_len, width) * cos + swap_halves(v, hd).reshape(n_src, seqs, p_len, width) * sin
                        return out.astype(BF16)

                    src = span(i, n_src)
                    q_ref[0, src] = rope(t[:, :width] * q_scale)
                    k_ref[0, src] = rope(t[:, width:2 * width])
                    v_ref[0, src] = t[:, 2 * width:].reshape(n_src, seqs, p_len, width).astype(BF16)

            slot3 = lambda rows, cols, f=lambda s: s: pl.BlockSpec((1, rows, cols), lambda s: (f(s), 0, 0))

            def pipe(body, **specs):
                def run(*refs):
                    with jax.named_scope(body.__name__):
                        pltpu.emit_pipeline(body, _explicit_indices=True, **specs)(*refs)

                return run

            pipe(qkv_step, grid=(n_tp,), in_specs=[slot3(n3, dim)], out_specs=[pl.BlockSpec((1, n_tp, seqs, p_len, width), lambda s: (s, 0, 0, 0, 0))] * 3)(
                wq, q_hbm, k_hbm, v_hbm)

            srcs = qc // p_len
            lane = lax.broadcasted_iota(jnp.int32, (qc, width), 1)

            def attn_step(ps, q_ref, k_ref, v_ref):
                g, b = ps.index
                hooks(g * seqs + b, {
                    0: lambda: (net.got('wu_a'), net.start('wu_relay', 'dy')), 6: lambda: (net.got('wu_b'), net.start('wu_fwd')),
                    11: lambda: (net.got('wu_relay'), net.start('wu_last', 'wd_a', 'wd_b'))})
                bad = ok[b][:, 0:1] <= 0
                k = k_ref[0, :, 0].reshape(seq, width)
                v_t = v_ref[0, :, 0].reshape(seq, width).T
                for c in range(seq // qc):
                    src = slice(c * srcs, (c + 1) * srcs)
                    cols = slice(c * qc, (c + 1) * qc)
                    q = q_ref[0, src, 0].reshape(qc, width)
                    outs = []
                    for h in range(heads):
                        s = jnp.where(bad, NEG_LARGE, mm(k, jnp.where(lane // hd == h, q, jnp.zeros_like(q)), NT))
                        m = jnp.max(s, axis=0, keepdims=True)
                        e = jnp.exp(s - m)
                        r = 1.0 / col_sum(e)
                        outs.append(mm(v_t[h * hd:(h + 1) * hd], (e * r).astype(BF16), NN))
                        m_st[g, b, h:h + 1, cols] = m
                        l_st[g, b, h:h + 1, cols] = r
                    o4[src, b, :, span(g, width)] = jnp.concatenate(outs, axis=0).T.astype(BF16).reshape(srcs, p_len, width)

            head_blk = pl.BlockSpec((1, n_tp, 1, p_len, width), lambda g, b: (g, 0, b, 0, 0))
            pipe(attn_step, grid=(n_tp, seqs), in_specs=[head_blk] * 3)(q_hbm, k_hbm, v_hbm)

            net.got('wo_fwd', 'wo_last')

            @pl.loop(0, tok // (2 * chunk))
            def _(i):
                rows = span(i, 2 * chunk)
                o = o4[pl.ds(2 * i, 2)].reshape(2 * chunk, n_tp * width)
                low = (x[rows, :].astype(F32) + (mm(o, wo[...].reshape(n_tp * width, dim), NN) + bias_o[...])).astype(BF16)
                x1[rows, :] = low
                x_hat, _ = ln_stats(low.astype(F32))
                h2[rows, :] = (x_hat * gain2[...] + bias2[...]).astype(BF16)

            net.got('wu_fwd', 'wu_last', 'dy')

            def up_step(ps, w, act_ref, slope_ref):
                s = ps.index[0]
                hooks(s, {3: lambda: (net.got('wd_a'), net.start('wd_relay')), 5: lambda: (stored('dn', 0), net.start('dn_relay')),
                          6: lambda: (stored('dn', 1), net.start('dn_next')), 7: lambda: (stored('dn', 2), net.start('dn_prev'), net.got('wd_b'), net.start('wd_fwd'))})

                def gelu(rows):
                    pre = mm(h2[rows, :], w[0], NN) + b_ffn[order(s)]
                    erf_term = lax.erf(pre * INV_SQRT2)
                    act_ref[rows, :] = (0.5 * pre * (1.0 + erf_term)).astype(BF16)
                    slope_ref[rows, :] = 0.5 * (1.0 + erf_term) + pre * jnp.exp(-0.5 * pre * pre) * INV_SQRT_2PI

                loop_rows(tok, half, gelu)

                def tile(put):
                    put((pl.ds(0, ffn),), mm(act_ref[...], dy[...], TN))

                pair(s, 'dn', tile)

            cols = pl.BlockSpec((tok, ffn), lambda s: (0, order(s)))
            wu_spec, wd_spec = slot3(dim, ffn, order), slot3(ffn, dim, order)
            pair_begin(True)
            pipe(up_step, grid=(n_tp,), in_specs=[wu_spec], out_specs=[cols, cols])(wu, act_hbm, slope_hbm)

            net.got('wd_relay')
            net.start('wd_last')
            net.got('wd_fwd', 'wd_last')
            stored('dn', 3)
            pair_begin(False)

            def mlp_step(ps, wd_s, wu_s, act_ref, slope_ref):
                s = ps.index[0]
                hooks(s, {4: lambda: (net.got('dn_relay'), net.start('dn_load')),
                          5: lambda: (add_relayed('dn'), stored('up', 0), net.start('up_relay')),
                          6: lambda: (net.done('dn_store'), net.start('dn_sum'), stored('up', 1), net.start('up_next')),
                          7: lambda: (stored('up', 2), net.start('up_prev'))})

                @pl.when(s == 0)
                def _():
                    acc[...] = jnp.zeros_like(acc)
                    acc2[...] = jnp.zeros_like(acc2)

                gb[order(s)] = jnp.zeros_like(gb[0])

                def rows_step(rows):
                    d_pre = mm(dy[rows, :], wd_s[0], NT) * slope_ref[rows, :]
                    gb[order(s)] += col_sum(d_pre)
                    low = d_pre.astype(BF16)
                    dpre[rows, :] = low
                    acc[rows, :] += mm(act_ref[rows, :], wd_s[0], NN)
                    acc2[rows, :] += mm(low, wu_s[0], NT)

                loop_rows(tok, half, rows_step)

                def tile(put):
                    for i in range(2):
                        part = pl.ds(i * half, half)
                        put((pl.ds(0, ffn), part), mm(h2[:, part], dpre[...], TN))

                pair(s, 'up', tile)

            pipe(mlp_step, grid=(n_tp,), in_specs=[wd_spec, wu_spec, cols, cols])(wd, wu, act_hbm, slope_hbm)
            vec[...] = jnp.zeros_like(vec)

            @pl.loop(0, tok // (2 * chunk))
            def _(i):
                rows = span(i, 2 * chunk)
                x1_f, dy_f, dh = x1[rows, :].astype(F32), dy[rows, :].astype(F32), acc2[rows, :]
                x1[rows, :] = (x1_f + (acc[rows, :] + bias_d[...])).astype(BF16)
                x_hat, inv_std = ln_stats(x1_f)
                d_x1 = dy_f + ln_grad(dh, x_hat, inv_std, gain2[...])
                acc2[rows, :] = d_x1
                low = d_x1.astype(BF16)
                dx1b[rows, :] = low
                d_o = mm(low, wo[...].reshape(n_tp * width, dim), NT).astype(BF16)
                do4[pl.ds(2 * i, 2)] = d_o.reshape(2, seqs, p_len, n_tp * width)
                for n, t in enumerate((d_x1, dh * x_hat, dh, dy_f)):
                    vec[2 + n:3 + n, :] += col_sum(t)

            stored('up', 3)
            pair_begin(False)

            def bwd_step(ps, q_ref, k_ref, v_ref, w):
                step = ps.index[0]
                g = order(step)
                hooks(step, {0: lambda: net.start('y', 'y_own'), 4: lambda: (net.got('up_relay'), net.start('up_load')),
                             5: lambda: (add_relayed('up'), stored('at', 0), net.start('at_relay')),
                             6: lambda: (net.done('up_store'), net.start('up_sum'), stored('at', 1), net.start('at_next')),
                             7: lambda: (stored('at', 2), net.start('at_prev'))})
                b8[g] = jnp.zeros_like(b8[0])
                for i in range(ffn // LANES):
                    b8[g, 3 + i:4 + i, :] = gb[g][:, i * LANES:(i + 1) * LANES]
                for b in range(seqs):
                    bad = ok[b][:, 0:1] <= 0
                    k = k_ref[0, :, b].reshape(seq, width)
                    v = v_ref[0, :, b].reshape(seq, width)
                    k_t = k.T
                    for c in range(seq // qc):
                        src = slice(c * srcs, (c + 1) * srcs)
                        at = slice(c * qc, (c + 1) * qc)
                        q = q_ref[0, src, b].reshape(qc, width)
                        d_o = do4[src, b, :, span(g, width)].reshape(qc, width)
                        dk = jnp.zeros((seq, width), F32)
                        dv = jnp.zeros((seq, width), F32)
                        dqs = []
                        for h in range(heads):
                            mine = lane // hd == h
                            q_h = jnp.where(mine, q, jnp.zeros_like(q))
                            do_h = jnp.where(mine, d_o, jnp.zeros_like(d_o))
                            s = jnp.where(bad, NEG_LARGE, mm(k, q_h, NT))
                            p = jnp.exp(s - m_st[g, b, h:h + 1, at]) * l_st[g, b, h:h + 1, at]
                            dv += mm(p.astype(BF16), do_h, NN)
                            dp = mm(v, do_h, NT)
                            ds = (p * (dp - col_sum(dp * p))).astype(BF16)
                            dk += mm(ds, q_h, NN)
                            dqs.append(mm(k_t[h * hd:(h + 1) * hd], ds, NN))
                        dq_acc[at, :] = jnp.concatenate(dqs, axis=0).T
                        dk_acc[...] = dk if c == 0 else dk_acc[...] + dk
                        dv_acc[...] = dv if c == 0 else dv_acc[...] + dv
                    cos, sin = cos_t[...], sin_t[...]
                    dq, dk, dv = dq_acc[...], dk_acc[...], dv_acc[...]
                    dq = (dq * cos - swap_halves(dq, hd) * sin) * q_scale
                    dk = dk * cos - swap_halves(dk, hd) * sin
                    for i, t in enumerate((dq, dk, dv)):
                        d4[:, b, :, i * width:(i + 1) * width] = t.astype(BF16).reshape(n_tp, p_len, width)
                        b8[g, i:i + 1, :] += col_sum(t)

                @pl.when(step == 0)
                def _():
                    acc[...] = jnp.zeros_like(acc)

                @pl.loop(0, 2)
                def _(i):
                    acc[span(i, half), :] += mm(d4[pl.ds(n_chips * i, n_chips)].reshape(half, n3), w[0], NN)

                def tile(put):
                    put((pl.ds(0, n3),), mm(d4[...].reshape(tok, n3), h1[...], TN))
                    put((pl.ds(n3, width),), mm(o4[:, :, :, span(g, width)].reshape(tok, width), dx1b[...], TN))

                pair(step, 'at', tile)

            slot_blk = pl.BlockSpec((1, n_tp, seqs, p_len, width), lambda s: (order(s), 0, 0, 0, 0))
            pipe(bwd_step, grid=(n_tp,), in_specs=[slot_blk] * 3 + [slot3(n3, dim, order)])(
                q_hbm, k_hbm, v_hbm, wq)

            def ln1_bwd(rows):
                x_hat, inv_std = ln_stats(x[rows, :].astype(F32))
                dh = acc[rows, :]
                h1[rows, :] = (acc2[rows, :] + ln_grad(dh, x_hat, inv_std, gain1[...])).astype(BF16)
                vec[0:1, :] += col_sum(dh * x_hat)
                vec[1:2, :] += col_sum(dh)

            loop_rows(tok, 2 * chunk, ln1_bwd)
            stored('at', 3)
            net.start('b8', 'vec', 'gx', 'gx_own')

            def total(name, out, n_in, block, at):
                def body(*blocks):
                    p_blk, more, o_blk = blocks[1], blocks[2:-1], blocks[-1]
                    v = p_blk[0]
                    for m in more:
                        v += m[...]
                    o_blk[...] = v

                p, _, _, early, last = parts[name]
                pipe(body, grid=(2,), in_specs=[pl.BlockSpec((1,) + block, lambda i: (0,) + at(i))] + [pl.BlockSpec(block, at)] * n_in,
                     out_specs=[pl.BlockSpec(block, lambda i: (i, 0))])(p, *(early, last)[:n_in], out)

            by_row, by_col = lambda i: (i, 0), lambda i: (0, i)
            net.got('dn_next', 'dn_prev', 'dn_sum')
            total('dn', g_down, 2, (t_half, dim), by_row)
            net.got('b8', 'vec')
            b_total, v_total = b8[0], vec[:, span(me, LANES)]
            for n in range(1, n_tp):
                b_total += b_in[n]
                v_total += v_in[n]
            b8[0] = b_total
            v_sum[...] = v_total
            v_all[:, span(me, LANES)] = v_total
            net.got('at_relay')
            net.start('at_load')
            add_relayed('at')
            net.done('at_store')
            net.start('v_sum', 'at_sum')
            net.got('up_next', 'up_prev', 'up_sum')
            total('up', g_up, 2, (n_tile, half), by_col)
            net.got('at_next', 'at_prev')
            total('at', g_at, 1, (t_half, dim), by_row)
            late = ('gx', 'v_sum', 'at_sum')
            local_ends = ('_own', '_load', '_store')
            for name in net.copies:
                if name not in ('load', 'store', 'own', 'write') + late and not name.endswith(local_ends):
                    net.sent(name)
            net.got('gx', 'y', 'v_sum')
            net.start('write')
            net.done('y_own', 'gx_own', 'write')
            net.sent('gx', 'v_sum')
            net.got('at_sum')
            net.sent('at_sum')

        big = (tok, dim)
        shapes = lambda *dims, dtype=F32: sds(dims, dtype)
        flat = lambda t: t.reshape(tok, dim)
        inv_freq = ROPE_BASE ** (-2.0 * np.arange(hd // 2) / hd)
        sign = np.repeat([-1.0, 1.0], hd // 2)
        freq = np.stack([np.tile(inv_freq, 2 * heads), np.tile(sign, heads)]).astype(np.float32)
        line = lambda v: v.reshape(1, -1)
        sem = lambda n: pltpu.SemaphoreType.DMA((n,))
        low = functools.partial(shapes, dtype=BF16)
        weights = [low(n_tp, n3, dim), low(n_tp, dim, ffn), low(n_tp, ffn, dim)]
        reduction = [shapes(n_chips, n_tile, dim), shapes(2, n_tile // 2, dim), shapes(2, n_tile // 2, dim), shapes(n_tile, dim), shapes(n_tile, dim)]
        out_shape = ([low(*big)] * 2 + [shapes(dim, ffn), shapes(ffn, dim), shapes(n_tile, dim), shapes(8, dim), shapes(8, LANES)] + weights
                     + [low(n_tp, n_tp, seqs, p_len, width)] * 3 + [low(tok, n_tp * ffn), shapes(tok, n_tp * ffn)] + reduction * 3)
        plain = [pad_mask] + [line(v) for v in (ln1_gain, ln1_bias, b_out, ln2_gain, b_down, ln2_bias)] + [freq]
        heads4 = low(n_tp, seqs, p_len, n_tp * width)
        stat = shapes(n_tp, seqs, heads, seq)
        tile8 = shapes(n_tp, 8, LANES)
        row_ffn = shapes(n_tp, 1, ffn)
        scratch = ([low(*big)] * 6 + [heads4, heads4, low(n_tp, width, dim)] + [shapes(*big)] * 2
                   + [shapes(n_chips, n_tile, dim)] + [shapes(2, n_tile, dim)] + [shapes(2, n_tile // 2, dim)] * 2 + [low(n_tp, seqs, p_len, n3)]
                   + [shapes(seq, width)] * 5 + [shapes(seqs, seq, LANES), stat, stat, shapes(n_tp, 1, n3), row_ffn, row_ffn, row_ffn]
                   + [shapes(n_tp, *b_qkv.shape), tile8, tile8, shapes(8, dim), tile8, shapes(8, LANES), shapes(8, dim), low(tok, ffn)] + plain)
        outs = pl.pallas_call(
            kernel, name='layer', out_shape=out_shape, in_specs=[ANY] * 16, out_specs=[ANY] * len(out_shape),
            scratch_shapes=[pltpu.VMEM(v.shape, v.dtype) for v in scratch]
            + [sem(128), sem(128), sem(64), sem(4 * n_chips), sem(3 * n_chips), pltpu.SemaphoreType.REGULAR],
            compiler_params=pltpu.CompilerParams(collective_id=0, has_side_effects=True, vmem_limit_bytes=VMEM_LIMIT),
        )(flat(x_in), flat(grad_y), w_qkv.transpose(0, 2, 3, 1).reshape(n3, dim), b_qkv, w_out.reshape(width, dim),
          w_up, line(b_up), w_down, *plain)

        def finish(y_ref, gx_ref, gu_ref, gd_ref, v_ref, b_ref, pq, po, lq, lo, y_o, gx_o, gu_o, gd_o, gq_o, go_o, bq_o, bu_o, *v_o):
            y_o[...], gx_o[...], gu_o[...], gd_o[...] = y_ref[...], gx_ref[...], gu_ref[...], gd_ref[...]
            gq_o[...] = pq[...] + lq[...]
            go_o[...] = po[...] + lo[...]
            for i in range(3):
                for h in range(heads):
                    bq_o[i, h:h + 1, :] = b_ref[i:i + 1, h * hd:(h + 1) * hd]
            for i in range(ffn // LANES):
                bu_o[:, i * LANES:(i + 1) * LANES] = b_ref[3 + i:4 + i, :]
            for i, ref in enumerate(v_o):
                ref[...] = v_ref[i:i + 1, :]

        n_step = 4

        def cut(rows, cols, first=0):
            return pl.BlockSpec((rows // n_step, cols), lambda i: (first * n_step // rows + i, 0))

        def const(*dims):
            return pl.BlockSpec(dims, lambda i: (0,) * len(dims))

        main = [cut(tok, dim), cut(tok, dim), cut(dim, ffn), cut(ffn, dim)]
        att = [cut(n3, dim), cut(width, dim, n3)]
        res = pl.pallas_call(
            finish, name='finish', grid=(n_step,),
            out_shape=(sds(big, BF16), sds(big, BF16), shapes(dim, ffn), shapes(ffn, dim), shapes(n3, dim), shapes(width, dim),
                       shapes(*b_qkv.shape), shapes(1, ffn)) + (shapes(1, dim),) * 6,
            in_specs=main + [const(8, dim), const(8, LANES)] + att * 2,
            out_specs=tuple(main) + (cut(n3, dim), cut(width, dim), const(*b_qkv.shape), const(1, ffn)) + (const(1, dim),) * 6,
            compiler_params=pltpu.CompilerParams(vmem_limit_bytes=VMEM_LIMIT),
        )(*outs[:4], *outs[5:7], outs[4], outs[4], outs[-1], outs[-1])
        y_out, grad_x, grad_w_up, grad_w_down, gq, go, grad_b_qkv, grad_b_up = res[:8]
        v = [t.reshape(dim) for t in res[8:]]
        return (y_out.reshape(x_in.shape), grad_x.reshape(x_in.shape), v[0], v[1], gq.reshape(3, heads, hd, dim).transpose(0, 3, 1, 2),
                grad_b_qkv, go.reshape(heads, hd, dim), v[2], v[3], v[4], grad_w_up, grad_b_up.reshape(ffn), grad_w_down, v[5])

    return jax.shard_map(device_step, mesh=mesh, in_specs=in_specs, out_specs=out_specs, check_vma=False)
```

```python
import functools

import jax
import jax.numpy as jnp
import numpy as np
from jax import lax
from jax.experimental import pallas as pl
from jax.experimental.pallas import tpu as pltpu
from jax.sharding import PartitionSpec as P

LN_EPS = 1e-5
ROPE_BASE = 10000.0
INV_SQRT2 = 0.7071067811865476
INV_SQRT_2PI = 0.3989422804014327
NEG_LARGE = -1e30
F32 = jnp.float32
BF16 = jnp.bfloat16
VMEM_LIMIT = 66_500_000
LANES = 128
NN = (((1,), (0,)), ((), ()))
NT = (((1,), (1,)), ((), ()))
TN = (((0,), (0,)), ((), ()))
PAIR, FAR, CROSS = 1, 2, 3
ANY = pl.BlockSpec(memory_space=pl.ANY)


def mm(a, b, dims):
    return lax.dot_general(a, b, dims, preferred_element_type=F32)


def ln_stats(v):
    centered = v - jnp.mean(v, axis=-1, keepdims=True)
    inv_std = lax.rsqrt(jnp.mean(centered * centered, axis=-1, keepdims=True) + LN_EPS)
    return centered * inv_std, inv_std


def ln_grad(d_out, x_hat, inv_std, gain):
    d_hat = d_out * gain
    return inv_std * (d_hat - jnp.mean(d_hat, axis=-1, keepdims=True) - x_hat * jnp.mean(d_hat * x_hat, axis=-1, keepdims=True))


def col_sum(t):
    return jnp.sum(t, axis=0, keepdims=True)


def swap_halves(t, head_dim):
    half = head_dim // 2
    lane = lax.broadcasted_iota(jnp.int32, t.shape, t.ndim - 1)
    return jnp.where(lane % head_dim < half, pltpu.roll(t, t.shape[-1] - half, t.ndim - 1), pltpu.roll(t, half, t.ndim - 1))


def span(i, n):
    return pl.ds(pl.multiple_of(i * n, n), n)


def loop_rows(total, n, body):
    @pl.loop(0, total // n)
    def _(i):
        body(span(i, n))


class Net:
    def __init__(self, n_tp, send, recv, local):
        self.n_tp, self.send, self.recv, self.local = n_tp, send, recv, local
        self.copies, self.count, self.n_local = {}, 0, 0

    def peer(self, chip, core=0):
        me = lax.axis_index('tp')
        way = 1 - 2 * lax.rem(lax.div(me, 2), 2)
        at = lax.rem(me + 2 * chip * way + self.n_tp, self.n_tp) if chip else me
        return at + 1 - 2 * lax.rem(at, 2) if core else at

    def add(self, name, src, dst, chip, core=0):
        n = self.count
        self.count += 1

        def make():
            return pltpu.make_async_remote_copy(
                src_ref=src(), dst_ref=dst(), send_sem=self.send.at[n], recv_sem=self.recv.at[n],
                device_id={'tp': self.peer(chip, core)}, device_id_type=pl.DeviceIdType.MESH)

        self.copies.setdefault(name, []).append(make)

    def add_local(self, name, src, dst):
        n = self.n_local
        self.n_local += 1
        self.copies.setdefault(name, []).append(lambda: pltpu.make_async_copy(src(), dst(), self.local.at[n]))

    def start(self, *names):
        for name in names:
            for make in self.copies[name]:
                make().start()

    def got(self, *names):
        for name in names:
            with jax.named_scope('got_' + name):
                for make in self.copies[name]:
                    make().wait_recv()

    def sent(self, *names):
        for name in names:
            for make in self.copies[name]:
                make().wait_send()

    def done(self, *names):
        for name in names:
            with jax.named_scope('done_' + name):
                for make in self.copies[name]:
                    make().wait()

    def gather(self, name, own, buf, via):
        for stage, chip in (('p', PAIR), ('c', CROSS)):
            self.add(name + stage, lambda: own, lambda c=chip: buf.at[2 * c], chip)
        self.add(name + 'm', lambda: own, lambda: buf.at[1], 0, 1)
        self.add(name + 'r', lambda: buf.at[2 * (PAIR + CROSS - via)], lambda: buf.at[2 * FAR], via)
        for stage, chip in (('f', PAIR), ('g', CROSS), ('l', FAR)):
            self.add(name + stage, lambda c=chip: buf.at[2 * c], lambda c=chip: buf.at[2 * c + 1], 0, 1)

    def exchange(self, name, src, dst, rows):
        me = lax.axis_index('tp')
        for core in range(2):
            for chip in (PAIR, CROSS, FAR, 0):
                if chip + core:
                    self.add(name, lambda c=chip, k=core: src.at[span(self.peer(c, k), rows)], lambda: dst.at[span(me, rows)], chip, core)
        self.add_local(name + '_own', lambda: src.at[span(me, rows)], lambda: dst.at[span(me, rows)])

    def multicast(self, name, src, dst, pair_dst, rows):
        me = lax.axis_index('tp')
        at = lambda buf: (lambda: buf.at[span(me, rows)])
        other = {0: PAIR, PAIR: 0, CROSS: FAR}
        for chip, stage in ((CROSS, '_cross'), (PAIR, '_pair'), (0, '_pair')):
            for core in range(2):
                if chip + core:
                    for c, buf in ((chip, dst), (other[chip], pair_dst)):
                        self.add(name + stage, lambda c=c, k=core: src.at[span(self.peer(c, k), rows)], at(buf), chip, core)
        for c, buf in ((0, dst), (PAIR, pair_dst)):
            self.add_local(name + '_own', lambda c=c: src.at[span(self.peer(c), rows)], at(buf))
        came = lambda buf: (lambda: buf.at[span(lax.div(self.peer(CROSS), 2), 2 * rows)])
        self.add(name + '_fwd', came(dst), came(pair_dst), PAIR)
        self.add(name + '_fwd', came(pair_dst), came(dst), PAIR)


def solution(mesh):
    n_tp = mesh.shape['tp']
    n_chips = n_tp // 2
    act_spec = P('dp', 'tp', None)
    rep_vec = P(None)
    part_vec = P('dp')
    in_specs = (act_spec, act_spec, P('dp', None), rep_vec, rep_vec, P(None, None, 'tp', None), P(None, 'tp', None),
                P('tp', None, None), rep_vec, rep_vec, rep_vec, P(None, 'tp'), P('tp'), P('tp', None), rep_vec)
    out_specs = (act_spec, act_spec, part_vec, part_vec, P('dp', None, 'tp', None), P('dp', 'tp', None),
                 P(('dp', 'tp'), None, None), part_vec, part_vec, part_vec, P('dp', 'tp'), P(('dp', 'tp')),
                 P(('dp', 'tp'), None), part_vec)

    def device_step(x_in, grad_y, pad_mask, ln1_gain, ln1_bias, w_qkv, b_qkv, w_out, b_out, ln2_gain, ln2_bias, w_up, b_up, w_down, b_down):
        batch, p_len, dim = x_in.shape
        seq = pad_mask.shape[1]
        _, _, heads, hd = w_qkv.shape
        seqs = batch // n_tp
        ffn = w_up.shape[1]
        width = heads * hd
        n3 = 3 * width
        tok = seqs * seq
        chunk = seqs * p_len
        qc = seq // 2
        q_scale = hd ** -0.5
        sds = jax.ShapeDtypeStruct
        n_tile = n3 + width
        half = dim // 2

        def kernel(*refs):
            it = iter(refs)
            take = lambda n: [next(it) for _ in range(n)]
            (x_ref, dy_ref, wq_ref, bq_ref, wo_ref, wu_ref, bu_ref, wd_ref), plain = take(8), take(8)
            y_out, gx_out, g_up, g_down, g_at, g_vec, g_b, wq, wu, wd, q_hbm, k_hbm, v_hbm, act_hbm, slope_hbm = take(15)
            p_at, got_at, sum_at, early_at, last_at, x_dn, x_up, p_dn, p_up, r_dn, r_up = take(11)
            x, h1, dy, x1, h2, dx1b, h2p, dyp, o4, do4, wo, acc, acc2, p_rcv, p_snd, d4 = take(16)
            dq_acc, dk_acc, dv_acc, cos_t, sin_t, ok, m_st, l_st, b_att, b_ffn, u_all, gb, b_all, b8, b_in, vec, v_in, v_own = take(18)
            dpre, act_p, dpre_p = take(3)
            here = take(8)
            send, recv, local, pair_send, pair_recv, pair_ready = take(6)
            net = Net(n_tp, send, recv, local)
            me = lax.axis_index('tp')
            mask_ref, gain1, bias1, bias_o, gain2, bias_d, bias2, freq_ref = here

            net.gather('q', wq_ref, wq, CROSS)
            net.gather('o', wo_ref, wo, CROSS)
            net.gather('u', wu_ref, wu, CROSS)
            net.gather('d', wd_ref, wd, PAIR)
            net.exchange('x', x_ref, x, chunk)
            net.multicast('dy', dy_ref, dy, dyp, chunk)
            net.exchange('y', x1, y_out, chunk)
            net.exchange('gx', h1, gx_out, chunk)
            for chip in range(n_chips):
                for core in range(2):
                    if chip + core:
                        slot = 2 * chip + core
                        net.add('bias', lambda: bq_ref, lambda n=slot: b_all.at[n], chip, core)
                        net.add('bias', lambda: bu_ref, lambda n=slot: u_all.at[n], chip, core)
                        net.add('b8', lambda n=slot: b8.at[n], lambda n=slot: b_in.at[n], chip, core)
                        for r, rows in enumerate((pl.ds(0, 2 * n_tp), pl.ds(2 * n_tp, 4 * n_tp))):
                            net.add(f'v{r}', lambda p=rows: v_own.at[p], lambda n=slot, p=rows: v_in.at[n, p], chip, core)
            net.add('h2p', lambda: h2, lambda: h2p, PAIR)
            net.add('dn_x', lambda: x_dn, lambda: r_dn, CROSS)
            net.add('up_x', lambda: x_up, lambda: r_up, CROSS)
            net.add('at_early', lambda: p_at.at[PAIR], lambda: early_at, PAIR)
            t_half = n_tile // 2
            for i, part in enumerate((pl.ds(0, t_half), pl.ds(t_half, t_half))):
                net.add(f'at_relay{i}', lambda p=part: p_at.at[FAR, p], lambda p=part: got_at.at[p], PAIR)
                net.add(f'at_sum{i}', lambda p=part: sum_at.at[p], lambda p=part: last_at.at[p], CROSS)
                net.add_local(f'at{i}_load', lambda p=part: got_at.at[p], lambda p=part: p_rcv.at[0, p])
                net.add_local(f'at{i}_load', lambda p=part: p_at.at[CROSS, p], lambda p=part: p_rcv.at[1, p])
                net.add_local(f'at{i}_store', lambda p=part: p_rcv.at[1, p], lambda p=part: sum_at.at[p])
            for src, dst in zip(plain, here):
                net.add_local('own', lambda r=src: r, lambda r=dst: r)
            net.add_local('write', lambda: v_own, lambda: g_vec)
            net.add_local('write', lambda: b8.at[0], lambda: g_b)
            for ref, tmp, buf in ((wq_ref, lambda: h2.at[pl.ds(0, n3)], wq), (wu_ref, lambda: x1.at[:, pl.ds(0, ffn)], wu),
                                        (wd_ref, lambda: dx1b.at[pl.ds(0, ffn)], wd)):
                net.add_local('load', lambda r=ref: r, tmp)
                net.add_local('store', tmp, lambda b=buf: b.at[0])
            net.add_local('own', lambda: wo_ref, lambda: wo.at[0])
            net.add_local('own', lambda: bq_ref, lambda: b_all.at[0])
            net.add_local('own', lambda: bu_ref, lambda: u_all.at[0])
            def pass_on(i):
                net.got(f'at_relay{i}')
                net.start(f'at{i}_load')
                net.done(f'at{i}_load')

                def body(rows):
                    rows = pl.ds(i * t_half + rows.start, rows.size)
                    p_rcv[1, rows] += p_rcv[0, rows]

                loop_rows(t_half, 8, body)
                net.start(f'at{i}_store')
                net.done(f'at{i}_store')
                net.start(f'at_sum{i}')

            def pack(lo, hi):
                for r in range(lo, hi):
                    for i in range(n_tp):
                        v_own[r * n_tp + i:r * n_tp + i + 1, :] = vec[r:r + 1, i * LANES:(i + 1) * LANES]

            def hooks(step, table):
                for at, act in table.items():
                    @pl.when(step == at)
                    def _(act=act):
                        act()

            tile_order = (FAR, PAIR, CROSS, 0)

            def place(i):
                return jnp.where(i == 0, FAR, jnp.where(i == 1, PAIR, jnp.where(i == 2, CROSS, 0)))

            def order(s):
                return 2 * place(lax.div(s, 2)) + 1 - lax.rem(s, 2)

            def to_partner(src, dst, sem):
                return pltpu.make_async_remote_copy(
                    src_ref=p_snd.at[src], dst_ref=p_rcv.at[dst], send_sem=pair_send.at[sem], recv_sem=pair_recv.at[sem],
                    device_id={'tp': net.peer(0, 1)}, device_id_type=pl.DeviceIdType.MESH)

            def keep(i, to):
                return pltpu.make_async_copy(p_rcv.at[i], to, pair_send.at[2 * n_tp + i])

            def into(i):
                return lambda at, v: p_snd.__setitem__((i,) + at, v)

            def add_sent(i, j):
                def body(rows):
                    p_rcv[j, rows] += p_snd[i, rows]

                loop_rows(n_tile, 16, body)

            def pair_go(s):
                @pl.when(lax.rem(s, 2) == 1)
                def _():
                    to_partner(0, lax.div(s, 2), lax.div(s, 2)).start()

            def pair(s, tile):
                j = lax.div(s, 2)
                odd = lax.rem(s, 2)
                tile(into(odd))

                @pl.when(odd == 1)
                def _():
                    copy = to_partner(0, j, j)
                    copy.wait_send()
                    copy.wait_recv()
                    add_sent(1, j)
                    keep(j, p_at.at[place(j)]).start()

            def stored(i):
                keep(i, p_at.at[tile_order[i]]).wait()

            def pair_begin():
                pl.semaphore_signal(pair_ready, inc=1, device_id={'tp': net.peer(0, 1)}, device_id_type=pl.DeviceIdType.MESH)
                pl.semaphore_wait(pair_ready, 1)

            barrier = pltpu.get_barrier_semaphore()
            for chip in range(n_chips):
                for core in range(2):
                    if chip + core:
                        pl.semaphore_signal(barrier, inc=1, device_id={'tp': net.peer(chip, core)}, device_id_type=pl.DeviceIdType.MESH)
            pl.semaphore_wait(barrier, n_tp - 1)
            net.start('qp', 'qc', 'x', 'qm', 'bias', 'own', 'load', 'x_own', 'dy_own')
            net.done('own')
            angle = lax.broadcasted_iota(jnp.int32, (seq, width), 0).astype(F32) * freq_ref[0:1, :]
            cos_t[...] = jnp.cos(angle)
            sin_t[...] = jnp.sin(angle) * freq_ref[1:2, :]
            for b in range(seqs):
                row = mask_ref[pl.ds(me * seqs + b, 1), :].astype(F32)
                ok[b] = jnp.broadcast_to(row, (LANES, seq)).T
            net.done('load')
            net.start('store')
            net.got('qp', 'qc')
            net.start('qr', 'dy_cross', 'oc', 'op', 'up', 'dy_pair', 'qf', 'qg', 'om')
            net.done('x_own', 'dy_own')
            net.got('bias')
            for n in range(n_tp):
                b = b_all[n]
                b_att[n] = jnp.concatenate([b[i // heads, i % heads:i % heads + 1, :] for i in range(3 * heads)], axis=1)
                b_ffn[n] = u_all[n]
            net.got('x')

            def ln1(rows):
                x_hat, _ = ln_stats(x[rows, :].astype(F32))
                h1[rows, :] = (x_hat * gain1[...] + bias1[...]).astype(BF16)

            loop_rows(tok, chunk, ln1)
            net.done('store')
            net.got('qm', 'qf', 'qg')

            def arrival(s):
                return s + 2 * lax.div(s, n_chips) - n_chips * lax.div(s, n_chips + 2)

            def qkv_step(ps, w, q_ref, k_ref, v_ref):
                s = ps.index[0]
                hooks(s, {2: lambda: (net.got('op'), net.start('or', 'uc', 'um', 'of')), 4: lambda: (net.got('qr'), net.start('ql')),
                          5: lambda: net.got('ql')})
                n_src = tok // chunk // 2

                @pl.loop(0, 2)
                def _(i):
                    rows = span(i, tok // 2)
                    t = mm(h1[rows, :], w[0], NT) + b_att[arrival(s)]
                    cos, sin = (t_ref[span(i, seq // 2), :].reshape(n_src, 1, p_len, width) for t_ref in (cos_t, sin_t))

                    def rope(v):
                        out = v.reshape(n_src, seqs, p_len, width) * cos + swap_halves(v, hd).reshape(n_src, seqs, p_len, width) * sin
                        return out.astype(BF16)

                    src = span(i, n_src)
                    q_ref[0, src] = rope(t[:, :width] * q_scale)
                    k_ref[0, src] = rope(t[:, width:2 * width])
                    v_ref[0, src] = t[:, 2 * width:].reshape(n_src, seqs, p_len, width).astype(BF16)

            slot3 = lambda rows, cols, f=lambda s: s: pl.BlockSpec((1, rows, cols), lambda s: (f(s), 0, 0))

            def pipe(body, **specs):
                def run(*refs):
                    with jax.named_scope(body.__name__):
                        pltpu.emit_pipeline(body, _explicit_indices=True, **specs)(*refs)

                return run

            pipe(qkv_step, grid=(n_tp,), in_specs=[slot3(n3, dim, arrival)],
                 out_specs=[pl.BlockSpec((1, n_tp, seqs, p_len, width), lambda s: (arrival(s), 0, 0, 0, 0))] * 3)(
                wq, q_hbm, k_hbm, v_hbm)

            srcs = qc // p_len
            lane = lax.broadcasted_iota(jnp.int32, (qc, width), 1)

            def attn_step(ps, q_ref, k_ref, v_ref):
                g, b = ps.index
                hooks(g * seqs + b, {
                    8: lambda: (net.got('dy_cross'), net.start('dy_fwd')), 9: lambda: (net.got('up'), net.start('ur', 'dc', 'dm', 'uf')),
                    14: lambda: (net.got('oc', 'or'), net.start('og', 'ol'))})
                bad = ok[b][:, 0:1] <= 0
                k = k_ref[0, :, 0].reshape(seq, width)
                v_t = v_ref[0, :, 0].reshape(seq, width).T
                for c in range(seq // qc):
                    src = slice(c * srcs, (c + 1) * srcs)
                    cols = slice(c * qc, (c + 1) * qc)
                    q = q_ref[0, src, 0].reshape(qc, width)
                    outs = []
                    for h in range(heads):
                        s = jnp.where(bad, NEG_LARGE, mm(k, jnp.where(lane // hd == h, q, jnp.zeros_like(q)), NT))
                        m = jnp.max(s, axis=0, keepdims=True)
                        e = jnp.exp(s - m)
                        r = 1.0 / col_sum(e)
                        outs.append(mm(v_t[h * hd:(h + 1) * hd], (e * r).astype(BF16), NN))
                        m_st[g, b, h:h + 1, cols] = m
                        l_st[g, b, h:h + 1, cols] = r
                    o4[src, b, :, span(g, width)] = jnp.concatenate(outs, axis=0).T.astype(BF16).reshape(srcs, p_len, width)

            head_blk = pl.BlockSpec((1, n_tp, 1, p_len, width), lambda g, b: (g, 0, b, 0, 0))
            pipe(attn_step, grid=(n_tp, seqs), in_specs=[head_blk] * 3)(q_hbm, k_hbm, v_hbm)

            net.got('om', 'of', 'og', 'ol')

            @pl.loop(0, tok // (2 * chunk))
            def _(i):
                rows = span(i, 2 * chunk)
                o = o4[pl.ds(2 * i, 2)].reshape(2 * chunk, n_tp * width)
                low = (x[rows, :].astype(F32) + (mm(o, wo[...].reshape(n_tp * width, dim), NN) + bias_o[...])).astype(BF16)
                x1[rows, :] = low
                x_hat, _ = ln_stats(low.astype(F32))
                h2[rows, :] = (x_hat * gain2[...] + bias2[...]).astype(BF16)

            net.start('h2p', 'dp')

            def gelu(pre):
                erf_term = lax.erf(pre * INV_SQRT2)
                act = (0.5 * pre * (1.0 + erf_term)).astype(BF16)
                return act, 0.5 * (1.0 + erf_term) + pre * jnp.exp(-0.5 * pre * pre) * INV_SQRT_2PI

            def up_step(ps, w, act_ref, slope_ref):
                s = ps.index[0]
                hooks(s, {2: lambda: (net.got('uc'), net.start('ug')), 3: lambda: net.got('ug'), 4: lambda: (net.got('ur'), net.start('ul')),
                          5: lambda: net.got('ul')})

                def body(rows):
                    act_ref[rows, :], slope_ref[rows, :] = gelu(mm(h2[rows, :], w[0], NN) + b_ffn[arrival(s)])

                loop_rows(tok, half, body)

            cols = lambda f: pl.BlockSpec((tok, ffn), lambda s: (0, f(s)))
            wu_spec, wd_spec = functools.partial(slot3, dim, ffn), functools.partial(slot3, ffn, dim)
            net.got('um', 'uf')
            pipe(up_step, grid=(n_tp,), in_specs=[wu_spec(arrival)], out_specs=[cols(arrival)] * 2)(wu, act_hbm, slope_hbm)
            net.got('dy_pair', 'dy_fwd', 'dm')

            def backward(slot, wd_s, wu_s, act_ref, slope_ref, add):
                if add:
                    gb[slot] = jnp.zeros_like(gb[0])

                def body(rows):
                    d_pre = mm(dy[rows, :], wd_s[0], NT) * slope_ref[rows, :]
                    low = d_pre.astype(BF16)
                    dpre[rows, :] = low
                    if add:
                        gb[slot] += col_sum(d_pre)
                        acc[rows, :] += mm(act_ref[rows, :], wd_s[0], NN)
                        acc2[rows, :] += mm(low, wu_s[0], NT)

                loop_rows(tok, half, body)

            def mlp(n, f, table):
                def mlp_step(ps, wd_s, wu_s, act_ref, slope_ref):
                    s = ps.index[0]
                    backward(f(s), wd_s, wu_s, act_ref, slope_ref, True)
                    hooks(s, table)

                pipe(mlp_step, grid=(n,), in_specs=[wd_spec(f), wu_spec(f), cols(f), cols(f)])(wd, wu, act_hbm, slope_hbm)

            def grads(chip, at, x_refs, add, sends):
                f = lambda s: 2 * chip + 1 - s

                def grads_step(ps, wd_s, wu_s, act_ref, slope_ref):
                    s = ps.index[0]
                    slot = f(s)

                    @pl.when(s == 1)
                    def _():
                        for i in range(2):
                            to_partner(i, at + i, n_tp + at + i).start()

                    backward(slot, wd_s, wu_s, act_ref, slope_ref, add)

                    def body(rows):
                        act, slope = gelu(mm(h2p[rows, :], wu_s[0], NN) + b_ffn[slot])
                        act_p[rows, :] = act
                        dpre_p[rows, :] = (mm(dyp[rows, :], wd_s[0], NT) * slope).astype(BF16)

                    loop_rows(tok, half, body)

                    def down(put):
                        put((pl.ds(0, ffn),), mm(act_ref[...], dy[...], TN) + mm(act_p[...], dyp[...], TN))

                    def up(put):
                        for i in range(2):
                            part = pl.ds(i * half, half)
                            put((pl.ds(0, ffn), part), mm(h2[:, part], dpre[...], TN) + mm(h2p[:, part], dpre_p[...], TN))

                    for i, tile in enumerate((down, up)):
                        copy = to_partner(i, at + i, n_tp + at + i)

                        @pl.when(s == 1)
                        def _():
                            copy.wait_send()

                        tile(into(i))

                        @pl.when(s == 1)
                        def _():
                            copy.wait_recv()
                            add_sent(i, at + i)
                            keep(at + i, x_refs[i]).start()
                            if i:
                                keep(at, x_refs[0]).wait()
                                net.start(*sends[:1])
                                keep(at + 1, x_refs[1]).wait()
                                net.start(*sends[1:])

                pipe(grads_step, grid=(2,), in_specs=[wd_spec(f), wu_spec(f), cols(f), cols(f)])(wd, wu, act_hbm, slope_hbm)

            acc[...] = jnp.zeros_like(acc)
            acc2[...] = jnp.zeros_like(acc2)
            mlp(2, lambda s: s, {})
            net.got('dc')
            net.start('dg', 'dr')
            net.got('dg', 'h2p')
            grads(CROSS, 0, (x_dn, x_up), True, ('dn_x', 'up_x'))
            net.got('dp')
            net.start('df')
            net.got('df')
            mlp(n_chips, lambda s: s + 2, {0: lambda: (net.got('dr'), net.start('dl'), net.got('dl'))})
            vec[...] = jnp.zeros_like(vec)

            @pl.loop(0, tok // (2 * chunk))
            def _(i):
                rows = span(i, 2 * chunk)
                x1_f, dy_f, dh = x1[rows, :].astype(F32), dy[rows, :].astype(F32), acc2[rows, :]
                x1[rows, :] = (x1_f + (acc[rows, :] + bias_d[...])).astype(BF16)
                x_hat, inv_std = ln_stats(x1_f)
                d_x1 = dy_f + ln_grad(dh, x_hat, inv_std, gain2[...])
                acc2[rows, :] = d_x1
                low = d_x1.astype(BF16)
                dx1b[rows, :] = low
                d_o = mm(low, wo[...].reshape(n_tp * width, dim), NT).astype(BF16)
                do4[pl.ds(2 * i, 2)] = d_o.reshape(2, seqs, p_len, n_tp * width)
                for n, t in enumerate((d_x1, dh * x_hat, dh, dy_f)):
                    vec[2 + n:3 + n, :] += col_sum(t)

            pack(2, 6)
            pair_begin()

            def bwd_step(ps, q_ref, k_ref, v_ref, w):
                step = ps.index[0]
                g = order(step)
                hooks(step, {0: lambda: net.start('y', 'v1', 'y_own'), 2: lambda: (stored(0), net.start('at_relay0', 'at_relay1')),
                             4: lambda: (stored(1), net.start('at_early'))})
                pair_go(step)
                b8[g] = jnp.zeros_like(b8[0])
                for i in range(ffn // LANES):
                    b8[g, 3 + i:4 + i, :] = gb[g][:, i * LANES:(i + 1) * LANES]
                for b in range(seqs):
                    bad = ok[b][:, 0:1] <= 0
                    k = k_ref[0, :, b].reshape(seq, width)
                    v = v_ref[0, :, b].reshape(seq, width)
                    k_t = k.T
                    for c in range(seq // qc):
                        src = slice(c * srcs, (c + 1) * srcs)
                        at = slice(c * qc, (c + 1) * qc)
                        q = q_ref[0, src, b].reshape(qc, width)
                        d_o = do4[src, b, :, span(g, width)].reshape(qc, width)
                        dk = jnp.zeros((seq, width), F32)
                        dv = jnp.zeros((seq, width), F32)
                        dqs = []
                        for h in range(heads):
                            mine = lane // hd == h
                            q_h = jnp.where(mine, q, jnp.zeros_like(q))
                            do_h = jnp.where(mine, d_o, jnp.zeros_like(d_o))
                            s = jnp.where(bad, NEG_LARGE, mm(k, q_h, NT))
                            p = jnp.exp(s - m_st[g, b, h:h + 1, at]) * l_st[g, b, h:h + 1, at]
                            dv += mm(p.astype(BF16), do_h, NN)
                            dp = mm(v, do_h, NT)
                            ds = (p * (dp - col_sum(dp * p))).astype(BF16)
                            dk += mm(ds, q_h, NN)
                            dqs.append(mm(k_t[h * hd:(h + 1) * hd], ds, NN))
                        dq_acc[at, :] = jnp.concatenate(dqs, axis=0).T
                        dk_acc[...] = dk if c == 0 else dk_acc[...] + dk
                        dv_acc[...] = dv if c == 0 else dv_acc[...] + dv
                    cos, sin = cos_t[...], sin_t[...]
                    dq, dk, dv = dq_acc[...], dk_acc[...], dv_acc[...]
                    dq = (dq * cos - swap_halves(dq, hd) * sin) * q_scale
                    dk = dk * cos - swap_halves(dk, hd) * sin
                    for i, t in enumerate((dq, dk, dv)):
                        d4[:, b, :, i * width:(i + 1) * width] = t.astype(BF16).reshape(n_tp, p_len, width)
                        b8[g, i:i + 1, :] += col_sum(t)

                @pl.when(step == 0)
                def _():
                    acc[...] = jnp.zeros_like(acc)

                @pl.loop(0, 2)
                def _(i):
                    acc[span(i, half), :] += mm(d4[pl.ds(n_chips * i, n_chips)].reshape(half, n3), w[0], NN)

                def tile(put):
                    put((pl.ds(0, n3),), mm(d4[...].reshape(tok, n3), h1[...], TN))
                    put((pl.ds(n3, width),), mm(o4[:, :, :, span(g, width)].reshape(tok, width), dx1b[...], TN))

                pair(step, tile)

            slot_blk = pl.BlockSpec((1, n_tp, seqs, p_len, width), lambda s: (order(s), 0, 0, 0, 0))
            pipe(bwd_step, grid=(n_tp,), in_specs=[slot_blk] * 3 + [slot3(n3, dim, order)])(
                q_hbm, k_hbm, v_hbm, wq)

            def ln1_bwd(rows):
                x_hat, inv_std = ln_stats(x[rows, :].astype(F32))
                dh = acc[rows, :]
                h1[rows, :] = (acc2[rows, :] + ln_grad(dh, x_hat, inv_std, gain1[...])).astype(BF16)
                vec[0:1, :] += col_sum(dh * x_hat)
                vec[1:2, :] += col_sum(dh)

            loop_rows(tok, 2 * chunk, ln1_bwd)
            for i in (2, 3):
                stored(i)
            pack(0, 2)
            net.start('b8', 'v0')
            pass_on(0)

            pair_begin()
            grads(0, 2, (p_dn, p_up), False, ())
            pass_on(1)
            net.start('gx', 'gx_own')

            def total(refs, out, block, at):
                def body(*blocks):
                    v = blocks[1][...]
                    for more in blocks[2:-1]:
                        v += more[...]
                    blocks[-1][...] = v

                pipe(body, grid=(2,), in_specs=[pl.BlockSpec(block, at)] * len(refs),
                     out_specs=[pl.BlockSpec(block, lambda i: (i, 0))])(*refs, out)

            by_row, by_col = lambda i: (i, 0), lambda i: (0, i)
            net.got('b8', 'v0', 'v1')
            b_total, v_total = b8[0], v_own[...]
            for n in range(1, n_tp):
                b_total += b_in[n]
                v_total += v_in[n]
            net.got('dn_x', 'up_x')
            total((p_dn, r_dn), g_down, (t_half, dim), by_row)
            total((p_up, r_up), g_up, (n_tile, half), by_col)
            net.got('at_early', 'at_sum0', 'at_sum1')
            total((p_at.at[0], early_at, last_at), g_at, (t_half, dim), by_row)
            for name in net.copies:
                if name not in ('load', 'store', 'own', 'write', 'gx') and not name.endswith(('_own', '_load', '_store')):
                    net.sent(name)
            b8[0] = b_total
            v_own[...] = v_total
            net.got('y')
            net.start('write')
            net.done('y_own', 'gx_own', 'write')
            net.got('gx')
            net.sent('gx')

        big = (tok, dim)
        shapes = lambda *dims, dtype=F32: sds(dims, dtype)
        flat = lambda t: t.reshape(tok, dim)
        inv_freq = ROPE_BASE ** (-2.0 * np.arange(hd // 2) / hd)
        sign = np.repeat([-1.0, 1.0], hd // 2)
        freq = np.stack([np.tile(inv_freq, 2 * heads), np.tile(sign, heads)]).astype(np.float32)
        line = lambda v: v.reshape(1, -1)
        sem = lambda n: pltpu.SemaphoreType.DMA((n,))
        low = functools.partial(shapes, dtype=BF16)
        weights = [low(n_tp, n3, dim), low(n_tp, dim, ffn), low(n_tp, ffn, dim)]
        tiles = [shapes(n_chips, n_tile, dim)] + [shapes(n_tile, dim)] * 10
        out_shape = ([low(*big)] * 2 + [shapes(dim, ffn), shapes(ffn, dim), shapes(n_tile, dim), shapes(6 * n_tp, LANES), shapes(8, LANES)] + weights
                     + [low(n_tp, n_tp, seqs, p_len, width)] * 3 + [low(tok, n_tp * ffn), shapes(tok, n_tp * ffn)] + tiles)
        plain = [pad_mask] + [line(v) for v in (ln1_gain, ln1_bias, b_out, ln2_gain, b_down, ln2_bias)] + [freq]
        heads4 = low(n_tp, seqs, p_len, n_tp * width)
        stat = shapes(n_tp, seqs, heads, seq)
        tile8 = shapes(n_tp, 8, LANES)
        row_ffn = shapes(n_tp, 1, ffn)
        scratch = ([low(*big)] * 8 + [heads4, heads4, low(n_tp, width, dim)] + [shapes(*big)] * 2
                   + [shapes(n_chips, n_tile, dim), shapes(2, n_tile, dim), low(n_tp, seqs, p_len, n3)]
                   + [shapes(seq, width)] * 5 + [shapes(seqs, seq, LANES), stat, stat, shapes(n_tp, 1, n3), row_ffn, row_ffn, row_ffn]
                   + [shapes(n_tp, *b_qkv.shape), tile8, tile8, shapes(8, dim), shapes(n_tp, 6 * n_tp, LANES), shapes(6 * n_tp, LANES)]
                   + [low(tok, ffn)] * 3 + plain)
        outs = pl.pallas_call(
            kernel, name='layer', out_shape=out_shape, in_specs=[ANY] * 16, out_specs=[ANY] * len(out_shape),
            scratch_shapes=[pltpu.VMEM(v.shape, v.dtype) for v in scratch]
            + [sem(128), sem(128), sem(64), sem(3 * n_tp), sem(3 * n_tp), pltpu.SemaphoreType.REGULAR],
            compiler_params=pltpu.CompilerParams(collective_id=0, has_side_effects=True, vmem_limit_bytes=VMEM_LIMIT),
        )(flat(x_in), flat(grad_y), w_qkv.transpose(0, 2, 3, 1).reshape(n3, dim), b_qkv, w_out.reshape(width, dim),
          w_up, line(b_up), w_down, *plain)

        def finish(y_ref, gx_ref, gu_ref, gd_ref, v_ref, b_ref, pq, po, y_o, gx_o, gu_o, gd_o, gq_o, go_o, bq_o, bu_o, *v_o):
            y_o[...], gx_o[...], gu_o[...], gd_o[...] = y_ref[...], gx_ref[...], gu_ref[...], gd_ref[...]
            gq_o[...], go_o[...] = pq[...], po[...]
            for i in range(3):
                for h in range(heads):
                    bq_o[i, h:h + 1, :] = b_ref[i:i + 1, h * hd:(h + 1) * hd]
            for i in range(ffn // LANES):
                bu_o[:, i * LANES:(i + 1) * LANES] = b_ref[3 + i:4 + i, :]
            for r, ref in enumerate(v_o):
                for i in range(n_tp):
                    ref[:, i * LANES:(i + 1) * LANES] = v_ref[r * n_tp + i:r * n_tp + i + 1, :]

        n_step = 4

        def cut(rows, cols, first=0):
            return pl.BlockSpec((rows // n_step, cols), lambda i: (first * n_step // rows + i, 0))

        def const(*dims):
            return pl.BlockSpec(dims, lambda i: (0,) * len(dims))

        main = [cut(tok, dim), cut(tok, dim), cut(dim, ffn), cut(ffn, dim)]
        att = [cut(n3, dim), cut(width, dim, n3)]
        res = pl.pallas_call(
            finish, name='finish', grid=(n_step,),
            out_shape=(sds(big, BF16), sds(big, BF16), shapes(dim, ffn), shapes(ffn, dim), shapes(n3, dim), shapes(width, dim),
                       shapes(*b_qkv.shape), shapes(1, ffn)) + (shapes(1, dim),) * 6,
            in_specs=main + [const(6 * n_tp, LANES), const(8, LANES)] + att,
            out_specs=tuple(main) + (cut(n3, dim), cut(width, dim), const(*b_qkv.shape), const(1, ffn)) + (const(1, dim),) * 6,
            compiler_params=pltpu.CompilerParams(vmem_limit_bytes=VMEM_LIMIT),
        )(*outs[:4], *outs[5:7], outs[4], outs[4])
        y_out, grad_x, grad_w_up, grad_w_down, gq, go, grad_b_qkv, grad_b_up = res[:8]
        v = [t.reshape(dim) for t in res[8:]]
        return (y_out.reshape(x_in.shape), grad_x.reshape(x_in.shape), v[0], v[1], gq.reshape(3, heads, hd, dim).transpose(0, 3, 1, 2),
                grad_b_qkv, go.reshape(heads, hd, dim), v[2], v[3], v[4], grad_w_up, grad_b_up.reshape(ffn), grad_w_down, v[5])

    return jax.shard_map(device_step, mesh=mesh, in_specs=in_specs, out_specs=out_specs, check_vma=False)
```

```python
import functools

import jax
import jax.numpy as jnp
import numpy as np
from jax import lax
from jax.experimental import pallas as pl
from jax.experimental.pallas import tpu as pltpu
from jax.sharding import PartitionSpec as P

LN_EPS = 1e-5
ROPE_BASE = 10000.0
INV_SQRT2 = 0.7071067811865476
INV_SQRT_2PI = 0.3989422804014327
NEG_LARGE = -1e30
F32 = jnp.float32
BF16 = jnp.bfloat16
VMEM_LIMIT = 66_500_000
LANES = 128
NN = (((1,), (0,)), ((), ()))
NT = (((1,), (1,)), ((), ()))
TN = (((0,), (0,)), ((), ()))
PAIR, FAR, CROSS = 1, 2, 3
ANY = pl.BlockSpec(memory_space=pl.ANY)


def mm(a, b, dims):
    return lax.dot_general(a, b, dims, preferred_element_type=F32)


def ln_stats(v):
    centered = v - jnp.mean(v, axis=-1, keepdims=True)
    inv_std = lax.rsqrt(jnp.mean(centered * centered, axis=-1, keepdims=True) + LN_EPS)
    return centered * inv_std, inv_std


def ln_grad(d_out, x_hat, inv_std, gain):
    d_hat = d_out * gain
    return inv_std * (d_hat - jnp.mean(d_hat, axis=-1, keepdims=True) - x_hat * jnp.mean(d_hat * x_hat, axis=-1, keepdims=True))


def col_sum(t):
    return jnp.sum(t, axis=0, keepdims=True)


def swap_halves(t, head_dim):
    half = head_dim // 2
    lane = lax.broadcasted_iota(jnp.int32, t.shape, t.ndim - 1)
    return jnp.where(lane % head_dim < half, pltpu.roll(t, t.shape[-1] - half, t.ndim - 1), pltpu.roll(t, half, t.ndim - 1))


def span(i, n):
    return pl.ds(pl.multiple_of(i * n, n), n)


def loop_rows(total, n, body):
    @pl.loop(0, total // n)
    def _(i):
        body(span(i, n))


class Net:
    def __init__(self, n_tp, send, recv, local):
        self.n_tp, self.send, self.recv, self.local = n_tp, send, recv, local
        self.copies, self.count, self.n_local = {}, 0, 0

    def peer(self, chip, core=0):
        me = lax.axis_index('tp')
        way = 1 - 2 * lax.rem(lax.div(me, 2), 2)
        at = lax.rem(me + 2 * chip * way + self.n_tp, self.n_tp) if chip else me
        return at + 1 - 2 * lax.rem(at, 2) if core else at

    def add(self, name, src, dst, chip, core=0):
        n = self.count
        self.count += 1

        def make():
            return pltpu.make_async_remote_copy(
                src_ref=src(), dst_ref=dst(), send_sem=self.send.at[n], recv_sem=self.recv.at[n],
                device_id={'tp': self.peer(chip, core)}, device_id_type=pl.DeviceIdType.MESH)

        self.copies.setdefault(name, []).append(make)

    def add_local(self, name, src, dst):
        n = self.n_local
        self.n_local += 1
        self.copies.setdefault(name, []).append(lambda: pltpu.make_async_copy(src(), dst(), self.local.at[n]))

    def start(self, *names):
        for name in names:
            for make in self.copies[name]:
                make().start()

    def got(self, *names):
        for name in names:
            with jax.named_scope('got_' + name):
                for make in self.copies[name]:
                    make().wait_recv()

    def sent(self, *names):
        for name in names:
            for make in self.copies[name]:
                make().wait_send()

    def done(self, *names):
        for name in names:
            with jax.named_scope('done_' + name):
                for make in self.copies[name]:
                    make().wait()

    def gather(self, name, own, buf, via):
        for stage, chip in (('p', PAIR), ('c', CROSS)):
            self.add(name + stage, lambda: own, lambda c=chip: buf.at[2 * c], chip)
        self.add(name + 'm', lambda: own, lambda: buf.at[1], 0, 1)
        self.add(name + 'r', lambda: buf.at[2 * (PAIR + CROSS - via)], lambda: buf.at[2 * FAR], via)
        for stage, chip in (('f', PAIR), ('g', CROSS), ('l', FAR)):
            self.add(name + stage, lambda c=chip: buf.at[2 * c], lambda c=chip: buf.at[2 * c + 1], 0, 1)

    def exchange(self, name, src, dst, rows):
        me = lax.axis_index('tp')
        for core in range(2):
            for chip in (PAIR, CROSS, FAR, 0):
                if chip + core:
                    self.add(name, lambda c=chip, k=core: src.at[span(self.peer(c, k), rows)], lambda: dst.at[span(me, rows)], chip, core)
        self.add_local(name + '_own', lambda: src.at[span(me, rows)], lambda: dst.at[span(me, rows)])

    def multicast(self, name, src, dst, pair_dst, rows):
        me = lax.axis_index('tp')
        at = lambda buf: (lambda: buf.at[span(me, rows)])
        other = {0: PAIR, PAIR: 0, CROSS: FAR}
        for chip, stage in ((CROSS, '_cross'), (PAIR, '_pair'), (0, '_pair')):
            for core in range(2):
                if chip + core:
                    for c, buf in ((chip, dst), (other[chip], pair_dst)):
                        self.add(name + stage, lambda c=c, k=core: src.at[span(self.peer(c, k), rows)], at(buf), chip, core)
        for c, buf in ((0, dst), (PAIR, pair_dst)):
            self.add_local(name + '_own', lambda c=c: src.at[span(self.peer(c), rows)], at(buf))
        came = lambda buf: (lambda: buf.at[span(lax.div(self.peer(CROSS), 2), 2 * rows)])
        self.add(name + '_fwd', came(dst), came(pair_dst), PAIR)
        self.add(name + '_fwd', came(pair_dst), came(dst), PAIR)


def solution(mesh):
    n_tp = mesh.shape['tp']
    n_chips = n_tp // 2
    act_spec = P('dp', 'tp', None)
    rep_vec = P(None)
    part_vec = P('dp')
    in_specs = (act_spec, act_spec, P('dp', None), rep_vec, rep_vec, P(None, None, 'tp', None), P(None, 'tp', None),
                P('tp', None, None), rep_vec, rep_vec, rep_vec, P(None, 'tp'), P('tp'), P('tp', None), rep_vec)
    out_specs = (act_spec, act_spec, part_vec, part_vec, P('dp', None, 'tp', None), P('dp', 'tp', None),
                 P(('dp', 'tp'), None, None), part_vec, part_vec, part_vec, P('dp', 'tp'), P(('dp', 'tp')),
                 P(('dp', 'tp'), None), part_vec)

    def device_step(x_in, grad_y, pad_mask, ln1_gain, ln1_bias, w_qkv, b_qkv, w_out, b_out, ln2_gain, ln2_bias, w_up, b_up, w_down, b_down):
        batch, p_len, dim = x_in.shape
        seq = pad_mask.shape[1]
        _, _, heads, hd = w_qkv.shape
        seqs = batch // n_tp
        ffn = w_up.shape[1]
        width = heads * hd
        n3 = 3 * width
        tok = seqs * seq
        chunk = seqs * p_len
        qc = seq // 2
        q_scale = hd ** -0.5
        sds = jax.ShapeDtypeStruct
        n_tile = n3 + width
        half = dim // 2

        def kernel(*refs):
            it = iter(refs)
            take = lambda n: [next(it) for _ in range(n)]
            (x_ref, dy_ref, wq_ref, bq_ref, wo_ref, wu_ref, bu_ref, wd_ref), plain = take(8), take(8)
            y_out, gx_out, g_up, g_down, g_at, g_vec, g_b, wq, wu, wd, q_hbm, k_hbm, v_hbm, act_hbm, slope_hbm = take(15)
            p_at, got_at, sum_at, early_at, last_at, x_dn, x_up, p_dn, p_up, r_dn, r_up = take(11)
            x, h1, dy, x1, h2, dx1b, h2p, dyp, y, o4, do4, wo, acc, acc2, p_rcv, p_snd, d4 = take(17)
            dq_acc, dk_acc, dv_acc, cos_t, sin_t, ok, m_st, l_st, b_att, b_ffn, u_all, gb, b_all, b8, b_in, vec, v_in, v_own = take(18)
            dpre, act_p, dpre_p = take(3)
            here = take(8)
            send, recv, local, pair_send, pair_recv, pair_ready = take(6)
            net = Net(n_tp, send, recv, local)
            me = lax.axis_index('tp')
            mask_ref, gain1, bias1, bias_o, gain2, bias_d, bias2, freq_ref = here

            net.gather('q', wq_ref, wq, CROSS)
            net.gather('o', wo_ref, wo, CROSS)
            net.gather('u', wu_ref, wu, CROSS)
            net.gather('d', wd_ref, wd, PAIR)
            net.exchange('x', x_ref, x, chunk)
            net.multicast('dy', dy_ref, dy, dyp, chunk)
            net.exchange('y', y, y_out, chunk)
            net.exchange('gx', h1, gx_out, chunk)
            for chip in range(n_chips):
                for core in range(2):
                    if chip + core:
                        slot = 2 * chip + core
                        net.add('bias', lambda: bq_ref, lambda n=slot: b_all.at[n], chip, core)
                        net.add('bias', lambda: bu_ref, lambda n=slot: u_all.at[n], chip, core)
                        net.add('b8', lambda n=slot: b8.at[n], lambda n=slot: b_in.at[n], chip, core)
                        for r, rows in enumerate((pl.ds(0, 2 * n_tp), pl.ds(2 * n_tp, 4 * n_tp))):
                            net.add(f'v{r}', lambda p=rows: v_own.at[p], lambda n=slot, p=rows: v_in.at[n, p], chip, core)
            net.add('h2p', lambda: h2, lambda: h2p, PAIR)
            net.add('dn_x', lambda: x_dn, lambda: r_dn, CROSS)
            net.add('up_x', lambda: x_up, lambda: r_up, CROSS)
            net.add('at_early', lambda: p_at.at[PAIR], lambda: early_at, PAIR)
            t_half = n_tile // 2
            for i, part in enumerate((pl.ds(0, t_half), pl.ds(t_half, t_half))):
                net.add(f'at_relay{i}', lambda p=part: p_at.at[FAR, p], lambda p=part: got_at.at[p], PAIR)
                net.add(f'at_sum{i}', lambda p=part: sum_at.at[p], lambda p=part: last_at.at[p], CROSS)
                net.add_local(f'at{i}_load', lambda p=part: got_at.at[p], lambda p=part: p_rcv.at[0, p])
                net.add_local(f'at{i}_load', lambda p=part: p_at.at[CROSS, p], lambda p=part: p_rcv.at[1, p])
                net.add_local(f'at{i}_store', lambda p=part: p_rcv.at[1, p], lambda p=part: sum_at.at[p])
            for src, dst in zip(plain, here):
                net.add_local('own', lambda r=src: r, lambda r=dst: r)
            net.add_local('write', lambda: v_own, lambda: g_vec)
            net.add_local('write', lambda: b8.at[0], lambda: g_b)
            for ref, tmp, buf in ((wq_ref, lambda: h2.at[pl.ds(0, n3)], wq), (wu_ref, lambda: x1.at[:, pl.ds(0, ffn)], wu),
                                        (wd_ref, lambda: dx1b.at[pl.ds(0, ffn)], wd)):
                net.add_local('load', lambda r=ref: r, tmp)
                net.add_local('store', tmp, lambda b=buf: b.at[0])
            net.add_local('own', lambda: wo_ref, lambda: wo.at[0])
            net.add_local('own', lambda: bq_ref, lambda: b_all.at[0])
            net.add_local('own', lambda: bu_ref, lambda: u_all.at[0])
            def pass_on(i, stage):
                if stage == 0:
                    net.got(f'at_relay{i}')
                    net.start(f'at{i}_load')
                elif stage == 1:
                    net.done(f'at{i}_load')

                    def body(rows):
                        rows = pl.ds(i * t_half + rows.start, rows.size)
                        p_rcv[1, rows] += p_rcv[0, rows]

                    loop_rows(t_half, 8, body)
                    net.start(f'at{i}_store')
                else:
                    net.done(f'at{i}_store')
                    net.start(f'at_sum{i}')

            def pack(lo, hi):
                for r in range(lo, hi):
                    for i in range(n_tp):
                        v_own[r * n_tp + i:r * n_tp + i + 1, :] = vec[r:r + 1, i * LANES:(i + 1) * LANES]

            def hooks(step, table):
                for at, act in table.items():
                    @pl.when(step == at)
                    def _(act=act):
                        act()

            tile_order = (FAR, PAIR, CROSS, 0)

            def place(i):
                return jnp.where(i == 0, FAR, jnp.where(i == 1, PAIR, jnp.where(i == 2, CROSS, 0)))

            def order(s):
                return 2 * place(lax.div(s, 2)) + 1 - lax.rem(s, 2)

            def to_partner(src, dst, sem):
                return pltpu.make_async_remote_copy(
                    src_ref=p_snd.at[src], dst_ref=p_rcv.at[dst], send_sem=pair_send.at[sem], recv_sem=pair_recv.at[sem],
                    device_id={'tp': net.peer(0, 1)}, device_id_type=pl.DeviceIdType.MESH)

            def keep(i, to):
                return pltpu.make_async_copy(p_rcv.at[i], to, pair_send.at[2 * n_tp + i])

            def into(i):
                return lambda at, v: p_snd.__setitem__((i,) + at, v)

            def add_sent(i, j):
                def body(rows):
                    p_rcv[j, rows] += p_snd[i, rows]

                loop_rows(n_tile, 16, body)

            def pair_go(s):
                @pl.when(lax.rem(s, 2) == 1)
                def _():
                    to_partner(0, lax.div(s, 2), lax.div(s, 2)).start()

            def pair(s, tile):
                j = lax.div(s, 2)
                odd = lax.rem(s, 2)
                tile(into(odd))

                @pl.when(odd == 1)
                def _():
                    copy = to_partner(0, j, j)
                    copy.wait_send()
                    copy.wait_recv()
                    add_sent(1, j)
                    keep(j, p_at.at[place(j)]).start()

            def stored(i):
                keep(i, p_at.at[tile_order[i]]).wait()

            def pair_begin():
                pl.semaphore_signal(pair_ready, inc=1, device_id={'tp': net.peer(0, 1)}, device_id_type=pl.DeviceIdType.MESH)
                pl.semaphore_wait(pair_ready, 1)

            barrier = pltpu.get_barrier_semaphore()
            for chip in range(n_chips):
                for core in range(2):
                    if chip + core:
                        pl.semaphore_signal(barrier, inc=1, device_id={'tp': net.peer(chip, core)}, device_id_type=pl.DeviceIdType.MESH)
            pl.semaphore_wait(barrier, n_tp - 1)
            net.start('qp', 'qc', 'x', 'qm', 'bias', 'own', 'load', 'x_own', 'dy_own')
            net.done('own')
            angle = lax.broadcasted_iota(jnp.int32, (seq, width), 0).astype(F32) * freq_ref[0:1, :]
            cos_t[...] = jnp.cos(angle)
            sin_t[...] = jnp.sin(angle) * freq_ref[1:2, :]
            for b in range(seqs):
                row = mask_ref[pl.ds(me * seqs + b, 1), :].astype(F32)
                ok[b] = jnp.broadcast_to(row, (LANES, seq)).T
            net.done('load')
            net.start('store')
            net.got('qp', 'qc')
            net.start('qr', 'dy_cross', 'oc', 'op', 'up', 'dy_pair', 'qf', 'qg', 'om')
            net.done('x_own', 'dy_own')
            net.got('bias')
            for n in range(n_tp):
                b = b_all[n]
                b_att[n] = jnp.concatenate([b[i // heads, i % heads:i % heads + 1, :] for i in range(3 * heads)], axis=1)
                b_ffn[n] = u_all[n]
            net.got('x')

            def ln1(rows):
                x_hat, _ = ln_stats(x[rows, :].astype(F32))
                h1[rows, :] = (x_hat * gain1[...] + bias1[...]).astype(BF16)

            loop_rows(tok, chunk, ln1)
            net.done('store')
            net.got('qm', 'qf', 'qg')

            def arrival(s):
                return s + 2 * lax.div(s, n_chips) - n_chips * lax.div(s, n_chips + 2)

            def qkv_step(ps, w, q_ref, k_ref, v_ref):
                s = ps.index[0]
                hooks(s, {2: lambda: (net.got('op'), net.start('or', 'uc', 'um', 'of')), 4: lambda: (net.got('qr'), net.start('ql')),
                          5: lambda: net.got('ql')})
                n_src = tok // chunk // 2

                @pl.loop(0, 2)
                def _(i):
                    rows = span(i, tok // 2)
                    t = mm(h1[rows, :], w[0], NT) + b_att[arrival(s)]
                    cos, sin = (t_ref[span(i, seq // 2), :].reshape(n_src, 1, p_len, width) for t_ref in (cos_t, sin_t))

                    def rope(v):
                        out = v.reshape(n_src, seqs, p_len, width) * cos + swap_halves(v, hd).reshape(n_src, seqs, p_len, width) * sin
                        return out.astype(BF16)

                    src = span(i, n_src)
                    q_ref[0, src] = rope(t[:, :width] * q_scale)
                    k_ref[0, src] = rope(t[:, width:2 * width])
                    v_ref[0, src] = t[:, 2 * width:].reshape(n_src, seqs, p_len, width).astype(BF16)

            slot3 = lambda rows, cols, f=lambda s: s: pl.BlockSpec((1, rows, cols), lambda s: (f(s), 0, 0))

            def pipe(body, **specs):
                def run(*refs):
                    with jax.named_scope(body.__name__):
                        pltpu.emit_pipeline(body, _explicit_indices=True, **specs)(*refs)

                return run

            pipe(qkv_step, grid=(n_tp,), in_specs=[slot3(n3, dim, arrival)],
                 out_specs=[pl.BlockSpec((1, n_tp, seqs, p_len, width), lambda s: (arrival(s), 0, 0, 0, 0))] * 3)(
                wq, q_hbm, k_hbm, v_hbm)

            srcs = qc // p_len
            lane = lax.broadcasted_iota(jnp.int32, (qc, width), 1)

            def attn_step(ps, q_ref, k_ref, v_ref):
                g, b = ps.index
                hooks(g * seqs + b, {
                    8: lambda: (net.got('dy_cross'), net.start('dy_fwd')), 9: lambda: (net.got('up'), net.start('ur', 'dc', 'dm', 'uf')),
                    14: lambda: (net.got('oc', 'or'), net.start('og', 'ol'))})
                bad = ok[b][:, 0:1] <= 0
                k = k_ref[0, :, 0].reshape(seq, width)
                v_t = v_ref[0, :, 0].reshape(seq, width).T
                for c in range(seq // qc):
                    src = slice(c * srcs, (c + 1) * srcs)
                    cols = slice(c * qc, (c + 1) * qc)
                    q = q_ref[0, src, 0].reshape(qc, width)
                    outs = []
                    for h in range(heads):
                        s = jnp.where(bad, NEG_LARGE, mm(k, jnp.where(lane // hd == h, q, jnp.zeros_like(q)), NT))
                        m = jnp.max(s, axis=0, keepdims=True)
                        e = jnp.exp(s - m)
                        r = 1.0 / col_sum(e)
                        outs.append(mm(v_t[h * hd:(h + 1) * hd], (e * r).astype(BF16), NN))
                        m_st[g, b, h:h + 1, cols] = m
                        l_st[g, b, h:h + 1, cols] = r
                    o4[src, b, :, span(g, width)] = jnp.concatenate(outs, axis=0).T.astype(BF16).reshape(srcs, p_len, width)

            head_blk = pl.BlockSpec((1, n_tp, 1, p_len, width), lambda g, b: (g, 0, b, 0, 0))
            pipe(attn_step, grid=(n_tp, seqs), in_specs=[head_blk] * 3)(q_hbm, k_hbm, v_hbm)

            net.got('om', 'of', 'og', 'ol')

            @pl.loop(0, tok // (2 * chunk))
            def _(i):
                rows = span(i, 2 * chunk)
                o = o4[pl.ds(2 * i, 2)].reshape(2 * chunk, n_tp * width)
                low = (x[rows, :].astype(F32) + (mm(o, wo[...].reshape(n_tp * width, dim), NN) + bias_o[...])).astype(BF16)
                x1[rows, :] = low
                x_hat, _ = ln_stats(low.astype(F32))
                h2[rows, :] = (x_hat * gain2[...] + bias2[...]).astype(BF16)

            net.start('h2p', 'dp')

            def gelu(pre):
                erf_term = lax.erf(pre * INV_SQRT2)
                act = (0.5 * pre * (1.0 + erf_term)).astype(BF16)
                return act, 0.5 * (1.0 + erf_term) + pre * jnp.exp(-0.5 * pre * pre) * INV_SQRT_2PI

            def up_step(ps, w, act_ref, slope_ref):
                s = ps.index[0]
                hooks(s, {2: lambda: (net.got('uc'), net.start('ug')), 3: lambda: net.got('ug'), 4: lambda: (net.got('ur'), net.start('ul')),
                          5: lambda: net.got('ul')})

                def body(rows):
                    act_ref[rows, :], slope_ref[rows, :] = gelu(mm(h2[rows, :], w[0], NN) + b_ffn[arrival(s)])

                loop_rows(tok, half, body)

            cols = lambda f: pl.BlockSpec((tok, ffn), lambda s: (0, f(s)))
            wu_spec, wd_spec = functools.partial(slot3, dim, ffn), functools.partial(slot3, ffn, dim)
            net.got('um', 'uf')
            pipe(up_step, grid=(n_tp,), in_specs=[wu_spec(arrival)], out_specs=[cols(arrival)] * 2)(wu, act_hbm, slope_hbm)
            net.got('dy_pair', 'dy_fwd', 'dm')

            def backward(slot, wd_s, wu_s, act_ref, slope_ref, add):
                if add:
                    gb[slot] = jnp.zeros_like(gb[0])

                def body(rows):
                    d_pre = mm(dy[rows, :], wd_s[0], NT) * slope_ref[rows, :]
                    low = d_pre.astype(BF16)
                    dpre[rows, :] = low
                    if add:
                        gb[slot] += col_sum(d_pre)
                        acc[rows, :] += mm(act_ref[rows, :], wd_s[0], NN)
                        acc2[rows, :] += mm(low, wu_s[0], NT)

                loop_rows(tok, half, body)

            def mlp(n, f, table):
                def mlp_step(ps, wd_s, wu_s, act_ref, slope_ref):
                    s = ps.index[0]
                    backward(f(s), wd_s, wu_s, act_ref, slope_ref, True)
                    hooks(s, table)

                pipe(mlp_step, grid=(n,), in_specs=[wd_spec(f), wu_spec(f), cols(f), cols(f)])(wd, wu, act_hbm, slope_hbm)

            def grads(chip, at, x_refs, add, sends):
                f = lambda s: 2 * chip + 1 - s
                half_step = lambda rows, wu_s, slot: gelu(mm(h2p[rows, :], wu_s[0], NN) + b_ffn[slot])

                def run(i, prepare, tile, specs, refs):
                    copy = to_partner(i, at + i, n_tp + at + i)

                    def step(ps, *blocks):
                        s = ps.index[0]
                        first = lambda act: pl.when(s == 1)(act)
                        first(lambda: copy.start())
                        prepare(f(s), *blocks)
                        first(lambda: copy.wait_send())
                        tile(into(i), *blocks)

                        @pl.when(s == 1)
                        def _():
                            copy.wait_recv()
                            add_sent(i, at + i)
                            keep(at + i, x_refs[i]).start()

                    pipe(step, grid=(2,), in_specs=specs)(*refs)
                    keep(at + i, x_refs[i]).wait()
                    net.start(*sends[i:i + 1])

                def acts(slot, wu_s, act_ref):
                    def body(rows):
                        act_p[rows, :] = half_step(rows, wu_s, slot)[0]

                    loop_rows(tok, half, body)

                def down(put, wu_s, act_ref):
                    put((pl.ds(0, ffn),), mm(act_ref[...], dy[...], TN) + mm(act_p[...], dyp[...], TN))

                def dpres(slot, wd_s, wu_s, act_ref, slope_ref):
                    backward(slot, wd_s, wu_s, act_ref, slope_ref, add)

                    def body(rows):
                        dpre_p[rows, :] = (mm(dyp[rows, :], wd_s[0], NT) * half_step(rows, wu_s, slot)[1]).astype(BF16)

                    loop_rows(tok, half, body)

                def up(put, *_):
                    for i in range(2):
                        part = pl.ds(i * half, half)
                        put((pl.ds(0, ffn), part), mm(h2[:, part], dpre[...], TN) + mm(h2p[:, part], dpre_p[...], TN))

                run(0, acts, down, [wu_spec(f), cols(f)], (wu, act_hbm))
                run(1, dpres, up, [wd_spec(f), wu_spec(f), cols(f), cols(f)], (wd, wu, act_hbm, slope_hbm))

            acc[...] = jnp.zeros_like(acc)
            acc2[...] = jnp.zeros_like(acc2)
            mlp(2, lambda s: s, {})
            net.got('dc')
            net.start('dg', 'dr')
            net.got('dg', 'h2p')
            grads(CROSS, 0, (x_dn, x_up), True, ('dn_x', 'up_x'))
            net.got('dp')
            net.start('df')
            net.got('df')
            mlp(n_chips, lambda s: s + 2, {0: lambda: (net.got('dr'), net.start('dl'), net.got('dl'))})
            def y_rows(rows):
                y[rows, :] = (x1[rows, :].astype(F32) + (acc[rows, :] + bias_d[...])).astype(BF16)

            loop_rows(tok, 2 * chunk, y_rows)
            vec[...] = jnp.zeros_like(vec)
            net.start('y', 'y_own')

            @pl.loop(0, tok // (2 * chunk))
            def _(i):
                rows = span(i, 2 * chunk)
                x1_f, dy_f, dh = x1[rows, :].astype(F32), dy[rows, :].astype(F32), acc2[rows, :]
                x_hat, inv_std = ln_stats(x1_f)
                d_x1 = dy_f + ln_grad(dh, x_hat, inv_std, gain2[...])
                acc2[rows, :] = d_x1
                low = d_x1.astype(BF16)
                dx1b[rows, :] = low
                d_o = mm(low, wo[...].reshape(n_tp * width, dim), NT).astype(BF16)
                do4[pl.ds(2 * i, 2)] = d_o.reshape(2, seqs, p_len, n_tp * width)
                for n, t in enumerate((d_x1, dh * x_hat, dh, dy_f)):
                    vec[2 + n:3 + n, :] += col_sum(t)

            pack(2, 6)
            pair_begin()

            def bwd_step(ps, q_ref, k_ref, v_ref, w):
                step = ps.index[0]
                g = order(step)
                hooks(step, {0: lambda: net.start('v1'), 2: lambda: (stored(0), net.start('at_relay0', 'at_relay1')),
                             4: lambda: (stored(1), net.start('at_early')), 6: lambda: (stored(2), pass_on(0, 0)), 7: lambda: pass_on(0, 1)})
                pair_go(step)
                b8[g] = jnp.zeros_like(b8[0])
                for i in range(ffn // LANES):
                    b8[g, 3 + i:4 + i, :] = gb[g][:, i * LANES:(i + 1) * LANES]
                for b in range(seqs):
                    bad = ok[b][:, 0:1] <= 0
                    k = k_ref[0, :, b].reshape(seq, width)
                    v = v_ref[0, :, b].reshape(seq, width)
                    k_t = k.T
                    for c in range(seq // qc):
                        src = slice(c * srcs, (c + 1) * srcs)
                        at = slice(c * qc, (c + 1) * qc)
                        q = q_ref[0, src, b].reshape(qc, width)
                        d_o = do4[src, b, :, span(g, width)].reshape(qc, width)
                        dk = jnp.zeros((seq, width), F32)
                        dv = jnp.zeros((seq, width), F32)
                        dqs = []
                        for h in range(heads):
                            mine = lane // hd == h
                            q_h = jnp.where(mine, q, jnp.zeros_like(q))
                            do_h = jnp.where(mine, d_o, jnp.zeros_like(d_o))
                            s = jnp.where(bad, NEG_LARGE, mm(k, q_h, NT))
                            p = jnp.exp(s - m_st[g, b, h:h + 1, at]) * l_st[g, b, h:h + 1, at]
                            dv += mm(p.astype(BF16), do_h, NN)
                            dp = mm(v, do_h, NT)
                            ds = (p * (dp - col_sum(dp * p))).astype(BF16)
                            dk += mm(ds, q_h, NN)
                            dqs.append(mm(k_t[h * hd:(h + 1) * hd], ds, NN))
                        dq_acc[at, :] = jnp.concatenate(dqs, axis=0).T
                        dk_acc[...] = dk if c == 0 else dk_acc[...] + dk
                        dv_acc[...] = dv if c == 0 else dv_acc[...] + dv
                    cos, sin = cos_t[...], sin_t[...]
                    dq, dk, dv = dq_acc[...], dk_acc[...], dv_acc[...]
                    dq = (dq * cos - swap_halves(dq, hd) * sin) * q_scale
                    dk = dk * cos - swap_halves(dk, hd) * sin
                    for i, t in enumerate((dq, dk, dv)):
                        d4[:, b, :, i * width:(i + 1) * width] = t.astype(BF16).reshape(n_tp, p_len, width)
                        b8[g, i:i + 1, :] += col_sum(t)

                @pl.when(step == 0)
                def _():
                    acc[...] = jnp.zeros_like(acc)

                @pl.loop(0, 2)
                def _(i):
                    acc[span(i, half), :] += mm(d4[pl.ds(n_chips * i, n_chips)].reshape(half, n3), w[0], NN)

                def tile(put):
                    put((pl.ds(0, n3),), mm(d4[...].reshape(tok, n3), h1[...], TN))
                    put((pl.ds(n3, width),), mm(o4[:, :, :, span(g, width)].reshape(tok, width), dx1b[...], TN))

                pair(step, tile)

            slot_blk = pl.BlockSpec((1, n_tp, seqs, p_len, width), lambda s: (order(s), 0, 0, 0, 0))
            pipe(bwd_step, grid=(n_tp,), in_specs=[slot_blk] * 3 + [slot3(n3, dim, order)])(
                q_hbm, k_hbm, v_hbm, wq)

            pass_on(0, 2)
            pass_on(1, 0)

            def ln1_bwd(rows):
                x_hat, inv_std = ln_stats(x[rows, :].astype(F32))
                dh = acc[rows, :]
                h1[rows, :] = (acc2[rows, :] + ln_grad(dh, x_hat, inv_std, gain1[...])).astype(BF16)
                vec[0:1, :] += col_sum(dh * x_hat)
                vec[1:2, :] += col_sum(dh)

            loop_rows(tok, 2 * chunk, ln1_bwd)
            stored(3)
            pack(0, 2)
            pass_on(1, 1)
            net.start('b8', 'v0')
            pass_on(1, 2)
            net.start('gx', 'gx_own')

            pair_begin()
            grads(0, 2, (p_dn, p_up), False, ())

            def total(refs, out, block, at):
                def body(*blocks):
                    v = blocks[1][...]
                    for more in blocks[2:-1]:
                        v += more[...]
                    blocks[-1][...] = v

                pipe(body, grid=(2,), in_specs=[pl.BlockSpec(block, at)] * len(refs),
                     out_specs=[pl.BlockSpec(block, lambda i: (i, 0))])(*refs, out)

            by_row, by_col = lambda i: (i, 0), lambda i: (0, i)
            net.got('b8', 'v0', 'v1')
            b_total, v_total = b8[0], v_own[...]
            for n in range(1, n_tp):
                b_total += b_in[n]
                v_total += v_in[n]
            net.got('dn_x', 'up_x')
            total((p_dn, r_dn), g_down, (t_half, dim), by_row)
            total((p_up, r_up), g_up, (n_tile, half), by_col)
            net.got('at_early', 'at_sum0', 'at_sum1')
            total((p_at.at[0], early_at, last_at), g_at, (t_half, dim), by_row)
            for name in net.copies:
                if name not in ('load', 'store', 'own', 'write', 'gx') and not name.endswith(('_own', '_load', '_store')):
                    net.sent(name)
            b8[0] = b_total
            v_own[...] = v_total
            net.got('y')
            net.start('write')
            net.done('y_own', 'gx_own', 'write')
            net.got('gx')
            net.sent('gx')

        big = (tok, dim)
        shapes = lambda *dims, dtype=F32: sds(dims, dtype)
        flat = lambda t: t.reshape(tok, dim)
        inv_freq = ROPE_BASE ** (-2.0 * np.arange(hd // 2) / hd)
        sign = np.repeat([-1.0, 1.0], hd // 2)
        freq = np.stack([np.tile(inv_freq, 2 * heads), np.tile(sign, heads)]).astype(np.float32)
        line = lambda v: v.reshape(1, -1)
        sem = lambda n: pltpu.SemaphoreType.DMA((n,))
        low = functools.partial(shapes, dtype=BF16)
        weights = [low(n_tp, n3, dim), low(n_tp, dim, ffn), low(n_tp, ffn, dim)]
        tiles = [shapes(n_chips, n_tile, dim)] + [shapes(n_tile, dim)] * 10
        out_shape = ([low(*big)] * 2 + [shapes(dim, ffn), shapes(ffn, dim), shapes(n_tile, dim), shapes(6 * n_tp, LANES), shapes(8, LANES)] + weights
                     + [low(n_tp, n_tp, seqs, p_len, width)] * 3 + [low(tok, n_tp * ffn), shapes(tok, n_tp * ffn)] + tiles)
        plain = [pad_mask] + [line(v) for v in (ln1_gain, ln1_bias, b_out, ln2_gain, b_down, ln2_bias)] + [freq]
        heads4 = low(n_tp, seqs, p_len, n_tp * width)
        stat = shapes(n_tp, seqs, heads, seq)
        tile8 = shapes(n_tp, 8, LANES)
        row_ffn = shapes(n_tp, 1, ffn)
        scratch = ([low(*big)] * 9 + [heads4, heads4, low(n_tp, width, dim)] + [shapes(*big)] * 2
                   + [shapes(n_chips, n_tile, dim), shapes(2, n_tile, dim), low(n_tp, seqs, p_len, n3)]
                   + [shapes(seq, width)] * 5 + [shapes(seqs, seq, LANES), stat, stat, shapes(n_tp, 1, n3), row_ffn, row_ffn, row_ffn]
                   + [shapes(n_tp, *b_qkv.shape), tile8, tile8, shapes(8, dim), shapes(n_tp, 6 * n_tp, LANES), shapes(6 * n_tp, LANES)]
                   + [low(tok, ffn)] * 3 + plain)
        outs = pl.pallas_call(
            kernel, name='layer', out_shape=out_shape, in_specs=[ANY] * 16, out_specs=[ANY] * len(out_shape),
            scratch_shapes=[pltpu.VMEM(v.shape, v.dtype) for v in scratch]
            + [sem(128), sem(128), sem(64), sem(3 * n_tp), sem(3 * n_tp), pltpu.SemaphoreType.REGULAR],
            compiler_params=pltpu.CompilerParams(collective_id=0, has_side_effects=True, vmem_limit_bytes=VMEM_LIMIT),
        )(flat(x_in), flat(grad_y), w_qkv.transpose(0, 2, 3, 1).reshape(n3, dim), b_qkv, w_out.reshape(width, dim),
          w_up, line(b_up), w_down, *plain)

        def finish(y_ref, gx_ref, gu_ref, gd_ref, v_ref, b_ref, pq, po, y_o, gx_o, gu_o, gd_o, gq_o, go_o, bq_o, bu_o, *v_o):
            y_o[...], gx_o[...], gu_o[...], gd_o[...] = y_ref[...], gx_ref[...], gu_ref[...], gd_ref[...]
            gq_o[...], go_o[...] = pq[...], po[...]
            for i in range(3):
                for h in range(heads):
                    bq_o[i, h:h + 1, :] = b_ref[i:i + 1, h * hd:(h + 1) * hd]
            for i in range(ffn // LANES):
                bu_o[:, i * LANES:(i + 1) * LANES] = b_ref[3 + i:4 + i, :]
            for r, ref in enumerate(v_o):
                for i in range(n_tp):
                    ref[:, i * LANES:(i + 1) * LANES] = v_ref[r * n_tp + i:r * n_tp + i + 1, :]

        n_step = 4

        def cut(rows, cols, first=0):
            return pl.BlockSpec((rows // n_step, cols), lambda i: (first * n_step // rows + i, 0))

        def const(*dims):
            return pl.BlockSpec(dims, lambda i: (0,) * len(dims))

        main = [cut(tok, dim), cut(tok, dim), cut(dim, ffn), cut(ffn, dim)]
        att = [cut(n3, dim), cut(width, dim, n3)]
        res = pl.pallas_call(
            finish, name='finish', grid=(n_step,),
            out_shape=(sds(big, BF16), sds(big, BF16), shapes(dim, ffn), shapes(ffn, dim), shapes(n3, dim), shapes(width, dim),
                       shapes(*b_qkv.shape), shapes(1, ffn)) + (shapes(1, dim),) * 6,
            in_specs=main + [const(6 * n_tp, LANES), const(8, LANES)] + att,
            out_specs=tuple(main) + (cut(n3, dim), cut(width, dim), const(*b_qkv.shape), const(1, ffn)) + (const(1, dim),) * 6,
            compiler_params=pltpu.CompilerParams(vmem_limit_bytes=VMEM_LIMIT),
        )(*outs[:4], *outs[5:7], outs[4], outs[4])
        y_out, grad_x, grad_w_up, grad_w_down, gq, go, grad_b_qkv, grad_b_up = res[:8]
        v = [t.reshape(dim) for t in res[8:]]
        return (y_out.reshape(x_in.shape), grad_x.reshape(x_in.shape), v[0], v[1], gq.reshape(3, heads, hd, dim).transpose(0, 3, 1, 2),
                grad_b_qkv, go.reshape(heads, hd, dim), v[2], v[3], v[4], grad_w_up, grad_b_up.reshape(ffn), grad_w_down, v[5])

    return jax.shard_map(device_step, mesh=mesh, in_specs=in_specs, out_specs=out_specs, check_vma=False)
```

```python
import functools

import jax
import jax.numpy as jnp
import numpy as np
from jax import lax
from jax.experimental import pallas as pl
from jax.experimental.pallas import tpu as pltpu
from jax.sharding import PartitionSpec as P

LN_EPS = 1e-5
ROPE_BASE = 10000.0
INV_SQRT2 = 0.7071067811865476
INV_SQRT_2PI = 0.3989422804014327
NEG_LARGE = -1e30
F32 = jnp.float32
BF16 = jnp.bfloat16
VMEM_LIMIT = 66_500_000
LANES = 128
NN = (((1,), (0,)), ((), ()))
NT = (((1,), (1,)), ((), ()))
TN = (((0,), (0,)), ((), ()))
PAIR, FAR, CROSS = 1, 2, 3
ANY = pl.BlockSpec(memory_space=pl.ANY)


def mm(a, b, dims):
    return lax.dot_general(a, b, dims, preferred_element_type=F32)


def ln_stats(v):
    centered = v - jnp.mean(v, axis=-1, keepdims=True)
    inv_std = lax.rsqrt(jnp.mean(centered * centered, axis=-1, keepdims=True) + LN_EPS)
    return centered * inv_std, inv_std


def ln_grad(d_out, x_hat, inv_std, gain):
    d_hat = d_out * gain
    return inv_std * (d_hat - jnp.mean(d_hat, axis=-1, keepdims=True) - x_hat * jnp.mean(d_hat * x_hat, axis=-1, keepdims=True))


def col_sum(t):
    return jnp.sum(t, axis=0, keepdims=True)


def swap_halves(t, head_dim):
    half = head_dim // 2
    lane = lax.broadcasted_iota(jnp.int32, t.shape, t.ndim - 1)
    return jnp.where(lane % head_dim < half, pltpu.roll(t, t.shape[-1] - half, t.ndim - 1), pltpu.roll(t, half, t.ndim - 1))


def span(i, n):
    return pl.ds(pl.multiple_of(i * n, n), n)


def loop_rows(total, n, body):
    @pl.loop(0, total // n)
    def _(i):
        body(span(i, n))


class Net:
    def __init__(self, n_tp, send, recv, local):
        self.n_tp, self.send, self.recv, self.local = n_tp, send, recv, local
        self.copies, self.count, self.n_local = {}, 0, 0

    def peer(self, chip, core=0):
        me = lax.axis_index('tp')
        way = 1 - 2 * lax.rem(lax.div(me, 2), 2)
        at = lax.rem(me + 2 * chip * way + self.n_tp, self.n_tp) if chip else me
        return at + 1 - 2 * lax.rem(at, 2) if core else at

    def add(self, name, src, dst, chip, core=0):
        n = self.count
        self.count += 1

        def make():
            return pltpu.make_async_remote_copy(
                src_ref=src(), dst_ref=dst(), send_sem=self.send.at[n], recv_sem=self.recv.at[n],
                device_id={'tp': self.peer(chip, core)}, device_id_type=pl.DeviceIdType.MESH)

        self.copies.setdefault(name, []).append(make)

    def add_local(self, name, src, dst):
        n = self.n_local
        self.n_local += 1
        self.copies.setdefault(name, []).append(lambda: pltpu.make_async_copy(src(), dst(), self.local.at[n]))

    def start(self, *names):
        for name in names:
            for make in self.copies[name]:
                make().start()

    def got(self, *names):
        for name in names:
            with jax.named_scope('got_' + name):
                for make in self.copies[name]:
                    make().wait_recv()

    def sent(self, *names):
        for name in names:
            for make in self.copies[name]:
                make().wait_send()

    def done(self, *names):
        for name in names:
            with jax.named_scope('done_' + name):
                for make in self.copies[name]:
                    make().wait()

    def gather(self, name, own, buf, via):
        for stage, chip in (('p', PAIR), ('c', CROSS)):
            self.add(name + stage, lambda: own, lambda c=chip: buf.at[2 * c], chip)
        self.add(name + 'm', lambda: own, lambda: buf.at[1], 0, 1)
        self.add(name + 'r', lambda: buf.at[2 * (PAIR + CROSS - via)], lambda: buf.at[2 * FAR], via)
        for stage, chip in (('f', PAIR), ('g', CROSS), ('l', FAR)):
            self.add(name + stage, lambda c=chip: buf.at[2 * c], lambda c=chip: buf.at[2 * c + 1], 0, 1)

    def exchange(self, name, src, dst, rows):
        me = lax.axis_index('tp')
        for core in range(2):
            for chip in (PAIR, CROSS, FAR, 0):
                if chip + core:
                    self.add(name, lambda c=chip, k=core: src.at[span(self.peer(c, k), rows)], lambda: dst.at[span(me, rows)], chip, core)
        self.add_local(name + '_own', lambda: src.at[span(me, rows)], lambda: dst.at[span(me, rows)])

    def multicast(self, name, src, dst, pair_dst, rows):
        me = lax.axis_index('tp')
        at = lambda buf: (lambda: buf.at[span(me, rows)])
        other = {0: PAIR, PAIR: 0, CROSS: FAR}
        for chip, stage in ((CROSS, '_cross'), (PAIR, '_pair'), (0, '_pair')):
            for core in range(2):
                if chip + core:
                    for c, buf in ((chip, dst), (other[chip], pair_dst)):
                        self.add(name + stage, lambda c=c, k=core: src.at[span(self.peer(c, k), rows)], at(buf), chip, core)
        for c, buf in ((0, dst), (PAIR, pair_dst)):
            self.add_local(name + '_own', lambda c=c: src.at[span(self.peer(c), rows)], at(buf))
        came = lambda buf: (lambda: buf.at[span(lax.div(self.peer(CROSS), 2), 2 * rows)])
        self.add(name + '_fwd', came(dst), came(pair_dst), PAIR)
        self.add(name + '_fwd', came(pair_dst), came(dst), PAIR)


def solution(mesh):
    n_tp = mesh.shape['tp']
    n_chips = n_tp // 2
    act_spec = P('dp', 'tp', None)
    rep_vec = P(None)
    part_vec = P('dp')
    in_specs = (act_spec, act_spec, P('dp', None), rep_vec, rep_vec, P(None, None, 'tp', None), P(None, 'tp', None),
                P('tp', None, None), rep_vec, rep_vec, rep_vec, P(None, 'tp'), P('tp'), P('tp', None), rep_vec)
    out_specs = (act_spec, act_spec, part_vec, part_vec, P('dp', None, 'tp', None), P('dp', 'tp', None),
                 P(('dp', 'tp'), None, None), part_vec, part_vec, part_vec, P('dp', 'tp'), P(('dp', 'tp')),
                 P(('dp', 'tp'), None), part_vec)

    def device_step(x_in, grad_y, pad_mask, ln1_gain, ln1_bias, w_qkv, b_qkv, w_out, b_out, ln2_gain, ln2_bias, w_up, b_up, w_down, b_down):
        batch, p_len, dim = x_in.shape
        seq = pad_mask.shape[1]
        _, _, heads, hd = w_qkv.shape
        seqs = batch // n_tp
        ffn = w_up.shape[1]
        width = heads * hd
        n3 = 3 * width
        tok = seqs * seq
        chunk = seqs * p_len
        qc = seq // 2
        q_scale = hd ** -0.5
        sds = jax.ShapeDtypeStruct
        n_tile = n3 + width
        half = dim // 2

        def kernel(*refs):
            it = iter(refs)
            take = lambda n: [next(it) for _ in range(n)]
            (x_ref, dy_ref, wq_ref, bq_ref, wo_ref, wu_ref, bu_ref, wd_ref), plain = take(8), take(8)
            y_out, gx_out, g_up, g_down, g_q, g_o, g_vec, g_b, wq, wu, wd, q_hbm, k_hbm, v_hbm, act_hbm, slope_hbm = take(16)
            p_at, got_at, sum_at, early_at, last_at, x_dn, x_up, p_dn, p_up, r_dn, r_up = take(11)
            x, h1, dy, x1, h2, dx1b, h2p, dyp, y, o4, do4, wo, acc, acc2, p_rcv, p_snd, d4 = take(17)
            dq_acc, dk_acc, dv_acc, cos_t, sin_t, ok, m_st, l_st, b_att, b_ffn, u_all, gb, b_all, b8, b_in, vec, v_in, v_own = take(18)
            dpre, act_p, dpre_p = take(3)
            here = take(8)
            send, recv, local, pair_send, pair_recv, pair_ready = take(6)
            net = Net(n_tp, send, recv, local)
            me = lax.axis_index('tp')
            mask_ref, gain1, bias1, bias_o, gain2, bias_d, bias2, freq_ref = here

            net.gather('q', wq_ref, wq, CROSS)
            net.gather('o', wo_ref, wo, CROSS)
            net.gather('u', wu_ref, wu, CROSS)
            net.gather('d', wd_ref, wd, PAIR)
            net.exchange('x', x_ref, x, chunk)
            net.multicast('dy', dy_ref, dy, dyp, chunk)
            net.exchange('y', y, y_out, chunk)
            net.exchange('gx', h1, gx_out, chunk)
            for chip in range(n_chips):
                for core in range(2):
                    if chip + core:
                        slot = 2 * chip + core
                        net.add('bias', lambda: bq_ref, lambda n=slot: b_all.at[n], chip, core)
                        net.add('bias', lambda: bu_ref, lambda n=slot: u_all.at[n], chip, core)
                        net.add('b8', lambda n=slot: b8.at[n], lambda n=slot: b_in.at[n], chip, core)
                        for r, rows in enumerate((pl.ds(0, 2 * n_tp), pl.ds(2 * n_tp, 4 * n_tp))):
                            net.add(f'v{r}', lambda p=rows: v_own.at[p], lambda n=slot, p=rows: v_in.at[n, p], chip, core)
            net.add('h2p', lambda: h2, lambda: h2p, PAIR)
            net.add('dn_x', lambda: x_dn, lambda: r_dn, CROSS)
            net.add('up_x', lambda: x_up, lambda: r_up, CROSS)
            net.add('at_early', lambda: p_at.at[PAIR], lambda: early_at, PAIR)
            t_half = n_tile // 2
            for i, part in enumerate((pl.ds(0, t_half), pl.ds(t_half, t_half))):
                net.add(f'at_relay{i}', lambda p=part: p_at.at[FAR, p], lambda p=part: got_at.at[p], PAIR)
                net.add(f'at_sum{i}', lambda p=part: sum_at.at[p], lambda p=part: last_at.at[p], CROSS)
                net.add_local(f'at{i}_load', lambda p=part: got_at.at[p], lambda p=part: p_rcv.at[0, p])
                net.add_local(f'at{i}_load', lambda p=part: p_at.at[CROSS, p], lambda p=part: p_rcv.at[1, p])
                net.add_local(f'at{i}_store', lambda p=part: p_rcv.at[1, p], lambda p=part: sum_at.at[p])
            for src, dst in zip(plain, here):
                net.add_local('own', lambda r=src: r, lambda r=dst: r)
            net.add_local('write', lambda: v_own, lambda: g_vec)
            net.add_local('write', lambda: b8.at[0], lambda: g_b)
            for ref, tmp, buf in ((wq_ref, lambda: h2.at[pl.ds(0, n3)], wq), (wu_ref, lambda: x1.at[:, pl.ds(0, ffn)], wu),
                                        (wd_ref, lambda: dx1b.at[pl.ds(0, ffn)], wd)):
                net.add_local('load', lambda r=ref: r, tmp)
                net.add_local('store', tmp, lambda b=buf: b.at[0])
            net.add_local('own', lambda: wo_ref, lambda: wo.at[0])
            net.add_local('own', lambda: bq_ref, lambda: b_all.at[0])
            net.add_local('own', lambda: bu_ref, lambda: u_all.at[0])
            def pass_on(i, stage):
                if stage == 0:
                    net.got(f'at_relay{i}')
                    net.start(f'at{i}_load')
                elif stage == 1:
                    net.done(f'at{i}_load')

                    def body(rows):
                        rows = pl.ds(i * t_half + rows.start, rows.size)
                        p_rcv[1, rows] += p_rcv[0, rows]

                    loop_rows(t_half, 8, body)
                    net.start(f'at{i}_store')
                else:
                    net.done(f'at{i}_store')
                    net.start(f'at_sum{i}')

            def pack(lo, hi):
                for r in range(lo, hi):
                    for i in range(n_tp):
                        v_own[r * n_tp + i:r * n_tp + i + 1, :] = vec[r:r + 1, i * LANES:(i + 1) * LANES]

            def hooks(step, table):
                for at, act in table.items():
                    @pl.when(step == at)
                    def _(act=act):
                        act()

            tile_order = (FAR, PAIR, CROSS, 0)

            def place(i):
                return jnp.where(i == 0, FAR, jnp.where(i == 1, PAIR, jnp.where(i == 2, CROSS, 0)))

            def order(s):
                return 2 * place(lax.div(s, 2)) + 1 - lax.rem(s, 2)

            def to_partner(src, dst, sem):
                return pltpu.make_async_remote_copy(
                    src_ref=p_snd.at[src], dst_ref=p_rcv.at[dst], send_sem=pair_send.at[sem], recv_sem=pair_recv.at[sem],
                    device_id={'tp': net.peer(0, 1)}, device_id_type=pl.DeviceIdType.MESH)

            def keep(i, to):
                return pltpu.make_async_copy(p_rcv.at[i], to, pair_send.at[2 * n_tp + i])

            def into(i):
                return lambda at, v: p_snd.__setitem__((i,) + at, v)

            def add_sent(i, j):
                def body(rows):
                    p_rcv[j, rows] += p_snd[i, rows]

                loop_rows(n_tile, 16, body)

            def pair_go(s):
                @pl.when(lax.rem(s, 2) == 1)
                def _():
                    to_partner(0, lax.div(s, 2), lax.div(s, 2)).start()

            def pair(s, tile):
                j = lax.div(s, 2)
                odd = lax.rem(s, 2)
                tile(into(odd))

                @pl.when(odd == 1)
                def _():
                    copy = to_partner(0, j, j)
                    copy.wait_send()
                    copy.wait_recv()
                    add_sent(1, j)
                    keep(j, p_at.at[place(j)]).start()

            def stored(i):
                keep(i, p_at.at[tile_order[i]]).wait()

            def pair_begin():
                pl.semaphore_signal(pair_ready, inc=1, device_id={'tp': net.peer(0, 1)}, device_id_type=pl.DeviceIdType.MESH)
                pl.semaphore_wait(pair_ready, 1)

            barrier = pltpu.get_barrier_semaphore()
            for chip in range(n_chips):
                for core in range(2):
                    if chip + core:
                        pl.semaphore_signal(barrier, inc=1, device_id={'tp': net.peer(chip, core)}, device_id_type=pl.DeviceIdType.MESH)
            pl.semaphore_wait(barrier, n_tp - 1)
            net.start('qp', 'qc', 'x', 'qm', 'bias', 'own', 'load', 'x_own', 'dy_own')
            net.done('own')
            angle = lax.broadcasted_iota(jnp.int32, (seq, width), 0).astype(F32) * freq_ref[0:1, :]
            cos_t[...] = jnp.cos(angle)
            sin_t[...] = jnp.sin(angle) * freq_ref[1:2, :]
            for b in range(seqs):
                row = mask_ref[pl.ds(me * seqs + b, 1), :].astype(F32)
                ok[b] = jnp.broadcast_to(row, (LANES, seq)).T
            net.done('load')
            net.start('store')
            net.got('qp', 'qc')
            net.start('qr', 'dy_cross', 'oc', 'op', 'up', 'dy_pair', 'qf', 'qg', 'om')
            net.done('x_own', 'dy_own')
            net.got('bias')
            for n in range(n_tp):
                b = b_all[n]
                b_att[n] = jnp.concatenate([b[i // heads, i % heads:i % heads + 1, :] for i in range(3 * heads)], axis=1)
                b_ffn[n] = u_all[n]
            net.got('x')

            def ln1(rows):
                x_hat, _ = ln_stats(x[rows, :].astype(F32))
                h1[rows, :] = (x_hat * gain1[...] + bias1[...]).astype(BF16)

            loop_rows(tok, chunk, ln1)
            net.done('store')
            net.got('qm', 'qf', 'qg')

            def arrival(s):
                return s + 2 * lax.div(s, n_chips) - n_chips * lax.div(s, n_chips + 2)

            def qkv_step(ps, w, q_ref, k_ref, v_ref):
                s = ps.index[0]
                hooks(s, {2: lambda: (net.got('op'), net.start('or', 'uc', 'um', 'of')), 4: lambda: (net.got('qr'), net.start('ql')),
                          5: lambda: net.got('ql')})
                n_src = tok // chunk // 2

                @pl.loop(0, 2)
                def _(i):
                    rows = span(i, tok // 2)
                    t = mm(h1[rows, :], w[0], NT) + b_att[arrival(s)]
                    cos, sin = (t_ref[span(i, seq // 2), :].reshape(n_src, 1, p_len, width) for t_ref in (cos_t, sin_t))

                    def rope(v):
                        out = v.reshape(n_src, seqs, p_len, width) * cos + swap_halves(v, hd).reshape(n_src, seqs, p_len, width) * sin
                        return out.astype(BF16)

                    src = span(i, n_src)
                    q_ref[0, src] = rope(t[:, :width] * q_scale)
                    k_ref[0, src] = rope(t[:, width:2 * width])
                    v_ref[0, src] = t[:, 2 * width:].reshape(n_src, seqs, p_len, width).astype(BF16)

            slot3 = lambda rows, cols, f=lambda s: s: pl.BlockSpec((1, rows, cols), lambda s: (f(s), 0, 0))

            def pipe(body, **specs):
                def run(*refs):
                    with jax.named_scope(body.__name__):
                        pltpu.emit_pipeline(body, _explicit_indices=True, **specs)(*refs)

                return run

            pipe(qkv_step, grid=(n_tp,), in_specs=[slot3(n3, dim, arrival)],
                 out_specs=[pl.BlockSpec((1, n_tp, seqs, p_len, width), lambda s: (arrival(s), 0, 0, 0, 0))] * 3)(
                wq, q_hbm, k_hbm, v_hbm)

            srcs = qc // p_len
            lane = lax.broadcasted_iota(jnp.int32, (qc, width), 1)

            def attn_step(ps, q_ref, k_ref, v_ref):
                g, b = ps.index
                hooks(g * seqs + b, {
                    8: lambda: (net.got('dy_cross'), net.start('dy_fwd')), 9: lambda: (net.got('up'), net.start('ur', 'dc', 'dm', 'uf')),
                    14: lambda: (net.got('oc', 'or'), net.start('og', 'ol'))})
                bad = ok[b][:, 0:1] <= 0
                k = k_ref[0, :, 0].reshape(seq, width)
                v_t = v_ref[0, :, 0].reshape(seq, width).T
                for c in range(seq // qc):
                    src = slice(c * srcs, (c + 1) * srcs)
                    cols = slice(c * qc, (c + 1) * qc)
                    q = q_ref[0, src, 0].reshape(qc, width)
                    outs = []
                    for h in range(heads):
                        s = jnp.where(bad, NEG_LARGE, mm(k, jnp.where(lane // hd == h, q, jnp.zeros_like(q)), NT))
                        m = jnp.max(s, axis=0, keepdims=True)
                        e = jnp.exp(s - m)
                        r = 1.0 / col_sum(e)
                        outs.append(mm(v_t[h * hd:(h + 1) * hd], (e * r).astype(BF16), NN))
                        m_st[g, b, h:h + 1, cols] = m
                        l_st[g, b, h:h + 1, cols] = r
                    o4[src, b, :, span(g, width)] = jnp.concatenate(outs, axis=0).T.astype(BF16).reshape(srcs, p_len, width)

            head_blk = pl.BlockSpec((1, n_tp, 1, p_len, width), lambda g, b: (g, 0, b, 0, 0))
            pipe(attn_step, grid=(n_tp, seqs), in_specs=[head_blk] * 3)(q_hbm, k_hbm, v_hbm)

            net.got('om', 'of', 'og', 'ol')

            @pl.loop(0, tok // (2 * chunk))
            def _(i):
                rows = span(i, 2 * chunk)
                o = o4[pl.ds(2 * i, 2)].reshape(2 * chunk, n_tp * width)
                low = (x[rows, :].astype(F32) + (mm(o, wo[...].reshape(n_tp * width, dim), NN) + bias_o[...])).astype(BF16)
                x1[rows, :] = low
                x_hat, _ = ln_stats(low.astype(F32))
                h2[rows, :] = (x_hat * gain2[...] + bias2[...]).astype(BF16)

            net.start('h2p', 'dp')

            def gelu(pre):
                erf_term = lax.erf(pre * INV_SQRT2)
                act = (0.5 * pre * (1.0 + erf_term)).astype(BF16)
                return act, 0.5 * (1.0 + erf_term) + pre * jnp.exp(-0.5 * pre * pre) * INV_SQRT_2PI

            def up_step(ps, w, act_ref, slope_ref):
                s = ps.index[0]
                hooks(s, {2: lambda: (net.got('uc'), net.start('ug')), 3: lambda: net.got('ug'), 4: lambda: (net.got('ur'), net.start('ul')),
                          5: lambda: net.got('ul')})

                def body(rows):
                    act_ref[rows, :], slope_ref[rows, :] = gelu(mm(h2[rows, :], w[0], NN) + b_ffn[arrival(s)])

                loop_rows(tok, half, body)

            cols = lambda f: pl.BlockSpec((tok, ffn), lambda s: (0, f(s)))
            wu_spec, wd_spec = functools.partial(slot3, dim, ffn), functools.partial(slot3, ffn, dim)
            net.got('um', 'uf')
            pipe(up_step, grid=(n_tp,), in_specs=[wu_spec(arrival)], out_specs=[cols(arrival)] * 2)(wu, act_hbm, slope_hbm)
            net.got('dy_pair', 'dy_fwd', 'dm')

            def backward(slot, wd_s, wu_s, act_ref, slope_ref, add):
                if add:
                    gb[slot] = jnp.zeros_like(gb[0])

                def body(rows):
                    d_pre = mm(dy[rows, :], wd_s[0], NT) * slope_ref[rows, :]
                    low = d_pre.astype(BF16)
                    dpre[rows, :] = low
                    if add:
                        gb[slot] += col_sum(d_pre)
                        acc[rows, :] += mm(act_ref[rows, :], wd_s[0], NN)
                        acc2[rows, :] += mm(low, wu_s[0], NT)

                loop_rows(tok, half, body)

            def mlp(n, f, table):
                def mlp_step(ps, wd_s, wu_s, act_ref, slope_ref):
                    s = ps.index[0]
                    backward(f(s), wd_s, wu_s, act_ref, slope_ref, True)
                    hooks(s, table)

                pipe(mlp_step, grid=(n,), in_specs=[wd_spec(f), wu_spec(f), cols(f), cols(f)])(wd, wu, act_hbm, slope_hbm)

            def grads(chip, at, x_refs, add, sends, then):
                f = lambda s: 2 * chip + 1 - s
                half_step = lambda rows, wu_s, slot: gelu(mm(h2p[rows, :], wu_s[0], NN) + b_ffn[slot])

                def run(i, prepare, tile, specs, refs, then):
                    copy = to_partner(i, at + i, n_tp + at + i)

                    def step(ps, *blocks):
                        s = ps.index[0]
                        first = lambda act: pl.when(s == 1)(act)
                        first(lambda: (copy.start(), then()) and None)
                        prepare(f(s), *blocks)
                        first(lambda: copy.wait_send())
                        tile(into(i), *blocks)

                        @pl.when(s == 1)
                        def _():
                            copy.wait_recv()
                            add_sent(i, at + i)
                            keep(at + i, x_refs[i]).start()

                    pipe(step, grid=(2,), in_specs=specs)(*refs)
                    keep(at + i, x_refs[i]).wait()
                    net.start(*sends[i:i + 1])

                def acts(slot, wu_s, act_ref):
                    def body(rows):
                        act_p[rows, :] = half_step(rows, wu_s, slot)[0]

                    loop_rows(tok, half, body)

                def down(put, wu_s, act_ref):
                    put((pl.ds(0, ffn),), mm(act_ref[...], dy[...], TN) + mm(act_p[...], dyp[...], TN))

                def dpres(slot, wd_s, wu_s, act_ref, slope_ref):
                    backward(slot, wd_s, wu_s, act_ref, slope_ref, add)

                    def body(rows):
                        dpre_p[rows, :] = (mm(dyp[rows, :], wd_s[0], NT) * half_step(rows, wu_s, slot)[1]).astype(BF16)

                    loop_rows(tok, half, body)

                def up(put, *_):
                    for i in range(2):
                        part = pl.ds(i * half, half)
                        put((pl.ds(0, ffn), part), mm(h2[:, part], dpre[...], TN) + mm(h2p[:, part], dpre_p[...], TN))

                run(0, acts, down, [wu_spec(f), cols(f)], (wu, act_hbm), lambda: None)
                run(1, dpres, up, [wd_spec(f), wu_spec(f), cols(f), cols(f)], (wd, wu, act_hbm, slope_hbm), then)

            acc[...] = jnp.zeros_like(acc)
            acc2[...] = jnp.zeros_like(acc2)
            mlp(2, lambda s: s, {})
            net.got('dc')
            net.start('dg', 'dr')
            net.got('dg', 'h2p')
            grads(CROSS, 0, (x_dn, x_up), True, ('dn_x', 'up_x'), lambda: (net.got('dp'), net.start('df')))
            net.got('df')
            mlp(n_chips, lambda s: s + 2, {0: lambda: (net.got('dr'), net.start('dl')), 1: lambda: net.got('dl')})
            def y_rows(rows):
                y[rows, :] = (x1[rows, :].astype(F32) + (acc[rows, :] + bias_d[...])).astype(BF16)

            loop_rows(tok, 2 * chunk, y_rows)
            vec[...] = jnp.zeros_like(vec)
            net.start('y', 'y_own')

            @pl.loop(0, tok // (2 * chunk))
            def _(i):
                rows = span(i, 2 * chunk)
                x1_f, dy_f, dh = x1[rows, :].astype(F32), dy[rows, :].astype(F32), acc2[rows, :]
                x_hat, inv_std = ln_stats(x1_f)
                d_x1 = dy_f + ln_grad(dh, x_hat, inv_std, gain2[...])
                acc2[rows, :] = d_x1
                low = d_x1.astype(BF16)
                dx1b[rows, :] = low
                d_o = mm(low, wo[...].reshape(n_tp * width, dim), NT).astype(BF16)
                do4[pl.ds(2 * i, 2)] = d_o.reshape(2, seqs, p_len, n_tp * width)
                for n, t in enumerate((d_x1, dh * x_hat, dh, dy_f)):
                    vec[2 + n:3 + n, :] += col_sum(t)

            pack(2, 6)
            pair_begin()

            def bwd_step(ps, q_ref, k_ref, v_ref, w):
                step = ps.index[0]
                g = order(step)
                hooks(step, {0: lambda: net.start('v1'), 2: lambda: (stored(0), net.start('at_relay0', 'at_relay1')),
                             4: lambda: (stored(1), net.start('at_early')), 6: lambda: (stored(2), pass_on(0, 0)), 7: lambda: pass_on(0, 2)})
                pair_go(step)
                b8[g] = jnp.zeros_like(b8[0])
                for i in range(ffn // LANES):
                    b8[g, 3 + i:4 + i, :] = gb[g][:, i * LANES:(i + 1) * LANES]
                for b in range(seqs):
                    bad = ok[b][:, 0:1] <= 0
                    k = k_ref[0, :, b].reshape(seq, width)
                    v = v_ref[0, :, b].reshape(seq, width)
                    k_t = k.T
                    for c in range(seq // qc):
                        src = slice(c * srcs, (c + 1) * srcs)
                        at = slice(c * qc, (c + 1) * qc)
                        q = q_ref[0, src, b].reshape(qc, width)
                        d_o = do4[src, b, :, span(g, width)].reshape(qc, width)
                        dk = jnp.zeros((seq, width), F32)
                        dv = jnp.zeros((seq, width), F32)
                        dqs = []
                        for h in range(heads):
                            mine = lane // hd == h
                            q_h = jnp.where(mine, q, jnp.zeros_like(q))
                            do_h = jnp.where(mine, d_o, jnp.zeros_like(d_o))
                            s = jnp.where(bad, NEG_LARGE, mm(k, q_h, NT))
                            p = jnp.exp(s - m_st[g, b, h:h + 1, at]) * l_st[g, b, h:h + 1, at]
                            dv += mm(p.astype(BF16), do_h, NN)
                            dp = mm(v, do_h, NT)
                            ds = (p * (dp - col_sum(dp * p))).astype(BF16)
                            dk += mm(ds, q_h, NN)
                            dqs.append(mm(k_t[h * hd:(h + 1) * hd], ds, NN))
                        dq_acc[at, :] = jnp.concatenate(dqs, axis=0).T
                        dk_acc[...] = dk if c == 0 else dk_acc[...] + dk
                        dv_acc[...] = dv if c == 0 else dv_acc[...] + dv
                    cos, sin = cos_t[...], sin_t[...]
                    dq, dk, dv = dq_acc[...], dk_acc[...], dv_acc[...]
                    dq = (dq * cos - swap_halves(dq, hd) * sin) * q_scale
                    dk = dk * cos - swap_halves(dk, hd) * sin
                    for i, t in enumerate((dq, dk, dv)):
                        d4[:, b, :, i * width:(i + 1) * width] = t.astype(BF16).reshape(n_tp, p_len, width)
                        b8[g, i:i + 1, :] += col_sum(t)

                @pl.when(step == 0)
                def _():
                    acc[...] = jnp.zeros_like(acc)

                @pl.loop(0, 2)
                def _(i):
                    acc[span(i, half), :] += mm(d4[pl.ds(n_chips * i, n_chips)].reshape(half, n3), w[0], NN)

                def tile(put):
                    put((pl.ds(0, n3),), mm(d4[...].reshape(tok, n3), h1[...], TN))
                    put((pl.ds(n3, width),), mm(o4[:, :, :, span(g, width)].reshape(tok, width), dx1b[...], TN))

                pair(step, tile)
                hooks(step, {6: lambda: pass_on(0, 1)})

            slot_blk = pl.BlockSpec((1, n_tp, seqs, p_len, width), lambda s: (order(s), 0, 0, 0, 0))
            pipe(bwd_step, grid=(n_tp,), in_specs=[slot_blk] * 3 + [slot3(n3, dim, order)])(
                q_hbm, k_hbm, v_hbm, wq)

            pass_on(1, 0)

            def ln1_bwd(rows):
                x_hat, inv_std = ln_stats(x[rows, :].astype(F32))
                dh = acc[rows, :]
                h1[rows, :] = (acc2[rows, :] + ln_grad(dh, x_hat, inv_std, gain1[...])).astype(BF16)
                vec[0:1, :] += col_sum(dh * x_hat)
                vec[1:2, :] += col_sum(dh)

            loop_rows(tok, 2 * chunk, ln1_bwd)
            stored(3)
            pack(0, 2)
            pass_on(1, 1)
            net.start('b8', 'v0')
            pass_on(1, 2)
            net.start('gx', 'gx_own')

            pair_begin()
            grads(0, 2, (p_dn, p_up), False, (), lambda: None)

            def total(refs, out, block, at):
                def body(*blocks):
                    v = blocks[1][...]
                    for more in blocks[2:-1]:
                        v += more[...]
                    blocks[-1][...] = v

                pipe(body, grid=(2,), in_specs=[pl.BlockSpec(block, at)] * len(refs),
                     out_specs=[pl.BlockSpec(block, lambda i: (i, 0))])(*refs, out)

            by_row, by_col = lambda i: (i, 0), lambda i: (0, i)
            net.got('b8', 'v0', 'v1')
            b_total, v_total = b8[0], v_own[...]
            for n in range(1, n_tp):
                b_total += b_in[n]
                v_total += v_in[n]
            net.got('dn_x', 'up_x')
            total((p_dn, r_dn), g_down, (t_half, dim), by_row)
            total((p_up, r_up), g_up, (n_tile, half), by_col)
            net.got('at_early', 'at_sum0', 'at_sum1')
            for rows, out, n in ((pl.ds(0, n3), g_q, n3), (pl.ds(n3, width), g_o, width)):
                total((p_at.at[0, rows], early_at.at[rows], last_at.at[rows]), out, (n // 2, dim), by_row)
            for name in net.copies:
                if name not in ('load', 'store', 'own', 'write', 'gx') and not name.endswith(('_own', '_load', '_store')):
                    net.sent(name)
            b8[0] = b_total
            v_own[...] = v_total
            net.got('y')
            net.start('write')
            net.done('y_own', 'gx_own', 'write')
            net.got('gx')
            net.sent('gx')

        big = (tok, dim)
        shapes = lambda *dims, dtype=F32: sds(dims, dtype)
        flat = lambda t: t.reshape(tok, dim)
        inv_freq = ROPE_BASE ** (-2.0 * np.arange(hd // 2) / hd)
        sign = np.repeat([-1.0, 1.0], hd // 2)
        freq = np.stack([np.tile(inv_freq, 2 * heads), np.tile(sign, heads)]).astype(np.float32)
        line = lambda v: v.reshape(1, -1)
        sem = lambda n: pltpu.SemaphoreType.DMA((n,))
        low = functools.partial(shapes, dtype=BF16)
        weights = [low(n_tp, n3, dim), low(n_tp, dim, ffn), low(n_tp, ffn, dim)]
        tiles = [shapes(n_chips, n_tile, dim)] + [shapes(n_tile, dim)] * 10
        out_shape = ([low(*big)] * 2 + [shapes(dim, ffn), shapes(ffn, dim), shapes(n3, dim), shapes(width, dim), shapes(6 * n_tp, LANES), shapes(8, LANES)] + weights
                     + [low(n_tp, n_tp, seqs, p_len, width)] * 3 + [low(tok, n_tp * ffn), shapes(tok, n_tp * ffn)] + tiles)
        plain = [pad_mask] + [line(v) for v in (ln1_gain, ln1_bias, b_out, ln2_gain, b_down, ln2_bias)] + [freq]
        heads4 = low(n_tp, seqs, p_len, n_tp * width)
        stat = shapes(n_tp, seqs, heads, seq)
        tile8 = shapes(n_tp, 8, LANES)
        row_ffn = shapes(n_tp, 1, ffn)
        scratch = ([low(*big)] * 9 + [heads4, heads4, low(n_tp, width, dim)] + [shapes(*big)] * 2
                   + [shapes(n_chips, n_tile, dim), shapes(2, n_tile, dim), low(n_tp, seqs, p_len, n3)]
                   + [shapes(seq, width)] * 5 + [shapes(seqs, seq, LANES), stat, stat, shapes(n_tp, 1, n3), row_ffn, row_ffn, row_ffn]
                   + [shapes(n_tp, *b_qkv.shape), tile8, tile8, shapes(8, dim), shapes(n_tp, 6 * n_tp, LANES), shapes(6 * n_tp, LANES)]
                   + [low(tok, ffn)] * 3 + plain)
        outs = pl.pallas_call(
            kernel, name='layer', out_shape=out_shape, in_specs=[ANY] * 16, out_specs=[ANY] * len(out_shape),
            scratch_shapes=[pltpu.VMEM(v.shape, v.dtype) for v in scratch]
            + [sem(112), sem(112), sem(48), sem(3 * n_tp), sem(3 * n_tp), pltpu.SemaphoreType.REGULAR],
            compiler_params=pltpu.CompilerParams(collective_id=0, has_side_effects=True, vmem_limit_bytes=VMEM_LIMIT),
        )(flat(x_in), flat(grad_y), w_qkv.transpose(0, 2, 3, 1).reshape(n3, dim), b_qkv, w_out.reshape(width, dim),
          w_up, line(b_up), w_down, *plain)

        def finish(*refs):
            src, (v_ref, b_ref), out, (bq_o, bu_o), v_o = refs[:6], refs[6:8], refs[8:14], refs[14:16], refs[16:22]
            bufs, (took, gave) = refs[22:28], refs[28:]
            cuts = [(n, pl.ds(i * (r.shape[0] // 2), r.shape[0] // 2)) for i in range(2) for n, r in enumerate(src)]
            loads = [pltpu.make_async_copy(src[n].at[p], bufs[n].at[p], took.at[i]) for i, (n, p) in enumerate(cuts)]
            stores = [pltpu.make_async_copy(bufs[n].at[p], out[n].at[p], gave.at[i]) for i, (n, p) in enumerate(cuts)]
            for c in loads:
                c.start()
            for i in range(3):
                for h in range(heads):
                    bq_o[i, h:h + 1, :] = b_ref[i:i + 1, h * hd:(h + 1) * hd]
            for i in range(ffn // LANES):
                bu_o[:, i * LANES:(i + 1) * LANES] = b_ref[3 + i:4 + i, :]
            for r, ref in enumerate(v_o):
                for i in range(n_tp):
                    ref[:, i * LANES:(i + 1) * LANES] = v_ref[r * n_tp + i:r * n_tp + i + 1, :]
            for load, give in zip(loads, stores):
                load.wait()
                give.start()
            for c in stores:
                c.wait()

        large = [low(*big)] * 2 + [shapes(dim, ffn), shapes(ffn, dim), shapes(n3, dim), shapes(width, dim)]
        small = [shapes(*b_qkv.shape), shapes(1, ffn)] + [shapes(1, dim)] * 6
        vmem = pl.BlockSpec(memory_space=pltpu.VMEM)
        res = pl.pallas_call(
            finish, name='finish', out_shape=large + small, in_specs=[ANY] * 6 + [vmem] * 2, out_specs=[ANY] * 6 + [vmem] * 8,
            scratch_shapes=[pltpu.VMEM(v.shape, v.dtype) for v in large] + [sem(12)] * 2,
            compiler_params=pltpu.CompilerParams(vmem_limit_bytes=VMEM_LIMIT),
        )(*outs[:8])
        y_out, grad_x, grad_w_up, grad_w_down, gq, go, grad_b_qkv, grad_b_up = res[:8]
        v = [t.reshape(dim) for t in res[8:]]
        return (y_out.reshape(x_in.shape), grad_x.reshape(x_in.shape), v[0], v[1], gq.reshape(3, heads, hd, dim).transpose(0, 3, 1, 2),
                grad_b_qkv, go.reshape(heads, hd, dim), v[2], v[3], v[4], grad_w_up, grad_b_up.reshape(ffn), grad_w_down, v[5])

    return jax.shard_map(device_step, mesh=mesh, in_specs=in_specs, out_specs=out_specs, check_vma=False)
```

```python
import functools

import jax
import jax.numpy as jnp
import numpy as np
from jax import lax
from jax.experimental import pallas as pl
from jax.experimental.pallas import tpu as pltpu
from jax.sharding import PartitionSpec as P

LN_EPS = 1e-5
ROPE_BASE = 10000.0
INV_SQRT2 = 0.7071067811865476
INV_SQRT_2PI = 0.3989422804014327
NEG_LARGE = -1e30
F32 = jnp.float32
BF16 = jnp.bfloat16
VMEM_LIMIT = 66_500_000
LANES = 128
NN = (((1,), (0,)), ((), ()))
NT = (((1,), (1,)), ((), ()))
TN = (((0,), (0,)), ((), ()))
PAIR, FAR, CROSS = 1, 2, 3
BOTH = range(2)
ANY = pl.BlockSpec(memory_space=pl.ANY)


def mm(a, b, dims):
    return lax.dot_general(a, b, dims, preferred_element_type=F32)


def ln_stats(v):
    centered = v - jnp.mean(v, axis=-1, keepdims=True)
    inv_std = lax.rsqrt(jnp.mean(centered * centered, axis=-1, keepdims=True) + LN_EPS)
    return centered * inv_std, inv_std


def ln_grad(d_out, x_hat, inv_std, gain):
    d_hat = d_out * gain
    return inv_std * (d_hat - jnp.mean(d_hat, axis=-1, keepdims=True) - x_hat * jnp.mean(d_hat * x_hat, axis=-1, keepdims=True))


def col_sum(t):
    return jnp.sum(t, axis=0, keepdims=True)


def swap_halves(t, head_dim):
    half = head_dim // 2
    lane = lax.broadcasted_iota(jnp.int32, t.shape, t.ndim - 1)
    return jnp.where(lane % head_dim < half, pltpu.roll(t, t.shape[-1] - half, t.ndim - 1), pltpu.roll(t, half, t.ndim - 1))


def span(i, n):
    return pl.ds(pl.multiple_of(i * n, n), n)


def fold(row, out, first):
    for i in range(row.shape[-1] // LANES):
        out[pl.ds(first + i, 1), :] = row[:, i * LANES:(i + 1) * LANES]


def unfold(src, first, out):
    for i in range(out.shape[-1] // LANES):
        out[:, pl.ds(i * LANES, LANES)] = src[pl.ds(first + i, 1), :]


def loop_rows(total, n, body):
    @pl.loop(0, total // n)
    def _(i):
        body(span(i, n))


class Net:
    def __init__(self, n_tp, send, recv, local):
        self.n_tp, self.send, self.recv, self.local = n_tp, send, recv, local
        self.copies, self.count, self.n_local = {}, 0, 0

    def peer(self, chip, core=0):
        me = lax.axis_index('tp')
        way = 1 - 2 * lax.rem(lax.div(me, 2), 2)
        at = lax.rem(me + 2 * chip * way + self.n_tp, self.n_tp) if chip else me
        return at + 1 - 2 * lax.rem(at, 2) if core else at

    def add(self, name, src, dst, chip, core=0):
        n = self.count
        self.count += 1

        def make():
            return pltpu.make_async_remote_copy(
                src_ref=src(), dst_ref=dst(), send_sem=self.send.at[n], recv_sem=self.recv.at[n],
                device_id={'tp': self.peer(chip, core)}, device_id_type=pl.DeviceIdType.MESH)

        self.copies.setdefault(name, []).append(make)

    def add_local(self, name, src, dst):
        n = self.n_local
        self.n_local += 1
        self.copies.setdefault(name, []).append(lambda: pltpu.make_async_copy(src(), dst(), self.local.at[n]))

    def start(self, *names):
        for name in names:
            for make in self.copies[name]:
                make().start()

    def got(self, *names):
        for name in names:
            with jax.named_scope('got_' + name):
                for make in self.copies[name]:
                    make().wait_recv()

    def sent(self, *names):
        for name in names:
            for make in self.copies[name]:
                make().wait_send()

    def done(self, *names):
        for name in names:
            with jax.named_scope('done_' + name):
                for make in self.copies[name]:
                    make().wait()

    def gather(self, name, own, buf, via, far=None):
        rows = own.shape[0]
        at = (lambda n: far.at[pl.ds((n - 2 * FAR) * rows, rows)] if far is not None and n // 2 == FAR else buf.at[n])
        for stage, chip in (('p', PAIR), ('c', CROSS)):
            self.add(name + stage, lambda: own, lambda c=chip: buf.at[2 * c], chip)
        self.add(name + 'm', lambda: own, lambda: buf.at[1], 0, 1)
        self.add(name + 'r', lambda: buf.at[2 * (PAIR + CROSS - via)], lambda: at(2 * FAR), via)
        for stage, chip in (('f', PAIR), ('g', CROSS), ('l', FAR)):
            self.add(name + stage, lambda c=chip: at(2 * c), lambda c=chip: at(2 * c + 1), 0, 1)

    def exchange(self, name, src, dst, rows):
        me = lax.axis_index('tp')
        for core in BOTH:
            for chip in (PAIR, CROSS, FAR, 0):
                if chip + core:
                    self.add(name, lambda c=chip, k=core: src.at[span(self.peer(c, k), rows)], lambda: dst.at[span(me, rows)], chip, core)
        self.add_local(name + '_own', lambda: src.at[span(me, rows)], lambda: dst.at[span(me, rows)])

    def multicast(self, name, src, dst, pair_dst, rows):
        me = lax.axis_index('tp')
        at = lambda buf: (lambda: buf.at[span(me, rows)])
        other = {0: PAIR, PAIR: 0, CROSS: FAR}
        for chip, stage in ((CROSS, '_cross'), (PAIR, '_pair'), (0, '_pair')):
            for core in BOTH:
                if chip + core:
                    for c, buf in ((chip, dst), (other[chip], pair_dst)):
                        self.add(name + stage, lambda c=c, k=core: src.at[span(self.peer(c, k), rows)], at(buf), chip, core)
        for c, buf in ((0, dst), (PAIR, pair_dst)):
            self.add_local(name + '_own', lambda c=c: src.at[span(self.peer(c), rows)], at(buf))
        came = lambda buf: (lambda: buf.at[span(lax.div(self.peer(CROSS), 2), 2 * rows)])
        self.add(name + '_fwd', came(dst), came(pair_dst), PAIR)
        self.add(name + '_fwd', came(pair_dst), came(dst), PAIR)


def solution(mesh):
    n_tp = mesh.shape['tp']
    n_chips = n_tp // 2
    act_spec = P('dp', 'tp', None)
    rep_vec = P(None)
    part_vec = P('dp')
    in_specs = (act_spec, act_spec, P('dp', None), rep_vec, rep_vec, P(None, None, 'tp', None), P(None, 'tp', None),
                P('tp', None, None), rep_vec, rep_vec, rep_vec, P(None, 'tp'), P('tp'), P('tp', None), rep_vec)
    out_specs = (act_spec, act_spec, part_vec, part_vec, P('dp', None, 'tp', None), P('dp', 'tp', None),
                 P(('dp', 'tp'), None, None), part_vec, part_vec, part_vec, P('dp', 'tp'), P(('dp', 'tp')),
                 P(('dp', 'tp'), None), part_vec)

    def device_step(x_in, grad_y, pad_mask, ln1_gain, ln1_bias, w_qkv, b_qkv, w_out, b_out, ln2_gain, ln2_bias, w_up, b_up, w_down, b_down):
        batch, p_len, dim = x_in.shape
        seq = pad_mask.shape[1]
        _, _, heads, hd = w_qkv.shape
        seqs = batch // n_tp
        ffn = w_up.shape[1]
        width = heads * hd
        n3 = 3 * width
        tok = seqs * seq
        chunk = seqs * p_len
        qc = seq // 2
        q_scale = hd ** -0.5
        sds = jax.ShapeDtypeStruct
        n_tile = n3 + width
        half = dim // 2
        twice = n_tp + n_tp

        def kernel(*refs):
            it = iter(refs)
            take = lambda n: [next(it) for _ in range(n)]
            (x_ref, dy_ref, wq_ref, bq_ref, wo_ref, wu_ref, bu_ref, wd_ref), plain = take(8), take(8)
            y_out, gx_out, g_up, g_down, g_q, g_o, g_vec, g_b, wq, wu, wd, q_hbm, k_hbm, v_hbm, act_hbm, slope_hbm = take(16)
            p_at, got_at, sum_at, early_at, last_at, x_dn, x_up, p_dn, p_up, r_dn, r_up = take(11)
            x, h1, dy, x1, h2, dx1b, h2p, dyp, y, o4, do4, wo, acc, acc2, p_rcv, p_snd, d4 = take(17)
            dq_acc, dk_acc, dv_acc, cos_t, sin_t, ok, m_st, l_st, b_att, b_ffn, u_all, gb, b_all, b8, late, late_in, vec, v_in, v_own = take(19)
            dpre = next(it)
            act_p, dpre_p = (y.at[:, pl.ds(i * ffn, ffn)] for i in BOTH)
            here = take(8)
            send, recv, local, pair_send, pair_recv, pair_ready = take(6)
            net = Net(n_tp, send, recv, local)
            me = lax.axis_index('tp')
            mask_ref, gain1, bias1, bias_o, gain2, bias_d, bias2, freq_ref = here

            net.gather('q', wq_ref, wq, CROSS)
            net.gather('o', wo_ref, wo, CROSS)
            net.gather('u', wu_ref, wu, CROSS)
            net.gather('d', wd_ref, wd, PAIR, dx1b)
            net.exchange('x', x_ref, x, chunk)
            net.multicast('dy', dy_ref, dy, dyp, chunk)
            net.exchange('y', y, y_out, chunk)
            net.exchange('gx', h1, gx_out, chunk)
            for chip in range(n_chips):
                for core in BOTH:
                    if chip + core:
                        slot = 2 * chip + core
                        net.add('bias', lambda: bq_ref, lambda n=slot: b_all.at[n], chip, core)
                        net.add('bias', lambda: bu_ref, lambda n=slot: u_all.at[n], chip, core)
                        net.add('late', lambda n=slot: late.at[n], lambda n=slot: late_in.at[n], chip, core)
                        net.add('early', lambda: v_own.at[pl.ds(twice, 2 * twice)], lambda n=slot: v_in.at[n], chip, core)
            for i in BOTH:
                net.add(f'h{i}', lambda p=pl.ds(i * half, half): h2.at[p], lambda p=pl.ds(i * half, half): h2p.at[p], PAIR)
            net.add('dn_x', lambda: x_dn, lambda: r_dn, CROSS)
            net.add('up_x', lambda: x_up, lambda: r_up, CROSS)
            net.add('at_early', lambda: p_at.at[PAIR], lambda: early_at, PAIR)
            t_half = n_tile // 2
            for i, part in enumerate((pl.ds(0, t_half), pl.ds(t_half, t_half))):
                net.add(f'at_relay{i}', lambda p=part: p_at.at[FAR, p], lambda p=part: got_at.at[p], PAIR)
                net.add(f'at_sum{i}', lambda p=part: sum_at.at[p], lambda p=part: last_at.at[p], CROSS)
                net.add_local(f'at{i}_load', lambda p=part: got_at.at[p], lambda p=part: p_rcv.at[0, p])
                net.add_local(f'at{i}_load', lambda p=part: p_at.at[CROSS, p], lambda p=part: p_rcv.at[1, p])
                net.add_local(f'at{i}_store', lambda p=part: p_rcv.at[1, p], lambda p=part: sum_at.at[p])
            for src, dst in zip(plain, here):
                net.add_local('own', lambda r=src: r, lambda r=dst: r)
            net.add_local('write', lambda: v_own, lambda: g_vec)
            net.add_local('write', lambda: b8.at[0], lambda: g_b)
            for ref, tmp, buf in ((wq_ref, lambda: h2.at[pl.ds(0, n3)], wq), (wu_ref, lambda: x1.at[:, pl.ds(0, ffn)], wu),
                                        (wd_ref, lambda: dx1b.at[pl.ds(0, ffn)], wd)):
                net.add_local('load', lambda r=ref: r, tmp)
                net.add_local('store', tmp, lambda b=buf: b.at[0])
            net.add_local('own', lambda: wo_ref, lambda: wo.at[0])
            net.add_local('own', lambda: bq_ref, lambda: b_all.at[0])
            net.add_local('own', lambda: bu_ref, lambda: u_all.at[0])
            def pass_on(i, stage):
                if stage == 0:
                    net.got(f'at_relay{i}')
                    net.start(f'at{i}_load')
                elif stage == 1:
                    net.done(f'at{i}_load')

                    def body(rows):
                        rows = pl.ds(i * t_half + rows.start, rows.size)
                        p_rcv[1, rows] += p_rcv[0, rows]

                    loop_rows(t_half, 8, body)
                    net.start(f'at{i}_store')
                else:
                    net.done(f'at{i}_store')
                    net.start(f'at_sum{i}')

            def pack(lo, hi):
                for r in range(lo, hi):
                    fold(vec[pl.ds(r, 1), :], v_own, r * n_tp)

            def hooks(step, table):
                for at, act in table.items():
                    @pl.when(step == at)
                    def _(act=act):
                        act()

            tile_order = (FAR, PAIR, CROSS, 0)

            def place(i):
                return jnp.where(i == 0, FAR, jnp.where(i == 1, PAIR, jnp.where(i == 2, CROSS, 0)))

            def order(s):
                return 2 * place(lax.div(s, 2)) + 1 - lax.rem(s, 2)

            def to_partner(src, dst, sem):
                return pltpu.make_async_remote_copy(
                    src_ref=p_snd.at[src], dst_ref=p_rcv.at[dst], send_sem=pair_send.at[sem], recv_sem=pair_recv.at[sem],
                    device_id={'tp': net.peer(0, 1)}, device_id_type=pl.DeviceIdType.MESH)

            def keep(i, to):
                return pltpu.make_async_copy(p_rcv.at[i], to, pair_send.at[twice + i])

            def into(i):
                return lambda at, v: p_snd.__setitem__((i,) + at, v)

            def add_sent(i, j):
                def body(rows):
                    p_rcv[j, rows] += p_snd[i, rows]

                loop_rows(n_tile, 16, body)

            def pair_go(s):
                @pl.when(lax.rem(s, 2) == 1)
                def _():
                    to_partner(0, lax.div(s, 2), lax.div(s, 2)).start()

            def pair(s, tile):
                j = lax.div(s, 2)
                odd = lax.rem(s, 2)
                tile(into(odd))

                @pl.when(odd == 1)
                def _():
                    copy = to_partner(0, j, j)
                    copy.wait_send()
                    copy.wait_recv()
                    add_sent(1, j)
                    keep(j, p_at.at[place(j)]).start()

            def stored(i):
                keep(i, p_at.at[tile_order[i]]).wait()

            def pair_begin():
                pl.semaphore_signal(pair_ready, inc=1, device_id={'tp': net.peer(0, 1)}, device_id_type=pl.DeviceIdType.MESH)
                pl.semaphore_wait(pair_ready, 1)

            barrier = pltpu.get_barrier_semaphore()
            for chip in range(n_chips):
                for core in BOTH:
                    if chip + core:
                        pl.semaphore_signal(barrier, inc=1, device_id={'tp': net.peer(chip, core)}, device_id_type=pl.DeviceIdType.MESH)
            pl.semaphore_wait(barrier, n_tp - 1)
            net.start('qp', 'qc', 'x', 'qm', 'bias', 'own', 'load', 'x_own', 'dy_own')
            net.done('own')
            angle = lax.broadcasted_iota(jnp.int32, (seq, width), 0).astype(F32) * freq_ref[0:1, :]
            cos_t[...] = jnp.cos(angle)
            sin_t[...] = jnp.sin(angle) * freq_ref[1:2, :]
            for b in range(seqs):
                row = mask_ref[pl.ds(me * seqs + b, 1), :].astype(F32)
                ok[b] = jnp.broadcast_to(row, (LANES, seq)).T
            net.done('load')
            net.start('store')
            net.got('qp', 'qc')
            net.start('qr', 'dy_cross', 'oc', 'op', 'up', 'dy_pair', 'qf', 'qg', 'om')
            net.done('x_own', 'dy_own')
            net.got('bias')
            for n in range(n_tp):
                b = b_all[n]
                b_att[n] = jnp.concatenate([b[i // heads, i % heads:i % heads + 1, :] for i in range(3 * heads)], axis=1)
                b_ffn[n] = u_all[n]
            net.got('x')

            def ln1(rows):
                x_hat, _ = ln_stats(x[rows, :].astype(F32))
                h1[rows, :] = (x_hat * gain1[...] + bias1[...]).astype(BF16)

            loop_rows(tok, chunk, ln1)
            net.done('store')
            net.got('qm', 'qf', 'qg')

            def arrival(s):
                return s + 2 * lax.div(s, n_chips) - n_chips * lax.div(s, n_chips + 2)

            def qkv_step(ps, w, q_ref, k_ref, v_ref):
                s = ps.index[0]
                hooks(s, {2: lambda: (net.got('op'), net.start('or', 'uc', 'um', 'of')), 4: lambda: (net.got('qr'), net.start('ql')),
                          5: lambda: net.got('ql')})
                n_src = tok // chunk // 2

                @pl.loop(0, 2)
                def _(i):
                    rows = span(i, tok // 2)
                    t = mm(h1[rows, :], w[0], NT) + b_att[arrival(s)]
                    cos, sin = (t_ref[span(i, seq // 2), :].reshape(n_src, 1, p_len, width) for t_ref in (cos_t, sin_t))

                    def rope(v):
                        out = v.reshape(n_src, seqs, p_len, width) * cos + swap_halves(v, hd).reshape(n_src, seqs, p_len, width) * sin
                        return out.astype(BF16)

                    src = span(i, n_src)
                    q_ref[0, src] = rope(t[:, :width] * q_scale)
                    k_ref[0, src] = rope(t[:, width:2 * width])
                    v_ref[0, src] = t[:, 2 * width:].reshape(n_src, seqs, p_len, width).astype(BF16)

            slot3 = lambda rows, cols, f=lambda s: s: pl.BlockSpec((1, rows, cols), lambda s: (f(s), 0, 0))

            def pipe(body, **specs):
                def run(*refs):
                    with jax.named_scope(body.__name__):
                        pltpu.emit_pipeline(body, _explicit_indices=True, **specs)(*refs)

                return run

            pipe(qkv_step, grid=(n_tp,), in_specs=[slot3(n3, dim, arrival)],
                 out_specs=[pl.BlockSpec((1, n_tp, seqs, p_len, width), lambda s: (arrival(s), 0, 0, 0, 0))] * 3)(
                wq, q_hbm, k_hbm, v_hbm)

            srcs = qc // p_len
            lane = lax.broadcasted_iota(jnp.int32, (qc, width), 1)

            def attn_step(ps, q_ref, k_ref, v_ref):
                g, b = ps.index
                hooks(g * seqs + b, {
                    8: lambda: (net.got('dy_cross'), net.start('dy_fwd')), 9: lambda: (net.got('up'), net.start('ur', 'dc', 'dm', 'uf')),
                    14: lambda: (net.got('oc', 'or'), net.start('og', 'ol'))})
                bad = ok[b][:, 0:1] <= 0
                k = k_ref[0, :, 0].reshape(seq, width)
                v_t = v_ref[0, :, 0].reshape(seq, width).T
                for c in range(seq // qc):
                    src = slice(c * srcs, (c + 1) * srcs)
                    cols = slice(c * qc, (c + 1) * qc)
                    q = q_ref[0, src, 0].reshape(qc, width)
                    outs = []
                    for h in range(heads):
                        s = jnp.where(bad, NEG_LARGE, mm(k, jnp.where(lane // hd == h, q, jnp.zeros_like(q)), NT))
                        m = jnp.max(s, axis=0, keepdims=True)
                        e = jnp.exp(s - m)
                        r = 1.0 / col_sum(e)
                        outs.append(mm(v_t[h * hd:(h + 1) * hd], (e * r).astype(BF16), NN))
                        m_st[g, b, h:h + 1, cols] = m
                        l_st[g, b, h:h + 1, cols] = r
                    o4[src, b, :, span(g, width)] = jnp.concatenate(outs, axis=0).T.astype(BF16).reshape(srcs, p_len, width)

            head_blk = pl.BlockSpec((1, n_tp, 1, p_len, width), lambda g, b: (g, 0, b, 0, 0))
            pipe(attn_step, grid=(n_tp, seqs), in_specs=[head_blk] * 3)(q_hbm, k_hbm, v_hbm)

            net.got('om', 'of', 'og', 'ol')

            @pl.loop(0, tok // (2 * chunk))
            def _(i):
                rows = span(i, 2 * chunk)
                o = o4[pl.ds(2 * i, 2)].reshape(2 * chunk, n_tp * width)
                low = (x[rows, :].astype(F32) + (mm(o, wo[...].reshape(n_tp * width, dim), NN) + bias_o[...])).astype(BF16)
                x1[rows, :] = low
                x_hat, _ = ln_stats(low.astype(F32))
                h2[rows, :] = (x_hat * gain2[...] + bias2[...]).astype(BF16)

            net.start('h0', 'h1', 'dp')

            def gelu(pre):
                erf_term = lax.erf(pre * INV_SQRT2)
                act = (0.5 * pre * (1.0 + erf_term)).astype(BF16)
                return act, 0.5 * (1.0 + erf_term) + pre * jnp.exp(-0.5 * pre * pre) * INV_SQRT_2PI

            cols = lambda f: pl.BlockSpec((tok, ffn), lambda s: (0, f(s)))
            wu_spec, wd_spec = functools.partial(slot3, dim, ffn), functools.partial(slot3, ffn, dim)

            def mlp_up(n, f, table):
                def up_step(ps, w, act_ref, slope_ref):
                    s = ps.index[0]
                    hooks(s, table)

                    def body(rows):
                        act_ref[rows, :], slope_ref[rows, :] = gelu(mm(h2[rows, :], w[0], NN) + b_ffn[f(s)])

                    loop_rows(tok, half, body)

                pipe(up_step, grid=(n,), in_specs=[wu_spec(f)], out_specs=[cols(f)] * 2)(wu, act_hbm, slope_hbm)

            net.got('um', 'uf')
            mlp_up(n_tp - 2, arrival, {2: lambda: (net.got('uc'), net.start('ug')), 3: lambda: net.got('ug')})
            net.got('dy_pair', 'dy_fwd', 'dm')

            def backward(slot, w_d, w_u, act_ref, slope_ref, add):
                if add:
                    gb[slot] = jnp.zeros_like(gb[0])

                def body(rows):
                    d_pre = mm(dy[rows, :], w_d, NT) * slope_ref[rows, :]
                    low = d_pre.astype(BF16)
                    dpre[rows, :] = low
                    if add:
                        gb[slot] += col_sum(d_pre)
                        acc[rows, :] += mm(act_ref[rows, :], w_d, NN)
                        acc2[rows, :] += mm(low, w_u, NT)

                loop_rows(tok, half, body)

            def pair_gelu(rows, w_u, slot):
                return gelu(mm(h2p[rows, :], w_u, NN) + b_ffn[slot])

            def grads(chip, at, x_refs, sends):
                f = lambda s: 2 * chip + 1 - s
                copy = to_partner(0, at, n_tp + at)

                def first(ps, w_u, act_ref):
                    s = ps.index[0]
                    rows = pl.ds(0, half)
                    act_p[rows, :] = pair_gelu(rows, w_u[0], f(s))[0]
                    p_snd[s] = mm(act_ref[...], dy[...], TN) + mm(act_p[rows, :], dyp[rows, :], TN)

                def second(ps, w_u):
                    s = ps.index[0]
                    pl.when(s == 1)(lambda: copy.start())
                    rows = pl.ds(half, half)
                    act_p[rows, :] = pair_gelu(rows, w_u[0], f(s))[0]
                    p_snd[s] += mm(act_p[rows, :], dyp[rows, :], TN)

                    @pl.when(s == 1)
                    def _():
                        copy.wait_recv()
                        add_sent(1, at)
                        keep(at, x_refs[0]).start()
                        copy.wait_send()

                pipe(first, grid=(len(BOTH),), in_specs=[wu_spec(f), cols(f)])(wu, act_hbm)
                net.got(*sends[2:])
                pipe(second, grid=(len(BOTH),), in_specs=[wu_spec(f)])(wu)
                keep(at, x_refs[0]).wait()
                net.start(*sends[:1])

            def mlp(n, f, add, table, last=None):
                def mlp_step(ps, wd_s, wu_s, act_ref, slope_ref):
                    s = ps.index[0]
                    backward(f(s), wd_s[0], wu_s[0], act_ref, slope_ref, add)
                    if last:
                        at, ref, send = last
                        copy = to_partner(0, at + 1, n_tp + at + 1)
                        pl.when(s == 1)(lambda: copy.start())

                        @pl.when(s < 2)
                        def _():
                            def body(rows):
                                dpre_p[rows, :] = (mm(dyp[rows, :], wd_s[0], NT) * pair_gelu(rows, wu_s[0], f(s))[1]).astype(BF16)

                            loop_rows(tok, half, body)
                            for i in BOTH:
                                part = pl.ds(i * half, half)
                                p_snd[s, pl.ds(0, ffn), part] = mm(h2[:, part], dpre[...], TN) + mm(h2p[:, part], dpre_p[...], TN)

                        @pl.when(s == 1)
                        def _():
                            copy.wait_recv()
                            add_sent(1, at + 1)
                            keep(at + 1, ref).start()
                            copy.wait_send()

                    hooks(s, table)

                pipe(mlp_step, grid=(n,), in_specs=[wd_spec(f), wu_spec(f), cols(f), cols(f)])(wd, wu, act_hbm, slope_hbm)

            acc[...] = jnp.zeros_like(acc)
            acc2[...] = jnp.zeros_like(acc2)
            mlp(2, lambda s: s, True, {})
            net.got('ur')
            net.start('ul')
            net.got('ul')
            mlp_up(2, lambda s: s + 2 * FAR, {})
            net.got('h0')
            grads(CROSS, 0, (x_dn, x_up), ('dn_x', 'up_x', 'h1'))
            net.got('dc')
            net.start('dg', 'dr')
            net.got('dg')

            def sent_up():
                keep(1, x_up).wait()
                net.start('up_x')

            slots = lambda s: jnp.where(s < 2, 2 * CROSS + 1 - s, s)
            mlp(n_chips, slots, True, {0: lambda: (net.got('dp'), net.start('df')), 1: lambda: net.got('df'), 2: sent_up}, (0, x_up, 'up_x'))

            def far_step(ps, wu_s, act_ref, slope_ref):
                s = ps.index[0]
                hooks(s, {0: lambda: (net.got('dr'), net.start('dl')), 1: lambda: net.got('dl')})
                backward(s + 2 * FAR, dx1b[span(s, ffn), :], wu_s[0], act_ref, slope_ref, True)

            far = lambda s: s + 2 * FAR
            pipe(far_step, grid=(len(BOTH),), in_specs=[wu_spec(far), cols(far), cols(far)])(wu, act_hbm, slope_hbm)

            def y_rows(rows):
                y[rows, :] = (x1[rows, :].astype(F32) + (acc[rows, :] + bias_d[...])).astype(BF16)

            loop_rows(tok, 2 * chunk, y_rows)
            vec[...] = jnp.zeros_like(vec)
            net.start('y', 'y_own')
            net.sent('dl')

            @pl.loop(0, tok // (2 * chunk))
            def _(i):
                rows = span(i, 2 * chunk)
                x1_f, dy_f, dh = x1[rows, :].astype(F32), dy[rows, :].astype(F32), acc2[rows, :]
                x_hat, inv_std = ln_stats(x1_f)
                d_x1 = dy_f + ln_grad(dh, x_hat, inv_std, gain2[...])
                acc2[rows, :] = d_x1
                low = d_x1.astype(BF16)
                dx1b[rows, :] = low
                d_o = mm(low, wo[...].reshape(n_tp * width, dim), NT).astype(BF16)
                do4[pl.ds(2 * i, 2)] = d_o.reshape(2, seqs, p_len, n_tp * width)
                for n, t in enumerate((d_x1, dh * x_hat, dh, dy_f)):
                    vec[2 + n:3 + n, :] += col_sum(t)

            pack(2, 6)
            pair_begin()

            def bwd_step(ps, q_ref, k_ref, v_ref, w):
                step = ps.index[0]
                g = order(step)
                hooks(step, {0: lambda: net.start('early'), 2: lambda: (stored(0), net.start('at_relay0', 'at_relay1')),
                             4: lambda: (stored(1), net.start('at_early')), 6: lambda: (stored(2), pass_on(0, 0)), 7: lambda: pass_on(0, 2)})
                pair_go(step)
                b8[g] = jnp.zeros_like(b8[0])
                fold(gb[g], b8.at[g], 3)
                for b in range(seqs):
                    bad = ok[b][:, 0:1] <= 0
                    k = k_ref[0, :, b].reshape(seq, width)
                    v = v_ref[0, :, b].reshape(seq, width)
                    k_t = k.T
                    for c in range(seq // qc):
                        src = slice(c * srcs, (c + 1) * srcs)
                        at = slice(c * qc, (c + 1) * qc)
                        q = q_ref[0, src, b].reshape(qc, width)
                        d_o = do4[src, b, :, span(g, width)].reshape(qc, width)
                        dk = jnp.zeros((seq, width), F32)
                        dv = jnp.zeros((seq, width), F32)
                        dqs = []
                        for h in range(heads):
                            mine = lane // hd == h
                            q_h = jnp.where(mine, q, jnp.zeros_like(q))
                            do_h = jnp.where(mine, d_o, jnp.zeros_like(d_o))
                            s = jnp.where(bad, NEG_LARGE, mm(k, q_h, NT))
                            p = jnp.exp(s - m_st[g, b, h:h + 1, at]) * l_st[g, b, h:h + 1, at]
                            dv += mm(p.astype(BF16), do_h, NN)
                            dp = mm(v, do_h, NT)
                            ds = (p * (dp - col_sum(dp * p))).astype(BF16)
                            dk += mm(ds, q_h, NN)
                            dqs.append(mm(k_t[h * hd:(h + 1) * hd], ds, NN))
                        dq_acc[at, :] = jnp.concatenate(dqs, axis=0).T
                        dk_acc[...] = dk if c == 0 else dk_acc[...] + dk
                        dv_acc[...] = dv if c == 0 else dv_acc[...] + dv
                    cos, sin = cos_t[...], sin_t[...]
                    dq, dk, dv = dq_acc[...], dk_acc[...], dv_acc[...]
                    dq = (dq * cos - swap_halves(dq, hd) * sin) * q_scale
                    dk = dk * cos - swap_halves(dk, hd) * sin
                    for i, t in enumerate((dq, dk, dv)):
                        d4[:, b, :, i * width:(i + 1) * width] = t.astype(BF16).reshape(n_tp, p_len, width)
                        b8[g, i:i + 1, :] += col_sum(t)

                @pl.when(step == 0)
                def _():
                    acc[...] = jnp.zeros_like(acc)

                @pl.loop(0, 2)
                def _(i):
                    acc[span(i, half), :] += mm(d4[pl.ds(n_chips * i, n_chips)].reshape(half, n3), w[0], NN)

                def tile(put):
                    put((pl.ds(0, n3),), mm(d4[...].reshape(tok, n3), h1[...], TN))
                    put((pl.ds(n3, width),), mm(o4[:, :, :, span(g, width)].reshape(tok, width), dx1b[...], TN))

                pair(step, tile)
                hooks(step, {6: lambda: pass_on(0, 1)})

            slot_blk = pl.BlockSpec((1, n_tp, seqs, p_len, width), lambda s: (order(s), 0, 0, 0, 0))
            pipe(bwd_step, grid=(n_tp,), in_specs=[slot_blk] * 3 + [slot3(n3, dim, order)])(
                q_hbm, k_hbm, v_hbm, wq)

            pass_on(1, 0)

            def ln1_bwd(rows):
                x_hat, inv_std = ln_stats(x[rows, :].astype(F32))
                dh = acc[rows, :]
                h1[rows, :] = (acc2[rows, :] + ln_grad(dh, x_hat, inv_std, gain1[...])).astype(BF16)
                vec[0:1, :] += col_sum(dh * x_hat)
                vec[1:2, :] += col_sum(dh)

            loop_rows(tok, 2 * chunk, ln1_bwd)
            stored(3)
            pack(0, 2)
            pass_on(1, 1)
            for n in range(1, n_tp):
                late[n, 0:8] = b8[n]
                late[n, 8:] = v_own[0:twice]
            net.start('late')
            pass_on(1, 2)
            net.start('gx', 'gx_own')

            net.sent('y')
            net.done('y_own')
            pair_begin()
            grads(0, 2, (p_dn, p_up), ())
            mlp(2, lambda s: 1 - s, False, {}, (2, p_up, None))
            keep(3, p_up).wait()

            def total(refs, out, block, at):
                def body(*blocks):
                    v = blocks[1][...]
                    for more in blocks[2:-1]:
                        v += more[...]
                    blocks[-1][...] = v

                pipe(body, grid=(len(BOTH),), in_specs=[pl.BlockSpec(block, at)] * len(refs),
                     out_specs=[pl.BlockSpec(block, lambda i: (i, 0))])(*refs, out)

            by_row, by_col = lambda i: (i, 0), lambda i: (0, i)
            net.got('late', 'early')
            b_total, v_late, v_early = b8[0], v_own[0:twice], v_own[twice:]
            for n in range(1, n_tp):
                b_total += late_in[n, 0:8]
                v_late += late_in[n, 8:]
                v_early += v_in[n]
            net.got('dn_x', 'up_x')
            total((p_dn, r_dn), g_down, (t_half, dim), by_row)
            total((p_up, r_up), g_up, (n_tile, half), by_col)
            net.got('at_early', 'at_sum0', 'at_sum1')
            for rows, out, n in ((pl.ds(0, n3), g_q, n3), (pl.ds(n3, width), g_o, width)):
                total((p_at.at[0, rows], early_at.at[rows], last_at.at[rows]), out, (n // 2, dim), by_row)
            for name in net.copies:
                if name not in ('load', 'store', 'own', 'write', 'gx', 'y', 'dl') and not name.endswith(('_own', '_load', '_store')):
                    net.sent(name)
            b8[0] = b_total
            v_own[0:twice] = v_late
            v_own[twice:] = v_early
            net.got('y')
            net.start('write')
            net.done('gx_own', 'write')
            net.got('gx')
            net.sent('gx')

        big = (tok, dim)
        shapes = lambda *dims, dtype=F32: sds(dims, dtype)
        flat = lambda t: t.reshape(tok, dim)
        inv_freq = ROPE_BASE ** (-2.0 * np.arange(hd // 2) / hd)
        sign = np.repeat([-1.0, 1.0], hd // 2)
        freq = np.stack([np.tile(inv_freq, 2 * heads), np.tile(sign, heads)]).astype(np.float32)
        line = lambda v: v.reshape(1, -1)
        sem = lambda n: pltpu.SemaphoreType.DMA((n,))
        low = functools.partial(shapes, dtype=BF16)
        weights = [low(n_tp, n3, dim), low(n_tp, dim, ffn), low(n_tp, ffn, dim)]
        tiles = [shapes(n_chips, n_tile, dim)] + [shapes(n_tile, dim)] * 10
        out_shape = ([low(*big)] * 2 + [shapes(dim, ffn), shapes(ffn, dim), shapes(n3, dim), shapes(width, dim), shapes(6 * n_tp, LANES), shapes(8, LANES)] + weights
                     + [low(n_tp, n_tp, seqs, p_len, width)] * 3 + [low(tok, n_tp * ffn), shapes(tok, n_tp * ffn)] + tiles)
        plain = [pad_mask] + [line(v) for v in (ln1_gain, ln1_bias, b_out, ln2_gain, b_down, ln2_bias)] + [freq]
        heads4 = low(n_tp, seqs, p_len, n_tp * width)
        stat = shapes(n_tp, seqs, heads, seq)
        tile8 = shapes(n_tp, 8, LANES)
        late = shapes(n_tp, 8 + twice, LANES)
        row_ffn = shapes(n_tp, 1, ffn)
        scratch = ([low(*big)] * 9 + [heads4, heads4, low(n_tp, width, dim)] + [shapes(*big)] * 2
                   + [shapes(n_chips, n_tile, dim), shapes(2, n_tile, dim), low(n_tp, seqs, p_len, n3)]
                   + [shapes(seq, width)] * 5 + [shapes(seqs, seq, LANES), stat, stat, shapes(n_tp, 1, n3), row_ffn, row_ffn, row_ffn]
                   + [shapes(n_tp, *b_qkv.shape), tile8, late, late, shapes(8, dim), shapes(n_tp, 2 * twice, LANES), shapes(6 * n_tp, LANES)]
                   + [low(tok, ffn)] + plain)
        outs = pl.pallas_call(
            kernel, name='layer', out_shape=out_shape, in_specs=[ANY] * 16, out_specs=[ANY] * len(out_shape),
            scratch_shapes=[pltpu.VMEM(v.shape, v.dtype) for v in scratch]
            + [sem(112), sem(112), sem(48), sem(3 * n_tp), sem(3 * n_tp), pltpu.SemaphoreType.REGULAR],
            compiler_params=pltpu.CompilerParams(collective_id=0, has_side_effects=True, vmem_limit_bytes=VMEM_LIMIT),
        )(flat(x_in), flat(grad_y), w_qkv.transpose(0, 2, 3, 1).reshape(n3, dim), b_qkv, w_out.reshape(width, dim),
          w_up, line(b_up), w_down, *plain)

        def finish(*refs):
            src, (v_ref, b_ref), out, (bq_o, bu_o), v_o = refs[:6], refs[6:8], refs[8:14], refs[14:16], refs[16:]
            for a, b in zip(src, out):
                b[...] = a[...]
            for i in range(3):
                for h in range(heads):
                    bq_o[i, h:h + 1, :] = b_ref[i:i + 1, h * hd:(h + 1) * hd]
            unfold(b_ref, 3, bu_o)
            for r, ref in enumerate(v_o):
                unfold(v_ref, r * n_tp, ref)

        large = [low(*big)] * 2 + [shapes(dim, ffn), shapes(ffn, dim), shapes(n3, dim), shapes(width, dim)]
        small = [shapes(*b_qkv.shape), shapes(1, ffn)] + [shapes(1, dim)] * 6
        moving = [pl.BlockSpec((v.shape[0] // n_chips, v.shape[1]), lambda i: (i, 0)) for v in large]
        fixed = lambda vs: [pl.BlockSpec(v.shape, lambda i, n=len(v.shape): (0,) * n) for v in vs]
        res = pl.pallas_call(
            finish, name='finish', out_shape=large + small, grid=(n_chips,), in_specs=moving + fixed(outs[6:8]),
            out_specs=moving + fixed(small), compiler_params=pltpu.CompilerParams(vmem_limit_bytes=VMEM_LIMIT),
        )(*outs[:8])
        y_out, grad_x, grad_w_up, grad_w_down, gq, go, grad_b_qkv, grad_b_up = res[:8]
        v = [t.reshape(dim) for t in res[8:]]
        return (y_out.reshape(x_in.shape), grad_x.reshape(x_in.shape), v[0], v[1], gq.reshape(3, heads, hd, dim).transpose(0, 3, 1, 2),
                grad_b_qkv, go.reshape(heads, hd, dim), v[2], v[3], v[4], grad_w_up, grad_b_up.reshape(ffn), grad_w_down, v[5])

    return jax.shard_map(device_step, mesh=mesh, in_specs=in_specs, out_specs=out_specs, check_vma=False)
```

```python
import functools

import jax
import jax.numpy as jnp
import numpy as np
from jax import lax
from jax.experimental import pallas as pl
from jax.experimental.pallas import tpu as pltpu
from jax.sharding import PartitionSpec as P

LN_EPS = 1e-5
ROPE_BASE = 10000.0
INV_SQRT2 = 0.7071067811865476
INV_SQRT_2PI = 0.3989422804014327
NEG_LARGE = -1e30
F32 = jnp.float32
BF16 = jnp.bfloat16
VMEM_LIMIT = 66_500_000
LANES = 128
NN = (((1,), (0,)), ((), ()))
NT = (((1,), (1,)), ((), ()))
TN = (((0,), (0,)), ((), ()))
PAIR, FAR, CROSS = 1, 2, 3
FAR0 = FAR + FAR
FAR1 = FAR0 + 1
BOTH = range(2)
ANY = pl.BlockSpec(memory_space=pl.ANY)


def mm(a, b, dims):
    return lax.dot_general(a, b, dims, preferred_element_type=F32)


def ln_stats(v):
    centered = v - jnp.mean(v, axis=-1, keepdims=True)
    inv_std = lax.rsqrt(jnp.mean(centered * centered, axis=-1, keepdims=True) + LN_EPS)
    return centered * inv_std, inv_std


def ln_grad(d_out, x_hat, inv_std, gain):
    d_hat = d_out * gain
    return inv_std * (d_hat - jnp.mean(d_hat, axis=-1, keepdims=True) - x_hat * jnp.mean(d_hat * x_hat, axis=-1, keepdims=True))


def col_sum(t):
    return jnp.sum(t, axis=0, keepdims=True)


def swap_halves(t, head_dim):
    half = head_dim // 2
    lane = lax.broadcasted_iota(jnp.int32, t.shape, t.ndim - 1)
    return jnp.where(lane % head_dim < half, pltpu.roll(t, t.shape[-1] - half, t.ndim - 1), pltpu.roll(t, half, t.ndim - 1))


def span(i, n):
    return pl.ds(pl.multiple_of(i * n, n), n)


def fold(row, out, first):
    for i in range(row.shape[-1] // LANES):
        out[pl.ds(first + i, 1), :] = row[:, i * LANES:(i + 1) * LANES]


def unfold(src, first, out):
    for i in range(out.shape[-1] // LANES):
        out[:, pl.ds(i * LANES, LANES)] = src[pl.ds(first + i, 1), :]


def loop_rows(total, n, body):
    @pl.loop(0, total // n)
    def _(i):
        body(span(i, n))


class Net:
    def __init__(self, n_tp, send, recv, local):
        self.n_tp, self.send, self.recv, self.local = n_tp, send, recv, local
        self.copies, self.count, self.n_local = {}, 0, 0

    def peer(self, chip, core=0):
        me = lax.axis_index('tp')
        way = 1 - 2 * lax.rem(lax.div(me, 2), 2)
        at = lax.rem(me + 2 * chip * way + self.n_tp, self.n_tp) if chip else me
        return at + 1 - 2 * lax.rem(at, 2) if core else at

    def add(self, name, src, dst, chip, core=0):
        n = self.count
        self.count += 1

        def make():
            return pltpu.make_async_remote_copy(
                src_ref=src(), dst_ref=dst(), send_sem=self.send.at[n], recv_sem=self.recv.at[n],
                device_id={'tp': self.peer(chip, core)}, device_id_type=pl.DeviceIdType.MESH)

        self.copies.setdefault(name, []).append(make)

    def add_local(self, name, src, dst):
        n = self.n_local
        self.n_local += 1
        self.copies.setdefault(name, []).append(lambda: pltpu.make_async_copy(src(), dst(), self.local.at[n]))

    def start(self, *names):
        for name in names:
            for make in self.copies[name]:
                make().start()

    def got(self, *names):
        for name in names:
            with jax.named_scope('got_' + name):
                for make in self.copies[name]:
                    make().wait_recv()

    def sent(self, *names):
        for name in names:
            for make in self.copies[name]:
                make().wait_send()

    def done(self, *names):
        for name in names:
            with jax.named_scope('done_' + name):
                for make in self.copies[name]:
                    make().wait()

    def gather(self, name, own, buf):
        for stage, chip in (('p', PAIR), ('c', CROSS)):
            self.add(name + stage, lambda: own, lambda c=chip: buf.at[2 * c], chip)
        self.add(name + 'm', lambda: own, lambda: buf.at[1], 0, 1)
        for stage, chip in (('f', PAIR), ('g', CROSS)):
            self.add(name + stage, lambda c=chip: buf.at[2 * c], lambda c=chip: buf.at[2 * c + 1], 0, 1)

    def gather_far(self, name, src, here, other, via):
        self.add(name + 'r', src, here, via)
        self.add(name + 'l', here, other, 0, 1)

    def exchange(self, name, src, dst, rows):
        me = lax.axis_index('tp')
        for core in BOTH:
            for chip in (PAIR, CROSS, FAR, 0):
                if chip + core:
                    self.add(name, lambda c=chip, k=core: src.at[span(self.peer(c, k), rows)], lambda: dst.at[span(me, rows)], chip, core)
        self.add_local(name + '_own', lambda: src.at[span(me, rows)], lambda: dst.at[span(me, rows)])

    def multicast(self, name, src, dst, pair_dst, rows):
        me = lax.axis_index('tp')
        at = lambda buf: (lambda: buf.at[span(me, rows)])
        other = {0: PAIR, PAIR: 0, CROSS: FAR}
        for chip, stage in ((CROSS, '_cross'), (PAIR, '_pair'), (0, '_pair')):
            for core in BOTH:
                if chip + core:
                    for c, buf in ((chip, dst), (other[chip], pair_dst)):
                        self.add(name + stage, lambda c=c, k=core: src.at[span(self.peer(c, k), rows)], at(buf), chip, core)
        for c, buf in ((0, dst), (PAIR, pair_dst)):
            self.add_local(name + '_own', lambda c=c: src.at[span(self.peer(c), rows)], at(buf))
        came = lambda buf: (lambda: buf.at[span(lax.div(self.peer(CROSS), 2), 2 * rows)])
        self.add(name + '_fwd', came(dst), came(pair_dst), PAIR)
        self.add(name + '_fwd', came(pair_dst), came(dst), PAIR)


def solution(mesh):
    n_tp = mesh.shape['tp']
    n_chips = n_tp // 2
    act_spec = P('dp', 'tp', None)
    rep_vec = P(None)
    part_vec = P('dp')
    in_specs = (act_spec, act_spec, P('dp', None), rep_vec, rep_vec, P(None, None, 'tp', None), P(None, 'tp', None),
                P('tp', None, None), rep_vec, rep_vec, rep_vec, P(None, 'tp'), P('tp'), P('tp', None), rep_vec)
    out_specs = (act_spec, act_spec, part_vec, part_vec, P('dp', None, 'tp', None), P('dp', 'tp', None),
                 P(('dp', 'tp'), None, None), part_vec, part_vec, part_vec, P('dp', 'tp'), P(('dp', 'tp')),
                 P(('dp', 'tp'), None), part_vec)

    def device_step(x_in, grad_y, pad_mask, ln1_gain, ln1_bias, w_qkv, b_qkv, w_out, b_out, ln2_gain, ln2_bias, w_up, b_up, w_down, b_down):
        batch, p_len, dim = x_in.shape
        seq = pad_mask.shape[1]
        _, _, heads, hd = w_qkv.shape
        seqs = batch // n_tp
        ffn = w_up.shape[1]
        width = heads * hd
        n3 = 3 * width
        tok = seqs * seq
        chunk = seqs * p_len
        qc = seq // 2
        q_scale = hd ** -0.5
        sds = jax.ShapeDtypeStruct
        n_tile = n3 + width
        half = dim // 2
        twice = n_tp + n_tp
        quarter = ffn // 2

        def kernel(*refs):
            it = iter(refs)
            take = lambda n: [next(it) for _ in range(n)]
            (x_ref, dy_ref, wq_ref, bq_ref, wo_ref, wu_ref, bu_ref, wd_ref), plain = take(8), take(8)
            y_out, gx_out, g_up, g_down, g_q, g_o, g_vec, g_b, wq, wu, wd, q_hbm, k_hbm, v_hbm, act_hbm, slope_hbm = take(16)
            p_at, got_at, sum_at, early_at, last_at, x_dn, x_up, p_dn, p_up, r_dn, r_up = take(11)
            x, h1, dy, x1, h2, dx1b, h2p, dyp, y, o4, do4, wo, acc, acc2, p_rcv, p_snd, d4 = take(17)
            dq_acc, dk_acc, dv_acc, cos_t, sin_t, ok, m_st, l_st, b_att, b_ffn, u_all, gb, b_all, b8, late, late_in, vec, v_in, v_own = take(19)
            dpre = next(it)
            act_p, dpre_p = (y.at[:, pl.ds(i * ffn, ffn)] for i in BOTH)
            here = take(8)
            send, recv, local, pair_send, pair_recv, pair_ready = take(6)
            net = Net(n_tp, send, recv, local)
            me = lax.axis_index('tp')
            mask_ref, gain1, bias1, bias_o, gain2, bias_d, bias2, freq_ref = here

            net.gather('q', wq_ref, wq)
            net.gather('o', wo_ref, wo)
            net.gather('u', wu_ref, wu)
            net.gather('d', wd_ref, wd)
            for name, buf in (('q', wq), ('o', wo), ('u', wu)):
                net.gather_far(name, lambda b=buf: b.at[2 * PAIR], lambda b=buf: b.at[FAR0], lambda b=buf: b.at[FAR1], CROSS)
            for i in BOTH:
                mine = lambda core, i=i: dx1b.at[pl.ds(core * ffn + i * quarter, quarter)]
                net.gather_far(f'd{i}', lambda i=i: wd.at[2 * CROSS, pl.ds(i * quarter, quarter)], lambda m=mine: m(0), lambda m=mine: m(1), PAIR)
            net.exchange('x', x_ref, x, chunk)
            net.multicast('dy', dy_ref, dy, dyp, chunk)
            net.exchange('y', y, y_out, chunk)
            net.exchange('gx', h1, gx_out, chunk)
            for chip in range(n_chips):
                for core in BOTH:
                    if chip + core:
                        slot = 2 * chip + core
                        net.add('bias', lambda: bq_ref, lambda n=slot: b_all.at[n], chip, core)
                        net.add('bias', lambda: bu_ref, lambda n=slot: u_all.at[n], chip, core)
                        net.add('late', lambda n=slot: late.at[n], lambda n=slot: late_in.at[n], chip, core)
                        net.add('early', lambda: v_own.at[pl.ds(twice, 2 * twice)], lambda n=slot: v_in.at[n], chip, core)
            for i in BOTH:
                net.add(f'h{i}', lambda p=pl.ds(i * half, half): h2.at[p], lambda p=pl.ds(i * half, half): h2p.at[p], PAIR)
            net.add('dn_x', lambda: x_dn, lambda: r_dn, CROSS)
            net.add('up_x', lambda: x_up, lambda: r_up, CROSS)
            net.add('at_early', lambda: p_at.at[PAIR], lambda: early_at, PAIR)
            t_half = n_tile // 2
            for i, part in enumerate((pl.ds(0, t_half), pl.ds(t_half, t_half))):
                net.add(f'at_relay{i}', lambda p=part: p_at.at[FAR, p], lambda p=part: got_at.at[p], PAIR)
                net.add(f'at_sum{i}', lambda p=part: sum_at.at[p], lambda p=part: last_at.at[p], CROSS)
                net.add_local(f'at{i}_load', lambda p=part: got_at.at[p], lambda p=part: p_rcv.at[0, p])
                net.add_local(f'at{i}_load', lambda p=part: p_at.at[CROSS, p], lambda p=part: p_rcv.at[1, p])
                net.add_local(f'at{i}_store', lambda p=part: p_rcv.at[1, p], lambda p=part: sum_at.at[p])
            for src, dst in zip(plain, here):
                net.add_local('own', lambda r=src: r, lambda r=dst: r)
            net.add_local('write', lambda: v_own, lambda: g_vec)
            net.add_local('write', lambda: b8.at[0], lambda: g_b)
            for ref, tmp, buf in ((wq_ref, lambda: h2.at[pl.ds(0, n3)], wq), (wu_ref, lambda: x1.at[:, pl.ds(0, ffn)], wu),
                                        (wd_ref, lambda: dx1b.at[pl.ds(0, ffn)], wd)):
                net.add_local('load', lambda r=ref: r, tmp)
                net.add_local('store', tmp, lambda b=buf: b.at[0])
            net.add_local('own', lambda: wo_ref, lambda: wo.at[0])
            net.add_local('own', lambda: bq_ref, lambda: b_all.at[0])
            net.add_local('own', lambda: bu_ref, lambda: u_all.at[0])
            def pass_on(i, stage):
                if stage == 0:
                    net.got(f'at_relay{i}')
                    net.start(f'at{i}_load')
                elif stage == 1:
                    net.done(f'at{i}_load')

                    def body(rows):
                        rows = pl.ds(i * t_half + rows.start, rows.size)
                        p_rcv[1, rows] += p_rcv[0, rows]

                    loop_rows(t_half, 8, body)
                    net.start(f'at{i}_store')
                else:
                    net.done(f'at{i}_store')
                    net.start(f'at_sum{i}')

            def pack(lo, hi):
                for r in range(lo, hi):
                    fold(vec[pl.ds(r, 1), :], v_own, r * n_tp)

            def hooks(step, table):
                for at, act in table.items():
                    @pl.when(step == at)
                    def _(act=act):
                        act()

            tile_order = (FAR, PAIR, CROSS, 0)

            def place(i):
                return jnp.where(i == 0, FAR, jnp.where(i == 1, PAIR, jnp.where(i == 2, CROSS, 0)))

            def order(s):
                return 2 * place(lax.div(s, 2)) + 1 - lax.rem(s, 2)

            def to_partner(src, dst, sem):
                return pltpu.make_async_remote_copy(
                    src_ref=p_snd.at[src], dst_ref=p_rcv.at[dst], send_sem=pair_send.at[sem], recv_sem=pair_recv.at[sem],
                    device_id={'tp': net.peer(0, 1)}, device_id_type=pl.DeviceIdType.MESH)

            def keep(i, to):
                return pltpu.make_async_copy(p_rcv.at[i], to, pair_send.at[twice + i])

            def into(i):
                return lambda at, v: p_snd.__setitem__((i,) + at, v)

            def add_sent(i, j):
                def body(rows):
                    p_rcv[j, rows] += p_snd[i, rows]

                loop_rows(n_tile, 16, body)

            def pair_go(s):
                @pl.when(lax.rem(s, 2) == 1)
                def _():
                    to_partner(0, lax.div(s, 2), lax.div(s, 2)).start()

            def pair(s, tile):
                j = lax.div(s, 2)
                odd = lax.rem(s, 2)
                tile(into(odd))

                @pl.when(odd == 1)
                def _():
                    copy = to_partner(0, j, j)
                    copy.wait_send()
                    copy.wait_recv()
                    add_sent(1, j)
                    keep(j, p_at.at[place(j)]).start()

            def stored(i):
                keep(i, p_at.at[tile_order[i]]).wait()

            def pair_begin():
                pl.semaphore_signal(pair_ready, inc=1, device_id={'tp': net.peer(0, 1)}, device_id_type=pl.DeviceIdType.MESH)
                pl.semaphore_wait(pair_ready, 1)

            barrier = pltpu.get_barrier_semaphore()
            for chip in range(n_chips):
                for core in BOTH:
                    if chip + core:
                        pl.semaphore_signal(barrier, inc=1, device_id={'tp': net.peer(chip, core)}, device_id_type=pl.DeviceIdType.MESH)
            pl.semaphore_wait(barrier, n_tp - 1)
            net.start('qp', 'qc', 'x', 'qm', 'bias', 'own', 'load', 'x_own', 'dy_own')
            net.done('own')
            angle = lax.broadcasted_iota(jnp.int32, (seq, width), 0).astype(F32) * freq_ref[0:1, :]
            cos_t[...] = jnp.cos(angle)
            sin_t[...] = jnp.sin(angle) * freq_ref[1:2, :]
            for b in range(seqs):
                row = mask_ref[pl.ds(me * seqs + b, 1), :].astype(F32)
                ok[b] = jnp.broadcast_to(row, (LANES, seq)).T
            net.done('load')
            net.start('store')
            net.got('qp', 'qc')
            net.start('qr', 'dy_cross', 'oc', 'op', 'up', 'dy_pair', 'qf', 'qg', 'om')
            net.done('x_own', 'dy_own')
            net.got('bias')
            for n in range(n_tp):
                b = b_all[n]
                b_att[n] = jnp.concatenate([b[i // heads, i % heads:i % heads + 1, :] for i in range(3 * heads)], axis=1)
                b_ffn[n] = u_all[n]
            net.got('x')

            def ln1(rows):
                x_hat, _ = ln_stats(x[rows, :].astype(F32))
                h1[rows, :] = (x_hat * gain1[...] + bias1[...]).astype(BF16)

            loop_rows(tok, chunk, ln1)
            net.done('store')
            net.got('qm', 'qf', 'qg')

            def arrival(s):
                return s + 2 * lax.div(s, n_chips) - n_chips * lax.div(s, n_chips + 2)

            def qkv_step(ps, w, q_ref, k_ref, v_ref):
                s = ps.index[0]
                hooks(s, {2: lambda: (net.got('op'), net.start('or', 'uc', 'um', 'of')), 4: lambda: (net.got('qr'), net.start('ql')),
                          5: lambda: net.got('ql')})
                n_src = tok // chunk // 2

                @pl.loop(0, 2)
                def _(i):
                    rows = span(i, tok // 2)
                    t = mm(h1[rows, :], w[0], NT) + b_att[arrival(s)]
                    cos, sin = (t_ref[span(i, seq // 2), :].reshape(n_src, 1, p_len, width) for t_ref in (cos_t, sin_t))

                    def rope(v):
                        out = v.reshape(n_src, seqs, p_len, width) * cos + swap_halves(v, hd).reshape(n_src, seqs, p_len, width) * sin
                        return out.astype(BF16)

                    src = span(i, n_src)
                    q_ref[0, src] = rope(t[:, :width] * q_scale)
                    k_ref[0, src] = rope(t[:, width:2 * width])
                    v_ref[0, src] = t[:, 2 * width:].reshape(n_src, seqs, p_len, width).astype(BF16)

            slot3 = lambda rows, cols, f=lambda s: s: pl.BlockSpec((1, rows, cols), lambda s: (f(s), 0, 0))

            def pipe(body, **specs):
                def run(*refs):
                    with jax.named_scope(body.__name__):
                        pltpu.emit_pipeline(body, _explicit_indices=True, **specs)(*refs)

                return run

            pipe(qkv_step, grid=(n_tp,), in_specs=[slot3(n3, dim, arrival)],
                 out_specs=[pl.BlockSpec((1, n_tp, seqs, p_len, width), lambda s: (arrival(s), 0, 0, 0, 0))] * 3)(
                wq, q_hbm, k_hbm, v_hbm)

            srcs = qc // p_len
            lane = lax.broadcasted_iota(jnp.int32, (qc, width), 1)

            def attn_step(ps, q_ref, k_ref, v_ref):
                g, b = ps.index
                hooks(g * seqs + b, {
                    8: lambda: (net.got('dy_cross'), net.start('dy_fwd')), 9: lambda: (net.got('up'), net.start('ur', 'dc', 'dm', 'uf')),
                    14: lambda: (net.got('oc', 'or'), net.start('og', 'ol'))})
                bad = ok[b][:, 0:1] <= 0
                k = k_ref[0, :, 0].reshape(seq, width)
                v_t = v_ref[0, :, 0].reshape(seq, width).T
                for c in range(seq // qc):
                    src = slice(c * srcs, (c + 1) * srcs)
                    cols = slice(c * qc, (c + 1) * qc)
                    q = q_ref[0, src, 0].reshape(qc, width)
                    outs = []
                    for h in range(heads):
                        s = jnp.where(bad, NEG_LARGE, mm(k, jnp.where(lane // hd == h, q, jnp.zeros_like(q)), NT))
                        m = jnp.max(s, axis=0, keepdims=True)
                        e = jnp.exp(s - m)
                        r = 1.0 / col_sum(e)
                        outs.append(mm(v_t[h * hd:(h + 1) * hd], (e * r).astype(BF16), NN))
                        m_st[g, b, h:h + 1, cols] = m
                        l_st[g, b, h:h + 1, cols] = r
                    o4[src, b, :, span(g, width)] = jnp.concatenate(outs, axis=0).T.astype(BF16).reshape(srcs, p_len, width)

            head_blk = pl.BlockSpec((1, n_tp, 1, p_len, width), lambda g, b: (g, 0, b, 0, 0))
            pipe(attn_step, grid=(n_tp, seqs), in_specs=[head_blk] * 3)(q_hbm, k_hbm, v_hbm)

            net.got('om', 'of', 'og', 'ol')

            @pl.loop(0, tok // (2 * chunk))
            def _(i):
                rows = span(i, 2 * chunk)
                o = o4[pl.ds(2 * i, 2)].reshape(2 * chunk, n_tp * width)
                low = (x[rows, :].astype(F32) + (mm(o, wo[...].reshape(n_tp * width, dim), NN) + bias_o[...])).astype(BF16)
                x1[rows, :] = low
                x_hat, _ = ln_stats(low.astype(F32))
                h2[rows, :] = (x_hat * gain2[...] + bias2[...]).astype(BF16)

            net.start('h0', 'h1', 'dp')

            def gelu(pre):
                erf_term = lax.erf(pre * INV_SQRT2)
                act = (0.5 * pre * (1.0 + erf_term)).astype(BF16)
                return act, 0.5 * (1.0 + erf_term) + pre * jnp.exp(-0.5 * pre * pre) * INV_SQRT_2PI

            cols = lambda f: pl.BlockSpec((tok, ffn), lambda s: (0, f(s)))
            wu_spec, wd_spec = functools.partial(slot3, dim, ffn), functools.partial(slot3, ffn, dim)

            def mlp_up(n, f, table):
                def up_step(ps, w, act_ref, slope_ref):
                    s = ps.index[0]
                    hooks(s, table)

                    def body(rows):
                        act_ref[rows, :], slope_ref[rows, :] = gelu(mm(h2[rows, :], w[0], NN) + b_ffn[f(s)])

                    loop_rows(tok, half, body)

                pipe(up_step, grid=(n,), in_specs=[wu_spec(f)], out_specs=[cols(f)] * 2)(wu, act_hbm, slope_hbm)

            net.got('um', 'uf')
            mlp_up(n_tp - 2, arrival, {2: lambda: (net.got('uc'), net.start('ug')), 3: lambda: net.got('ug')})
            net.got('dy_pair', 'dy_fwd', 'dm')

            def backward(slot, w_d, w_u, act_ref, slope_ref, add):
                if add:
                    gb[slot] = jnp.zeros_like(gb[0])

                def body(rows):
                    d_pre = mm(dy[rows, :], w_d, NT) * slope_ref[rows, :]
                    low = d_pre.astype(BF16)
                    dpre[rows, :] = low
                    if add:
                        gb[slot] += col_sum(d_pre)
                        acc[rows, :] += mm(act_ref[rows, :], w_d, NN)
                        acc2[rows, :] += mm(low, w_u, NT)

                loop_rows(tok, half, body)

            def pair_gelu(rows, w_u, slot):
                return gelu(mm(h2p[rows, :], w_u, NN) + b_ffn[slot])

            def grads(chip, at, x_ref, between):
                f = lambda s: 2 * chip + 1 - s
                copy = to_partner(0, at, n_tp + at)

                def first(ps, w_u, act_ref):
                    s = ps.index[0]
                    rows = pl.ds(0, half)
                    act_p[rows, :] = pair_gelu(rows, w_u[0], f(s))[0]
                    p_snd[s] = mm(act_ref[...], dy[...], TN) + mm(act_p[rows, :], dyp[rows, :], TN)

                def second(ps, w_u):
                    s = ps.index[0]
                    pl.when(s == 1)(lambda: copy.start())
                    rows = pl.ds(half, half)
                    act_p[rows, :] = pair_gelu(rows, w_u[0], f(s))[0]
                    p_snd[s] += mm(act_p[rows, :], dyp[rows, :], TN)

                    @pl.when(s == 1)
                    def _():
                        copy.wait_recv()
                        add_sent(1, at)
                        keep(at, x_ref).start()
                        copy.wait_send()

                pipe(first, grid=(len(BOTH),), in_specs=[wu_spec(f), cols(f)])(wu, act_hbm)
                between()
                pipe(second, grid=(len(BOTH),), in_specs=[wu_spec(f)])(wu)
                keep(at, x_ref).wait()

            def mlp(n, f, add, table, last=None):
                def mlp_step(ps, wd_s, wu_s, act_ref, slope_ref):
                    s = ps.index[0]
                    backward(f(s), wd_s[0], wu_s[0], act_ref, slope_ref, add)
                    if last:
                        at, ref, send = last
                        copy = to_partner(0, at + 1, n_tp + at + 1)
                        pl.when(s == 1)(lambda: copy.start())

                        @pl.when(s < 2)
                        def _():
                            def body(rows):
                                dpre_p[rows, :] = (mm(dyp[rows, :], wd_s[0], NT) * pair_gelu(rows, wu_s[0], f(s))[1]).astype(BF16)

                            loop_rows(tok, half, body)
                            for i in BOTH:
                                part = pl.ds(i * half, half)
                                p_snd[s, pl.ds(0, ffn), part] = mm(h2[:, part], dpre[...], TN) + mm(h2p[:, part], dpre_p[...], TN)

                        @pl.when(s == 1)
                        def _():
                            copy.wait_recv()
                            add_sent(1, at + 1)
                            keep(at + 1, ref).start()
                            copy.wait_send()

                    hooks(s, table)

                pipe(mlp_step, grid=(n,), in_specs=[wd_spec(f), wu_spec(f), cols(f), cols(f)])(wd, wu, act_hbm, slope_hbm)

            acc[...] = jnp.zeros_like(acc)
            acc2[...] = jnp.zeros_like(acc2)
            mlp(2, lambda s: s, True, {})
            net.got('ur')
            net.start('ul')
            net.got('ul')
            mlp_up(2, lambda s: s + FAR0, {})
            net.got('h0')
            grads(CROSS, 0, x_dn, lambda: (net.got('dc'), net.start('dg', 'd0r', 'd1r'), net.got('h1')))
            net.start('dn_x')
            net.got('dg')

            def sent_up():
                keep(1, x_up).wait()
                net.start('up_x')

            slots = lambda s: jnp.where(s < 2, 2 * CROSS + 1 - s, s)
            mlp(n_chips, slots, True, {0: lambda: (net.got('dp'), net.start('df')), 1: lambda: net.got('df'), 2: sent_up}, (0, x_up, 'up_x'))

            for slot in (FAR0, FAR1):
                gb[slot] = jnp.zeros_like(gb[slot])

            def far_step(ps, w_u, act_ref, slope_ref):
                part, core = ps.index
                hooks(2 * part + core, {0: lambda: (net.got('d0r'), net.start('d0l')), 1: lambda: net.got('d0l'),
                                        2: lambda: (net.got('d1r'), net.start('d1l')), 3: lambda: net.got('d1l')})
                w_d = dx1b[pl.ds(pl.multiple_of(core * ffn + part * quarter, quarter), quarter), :]

                def body(rows):
                    d_pre = mm(dy[rows, :], w_d, NT) * slope_ref[rows, :]
                    gb[FAR0 + core, :, span(part, quarter)] += col_sum(d_pre)
                    acc[rows, :] += mm(act_ref[rows, :], w_d, NN)
                    acc2[rows, :] += mm(d_pre.astype(BF16), w_u[0], NT)

                loop_rows(tok, half, body)

            narrow = pl.BlockSpec((tok, quarter), lambda part, core: (0, 2 * (FAR0 + core) + part))
            pipe(far_step, grid=(len(BOTH),) * len(BOTH), in_specs=[pl.BlockSpec((1, dim, quarter), lambda part, core: (FAR0 + core, 0, part)), narrow, narrow])(
                wu, act_hbm, slope_hbm)

            def y_rows(rows):
                y[rows, :] = (x1[rows, :].astype(F32) + (acc[rows, :] + bias_d[...])).astype(BF16)

            loop_rows(tok, 2 * chunk, y_rows)
            vec[...] = jnp.zeros_like(vec)
            net.start('y', 'y_own')
            net.sent('d0l', 'd1l')

            @pl.loop(0, tok // (2 * chunk))
            def _(i):
                rows = span(i, 2 * chunk)
                x1_f, dy_f, dh = x1[rows, :].astype(F32), dy[rows, :].astype(F32), acc2[rows, :]
                x_hat, inv_std = ln_stats(x1_f)
                d_x1 = dy_f + ln_grad(dh, x_hat, inv_std, gain2[...])
                acc2[rows, :] = d_x1
                low = d_x1.astype(BF16)
                dx1b[rows, :] = low
                d_o = mm(low, wo[...].reshape(n_tp * width, dim), NT).astype(BF16)
                do4[pl.ds(2 * i, 2)] = d_o.reshape(2, seqs, p_len, n_tp * width)
                for n, t in enumerate((d_x1, dh * x_hat, dh, dy_f)):
                    vec[2 + n:3 + n, :] += col_sum(t)

            pack(2, 6)
            pair_begin()

            def bwd_step(ps, q_ref, k_ref, v_ref, w):
                step = ps.index[0]
                g = order(step)
                hooks(step, {0: lambda: net.start('early'), 2: lambda: (stored(0), net.start('at_relay0', 'at_relay1')),
                             4: lambda: (stored(1), net.start('at_early')), 6: lambda: (stored(2), pass_on(0, 0)), 7: lambda: pass_on(0, 2)})
                pair_go(step)
                b8[g] = jnp.zeros_like(b8[0])
                fold(gb[g], b8.at[g], 3)
                for b in range(seqs):
                    bad = ok[b][:, 0:1] <= 0
                    k = k_ref[0, :, b].reshape(seq, width)
                    v = v_ref[0, :, b].reshape(seq, width)
                    k_t = k.T
                    for c in range(seq // qc):
                        src = slice(c * srcs, (c + 1) * srcs)
                        at = slice(c * qc, (c + 1) * qc)
                        q = q_ref[0, src, b].reshape(qc, width)
                        d_o = do4[src, b, :, span(g, width)].reshape(qc, width)
                        dk = jnp.zeros((seq, width), F32)
                        dv = jnp.zeros((seq, width), F32)
                        dqs = []
                        for h in range(heads):
                            mine = lane // hd == h
                            q_h = jnp.where(mine, q, jnp.zeros_like(q))
                            do_h = jnp.where(mine, d_o, jnp.zeros_like(d_o))
                            s = jnp.where(bad, NEG_LARGE, mm(k, q_h, NT))
                            p = jnp.exp(s - m_st[g, b, h:h + 1, at]) * l_st[g, b, h:h + 1, at]
                            dv += mm(p.astype(BF16), do_h, NN)
                            dp = mm(v, do_h, NT)
                            ds = (p * (dp - col_sum(dp * p))).astype(BF16)
                            dk += mm(ds, q_h, NN)
                            dqs.append(mm(k_t[h * hd:(h + 1) * hd], ds, NN))
                        dq_acc[at, :] = jnp.concatenate(dqs, axis=0).T
                        dk_acc[...] = dk if c == 0 else dk_acc[...] + dk
                        dv_acc[...] = dv if c == 0 else dv_acc[...] + dv
                    cos, sin = cos_t[...], sin_t[...]
                    dq, dk, dv = dq_acc[...], dk_acc[...], dv_acc[...]
                    dq = (dq * cos - swap_halves(dq, hd) * sin) * q_scale
                    dk = dk * cos - swap_halves(dk, hd) * sin
                    for i, t in enumerate((dq, dk, dv)):
                        d4[:, b, :, i * width:(i + 1) * width] = t.astype(BF16).reshape(n_tp, p_len, width)
                        b8[g, i:i + 1, :] += col_sum(t)

                @pl.when(step == 0)
                def _():
                    acc[...] = jnp.zeros_like(acc)

                @pl.loop(0, 2)
                def _(i):
                    acc[span(i, half), :] += mm(d4[pl.ds(n_chips * i, n_chips)].reshape(half, n3), w[0], NN)

                def tile(put):
                    put((pl.ds(0, n3),), mm(d4[...].reshape(tok, n3), h1[...], TN))
                    put((pl.ds(n3, width),), mm(o4[:, :, :, span(g, width)].reshape(tok, width), dx1b[...], TN))

                pair(step, tile)
                hooks(step, {6: lambda: pass_on(0, 1)})

            slot_blk = pl.BlockSpec((1, n_tp, seqs, p_len, width), lambda s: (order(s), 0, 0, 0, 0))
            pipe(bwd_step, grid=(n_tp,), in_specs=[slot_blk] * 3 + [slot3(n3, dim, order)])(
                q_hbm, k_hbm, v_hbm, wq)

            pass_on(1, 0)

            def ln1_bwd(rows):
                x_hat, inv_std = ln_stats(x[rows, :].astype(F32))
                dh = acc[rows, :]
                h1[rows, :] = (acc2[rows, :] + ln_grad(dh, x_hat, inv_std, gain1[...])).astype(BF16)
                vec[0:1, :] += col_sum(dh * x_hat)
                vec[1:2, :] += col_sum(dh)

            loop_rows(tok, 2 * chunk, ln1_bwd)
            stored(3)
            pack(0, 2)
            pass_on(1, 1)
            for n in range(1, n_tp):
                late[n, 0:8] = b8[n]
                late[n, 8:] = v_own[0:twice]
            net.start('late')
            pass_on(1, 2)
            net.start('gx', 'gx_own')

            net.sent('y')
            net.done('y_own')
            pair_begin()
            grads(0, 2, p_dn, lambda: None)
            mlp(2, lambda s: 1 - s, False, {}, (2, p_up, None))
            keep(3, p_up).wait()

            def total(refs, out, block, at):
                def body(*blocks):
                    v = blocks[1][...]
                    for more in blocks[2:-1]:
                        v += more[...]
                    blocks[-1][...] = v

                pipe(body, grid=(len(BOTH),), in_specs=[pl.BlockSpec(block, at)] * len(refs),
                     out_specs=[pl.BlockSpec(block, lambda i: (i, 0))])(*refs, out)

            by_row, by_col = lambda i: (i, 0), lambda i: (0, i)
            net.got('late', 'early')
            b_total, v_late, v_early = b8[0], v_own[0:twice], v_own[twice:]
            for n in range(1, n_tp):
                b_total += late_in[n, 0:8]
                v_late += late_in[n, 8:]
                v_early += v_in[n]
            net.got('dn_x', 'up_x')
            total((p_dn, r_dn), g_down, (t_half, dim), by_row)
            total((p_up, r_up), g_up, (n_tile, half), by_col)
            net.got('at_early', 'at_sum0', 'at_sum1')
            for rows, out, n in ((pl.ds(0, n3), g_q, n3), (pl.ds(n3, width), g_o, width)):
                total((p_at.at[0, rows], early_at.at[rows], last_at.at[rows]), out, (n // 2, dim), by_row)
            for name in net.copies:
                if name not in ('load', 'store', 'own', 'write', 'gx', 'y', 'd0l', 'd1l') and not name.endswith(('_own', '_load', '_store')):
                    net.sent(name)
            b8[0] = b_total
            v_own[0:twice] = v_late
            v_own[twice:] = v_early
            net.got('y')
            net.start('write')
            net.done('gx_own', 'write')
            net.got('gx')
            net.sent('gx')

        big = (tok, dim)
        shapes = lambda *dims, dtype=F32: sds(dims, dtype)
        flat = lambda t: t.reshape(tok, dim)
        inv_freq = ROPE_BASE ** (-2.0 * np.arange(hd // 2) / hd)
        sign = np.repeat([-1.0, 1.0], hd // 2)
        freq = np.stack([np.tile(inv_freq, 2 * heads), np.tile(sign, heads)]).astype(np.float32)
        line = lambda v: v.reshape(1, -1)
        sem = lambda n: pltpu.SemaphoreType.DMA((n,))
        low = functools.partial(shapes, dtype=BF16)
        weights = [low(n_tp, n3, dim), low(n_tp, dim, ffn), low(n_tp, ffn, dim)]
        tiles = [shapes(n_chips, n_tile, dim)] + [shapes(n_tile, dim)] * 10
        out_shape = ([low(*big)] * 2 + [shapes(dim, ffn), shapes(ffn, dim), shapes(n3, dim), shapes(width, dim), shapes(6 * n_tp, LANES), shapes(8, LANES)] + weights
                     + [low(n_tp, n_tp, seqs, p_len, width)] * 3 + [low(tok, n_tp * ffn), shapes(tok, n_tp * ffn)] + tiles)
        plain = [pad_mask] + [line(v) for v in (ln1_gain, ln1_bias, b_out, ln2_gain, b_down, ln2_bias)] + [freq]
        heads4 = low(n_tp, seqs, p_len, n_tp * width)
        stat = shapes(n_tp, seqs, heads, seq)
        tile8 = shapes(n_tp, 8, LANES)
        late = shapes(n_tp, 8 + twice, LANES)
        row_ffn = shapes(n_tp, 1, ffn)
        scratch = ([low(*big)] * 9 + [heads4, heads4, low(n_tp, width, dim)] + [shapes(*big)] * 2
                   + [shapes(n_chips, n_tile, dim), shapes(2, n_tile, dim), low(n_tp, seqs, p_len, n3)]
                   + [shapes(seq, width)] * 5 + [shapes(seqs, seq, LANES), stat, stat, shapes(n_tp, 1, n3), row_ffn, row_ffn, row_ffn]
                   + [shapes(n_tp, *b_qkv.shape), tile8, late, late, shapes(8, dim), shapes(n_tp, 2 * twice, LANES), shapes(6 * n_tp, LANES)]
                   + [low(tok, ffn)] + plain)
        outs = pl.pallas_call(
            kernel, name='layer', out_shape=out_shape, in_specs=[ANY] * 16, out_specs=[ANY] * len(out_shape),
            scratch_shapes=[pltpu.VMEM(v.shape, v.dtype) for v in scratch]
            + [sem(100), sem(100), sem(30), sem(20), sem(12), pltpu.SemaphoreType.REGULAR],
            compiler_params=pltpu.CompilerParams(collective_id=0, has_side_effects=True, vmem_limit_bytes=VMEM_LIMIT),
        )(flat(x_in), flat(grad_y), w_qkv.transpose(0, 2, 3, 1).reshape(n3, dim), b_qkv, w_out.reshape(width, dim),
          w_up, line(b_up), w_down, *plain)

        def finish(*refs):
            src, (v_ref, b_ref), out, (bq_o, bu_o), v_o = refs[:6], refs[6:8], refs[8:14], refs[14:16], refs[16:]
            for a, b in zip(src, out):
                b[...] = a[...]
            for i in range(3):
                for h in range(heads):
                    bq_o[i, h:h + 1, :] = b_ref[i:i + 1, h * hd:(h + 1) * hd]
            unfold(b_ref, 3, bu_o)
            for r, ref in enumerate(v_o):
                unfold(v_ref, r * n_tp, ref)

        large = [low(*big)] * 2 + [shapes(dim, ffn), shapes(ffn, dim), shapes(n3, dim), shapes(width, dim)]
        small = [shapes(*b_qkv.shape), shapes(1, ffn)] + [shapes(1, dim)] * 6
        moving = [pl.BlockSpec((v.shape[0] // n_chips, v.shape[1]), lambda i: (i, 0)) for v in large]
        fixed = lambda vs: [pl.BlockSpec(v.shape, lambda i, n=len(v.shape): (0,) * n) for v in vs]
        res = pl.pallas_call(
            finish, name='finish', out_shape=large + small, grid=(n_chips,), in_specs=moving + fixed(outs[6:8]),
            out_specs=moving + fixed(small), compiler_params=pltpu.CompilerParams(vmem_limit_bytes=VMEM_LIMIT),
        )(*outs[:8])
        y_out, grad_x, grad_w_up, grad_w_down, gq, go, grad_b_qkv, grad_b_up = res[:8]
        v = [t.reshape(dim) for t in res[8:]]
        return (y_out.reshape(x_in.shape), grad_x.reshape(x_in.shape), v[0], v[1], gq.reshape(3, heads, hd, dim).transpose(0, 3, 1, 2),
                grad_b_qkv, go.reshape(heads, hd, dim), v[2], v[3], v[4], grad_w_up, grad_b_up.reshape(ffn), grad_w_down, v[5])

    return jax.shard_map(device_step, mesh=mesh, in_specs=in_specs, out_specs=out_specs, check_vma=False)
```

```python
import functools

import jax
import jax.numpy as jnp
import numpy as np
from jax import lax
from jax.experimental import pallas as pl
from jax.experimental.pallas import tpu as pltpu
from jax.sharding import PartitionSpec as P

LN_EPS = 1e-5
ROPE_BASE = 10000.0
INV_SQRT2 = 0.7071067811865476
INV_SQRT_2PI = 0.3989422804014327
NEG_LARGE = -1e30
F32 = jnp.float32
BF16 = jnp.bfloat16
VMEM_LIMIT = 66_500_000
LANES = 128
NN = (((1,), (0,)), ((), ()))
NT = (((1,), (1,)), ((), ()))
TN = (((0,), (0,)), ((), ()))
PAIR, FAR, CROSS = 1, 2, 3
FAR0 = FAR + FAR
FAR1 = FAR0 + 1
BOTH = range(2)
ANY = pl.BlockSpec(memory_space=pl.ANY)


def mm(a, b, dims):
    return lax.dot_general(a, b, dims, preferred_element_type=F32)


def ln_stats(v):
    centered = v - jnp.mean(v, axis=-1, keepdims=True)
    inv_std = lax.rsqrt(jnp.mean(centered * centered, axis=-1, keepdims=True) + LN_EPS)
    return centered * inv_std, inv_std


def ln_grad(d_out, x_hat, inv_std, gain):
    d_hat = d_out * gain
    return inv_std * (d_hat - jnp.mean(d_hat, axis=-1, keepdims=True) - x_hat * jnp.mean(d_hat * x_hat, axis=-1, keepdims=True))


def col_sum(t):
    return jnp.sum(t, axis=0, keepdims=True)


def swap_halves(t, head_dim):
    half = head_dim // 2
    lane = lax.broadcasted_iota(jnp.int32, t.shape, t.ndim - 1)
    return jnp.where(lane % head_dim < half, pltpu.roll(t, t.shape[-1] - half, t.ndim - 1), pltpu.roll(t, half, t.ndim - 1))


def span(i, n):
    return pl.ds(pl.multiple_of(i * n, n), n)


def fold(row, out, first):
    for i in range(row.shape[-1] // LANES):
        out[pl.ds(first + i, 1), :] = row[:, i * LANES:(i + 1) * LANES]


def unfold(src, first, out):
    for i in range(out.shape[-1] // LANES):
        out[:, pl.ds(i * LANES, LANES)] = src[pl.ds(first + i, 1), :]


def loop_rows(total, n, body):
    @pl.loop(0, total // n)
    def _(i):
        body(span(i, n))


class Net:
    def __init__(self, n_tp, send, recv, local):
        self.n_tp, self.send, self.recv, self.local = n_tp, send, recv, local
        self.copies, self.count, self.n_local = {}, 0, 0

    def peer(self, chip, core=0):
        me = lax.axis_index('tp')
        way = 1 - 2 * lax.rem(lax.div(me, 2), 2)
        at = lax.rem(me + 2 * chip * way + self.n_tp, self.n_tp) if chip else me
        return at + 1 - 2 * lax.rem(at, 2) if core else at

    def add(self, name, src, dst, chip, core=0):
        n = self.count
        self.count += 1

        def make():
            return pltpu.make_async_remote_copy(
                src_ref=src(), dst_ref=dst(), send_sem=self.send.at[n], recv_sem=self.recv.at[n],
                device_id={'tp': self.peer(chip, core)}, device_id_type=pl.DeviceIdType.MESH)

        self.copies.setdefault(name, []).append(make)

    def add_local(self, name, src, dst):
        n = self.n_local
        self.n_local += 1
        self.copies.setdefault(name, []).append(lambda: pltpu.make_async_copy(src(), dst(), self.local.at[n]))

    def start(self, *names):
        for name in names:
            for make in self.copies[name]:
                make().start()

    def got(self, *names):
        for name in names:
            with jax.named_scope('got_' + name):
                for make in self.copies[name]:
                    make().wait_recv()

    def sent(self, *names):
        for name in names:
            for make in self.copies[name]:
                make().wait_send()

    def done(self, *names):
        for name in names:
            with jax.named_scope('done_' + name):
                for make in self.copies[name]:
                    make().wait()

    def gather(self, name, own, buf):
        for stage, chip in (('p', PAIR), ('c', CROSS)):
            self.add(name + stage, lambda: own, lambda c=chip: buf.at[2 * c], chip)
        self.add(name + 'm', lambda: own, lambda: buf.at[1], 0, 1)
        for stage, chip in (('f', PAIR), ('g', CROSS)):
            self.add(name + stage, lambda c=chip: buf.at[2 * c], lambda c=chip: buf.at[2 * c + 1], 0, 1)

    def gather_far(self, name, src, here, other, via):
        self.add(name + 'r', src, here, via)
        self.add(name + 'l', here, other, 0, 1)

    def exchange(self, name, src, dst, rows):
        me = lax.axis_index('tp')
        for core in BOTH:
            for chip in (PAIR, CROSS, FAR, 0):
                if chip + core:
                    self.add(name, lambda c=chip, k=core: src.at[span(self.peer(c, k), rows)], lambda: dst.at[span(me, rows)], chip, core)
        self.add_local(name + '_own', lambda: src.at[span(me, rows)], lambda: dst.at[span(me, rows)])

    def multicast(self, name, src, dst, pair_dst, rows):
        me = lax.axis_index('tp')
        at = lambda buf: (lambda: buf.at[span(me, rows)])
        other = {0: PAIR, PAIR: 0, CROSS: FAR}
        for chip, stage in ((CROSS, '_cross'), (PAIR, '_pair'), (0, '_pair')):
            for core in BOTH:
                if chip + core:
                    for c, buf in ((chip, dst), (other[chip], pair_dst)):
                        self.add(name + stage, lambda c=c, k=core: src.at[span(self.peer(c, k), rows)], at(buf), chip, core)
        for c, buf in ((0, dst), (PAIR, pair_dst)):
            self.add_local(name + '_own', lambda c=c: src.at[span(self.peer(c), rows)], at(buf))
        came = lambda buf: (lambda: buf.at[span(lax.div(self.peer(CROSS), 2), 2 * rows)])
        self.add(name + '_fwd', came(dst), came(pair_dst), PAIR)
        self.add(name + '_fwd', came(pair_dst), came(dst), PAIR)


def solution(mesh):
    n_tp = mesh.shape['tp']
    n_chips = n_tp // 2
    act_spec = P('dp', 'tp', None)
    rep_vec = P(None)
    part_vec = P('dp')
    in_specs = (act_spec, act_spec, P('dp', None), rep_vec, rep_vec, P(None, None, 'tp', None), P(None, 'tp', None),
                P('tp', None, None), rep_vec, rep_vec, rep_vec, P(None, 'tp'), P('tp'), P('tp', None), rep_vec)
    out_specs = (act_spec, act_spec, part_vec, part_vec, P('dp', None, 'tp', None), P('dp', 'tp', None),
                 P(('dp', 'tp'), None, None), part_vec, part_vec, part_vec, P('dp', 'tp'), P(('dp', 'tp')),
                 P(('dp', 'tp'), None), part_vec)

    def device_step(x_in, grad_y, pad_mask, ln1_gain, ln1_bias, w_qkv, b_qkv, w_out, b_out, ln2_gain, ln2_bias, w_up, b_up, w_down, b_down):
        batch, p_len, dim = x_in.shape
        seq = pad_mask.shape[1]
        _, _, heads, hd = w_qkv.shape
        seqs = batch // n_tp
        ffn = w_up.shape[1]
        width = heads * hd
        n3 = 3 * width
        tok = seqs * seq
        chunk = seqs * p_len
        qc = seq // 2
        q_scale = hd ** -0.5
        sds = jax.ShapeDtypeStruct
        n_tile = n3 + width
        half = dim // 2
        twice = n_tp + n_tp
        quarter = ffn // 2
        v_half = 3 * n_tp

        def kernel(*refs):
            it = iter(refs)
            take = lambda n: [next(it) for _ in range(n)]
            (x_ref, dy_ref, wq_ref, bq_ref, wo_ref, wu_ref, bu_ref, wd_ref), plain = take(8), take(8)
            y_out, gx_out, g_up, g_down, g_q, g_o, g_vec, g_b, wq, wu, wd, q_hbm, k_hbm, v_hbm, act_hbm, slope_hbm = take(16)
            p_at, got_at, sum_at, early_at, last_at, x_dn, x_up, p_dn, p_up, r_dn, r_up = take(11)
            x, h1, dy, x1, h2, dx1b, h2p, dyp, y, o4, do4, wo, acc, acc2, p_rcv, p_snd, d4 = take(17)
            dq_acc, dk_acc, dv_acc, cos_t, sin_t, ok, m_st, l_st, b_att, b_ffn, u_all, gb, b_all, b8, late, late_in, vec, mate, mate_in, v_own = take(20)
            dpre = next(it)
            act_p, dpre_p = (y.at[:, pl.ds(i * ffn, ffn)] for i in BOTH)
            here = take(8)
            send, recv, local, pair_send, pair_recv, pair_ready = take(6)
            net = Net(n_tp, send, recv, local)
            me = lax.axis_index('tp')
            mask_ref, gain1, bias1, bias_o, gain2, bias_d, bias2, freq_ref = here

            net.gather('q', wq_ref, wq)
            net.gather('o', wo_ref, wo)
            net.gather('u', wu_ref, wu)
            net.gather('d', wd_ref, wd)
            for name, buf in (('q', wq), ('o', wo), ('u', wu)):
                net.gather_far(name, lambda b=buf: b.at[2 * PAIR], lambda b=buf: b.at[FAR0], lambda b=buf: b.at[FAR1], CROSS)
            for i in BOTH:
                mine = lambda core, i=i: dx1b.at[pl.ds(core * ffn + i * quarter, quarter)]
                net.gather_far(f'd{i}', lambda i=i: wd.at[2 * CROSS, pl.ds(i * quarter, quarter)], lambda m=mine: m(0), lambda m=mine: m(1), PAIR)
            net.exchange('x', x_ref, x, chunk)
            net.multicast('dy', dy_ref, dy, dyp, chunk)
            net.exchange('y', y, y_out, chunk)
            net.exchange('gx', h1, gx_out, chunk)
            for chip in range(n_chips):
                for core in BOTH:
                    if chip + core:
                        slot = 2 * chip + core
                        net.add('bias', lambda: bq_ref, lambda n=slot: b_all.at[n], chip, core)
                        net.add('bias', lambda: bu_ref, lambda n=slot: u_all.at[n], chip, core)
            for chip in (PAIR, CROSS, FAR):
                net.add('late', lambda n=chip: late.at[n], lambda n=chip: late_in.at[n], chip)
            side = lax.rem(me, 2)
            net.add('mate', lambda: mate, lambda: mate_in, 0, 1)
            net.add('final', lambda: v_own.at[span(side, v_half)], lambda: v_own.at[span(side, v_half)], 0, 1)
            for i in BOTH:
                net.add(f'h{i}', lambda p=pl.ds(i * half, half): h2.at[p], lambda p=pl.ds(i * half, half): h2p.at[p], PAIR)
            net.add('dn_x', lambda: x_dn, lambda: r_dn, CROSS)
            net.add('up_x', lambda: x_up, lambda: r_up, CROSS)
            net.add('at_early', lambda: p_at.at[PAIR], lambda: early_at, PAIR)
            t_half = n_tile // 2
            for i, part in enumerate((pl.ds(0, t_half), pl.ds(t_half, t_half))):
                net.add(f'at_relay{i}', lambda p=part: p_at.at[FAR, p], lambda p=part: got_at.at[p], PAIR)
                net.add(f'at_sum{i}', lambda p=part: sum_at.at[p], lambda p=part: last_at.at[p], CROSS)
                net.add_local(f'at{i}_load', lambda p=part: got_at.at[p], lambda p=part: p_rcv.at[0, p])
                net.add_local(f'at{i}_load', lambda p=part: p_at.at[CROSS, p], lambda p=part: p_rcv.at[1, p])
                net.add_local(f'at{i}_store', lambda p=part: p_rcv.at[1, p], lambda p=part: sum_at.at[p])
            for src, dst in zip(plain, here):
                net.add_local('own', lambda r=src: r, lambda r=dst: r)
            net.add_local('write', lambda: v_own, lambda: g_vec)
            net.add_local('write', lambda: b8.at[0], lambda: g_b)
            for ref, tmp, buf in ((wq_ref, lambda: h2.at[pl.ds(0, n3)], wq), (wu_ref, lambda: x1.at[:, pl.ds(0, ffn)], wu),
                                        (wd_ref, lambda: dx1b.at[pl.ds(0, ffn)], wd)):
                net.add_local('load', lambda r=ref: r, tmp)
                net.add_local('store', tmp, lambda b=buf: b.at[0])
            net.add_local('own', lambda: wo_ref, lambda: wo.at[0])
            net.add_local('own', lambda: bq_ref, lambda: b_all.at[0])
            net.add_local('own', lambda: bu_ref, lambda: u_all.at[0])
            def pass_on(i, stage):
                if stage == 0:
                    net.got(f'at_relay{i}')
                    net.start(f'at{i}_load')
                elif stage == 1:
                    net.done(f'at{i}_load')

                    def body(rows):
                        rows = pl.ds(i * t_half + rows.start, rows.size)
                        p_rcv[1, rows] += p_rcv[0, rows]

                    loop_rows(t_half, 8, body)
                    net.start(f'at{i}_store')
                else:
                    net.done(f'at{i}_store')
                    net.start(f'at_sum{i}')

            def hooks(step, table):
                for at, act in table.items():
                    @pl.when(step == at)
                    def _(act=act):
                        act()

            tile_order = (FAR, PAIR, CROSS, 0)

            def place(i):
                return jnp.where(i == 0, FAR, jnp.where(i == 1, PAIR, jnp.where(i == 2, CROSS, 0)))

            def order(s):
                return 2 * place(lax.div(s, 2)) + 1 - lax.rem(s, 2)

            def to_partner(src, dst, sem):
                return pltpu.make_async_remote_copy(
                    src_ref=p_snd.at[src], dst_ref=p_rcv.at[dst], send_sem=pair_send.at[sem], recv_sem=pair_recv.at[sem],
                    device_id={'tp': net.peer(0, 1)}, device_id_type=pl.DeviceIdType.MESH)

            def keep(i, to):
                return pltpu.make_async_copy(p_rcv.at[i], to, pair_send.at[twice + i])

            def into(i):
                return lambda at, v: p_snd.__setitem__((i,) + at, v)

            def add_sent(i, j):
                def body(rows):
                    p_rcv[j, rows] += p_snd[i, rows]

                loop_rows(n_tile, 16, body)

            def pair_go(s):
                @pl.when(lax.rem(s, 2) == 1)
                def _():
                    to_partner(0, lax.div(s, 2), lax.div(s, 2)).start()

            def pair(s, tile):
                j = lax.div(s, 2)
                odd = lax.rem(s, 2)
                tile(into(odd))

                @pl.when(odd == 1)
                def _():
                    copy = to_partner(0, j, j)
                    copy.wait_send()
                    copy.wait_recv()
                    add_sent(1, j)
                    keep(j, p_at.at[place(j)]).start()

            def stored(i):
                keep(i, p_at.at[tile_order[i]]).wait()

            def pair_begin():
                pl.semaphore_signal(pair_ready, inc=1, device_id={'tp': net.peer(0, 1)}, device_id_type=pl.DeviceIdType.MESH)
                pl.semaphore_wait(pair_ready, 1)

            barrier = pltpu.get_barrier_semaphore()
            for chip in range(n_chips):
                for core in BOTH:
                    if chip + core:
                        pl.semaphore_signal(barrier, inc=1, device_id={'tp': net.peer(chip, core)}, device_id_type=pl.DeviceIdType.MESH)
            pl.semaphore_wait(barrier, n_tp - 1)
            net.start('qp', 'qc', 'x', 'qm', 'bias', 'own', 'load', 'x_own', 'dy_own')
            net.done('own')
            angle = lax.broadcasted_iota(jnp.int32, (seq, width), 0).astype(F32) * freq_ref[0:1, :]
            cos_t[...] = jnp.cos(angle)
            sin_t[...] = jnp.sin(angle) * freq_ref[1:2, :]
            for b in range(seqs):
                row = mask_ref[pl.ds(me * seqs + b, 1), :].astype(F32)
                ok[b] = jnp.broadcast_to(row, (LANES, seq)).T
            net.done('load')
            net.start('store')
            net.got('qp', 'qc')
            net.start('qr', 'dy_cross', 'oc', 'op', 'up', 'dy_pair', 'qf', 'qg', 'om')
            net.done('x_own', 'dy_own')
            net.got('bias')
            for n in range(n_tp):
                b = b_all[n]
                b_att[n] = jnp.concatenate([b[i // heads, i % heads:i % heads + 1, :] for i in range(3 * heads)], axis=1)
                b_ffn[n] = u_all[n]
            net.got('x')

            def ln1(rows):
                x_hat, _ = ln_stats(x[rows, :].astype(F32))
                h1[rows, :] = (x_hat * gain1[...] + bias1[...]).astype(BF16)

            loop_rows(tok, chunk, ln1)
            net.done('store')
            net.got('qm', 'qf', 'qg')

            def arrival(s):
                return s + 2 * lax.div(s, n_chips) - n_chips * lax.div(s, n_chips + 2)

            def qkv_step(ps, w, q_ref, k_ref, v_ref):
                s = ps.index[0]
                hooks(s, {2: lambda: (net.got('op'), net.start('or', 'uc', 'um', 'of')), 4: lambda: (net.got('qr'), net.start('ql')),
                          5: lambda: net.got('ql')})
                n_src = tok // chunk // 2

                @pl.loop(0, 2)
                def _(i):
                    rows = span(i, tok // 2)
                    t = mm(h1[rows, :], w[0], NT) + b_att[arrival(s)]
                    cos, sin = (t_ref[span(i, seq // 2), :].reshape(n_src, 1, p_len, width) for t_ref in (cos_t, sin_t))

                    def rope(v):
                        out = v.reshape(n_src, seqs, p_len, width) * cos + swap_halves(v, hd).reshape(n_src, seqs, p_len, width) * sin
                        return out.astype(BF16)

                    src = span(i, n_src)
                    q_ref[0, src] = rope(t[:, :width] * q_scale)
                    k_ref[0, src] = rope(t[:, width:2 * width])
                    v_ref[0, src] = t[:, 2 * width:].reshape(n_src, seqs, p_len, width).astype(BF16)

            slot3 = lambda rows, cols, f=lambda s: s: pl.BlockSpec((1, rows, cols), lambda s: (f(s), 0, 0))

            def pipe(body, **specs):
                def run(*refs):
                    with jax.named_scope(body.__name__):
                        pltpu.emit_pipeline(body, _explicit_indices=True, **specs)(*refs)

                return run

            pipe(qkv_step, grid=(n_tp,), in_specs=[slot3(n3, dim, arrival)],
                 out_specs=[pl.BlockSpec((1, n_tp, seqs, p_len, width), lambda s: (arrival(s), 0, 0, 0, 0))] * 3)(
                wq, q_hbm, k_hbm, v_hbm)

            srcs = qc // p_len
            lane = lax.broadcasted_iota(jnp.int32, (qc, width), 1)

            def attn_step(ps, q_ref, k_ref, v_ref):
                g, b = ps.index
                hooks(g * seqs + b, {
                    8: lambda: (net.got('dy_cross'), net.start('dy_fwd')), 9: lambda: (net.got('up'), net.start('ur', 'dc', 'dm', 'uf')),
                    14: lambda: (net.got('oc', 'or'), net.start('og', 'ol'))})
                bad = ok[b][:, 0:1] <= 0
                k = k_ref[0, :, 0].reshape(seq, width)
                v_t = v_ref[0, :, 0].reshape(seq, width).T
                for c in range(seq // qc):
                    src = slice(c * srcs, (c + 1) * srcs)
                    cols = slice(c * qc, (c + 1) * qc)
                    q = q_ref[0, src, 0].reshape(qc, width)
                    outs = []
                    for h in range(heads):
                        s = jnp.where(bad, NEG_LARGE, mm(k, jnp.where(lane // hd == h, q, jnp.zeros_like(q)), NT))
                        m = jnp.max(s, axis=0, keepdims=True)
                        e = jnp.exp(s - m)
                        r = 1.0 / col_sum(e)
                        outs.append(mm(v_t[h * hd:(h + 1) * hd], (e * r).astype(BF16), NN))
                        m_st[g, b, h:h + 1, cols] = m
                        l_st[g, b, h:h + 1, cols] = r
                    o4[src, b, :, span(g, width)] = jnp.concatenate(outs, axis=0).T.astype(BF16).reshape(srcs, p_len, width)

            head_blk = pl.BlockSpec((1, n_tp, 1, p_len, width), lambda g, b: (g, 0, b, 0, 0))
            pipe(attn_step, grid=(n_tp, seqs), in_specs=[head_blk] * 3)(q_hbm, k_hbm, v_hbm)

            net.got('om', 'of', 'og', 'ol')

            @pl.loop(0, tok // (2 * chunk))
            def _(i):
                rows = span(i, 2 * chunk)
                o = o4[pl.ds(2 * i, 2)].reshape(2 * chunk, n_tp * width)
                low = (x[rows, :].astype(F32) + (mm(o, wo[...].reshape(n_tp * width, dim), NN) + bias_o[...])).astype(BF16)
                x1[rows, :] = low
                x_hat, _ = ln_stats(low.astype(F32))
                h2[rows, :] = (x_hat * gain2[...] + bias2[...]).astype(BF16)

            net.start('h0', 'h1', 'dp')

            def gelu(pre):
                erf_term = lax.erf(pre * INV_SQRT2)
                act = (0.5 * pre * (1.0 + erf_term)).astype(BF16)
                return act, 0.5 * (1.0 + erf_term) + pre * jnp.exp(-0.5 * pre * pre) * INV_SQRT_2PI

            cols = lambda f: pl.BlockSpec((tok, ffn), lambda s: (0, f(s)))
            wu_spec, wd_spec = functools.partial(slot3, dim, ffn), functools.partial(slot3, ffn, dim)

            def mlp_up(n, f, table):
                def up_step(ps, w, act_ref, slope_ref):
                    s = ps.index[0]
                    hooks(s, table)

                    def body(rows):
                        act_ref[rows, :], slope_ref[rows, :] = gelu(mm(h2[rows, :], w[0], NN) + b_ffn[f(s)])

                    loop_rows(tok, half, body)

                pipe(up_step, grid=(n,), in_specs=[wu_spec(f)], out_specs=[cols(f)] * 2)(wu, act_hbm, slope_hbm)

            net.got('um', 'uf')
            mlp_up(n_tp - 2, arrival, {2: lambda: (net.got('uc'), net.start('ug')), 3: lambda: net.got('ug')})
            net.got('dy_pair', 'dy_fwd', 'dm')

            def backward(slot, w_d, w_u, act_ref, slope_ref, add):
                if add:
                    gb[slot] = jnp.zeros_like(gb[0])

                def body(rows):
                    d_pre = mm(dy[rows, :], w_d, NT) * slope_ref[rows, :]
                    low = d_pre.astype(BF16)
                    dpre[rows, :] = low
                    if add:
                        gb[slot] += col_sum(d_pre)
                        acc[rows, :] += mm(act_ref[rows, :], w_d, NN)
                        acc2[rows, :] += mm(low, w_u, NT)

                loop_rows(tok, half, body)

            def pair_gelu(rows, w_u, slot):
                return gelu(mm(h2p[rows, :], w_u, NN) + b_ffn[slot])

            def grads(chip, at, x_ref, between):
                f = lambda s: 2 * chip + 1 - s
                copy = to_partner(0, at, n_tp + at)

                def first(ps, w_u, act_ref):
                    s = ps.index[0]
                    rows = pl.ds(0, half)
                    act_p[rows, :] = pair_gelu(rows, w_u[0], f(s))[0]
                    p_snd[s] = mm(act_ref[...], dy[...], TN) + mm(act_p[rows, :], dyp[rows, :], TN)

                def second(ps, w_u):
                    s = ps.index[0]
                    pl.when(s == 1)(lambda: copy.start())
                    rows = pl.ds(half, half)
                    act_p[rows, :] = pair_gelu(rows, w_u[0], f(s))[0]
                    p_snd[s] += mm(act_p[rows, :], dyp[rows, :], TN)

                    @pl.when(s == 1)
                    def _():
                        copy.wait_recv()
                        add_sent(1, at)
                        keep(at, x_ref).start()
                        copy.wait_send()

                pipe(first, grid=(len(BOTH),), in_specs=[wu_spec(f), cols(f)])(wu, act_hbm)
                between()
                pipe(second, grid=(len(BOTH),), in_specs=[wu_spec(f)])(wu)
                keep(at, x_ref).wait()

            def mlp(n, f, add, table, last=None):
                def mlp_step(ps, wd_s, wu_s, act_ref, slope_ref):
                    s = ps.index[0]
                    backward(f(s), wd_s[0], wu_s[0], act_ref, slope_ref, add)
                    if last:
                        at, ref, send = last
                        copy = to_partner(0, at + 1, n_tp + at + 1)
                        pl.when(s == 1)(lambda: copy.start())

                        @pl.when(s < 2)
                        def _():
                            def body(rows):
                                dpre_p[rows, :] = (mm(dyp[rows, :], wd_s[0], NT) * pair_gelu(rows, wu_s[0], f(s))[1]).astype(BF16)

                            loop_rows(tok, half, body)
                            for i in BOTH:
                                part = pl.ds(i * half, half)
                                p_snd[s, pl.ds(0, ffn), part] = mm(h2[:, part], dpre[...], TN) + mm(h2p[:, part], dpre_p[...], TN)

                        @pl.when(s == 1)
                        def _():
                            copy.wait_recv()
                            add_sent(1, at + 1)
                            keep(at + 1, ref).start()
                            copy.wait_send()

                    hooks(s, table)

                pipe(mlp_step, grid=(n,), in_specs=[wd_spec(f), wu_spec(f), cols(f), cols(f)])(wd, wu, act_hbm, slope_hbm)

            acc[...] = jnp.zeros_like(acc)
            acc2[...] = jnp.zeros_like(acc2)
            mlp(2, lambda s: s, True, {})
            net.got('ur')
            net.start('ul')
            net.got('ul')
            mlp_up(2, lambda s: s + FAR0, {})
            net.got('h0')
            grads(CROSS, 0, x_dn, lambda: (net.got('dc'), net.start('dg', 'd0r', 'd1r'), net.got('h1')))
            net.start('dn_x')
            net.got('dg')

            def sent_up():
                keep(1, x_up).wait()
                net.start('up_x')

            slots = lambda s: jnp.where(s < 2, 2 * CROSS + 1 - s, s)
            mlp(n_chips, slots, True, {0: lambda: (net.got('dp'), net.start('df')), 1: lambda: net.got('df'), 2: sent_up}, (0, x_up, 'up_x'))

            for slot in (FAR0, FAR1):
                gb[slot] = jnp.zeros_like(gb[slot])

            def far_step(ps, w_u, act_ref, slope_ref):
                part, core = ps.index
                hooks(2 * part + core, {0: lambda: (net.got('d0r'), net.start('d0l')), 1: lambda: net.got('d0l'),
                                        2: lambda: (net.got('d1r'), net.start('d1l')), 3: lambda: net.got('d1l')})
                w_d = dx1b[pl.ds(pl.multiple_of(core * ffn + part * quarter, quarter), quarter), :]

                def body(rows):
                    d_pre = mm(dy[rows, :], w_d, NT) * slope_ref[rows, :]
                    gb[FAR0 + core, :, span(part, quarter)] += col_sum(d_pre)
                    acc[rows, :] += mm(act_ref[rows, :], w_d, NN)
                    acc2[rows, :] += mm(d_pre.astype(BF16), w_u[0], NT)

                loop_rows(tok, half, body)

            narrow = pl.BlockSpec((tok, quarter), lambda part, core: (0, 2 * (FAR0 + core) + part))
            pipe(far_step, grid=(len(BOTH),) * len(BOTH), in_specs=[pl.BlockSpec((1, dim, quarter), lambda part, core: (FAR0 + core, 0, part)), narrow, narrow])(
                wu, act_hbm, slope_hbm)

            def y_rows(rows):
                y[rows, :] = (x1[rows, :].astype(F32) + (acc[rows, :] + bias_d[...])).astype(BF16)

            loop_rows(tok, 2 * chunk, y_rows)
            vec[...] = jnp.zeros_like(vec)
            net.start('y', 'y_own')
            net.sent('d0l', 'd1l')

            @pl.loop(0, tok // (2 * chunk))
            def _(i):
                rows = span(i, 2 * chunk)
                x1_f, dy_f, dh = x1[rows, :].astype(F32), dy[rows, :].astype(F32), acc2[rows, :]
                x_hat, inv_std = ln_stats(x1_f)
                d_x1 = dy_f + ln_grad(dh, x_hat, inv_std, gain2[...])
                acc2[rows, :] = d_x1
                low = d_x1.astype(BF16)
                dx1b[rows, :] = low
                d_o = mm(low, wo[...].reshape(n_tp * width, dim), NT).astype(BF16)
                do4[pl.ds(2 * i, 2)] = d_o.reshape(2, seqs, p_len, n_tp * width)
                for n, t in enumerate((d_x1, dh * x_hat, dh, dy_f)):
                    vec[2 + n:3 + n, :] += col_sum(t)

            pair_begin()

            def bwd_step(ps, q_ref, k_ref, v_ref, w):
                step = ps.index[0]
                g = order(step)
                hooks(step, {2: lambda: (stored(0), net.start('at_relay0', 'at_relay1')),
                             4: lambda: (stored(1), net.start('at_early')), 6: lambda: (stored(2), pass_on(0, 0)), 7: lambda: pass_on(0, 2)})
                pair_go(step)
                b8[g] = jnp.zeros_like(b8[0])
                fold(gb[g], b8.at[g], 3)
                for b in range(seqs):
                    bad = ok[b][:, 0:1] <= 0
                    k = k_ref[0, :, b].reshape(seq, width)
                    v = v_ref[0, :, b].reshape(seq, width)
                    k_t = k.T
                    for c in range(seq // qc):
                        src = slice(c * srcs, (c + 1) * srcs)
                        at = slice(c * qc, (c + 1) * qc)
                        q = q_ref[0, src, b].reshape(qc, width)
                        d_o = do4[src, b, :, span(g, width)].reshape(qc, width)
                        dk = jnp.zeros((seq, width), F32)
                        dv = jnp.zeros((seq, width), F32)
                        dqs = []
                        for h in range(heads):
                            mine = lane // hd == h
                            q_h = jnp.where(mine, q, jnp.zeros_like(q))
                            do_h = jnp.where(mine, d_o, jnp.zeros_like(d_o))
                            s = jnp.where(bad, NEG_LARGE, mm(k, q_h, NT))
                            p = jnp.exp(s - m_st[g, b, h:h + 1, at]) * l_st[g, b, h:h + 1, at]
                            dv += mm(p.astype(BF16), do_h, NN)
                            dp = mm(v, do_h, NT)
                            ds = (p * (dp - col_sum(dp * p))).astype(BF16)
                            dk += mm(ds, q_h, NN)
                            dqs.append(mm(k_t[h * hd:(h + 1) * hd], ds, NN))
                        dq_acc[at, :] = jnp.concatenate(dqs, axis=0).T
                        dk_acc[...] = dk if c == 0 else dk_acc[...] + dk
                        dv_acc[...] = dv if c == 0 else dv_acc[...] + dv
                    cos, sin = cos_t[...], sin_t[...]
                    dq, dk, dv = dq_acc[...], dk_acc[...], dv_acc[...]
                    dq = (dq * cos - swap_halves(dq, hd) * sin) * q_scale
                    dk = dk * cos - swap_halves(dk, hd) * sin
                    for i, t in enumerate((dq, dk, dv)):
                        d4[:, b, :, i * width:(i + 1) * width] = t.astype(BF16).reshape(n_tp, p_len, width)
                        b8[g, i:i + 1, :] += col_sum(t)

                @pl.when(step == 0)
                def _():
                    acc[...] = jnp.zeros_like(acc)

                @pl.loop(0, 2)
                def _(i):
                    acc[span(i, half), :] += mm(d4[pl.ds(n_chips * i, n_chips)].reshape(half, n3), w[0], NN)

                def tile(put):
                    put((pl.ds(0, n3),), mm(d4[...].reshape(tok, n3), h1[...], TN))
                    put((pl.ds(n3, width),), mm(o4[:, :, :, span(g, width)].reshape(tok, width), dx1b[...], TN))

                pair(step, tile)
                hooks(step, {6: lambda: pass_on(0, 1)})

            slot_blk = pl.BlockSpec((1, n_tp, seqs, p_len, width), lambda s: (order(s), 0, 0, 0, 0))
            pipe(bwd_step, grid=(n_tp,), in_specs=[slot_blk] * 3 + [slot3(n3, dim, order)])(
                q_hbm, k_hbm, v_hbm, wq)

            pass_on(1, 0)

            def ln1_bwd(rows):
                x_hat, inv_std = ln_stats(x[rows, :].astype(F32))
                dh = acc[rows, :]
                h1[rows, :] = (acc2[rows, :] + ln_grad(dh, x_hat, inv_std, gain1[...])).astype(BF16)
                vec[0:1, :] += col_sum(dh * x_hat)
                vec[1:2, :] += col_sum(dh)

            loop_rows(tok, 2 * chunk, ln1_bwd)
            stored(3)
            for r in range(6):
                fold(vec[pl.ds(r, 1), :], v_own, r * n_tp)
            mate[0:v_half] = v_own[span(1 - side, v_half), :]
            for n in range(n_chips):
                mate[pl.ds(v_half + n * 8, 8)] = b8[2 * n + 1]
            net.start('mate')
            pass_on(1, 1)
            net.got('mate')
            v_sum = v_own[span(side, v_half), :] + mate_in[0:v_half]
            for n in range(n_chips):
                late[n, 0:v_half] = v_sum
                late[n, v_half:] = b8[2 * n] + mate_in[pl.ds(v_half + n * 8, 8)]
            net.start('late')
            pass_on(1, 2)
            net.start('gx', 'gx_own')

            net.sent('y')
            net.done('y_own')
            pair_begin()
            grads(0, 2, p_dn, lambda: None)
            mlp(2, lambda s: 1 - s, False, {}, (2, p_up, None))
            keep(3, p_up).wait()

            def total(refs, out, block, at):
                def body(*blocks):
                    v = blocks[1][...]
                    for more in blocks[2:-1]:
                        v += more[...]
                    blocks[-1][...] = v

                pipe(body, grid=(len(BOTH),), in_specs=[pl.BlockSpec(block, at)] * len(refs),
                     out_specs=[pl.BlockSpec(block, lambda i: (i, 0))])(*refs, out)

            by_row, by_col = lambda i: (i, 0), lambda i: (0, i)
            net.got('late')
            late_sum = late[0]
            for n in range(1, n_chips):
                late_sum += late_in[n]
            v_own[span(side, v_half), :] = late_sum[0:v_half]
            b8[0] = late_sum[v_half:]
            net.start('final')
            net.got('dn_x', 'up_x')
            total((p_dn, r_dn), g_down, (t_half, dim), by_row)
            total((p_up, r_up), g_up, (n_tile, half), by_col)
            net.got('at_early', 'at_sum0', 'at_sum1')
            for rows, out, n in ((pl.ds(0, n3), g_q, n3), (pl.ds(n3, width), g_o, width)):
                total((p_at.at[0, rows], early_at.at[rows], last_at.at[rows]), out, (n // 2, dim), by_row)
            for name in net.copies:
                if name not in ('load', 'store', 'own', 'write', 'gx', 'y', 'd0l', 'd1l') and not name.endswith(('_own', '_load', '_store')):
                    net.sent(name)
            net.got('y', 'final')
            net.start('write')
            net.done('gx_own', 'write')
            net.got('gx')
            net.sent('gx')

        big = (tok, dim)
        shapes = lambda *dims, dtype=F32: sds(dims, dtype)
        flat = lambda t: t.reshape(tok, dim)
        inv_freq = ROPE_BASE ** (-2.0 * np.arange(hd // 2) / hd)
        sign = np.repeat([-1.0, 1.0], hd // 2)
        freq = np.stack([np.tile(inv_freq, 2 * heads), np.tile(sign, heads)]).astype(np.float32)
        line = lambda v: v.reshape(1, -1)
        sem = lambda n: pltpu.SemaphoreType.DMA((n,))
        low = functools.partial(shapes, dtype=BF16)
        weights = [low(n_tp, n3, dim), low(n_tp, dim, ffn), low(n_tp, ffn, dim)]
        tiles = [shapes(n_chips, n_tile, dim)] + [shapes(n_tile, dim)] * 10
        out_shape = ([low(*big)] * 2 + [shapes(dim, ffn), shapes(ffn, dim), shapes(n3, dim), shapes(width, dim), shapes(6 * n_tp, LANES), shapes(8, LANES)] + weights
                     + [low(n_tp, n_tp, seqs, p_len, width)] * 3 + [low(tok, n_tp * ffn), shapes(tok, n_tp * ffn)] + tiles)
        plain = [pad_mask] + [line(v) for v in (ln1_gain, ln1_bias, b_out, ln2_gain, b_down, ln2_bias)] + [freq]
        heads4 = low(n_tp, seqs, p_len, n_tp * width)
        stat = shapes(n_tp, seqs, heads, seq)
        tile8 = shapes(n_tp, 8, LANES)
        late = shapes(n_chips, v_half + 8, LANES)
        mate = shapes(v_half + 8 * n_chips, LANES)
        row_ffn = shapes(n_tp, 1, ffn)
        scratch = ([low(*big)] * 9 + [heads4, heads4, low(n_tp, width, dim)] + [shapes(*big)] * 2
                   + [shapes(n_chips, n_tile, dim), shapes(2, n_tile, dim), low(n_tp, seqs, p_len, n3)]
                   + [shapes(seq, width)] * 5 + [shapes(seqs, seq, LANES), stat, stat, shapes(n_tp, 1, n3), row_ffn, row_ffn, row_ffn]
                   + [shapes(n_tp, *b_qkv.shape), tile8, late, late, shapes(8, dim), mate, mate, shapes(6 * n_tp, LANES)]
                   + [low(tok, ffn)] + plain)
        outs = pl.pallas_call(
            kernel, name='layer', out_shape=out_shape, in_specs=[ANY] * 16, out_specs=[ANY] * len(out_shape),
            scratch_shapes=[pltpu.VMEM(v.shape, v.dtype) for v in scratch]
            + [sem(91), sem(91), sem(30), sem(20), sem(12), pltpu.SemaphoreType.REGULAR],
            compiler_params=pltpu.CompilerParams(collective_id=0, has_side_effects=True, vmem_limit_bytes=VMEM_LIMIT),
        )(flat(x_in), flat(grad_y), w_qkv.transpose(0, 2, 3, 1).reshape(n3, dim), b_qkv, w_out.reshape(width, dim),
          w_up, line(b_up), w_down, *plain)

        def finish(*refs):
            src, (v_ref, b_ref), out, (bq_o, bu_o), v_o = refs[:6], refs[6:8], refs[8:14], refs[14:16], refs[16:]
            for a, b in zip(src, out):
                b[...] = a[...]
            for i in range(3):
                for h in range(heads):
                    bq_o[i, h:h + 1, :] = b_ref[i:i + 1, h * hd:(h + 1) * hd]
            unfold(b_ref, 3, bu_o)
            for r, ref in enumerate(v_o):
                unfold(v_ref, r * n_tp, ref)

        large = [low(*big)] * 2 + [shapes(dim, ffn), shapes(ffn, dim), shapes(n3, dim), shapes(width, dim)]
        small = [shapes(*b_qkv.shape), shapes(1, ffn)] + [shapes(1, dim)] * 6
        moving = [pl.BlockSpec((v.shape[0] // n_tp, v.shape[1]), lambda i: (i, 0)) for v in large]
        fixed = lambda vs: [pl.BlockSpec(v.shape, lambda i, n=len(v.shape): (0,) * n) for v in vs]
        res = pl.pallas_call(
            finish, name='finish', out_shape=large + small, grid=(n_tp,), in_specs=moving + fixed(outs[6:8]),
            out_specs=moving + fixed(small), compiler_params=pltpu.CompilerParams(vmem_limit_bytes=VMEM_LIMIT),
        )(*outs[:8])
        y_out, grad_x, grad_w_up, grad_w_down, gq, go, grad_b_qkv, grad_b_up = res[:8]
        v = [t.reshape(dim) for t in res[8:]]
        return (y_out.reshape(x_in.shape), grad_x.reshape(x_in.shape), v[0], v[1], gq.reshape(3, heads, hd, dim).transpose(0, 3, 1, 2),
                grad_b_qkv, go.reshape(heads, hd, dim), v[2], v[3], v[4], grad_w_up, grad_b_up.reshape(ffn), grad_w_down, v[5])

    return jax.shard_map(device_step, mesh=mesh, in_specs=in_specs, out_specs=out_specs, check_vma=False)
```

```python
import functools

import jax
import jax.numpy as jnp
import numpy as np
from jax import lax
from jax.experimental import pallas as pl
from jax.experimental.pallas import tpu as pltpu
from jax.sharding import PartitionSpec as P

LN_EPS = 1e-5
ROPE_BASE = 10000.0
INV_SQRT2 = 0.7071067811865476
INV_SQRT_2PI = 0.3989422804014327
NEG_LARGE = -1e30
F32 = jnp.float32
BF16 = jnp.bfloat16
VMEM_LIMIT = 66_500_000
LANES = 128
NN = (((1,), (0,)), ((), ()))
NT = (((1,), (1,)), ((), ()))
TN = (((0,), (0,)), ((), ()))
PAIR, FAR, CROSS = 1, 2, 3
FAR0 = FAR + FAR
FAR1 = FAR0 + 1
BOTH = range(2)
ANY = pl.BlockSpec(memory_space=pl.ANY)


def mm(a, b, dims):
    return lax.dot_general(a, b, dims, preferred_element_type=F32)


def ln_stats(v):
    centered = v - jnp.mean(v, axis=-1, keepdims=True)
    inv_std = lax.rsqrt(jnp.mean(centered * centered, axis=-1, keepdims=True) + LN_EPS)
    return centered * inv_std, inv_std


def ln_grad(d_out, x_hat, inv_std, gain):
    d_hat = d_out * gain
    return inv_std * (d_hat - jnp.mean(d_hat, axis=-1, keepdims=True) - x_hat * jnp.mean(d_hat * x_hat, axis=-1, keepdims=True))


def col_sum(t):
    return jnp.sum(t, axis=0, keepdims=True)


def swap_halves(t, head_dim):
    half = head_dim // 2
    lane = lax.broadcasted_iota(jnp.int32, t.shape, t.ndim - 1)
    return jnp.where(lane % head_dim < half, pltpu.roll(t, t.shape[-1] - half, t.ndim - 1), pltpu.roll(t, half, t.ndim - 1))


def span(i, n):
    return pl.ds(pl.multiple_of(i * n, n), n)


def fold(row, out, first):
    for i in range(row.shape[-1] // LANES):
        out[pl.ds(first + i, 1), :] = row[:, i * LANES:(i + 1) * LANES]


def unfold(src, first, out):
    for i in range(out.shape[-1] // LANES):
        out[:, pl.ds(i * LANES, LANES)] = src[pl.ds(first + i, 1), :]


def loop_rows(total, n, body):
    @pl.loop(0, total // n)
    def _(i):
        body(span(i, n))


class Net:
    def __init__(self, n_tp, send, recv, local):
        self.n_tp, self.send, self.recv, self.local = n_tp, send, recv, local
        self.copies, self.count, self.n_local = {}, 0, 0

    def peer(self, chip, core=0):
        me = lax.axis_index('tp')
        way = 1 - 2 * lax.rem(lax.div(me, 2), 2)
        at = lax.rem(me + 2 * chip * way + self.n_tp, self.n_tp) if chip else me
        return at + 1 - 2 * lax.rem(at, 2) if core else at

    def add(self, name, src, dst, chip, core=0):
        n = self.count
        self.count += 1

        def make():
            return pltpu.make_async_remote_copy(
                src_ref=src(), dst_ref=dst(), send_sem=self.send.at[n], recv_sem=self.recv.at[n],
                device_id={'tp': self.peer(chip, core)}, device_id_type=pl.DeviceIdType.MESH)

        self.copies.setdefault(name, []).append(make)

    def add_local(self, name, src, dst):
        n = self.n_local
        self.n_local += 1
        self.copies.setdefault(name, []).append(lambda: pltpu.make_async_copy(src(), dst(), self.local.at[n]))

    def start(self, *names):
        for name in names:
            for make in self.copies[name]:
                make().start()

    def got(self, *names):
        for name in names:
            with jax.named_scope('got_' + name):
                for make in self.copies[name]:
                    make().wait_recv()

    def sent(self, *names):
        for name in names:
            for make in self.copies[name]:
                make().wait_send()

    def done(self, *names):
        for name in names:
            with jax.named_scope('done_' + name):
                for make in self.copies[name]:
                    make().wait()

    def gather(self, name, own, buf):
        for stage, chip in (('p', PAIR), ('c', CROSS)):
            self.add(name + stage, lambda: own, lambda c=chip: buf.at[2 * c], chip)
        self.add(name + 'm', lambda: own, lambda: buf.at[1], 0, 1)
        for stage, chip in (('f', PAIR), ('g', CROSS)):
            self.add(name + stage, lambda c=chip: buf.at[2 * c], lambda c=chip: buf.at[2 * c + 1], 0, 1)

    def gather_far(self, name, src, here, other, via):
        self.add(name + 'r', src, here, via)
        self.add(name + 'l', here, other, 0, 1)

    def exchange(self, name, src, dst, rows):
        me = lax.axis_index('tp')
        for core in BOTH:
            for chip in (PAIR, CROSS, FAR, 0):
                if chip + core:
                    self.add(name, lambda c=chip, k=core: src.at[span(self.peer(c, k), rows)], lambda: dst.at[span(me, rows)], chip, core)
        self.add_local(name + '_own', lambda: src.at[span(me, rows)], lambda: dst.at[span(me, rows)])

    def multicast(self, name, src, dst, pair_dst, rows):
        me = lax.axis_index('tp')
        at = lambda buf: (lambda: buf.at[span(me, rows)])
        other = {0: PAIR, PAIR: 0, CROSS: FAR}
        for chip, stage in ((CROSS, '_cross'), (PAIR, '_pair'), (0, '_pair')):
            for core in BOTH:
                if chip + core:
                    for c, buf in ((chip, dst), (other[chip], pair_dst)):
                        self.add(name + stage, lambda c=c, k=core: src.at[span(self.peer(c, k), rows)], at(buf), chip, core)
        for c, buf in ((0, dst), (PAIR, pair_dst)):
            self.add_local(name + '_own', lambda c=c: src.at[span(self.peer(c), rows)], at(buf))
        came = lambda buf: (lambda: buf.at[span(lax.div(self.peer(CROSS), 2), 2 * rows)])
        self.add(name + '_fwd', came(dst), came(pair_dst), PAIR)
        self.add(name + '_fwd', came(pair_dst), came(dst), PAIR)


def solution(mesh):
    n_tp = mesh.shape['tp']
    n_chips = n_tp // 2
    act_spec = P('dp', 'tp', None)
    rep_vec = P(None)
    part_vec = P('dp')
    in_specs = (act_spec, act_spec, P('dp', None), rep_vec, rep_vec, P(None, None, 'tp', None), P(None, 'tp', None),
                P('tp', None, None), rep_vec, rep_vec, rep_vec, P(None, 'tp'), P('tp'), P('tp', None), rep_vec)
    out_specs = (act_spec, act_spec, part_vec, part_vec, P('dp', None, 'tp', None), P('dp', 'tp', None),
                 P(('dp', 'tp'), None, None), part_vec, part_vec, part_vec, P('dp', 'tp'), P(('dp', 'tp')),
                 P(('dp', 'tp'), None), part_vec)

    def device_step(x_in, grad_y, pad_mask, ln1_gain, ln1_bias, w_qkv, b_qkv, w_out, b_out, ln2_gain, ln2_bias, w_up, b_up, w_down, b_down):
        batch, p_len, dim = x_in.shape
        seq = pad_mask.shape[1]
        _, _, heads, hd = w_qkv.shape
        seqs = batch // n_tp
        ffn = w_up.shape[1]
        width = heads * hd
        n3 = 3 * width
        tok = seqs * seq
        chunk = seqs * p_len
        qc = seq // 2
        q_scale = hd ** -0.5
        sds = jax.ShapeDtypeStruct
        n_tile = n3 + width
        half = dim // 2
        twice = n_tp + n_tp
        quarter = ffn // 2
        v_half = 3 * n_tp

        def kernel(*refs):
            it = iter(refs)
            take = lambda n: [next(it) for _ in range(n)]
            (x_ref, dy_ref, wq_ref, bq_ref, wo_ref, wu_ref, bu_ref, wd_ref), plain = take(8), take(8)
            y_out, gx_out, g_up, g_down, g_q, g_o, g_vec, g_b, wq, wu, wd, q_hbm, k_hbm, v_hbm, act_hbm, slope_hbm = take(16)
            p_at, got_at, sum_at, early_at, last_at, x_dn, x_up, p_dn, p_up, r_dn, r_up = take(11)
            x, h1, dy, x1, h2, dx1b, h2p, dyp, y, o4, do4, wo, acc, acc2, p_rcv, p_snd, d4 = take(17)
            dq_acc, dk_acc, dv_acc, cos_t, sin_t, ok, m_st, l_st, b_att, b_ffn, u_all, gb, b_all, b8, late, late_in, vec, mate, mate_in, v_own = take(20)
            dpre = next(it)
            act_p, dpre_p = (y.at[:, pl.ds(i * ffn, ffn)] for i in BOTH)
            here = take(8)
            send, recv, local, pair_send, pair_recv, pair_ready = take(6)
            net = Net(n_tp, send, recv, local)
            me = lax.axis_index('tp')
            mask_ref, gain1, bias1, bias_o, gain2, bias_d, bias2, freq_ref = here

            net.gather('q', wq_ref, wq)
            net.gather('o', wo_ref, wo)
            net.gather('u', wu_ref, wu)
            net.gather('d', wd_ref, wd)
            for name, buf in (('q', wq), ('o', wo), ('u', wu)):
                net.gather_far(name, lambda b=buf: b.at[2 * PAIR], lambda b=buf: b.at[FAR0], lambda b=buf: b.at[FAR1], CROSS)
            for i in BOTH:
                mine = lambda core, i=i: dx1b.at[pl.ds(core * ffn + i * quarter, quarter)]
                net.gather_far(f'd{i}', lambda i=i: wd.at[2 * CROSS, pl.ds(i * quarter, quarter)], lambda m=mine: m(0), lambda m=mine: m(1), PAIR)
            net.exchange('x', x_ref, x, chunk)
            net.multicast('dy', dy_ref, dy, dyp, chunk)
            net.exchange('y', y, y_out, chunk)
            net.exchange('gx', h1, gx_out, chunk)
            for chip in range(n_chips):
                for core in BOTH:
                    if chip + core:
                        slot = 2 * chip + core
                        net.add('bias', lambda: bq_ref, lambda n=slot: b_all.at[n], chip, core)
                        net.add('bias', lambda: bu_ref, lambda n=slot: u_all.at[n], chip, core)
            for chip in (PAIR, CROSS, FAR):
                net.add('late', lambda n=chip: late.at[n], lambda n=chip: late_in.at[n], chip)
            side = lax.rem(me, 2)
            net.add('mate', lambda: mate, lambda: mate_in, 0, 1)
            net.add('final', lambda: v_own.at[span(side, v_half)], lambda: v_own.at[span(side, v_half)], 0, 1)
            for i in BOTH:
                net.add(f'h{i}', lambda p=pl.ds(i * half, half): h2.at[p], lambda p=pl.ds(i * half, half): h2p.at[p], PAIR)
            net.add('dn_x', lambda: x_dn, lambda: r_dn, CROSS)
            net.add('up_x', lambda: x_up, lambda: r_up, CROSS)
            net.add('at_early', lambda: p_at.at[PAIR], lambda: early_at, PAIR)
            t_half = n_tile // 2
            for i, part in enumerate((pl.ds(0, t_half), pl.ds(t_half, t_half))):
                net.add(f'at_relay{i}', lambda p=part: p_at.at[FAR, p], lambda p=part: got_at.at[p], PAIR)
                net.add(f'at_sum{i}', lambda p=part: sum_at.at[p], lambda p=part: last_at.at[p], CROSS)
                net.add_local(f'at{i}_load', lambda p=part: got_at.at[p], lambda p=part: p_rcv.at[0, p])
                net.add_local(f'at{i}_load', lambda p=part: p_at.at[CROSS, p], lambda p=part: p_rcv.at[1, p])
                net.add_local(f'at{i}_store', lambda p=part: p_rcv.at[1, p], lambda p=part: sum_at.at[p])
            for src, dst in zip(plain, here):
                net.add_local('own', lambda r=src: r, lambda r=dst: r)
            net.add_local('write', lambda: v_own, lambda: g_vec)
            net.add_local('write', lambda: b8.at[0], lambda: g_b)
            for ref, tmp, buf in ((wq_ref, lambda: h2.at[pl.ds(0, n3)], wq), (wu_ref, lambda: x1.at[:, pl.ds(0, ffn)], wu),
                                        (wd_ref, lambda: dx1b.at[pl.ds(0, ffn)], wd)):
                net.add_local('load', lambda r=ref: r, tmp)
                net.add_local('store', tmp, lambda b=buf: b.at[0])
            net.add_local('own', lambda: wo_ref, lambda: wo.at[0])
            net.add_local('own', lambda: bq_ref, lambda: b_all.at[0])
            net.add_local('own', lambda: bu_ref, lambda: u_all.at[0])
            def pass_on(i, stage):
                if stage == 0:
                    net.got(f'at_relay{i}')
                    net.start(f'at{i}_load')
                elif stage == 1:
                    net.done(f'at{i}_load')

                    def body(rows):
                        rows = pl.ds(i * t_half + rows.start, rows.size)
                        p_rcv[1, rows] += p_rcv[0, rows]

                    loop_rows(t_half, 8, body)
                    net.start(f'at{i}_store')
                else:
                    net.done(f'at{i}_store')
                    net.start(f'at_sum{i}')

            def hooks(step, table):
                for at, act in table.items():
                    @pl.when(step == at)
                    def _(act=act):
                        act()

            tile_order = (FAR, PAIR, CROSS, 0)

            def place(i):
                return jnp.where(i == 0, FAR, jnp.where(i == 1, PAIR, jnp.where(i == 2, CROSS, 0)))

            def order(s):
                return 2 * place(lax.div(s, 2)) + 1 - lax.rem(s, 2)

            def to_partner(src, dst, sem):
                return pltpu.make_async_remote_copy(
                    src_ref=p_snd.at[src], dst_ref=p_rcv.at[dst], send_sem=pair_send.at[sem], recv_sem=pair_recv.at[sem],
                    device_id={'tp': net.peer(0, 1)}, device_id_type=pl.DeviceIdType.MESH)

            def keep(i, to):
                return pltpu.make_async_copy(p_rcv.at[i], to, pair_send.at[twice + i])

            def into(i):
                return lambda at, v: p_snd.__setitem__((i,) + at, v)

            def add_sent(i, j):
                def body(rows):
                    p_rcv[j, rows] += p_snd[i, rows]

                loop_rows(n_tile, 16, body)

            def pair_go(s):
                @pl.when(lax.rem(s, 2) == 1)
                def _():
                    to_partner(0, lax.div(s, 2), lax.div(s, 2)).start()

            def pair(s, tile):
                j = lax.div(s, 2)
                odd = lax.rem(s, 2)
                tile(into(odd))

                @pl.when(odd == 1)
                def _():
                    copy = to_partner(0, j, j)
                    copy.wait_send()
                    copy.wait_recv()
                    add_sent(1, j)
                    keep(j, p_at.at[place(j)]).start()

            def stored(i):
                keep(i, p_at.at[tile_order[i]]).wait()

            def pair_begin():
                pl.semaphore_signal(pair_ready, inc=1, device_id={'tp': net.peer(0, 1)}, device_id_type=pl.DeviceIdType.MESH)
                pl.semaphore_wait(pair_ready, 1)

            barrier = pltpu.get_barrier_semaphore()
            for chip in range(n_chips):
                for core in BOTH:
                    if chip + core:
                        pl.semaphore_signal(barrier, inc=1, device_id={'tp': net.peer(chip, core)}, device_id_type=pl.DeviceIdType.MESH)
            pl.semaphore_wait(barrier, n_tp - 1)
            net.start('qp', 'qc', 'x', 'qm', 'bias', 'own', 'load', 'x_own', 'dy_own')
            net.done('own')
            angle = lax.broadcasted_iota(jnp.int32, (seq, width), 0).astype(F32) * freq_ref[0:1, :]
            cos_t[...] = jnp.cos(angle)
            sin_t[...] = jnp.sin(angle) * freq_ref[1:2, :]
            for b in range(seqs):
                row = mask_ref[pl.ds(me * seqs + b, 1), :].astype(F32)
                ok[b] = jnp.broadcast_to(row, (LANES, seq)).T
            net.done('load')
            net.start('store')
            net.got('qp', 'qc')
            net.start('qr', 'dy_cross', 'oc', 'op', 'up', 'dy_pair', 'qf', 'qg', 'om')
            net.done('x_own', 'dy_own')
            net.got('bias')
            for n in range(n_tp):
                b = b_all[n]
                b_att[n] = jnp.concatenate([b[i // heads, i % heads:i % heads + 1, :] for i in range(3 * heads)], axis=1)
                b_ffn[n] = u_all[n]
            net.got('x')

            def ln1(rows):
                x_hat, _ = ln_stats(x[rows, :].astype(F32))
                h1[rows, :] = (x_hat * gain1[...] + bias1[...]).astype(BF16)

            loop_rows(tok, chunk, ln1)
            net.done('store')
            net.got('qm', 'qf', 'qg')

            def arrival(s):
                return s + 2 * lax.div(s, n_chips) - n_chips * lax.div(s, n_chips + 2)

            def qkv_step(ps, w, q_ref, k_ref, v_ref):
                s = ps.index[0]
                hooks(s, {2: lambda: (net.got('op'), net.start('or', 'uc', 'um', 'of')), 4: lambda: (net.got('qr'), net.start('ql')),
                          5: lambda: net.got('ql')})
                n_src = tok // chunk // 2

                @pl.loop(0, 2)
                def _(i):
                    rows = span(i, tok // 2)
                    t = mm(h1[rows, :], w[0], NT) + b_att[arrival(s)]
                    cos, sin = (t_ref[span(i, seq // 2), :].reshape(n_src, 1, p_len, width) for t_ref in (cos_t, sin_t))

                    def rope(v):
                        out = v.reshape(n_src, seqs, p_len, width) * cos + swap_halves(v, hd).reshape(n_src, seqs, p_len, width) * sin
                        return out.astype(BF16)

                    src = span(i, n_src)
                    q_ref[0, src] = rope(t[:, :width] * q_scale)
                    k_ref[0, src] = rope(t[:, width:2 * width])
                    v_ref[0, src] = t[:, 2 * width:].reshape(n_src, seqs, p_len, width).astype(BF16)

            slot3 = lambda rows, cols, f=lambda s: s: pl.BlockSpec((1, rows, cols), lambda s: (f(s), 0, 0))

            def pipe(body, **specs):
                def run(*refs):
                    with jax.named_scope(body.__name__):
                        pltpu.emit_pipeline(body, _explicit_indices=True, **specs)(*refs)

                return run

            pipe(qkv_step, grid=(n_tp,), in_specs=[slot3(n3, dim, arrival)],
                 out_specs=[pl.BlockSpec((1, n_tp, seqs, p_len, width), lambda s: (arrival(s), 0, 0, 0, 0))] * 3)(
                wq, q_hbm, k_hbm, v_hbm)

            srcs = qc // p_len
            lane = lax.broadcasted_iota(jnp.int32, (qc, width), 1)

            def attn_step(ps, q_ref, k_ref, v_ref):
                g, b = ps.index
                hooks(g * seqs + b, {
                    8: lambda: (net.got('dy_cross'), net.start('dy_fwd')), 9: lambda: (net.got('up'), net.start('ur', 'dc', 'dm', 'uf')),
                    14: lambda: (net.got('oc', 'or'), net.start('og', 'ol'))})
                bad = ok[b][:, 0:1] <= 0
                k = k_ref[0, :, 0].reshape(seq, width)
                v_t = v_ref[0, :, 0].reshape(seq, width).T
                for c in range(seq // qc):
                    src = slice(c * srcs, (c + 1) * srcs)
                    cols = slice(c * qc, (c + 1) * qc)
                    q = q_ref[0, src, 0].reshape(qc, width)
                    outs = []
                    for h in range(heads):
                        s = jnp.where(bad, NEG_LARGE, mm(k, jnp.where(lane // hd == h, q, jnp.zeros_like(q)), NT))
                        m = jnp.max(s, axis=0, keepdims=True)
                        e = jnp.exp(s - m)
                        r = 1.0 / col_sum(e)
                        outs.append(mm(v_t[h * hd:(h + 1) * hd], (e * r).astype(BF16), NN))
                        m_st[g, b, h:h + 1, cols] = m
                        l_st[g, b, h:h + 1, cols] = r
                    o4[src, b, :, span(g, width)] = jnp.concatenate(outs, axis=0).T.astype(BF16).reshape(srcs, p_len, width)

            head_blk = pl.BlockSpec((1, n_tp, 1, p_len, width), lambda g, b: (g, 0, b, 0, 0))
            pipe(attn_step, grid=(n_tp, seqs), in_specs=[head_blk] * 3)(q_hbm, k_hbm, v_hbm)

            net.got('om', 'of', 'og', 'ol')

            @pl.loop(0, tok // (2 * chunk))
            def _(i):
                rows = span(i, 2 * chunk)
                o = o4[pl.ds(2 * i, 2)].reshape(2 * chunk, n_tp * width)
                low = (x[rows, :].astype(F32) + (mm(o, wo[...].reshape(n_tp * width, dim), NN) + bias_o[...])).astype(BF16)
                x1[rows, :] = low
                x_hat, _ = ln_stats(low.astype(F32))
                h2[rows, :] = (x_hat * gain2[...] + bias2[...]).astype(BF16)

            net.start('h0', 'h1', 'dp')

            def gelu(pre):
                erf_term = lax.erf(pre * INV_SQRT2)
                act = (0.5 * pre * (1.0 + erf_term)).astype(BF16)
                return act, 0.5 * (1.0 + erf_term) + pre * jnp.exp(-0.5 * pre * pre) * INV_SQRT_2PI

            cols = lambda f: pl.BlockSpec((tok, ffn), lambda s: (0, f(s)))
            wu_spec, wd_spec = functools.partial(slot3, dim, ffn), functools.partial(slot3, ffn, dim)

            def mlp_up(n, f, table):
                def up_step(ps, w, act_ref, slope_ref):
                    s = ps.index[0]
                    hooks(s, table)

                    def body(rows):
                        act_ref[rows, :], slope_ref[rows, :] = gelu(mm(h2[rows, :], w[0], NN) + b_ffn[f(s)])

                    loop_rows(tok, half, body)

                pipe(up_step, grid=(n,), in_specs=[wu_spec(f)], out_specs=[cols(f)] * 2)(wu, act_hbm, slope_hbm)

            net.got('um', 'uf')
            mlp_up(n_tp - 2, arrival, {2: lambda: (net.got('uc'), net.start('ug')), 3: lambda: net.got('ug')})
            net.got('dy_pair', 'dy_fwd', 'dm')

            def backward(slot, w_d, w_u, act_ref, slope_ref, add):
                if add:
                    gb[slot] = jnp.zeros_like(gb[0])

                def body(rows):
                    d_pre = mm(dy[rows, :], w_d, NT) * slope_ref[rows, :]
                    low = d_pre.astype(BF16)
                    dpre[rows, :] = low
                    if add:
                        gb[slot] += col_sum(d_pre)
                        acc[rows, :] += mm(act_ref[rows, :], w_d, NN)
                        acc2[rows, :] += mm(low, w_u, NT)

                loop_rows(tok, half, body)

            def pair_gelu(rows, w_u, slot):
                return gelu(mm(h2p[rows, :], w_u, NN) + b_ffn[slot])

            def grads(chip, at, x_ref, between):
                f = lambda s: 2 * chip + 1 - s
                copy = to_partner(0, at, n_tp + at)

                def first(ps, w_u, act_ref):
                    s = ps.index[0]
                    rows = pl.ds(0, half)
                    act_p[rows, :] = pair_gelu(rows, w_u[0], f(s))[0]
                    p_snd[s] = mm(act_ref[...], dy[...], TN) + mm(act_p[rows, :], dyp[rows, :], TN)

                def second(ps, w_u):
                    s = ps.index[0]
                    pl.when(s == 1)(lambda: copy.start())
                    rows = pl.ds(half, half)
                    act_p[rows, :] = pair_gelu(rows, w_u[0], f(s))[0]
                    p_snd[s] += mm(act_p[rows, :], dyp[rows, :], TN)

                    @pl.when(s == 1)
                    def _():
                        copy.wait_recv()
                        add_sent(1, at)
                        keep(at, x_ref).start()
                        copy.wait_send()

                pipe(first, grid=(len(BOTH),), in_specs=[wu_spec(f), cols(f)])(wu, act_hbm)
                between()
                pipe(second, grid=(len(BOTH),), in_specs=[wu_spec(f)])(wu)
                keep(at, x_ref).wait()

            def mlp(n, f, add, table, last=None):
                def mlp_step(ps, wd_s, wu_s, act_ref, slope_ref):
                    s = ps.index[0]
                    backward(f(s), wd_s[0], wu_s[0], act_ref, slope_ref, add)
                    if last:
                        at, ref, send = last
                        copy = to_partner(0, at + 1, n_tp + at + 1)
                        pl.when(s == 1)(lambda: copy.start())

                        @pl.when(s < 2)
                        def _():
                            def body(rows):
                                dpre_p[rows, :] = (mm(dyp[rows, :], wd_s[0], NT) * pair_gelu(rows, wu_s[0], f(s))[1]).astype(BF16)

                            loop_rows(tok, half, body)
                            for i in BOTH:
                                part = pl.ds(i * half, half)
                                p_snd[s, pl.ds(0, ffn), part] = mm(h2[:, part], dpre[...], TN) + mm(h2p[:, part], dpre_p[...], TN)

                        @pl.when(s == 1)
                        def _():
                            copy.wait_recv()
                            add_sent(1, at + 1)
                            keep(at + 1, ref).start()
                            copy.wait_send()

                    hooks(s, table)

                pipe(mlp_step, grid=(n,), in_specs=[wd_spec(f), wu_spec(f), cols(f), cols(f)])(wd, wu, act_hbm, slope_hbm)

            acc[...] = jnp.zeros_like(acc)
            acc2[...] = jnp.zeros_like(acc2)
            mlp(2, lambda s: s, True, {})
            net.got('ur')
            net.start('ul')
            net.got('ul')
            mlp_up(2, lambda s: s + FAR0, {})
            net.got('h0')
            grads(CROSS, 0, x_dn, lambda: (net.got('dc'), net.start('dg', 'd0r', 'd1r'), net.got('h1')))
            net.start('dn_x')
            net.got('dg')

            def sent_up():
                keep(1, x_up).wait()
                net.start('up_x')

            slots = lambda s: jnp.where(s < 2, 2 * CROSS + 1 - s, s)
            mlp(n_chips, slots, True, {0: lambda: (net.got('dp'), net.start('df')), 1: lambda: net.got('df'), 2: sent_up}, (0, x_up, 'up_x'))

            for slot in (FAR0, FAR1):
                gb[slot] = jnp.zeros_like(gb[slot])

            def far_step(ps, w_u, act_ref, slope_ref):
                part, core = ps.index
                hooks(2 * part + core, {0: lambda: (net.got('d0r'), net.start('d0l')), 1: lambda: net.got('d0l'),
                                        2: lambda: (net.got('d1r'), net.start('d1l')), 3: lambda: net.got('d1l')})
                w_d = dx1b[pl.ds(pl.multiple_of(core * ffn + part * quarter, quarter), quarter), :]

                def body(rows):
                    d_pre = mm(dy[rows, :], w_d, NT) * slope_ref[rows, :]
                    gb[FAR0 + core, :, span(part, quarter)] += col_sum(d_pre)
                    acc[rows, :] += mm(act_ref[rows, :], w_d, NN)
                    acc2[rows, :] += mm(d_pre.astype(BF16), w_u[0], NT)

                loop_rows(tok, half, body)

            narrow = pl.BlockSpec((tok, quarter), lambda part, core: (0, 2 * (FAR0 + core) + part))
            pipe(far_step, grid=(len(BOTH),) * len(BOTH), in_specs=[pl.BlockSpec((1, dim, quarter), lambda part, core: (FAR0 + core, 0, part)), narrow, narrow])(
                wu, act_hbm, slope_hbm)

            def y_rows(rows):
                y[rows, :] = (x1[rows, :].astype(F32) + (acc[rows, :] + bias_d[...])).astype(BF16)

            loop_rows(tok, 2 * chunk, y_rows)
            vec[...] = jnp.zeros_like(vec)
            net.start('y', 'y_own')
            net.sent('d0l', 'd1l')

            @pl.loop(0, tok // (2 * chunk))
            def _(i):
                rows = span(i, 2 * chunk)
                x1_f, dy_f, dh = x1[rows, :].astype(F32), dy[rows, :].astype(F32), acc2[rows, :]
                x_hat, inv_std = ln_stats(x1_f)
                d_x1 = dy_f + ln_grad(dh, x_hat, inv_std, gain2[...])
                acc2[rows, :] = d_x1
                low = d_x1.astype(BF16)
                dx1b[rows, :] = low
                d_o = mm(low, wo[...].reshape(n_tp * width, dim), NT).astype(BF16)
                do4[pl.ds(2 * i, 2)] = d_o.reshape(2, seqs, p_len, n_tp * width)
                for n, t in enumerate((d_x1, dh * x_hat, dh, dy_f)):
                    vec[2 + n:3 + n, :] += col_sum(t)

            pair_begin()

            def bwd_step(ps, q_ref, k_ref, v_ref, w):
                step = ps.index[0]
                g = order(step)
                hooks(step, {2: lambda: (stored(0), net.start('at_relay0', 'at_relay1')),
                             4: lambda: (stored(1), net.start('at_early')), 6: lambda: (stored(2), pass_on(0, 0)), 7: lambda: pass_on(0, 2)})
                pair_go(step)
                b8[g] = jnp.zeros_like(b8[0])
                fold(gb[g], b8.at[g], 3)
                for b in range(seqs):
                    bad = ok[b][:, 0:1] <= 0
                    k = k_ref[0, :, b].reshape(seq, width)
                    v = v_ref[0, :, b].reshape(seq, width)
                    k_t = k.T
                    for c in range(seq // qc):
                        src = slice(c * srcs, (c + 1) * srcs)
                        at = slice(c * qc, (c + 1) * qc)
                        q = q_ref[0, src, b].reshape(qc, width)
                        d_o = do4[src, b, :, span(g, width)].reshape(qc, width)
                        dk = jnp.zeros((seq, width), F32)
                        dv = jnp.zeros((seq, width), F32)
                        dqs = []
                        for h in range(heads):
                            mine = lane // hd == h
                            q_h = jnp.where(mine, q, jnp.zeros_like(q))
                            do_h = jnp.where(mine, d_o, jnp.zeros_like(d_o))
                            s = jnp.where(bad, NEG_LARGE, mm(k, q_h, NT))
                            p = jnp.exp(s - m_st[g, b, h:h + 1, at]) * l_st[g, b, h:h + 1, at]
                            dv += mm(p.astype(BF16), do_h, NN)
                            dp = mm(v, do_h, NT)
                            ds = (p * (dp - col_sum(dp * p))).astype(BF16)
                            dk += mm(ds, q_h, NN)
                            dqs.append(mm(k_t[h * hd:(h + 1) * hd], ds, NN))
                        dq_acc[at, :] = jnp.concatenate(dqs, axis=0).T
                        dk_acc[...] = dk if c == 0 else dk_acc[...] + dk
                        dv_acc[...] = dv if c == 0 else dv_acc[...] + dv
                    cos, sin = cos_t[...], sin_t[...]
                    dq, dk, dv = dq_acc[...], dk_acc[...], dv_acc[...]
                    dq = (dq * cos - swap_halves(dq, hd) * sin) * q_scale
                    dk = dk * cos - swap_halves(dk, hd) * sin
                    for i, t in enumerate((dq, dk, dv)):
                        d4[:, b, :, i * width:(i + 1) * width] = t.astype(BF16).reshape(n_tp, p_len, width)
                        b8[g, i:i + 1, :] += col_sum(t)

                @pl.when(step == 0)
                def _():
                    acc[...] = jnp.zeros_like(acc)

                @pl.loop(0, 2)
                def _(i):
                    acc[span(i, half), :] += mm(d4[pl.ds(n_chips * i, n_chips)].reshape(half, n3), w[0], NN)

                def tile(put):
                    put((pl.ds(0, n3),), mm(d4[...].reshape(tok, n3), h1[...], TN))
                    put((pl.ds(n3, width),), mm(o4[:, :, :, span(g, width)].reshape(tok, width), dx1b[...], TN))

                pair(step, tile)
                hooks(step, {6: lambda: pass_on(0, 1)})

            slot_blk = pl.BlockSpec((1, n_tp, seqs, p_len, width), lambda s: (order(s), 0, 0, 0, 0))
            pipe(bwd_step, grid=(n_tp,), in_specs=[slot_blk] * 3 + [slot3(n3, dim, order)])(
                q_hbm, k_hbm, v_hbm, wq)

            pass_on(1, 0)

            def ln1_bwd(rows):
                x_hat, inv_std = ln_stats(x[rows, :].astype(F32))
                dh = acc[rows, :]
                h1[rows, :] = (acc2[rows, :] + ln_grad(dh, x_hat, inv_std, gain1[...])).astype(BF16)
                vec[0:1, :] += col_sum(dh * x_hat)
                vec[1:2, :] += col_sum(dh)

            loop_rows(tok, 2 * chunk, ln1_bwd)
            stored(3)
            for r in range(6):
                fold(vec[pl.ds(r, 1), :], v_own, r * n_tp)
            mate[0:v_half] = v_own[span(1 - side, v_half), :]
            for n in range(n_chips):
                mate[pl.ds(v_half + n * 8, 8)] = b8[2 * n + 1]
            net.start('mate')
            pass_on(1, 1)
            net.got('mate')
            v_sum = v_own[span(side, v_half), :] + mate_in[0:v_half]
            for n in range(n_chips):
                late[n, 0:v_half] = v_sum
                late[n, v_half:] = b8[2 * n] + mate_in[pl.ds(v_half + n * 8, 8)]
            net.start('late')
            pass_on(1, 2)
            net.start('gx', 'gx_own')

            net.sent('y')
            net.done('y_own')
            pair_begin()
            grads(0, 2, p_dn, lambda: None)
            mlp(2, lambda s: 1 - s, False, {}, (2, p_up, None))
            keep(3, p_up).wait()

            def total(refs, out, block, at):
                def body(*blocks):
                    v = blocks[1][...]
                    for more in blocks[2:-1]:
                        v += more[...]
                    blocks[-1][...] = v

                pipe(body, grid=(len(BOTH),), in_specs=[pl.BlockSpec(block, at)] * len(refs),
                     out_specs=[pl.BlockSpec(block, lambda i: (i, 0))])(*refs, out)

            by_row, by_col = lambda i: (i, 0), lambda i: (0, i)
            net.got('late')
            late_sum = late[0]
            for n in range(1, n_chips):
                late_sum += late_in[n]
            v_own[span(side, v_half), :] = late_sum[0:v_half]
            b8[0] = late_sum[v_half:]
            net.start('final')
            net.got('dn_x', 'up_x')
            total((p_dn, r_dn), g_down, (t_half, dim), by_row)
            total((p_up, r_up), g_up, (n_tile, half), by_col)
            net.got('at_early', 'at_sum0', 'at_sum1')
            for rows, out, n in ((pl.ds(0, n3), g_q, n3), (pl.ds(n3, width), g_o, width)):
                total((p_at.at[0, rows], early_at.at[rows], last_at.at[rows]), out, (n // 2, dim), by_row)
            for name in net.copies:
                if name not in ('load', 'store', 'own', 'write', 'gx', 'y', 'd0l', 'd1l') and not name.endswith(('_own', '_load', '_store')):
                    net.sent(name)
            net.got('y', 'final')
            net.start('write')
            net.done('gx_own', 'write')
            net.got('gx')
            net.sent('gx')

        big = (tok, dim)
        shapes = lambda *dims, dtype=F32: sds(dims, dtype)
        flat = lambda t: t.reshape(tok, dim)
        inv_freq = ROPE_BASE ** (-2.0 * np.arange(hd // 2) / hd)
        sign = np.repeat([-1.0, 1.0], hd // 2)
        freq = np.stack([np.tile(inv_freq, 2 * heads), np.tile(sign, heads)]).astype(np.float32)
        line = lambda v: v.reshape(1, -1)
        sem = lambda n: pltpu.SemaphoreType.DMA((n,))
        low = functools.partial(shapes, dtype=BF16)
        weights = [low(n_tp, n3, dim), low(n_tp, dim, ffn), low(n_tp, ffn, dim)]
        tiles = [shapes(n_chips, n_tile, dim)] + [shapes(n_tile, dim)] * 10
        out_shape = ([low(*big)] * 2 + [shapes(dim, ffn), shapes(ffn, dim), shapes(n3, dim), shapes(width, dim), shapes(6 * n_tp, LANES), shapes(8, LANES)] + weights
                     + [low(n_tp, n_tp, seqs, p_len, width)] * 3 + [low(tok, n_tp * ffn), shapes(tok, n_tp * ffn)] + tiles)
        plain = [pad_mask] + [line(v) for v in (ln1_gain, ln1_bias, b_out, ln2_gain, b_down, ln2_bias)] + [freq]
        heads4 = low(n_tp, seqs, p_len, n_tp * width)
        stat = shapes(n_tp, seqs, heads, seq)
        tile8 = shapes(n_tp, 8, LANES)
        late = shapes(n_chips, v_half + 8, LANES)
        mate = shapes(v_half + 8 * n_chips, LANES)
        row_ffn = shapes(n_tp, 1, ffn)
        scratch = ([low(*big)] * 9 + [heads4, heads4, low(n_tp, width, dim)] + [shapes(*big)] * 2
                   + [shapes(n_chips, n_tile, dim), shapes(2, n_tile, dim), low(n_tp, seqs, p_len, n3)]
                   + [shapes(seq, width)] * 5 + [shapes(seqs, seq, LANES), stat, stat, shapes(n_tp, 1, n3), row_ffn, row_ffn, row_ffn]
                   + [shapes(n_tp, *b_qkv.shape), tile8, late, late, shapes(8, dim), mate, mate, shapes(6 * n_tp, LANES)]
                   + [low(tok, ffn)] + plain)
        outs = pl.pallas_call(
            kernel, name='layer', out_shape=out_shape, in_specs=[ANY] * 16, out_specs=[ANY] * len(out_shape),
            scratch_shapes=[pltpu.VMEM(v.shape, v.dtype) for v in scratch]
            + [sem(91), sem(91), sem(30), sem(20), sem(12), pltpu.SemaphoreType.REGULAR],
            compiler_params=pltpu.CompilerParams(collective_id=0, has_side_effects=True, vmem_limit_bytes=VMEM_LIMIT),
        )(flat(x_in), flat(grad_y), w_qkv.transpose(0, 2, 3, 1).reshape(n3, dim), b_qkv, w_out.reshape(width, dim),
          w_up, line(b_up), w_down, *plain)

        def finish(*refs):
            src, (v_ref, b_ref), out, (bq_o, bu_o), v_o = refs[:6], refs[6:8], refs[8:14], refs[14:16], refs[16:]
            for a, b in zip(src, out):
                b[...] = a[...]
            for i in range(3):
                for h in range(heads):
                    bq_o[i, h:h + 1, :] = b_ref[i:i + 1, h * hd:(h + 1) * hd]
            unfold(b_ref, 3, bu_o)
            for r, ref in enumerate(v_o):
                unfold(v_ref, r * n_tp, ref)

        large = [low(*big)] * 2 + [shapes(dim, ffn), shapes(ffn, dim), shapes(n3, dim), shapes(width, dim)]
        small = [shapes(*b_qkv.shape), shapes(1, ffn)] + [shapes(1, dim)] * 6
        moving = [pl.BlockSpec((v.shape[0] // n_chips, v.shape[1]), lambda i: (i, 0)) for v in large]
        fixed = lambda vs: [pl.BlockSpec(v.shape, lambda i, n=len(v.shape): (0,) * n) for v in vs]
        res = pl.pallas_call(
            finish, name='finish', out_shape=large + small, grid=(n_chips,), in_specs=moving + fixed(outs[6:8]),
            out_specs=moving + fixed(small), compiler_params=pltpu.CompilerParams(vmem_limit_bytes=VMEM_LIMIT),
        )(*outs[:8])
        y_out, grad_x, grad_w_up, grad_w_down, gq, go, grad_b_qkv, grad_b_up = res[:8]
        v = [t.reshape(dim) for t in res[8:]]
        return (y_out.reshape(x_in.shape), grad_x.reshape(x_in.shape), v[0], v[1], gq.reshape(3, heads, hd, dim).transpose(0, 3, 1, 2),
                grad_b_qkv, go.reshape(heads, hd, dim), v[2], v[3], v[4], grad_w_up, grad_b_up.reshape(ffn), grad_w_down, v[5])

    return jax.shard_map(device_step, mesh=mesh, in_specs=in_specs, out_specs=out_specs, check_vma=False)
```

```python
import functools
import itertools

import jax
import jax.numpy as jnp
import numpy as np
from jax import lax
from jax.experimental import pallas as pl
from jax.experimental.pallas import tpu as pltpu
from jax.sharding import PartitionSpec as P

LN_EPS = 1e-5
ROPE_BASE = 10000.0
INV_SQRT2 = 0.7071067811865476
INV_SQRT_2PI = 0.3989422804014327
NEG_LARGE = -1e30
F32 = jnp.float32
BF16 = jnp.bfloat16
VMEM_LIMIT = 66_500_000
LANES = 128
NN = (((1,), (0,)), ((), ()))
NT = (((1,), (1,)), ((), ()))
TN = (((0,), (0,)), ((), ()))
PAIR, FAR, CROSS = 1, 2, 3
FAR0 = FAR + FAR
FAR1 = FAR0 + 1
BOTH = range(2)
ANY = pl.BlockSpec(memory_space=pl.ANY)


def mm(a, b, dims):
    return lax.dot_general(a, b, dims, preferred_element_type=F32)


def ln_stats(v):
    centered = v - jnp.mean(v, axis=-1, keepdims=True)
    inv_std = lax.rsqrt(jnp.mean(centered * centered, axis=-1, keepdims=True) + LN_EPS)
    return centered * inv_std, inv_std


def ln_grad(d_out, x_hat, inv_std, gain):
    d_hat = d_out * gain
    return inv_std * (d_hat - jnp.mean(d_hat, axis=-1, keepdims=True) - x_hat * jnp.mean(d_hat * x_hat, axis=-1, keepdims=True))


def col_sum(t):
    return jnp.sum(t, axis=0, keepdims=True)


def swap_halves(t, head_dim):
    half = head_dim // 2
    lane = lax.broadcasted_iota(jnp.int32, t.shape, t.ndim - 1)
    return jnp.where(lane % head_dim < half, pltpu.roll(t, t.shape[-1] - half, t.ndim - 1), pltpu.roll(t, half, t.ndim - 1))


def span(i, n):
    return pl.ds(pl.multiple_of(i * n, n), n)


def fold(row, out, first):
    for i in range(row.shape[-1] // LANES):
        out[pl.ds(first + i, 1), :] = row[:, i * LANES:(i + 1) * LANES]


def unfold(src, first, out):
    for i in range(out.shape[-1] // LANES):
        out[:, pl.ds(i * LANES, LANES)] = src[pl.ds(first + i, 1), :]


def loop_rows(total, n, body):
    @pl.loop(0, total // n)
    def _(i):
        body(span(i, n))


class Net:
    def __init__(self, n_tp, send, recv, local):
        self.n_tp, self.send, self.recv, self.local = n_tp, send, recv, local
        self.copies, self.count, self.n_local = {}, 0, 0

    def peer(self, chip, core=0):
        me = lax.axis_index('tp')
        way = 1 - 2 * lax.rem(lax.div(me, 2), 2)
        at = lax.rem(me + 2 * chip * way + self.n_tp, self.n_tp) if chip else me
        return at + 1 - 2 * lax.rem(at, 2) if core else at

    def add(self, name, src, dst, chip, core=0):
        n = self.count
        self.count += 1

        def make():
            return pltpu.make_async_remote_copy(
                src_ref=src(), dst_ref=dst(), send_sem=self.send.at[n], recv_sem=self.recv.at[n],
                device_id={'tp': self.peer(chip, core)}, device_id_type=pl.DeviceIdType.MESH)

        self.copies.setdefault(name, []).append(make)

    def add_local(self, name, src, dst):
        n = self.n_local
        self.n_local += 1
        self.copies.setdefault(name, []).append(lambda: pltpu.make_async_copy(src(), dst(), self.local.at[n]))

    def start(self, *names):
        for name in names:
            for make in self.copies[name]:
                make().start()

    def got(self, *names):
        for name in names:
            with jax.named_scope('got_' + name):
                for make in self.copies[name]:
                    make().wait_recv()

    def sent(self, *names):
        for name in names:
            for make in self.copies[name]:
                make().wait_send()

    def done(self, *names):
        for name in names:
            with jax.named_scope('done_' + name):
                for make in self.copies[name]:
                    make().wait()

    def gather(self, name, own, buf):
        for stage, chip in (('p', PAIR), ('c', CROSS)):
            self.add(name + stage, lambda: own, lambda c=chip: buf.at[2 * c], chip)
        self.add(name + 'm', lambda: own, lambda: buf.at[1], 0, 1)
        for stage, chip in (('f', PAIR), ('g', CROSS)):
            self.add(name + stage, lambda c=chip: buf.at[2 * c], lambda c=chip: buf.at[2 * c + 1], 0, 1)

    def gather_far(self, name, src, here, other, via):
        self.add(name + 'r', src, here, via)
        self.add(name + 'l', here, other, 0, 1)

    def exchange(self, name, src, dst, rows):
        me = lax.axis_index('tp')
        for core in BOTH:
            for chip in (PAIR, CROSS, FAR, 0):
                if chip + core:
                    self.add(name + '_far' * (chip == FAR), lambda c=chip, k=core: src.at[span(self.peer(c, k), rows)],
                             lambda: dst.at[span(me, rows)], chip, core)
        self.add_local(name + '_own', lambda: src.at[span(me, rows)], lambda: dst.at[span(me, rows)])

    def multicast(self, name, src, dst, pair_dst, rows):
        me = lax.axis_index('tp')
        at = lambda buf: (lambda: buf.at[span(me, rows)])
        other = {0: PAIR, PAIR: 0, CROSS: FAR}
        for chip, stage in ((CROSS, '_cross'), (PAIR, '_pair'), (0, '_pair')):
            for core in BOTH:
                if chip + core:
                    for c, buf in ((chip, dst), (other[chip], pair_dst)):
                        self.add(name + stage, lambda c=c, k=core: src.at[span(self.peer(c, k), rows)], at(buf), chip, core)
        for c, buf in ((0, dst), (PAIR, pair_dst)):
            self.add_local(name + '_own', lambda c=c: src.at[span(self.peer(c), rows)], at(buf))
        came = lambda buf: (lambda: buf.at[span(lax.div(self.peer(CROSS), 2), 2 * rows)])
        self.add(name + '_fwd', came(dst), came(pair_dst), PAIR)
        self.add(name + '_fwd', came(pair_dst), came(dst), PAIR)


def solution(mesh):
    n_tp = mesh.shape['tp']
    n_chips = n_tp // 2
    act_spec = P('dp', 'tp', None)
    rep_vec = P(None)
    part_vec = P('dp')
    in_specs = (act_spec, act_spec, P('dp', None), rep_vec, rep_vec, P(None, None, 'tp', None), P(None, 'tp', None),
                P('tp', None, None), rep_vec, rep_vec, rep_vec, P(None, 'tp'), P('tp'), P('tp', None), rep_vec)
    out_specs = (act_spec, act_spec, part_vec, part_vec, P('dp', None, 'tp', None), P('dp', 'tp', None),
                 P(('dp', 'tp'), None, None), part_vec, part_vec, part_vec, P('dp', 'tp'), P(('dp', 'tp')),
                 P(('dp', 'tp'), None), part_vec)

    def device_step(x_in, grad_y, pad_mask, ln1_gain, ln1_bias, w_qkv, b_qkv, w_out, b_out, ln2_gain, ln2_bias, w_up, b_up, w_down, b_down):
        batch, p_len, dim = x_in.shape
        seq = pad_mask.shape[1]
        _, _, heads, hd = w_qkv.shape
        seqs = batch // n_tp
        ffn = w_up.shape[1]
        width = heads * hd
        n3 = 3 * width
        tok = seqs * seq
        chunk = seqs * p_len
        qc = seq // 2
        q_scale = hd ** -0.5
        sds = jax.ShapeDtypeStruct
        n_tile = n3 + width
        half = dim // 2
        twice = n_tp + n_tp
        quarter = ffn // 2
        v_half = 3 * n_tp

        def kernel(*refs):
            it = iter(refs)
            take = lambda n: [next(it) for _ in range(n)]
            (x_ref, dy_ref, wq_ref, bq_ref, wo_ref, wu_ref, bu_ref, wd_ref), plain = take(8), take(8)
            y_out, gx_out, g_up, g_down, g_q, g_o, g_vec, g_b, wq, wu, wd, q_hbm, k_hbm, v_hbm, act_hbm, slope_hbm = take(16)
            p_at, got_at, sum_at, early_at, last_at, x_dn, x_up, p_dn, p_up, r_dn, r_up = take(11)
            x, h1, dy, x1, h2, dx1b, h2p, dyp, y, o4, do4, wo, acc, acc2, p_rcv, p_snd, d4 = take(17)
            dq_acc, dk_acc, dv_acc, cos_t, sin_t, ok, m_st, l_st, b_att, b_ffn, u_all, gb, b_all, b8, late, late_in, vec, mate, mate_in, v_own = take(20)
            dpre = next(it)
            act_p, dpre_p = (y.at[:, pl.ds(i * ffn, ffn)] for i in BOTH)
            here = take(8)
            send, recv, local, pair_send, pair_recv, pair_ready = take(6)
            net = Net(n_tp, send, recv, local)
            me = lax.axis_index('tp')
            mask_ref, gain1, bias1, bias_o, gain2, bias_d, bias2, freq_ref = here

            net.gather('q', wq_ref, wq)
            net.gather('o', wo_ref, wo)
            net.gather('u', wu_ref, wu)
            net.gather('d', wd_ref, wd)
            for name, buf in (('q', wq), ('o', wo), ('u', wu)):
                net.gather_far(name, lambda b=buf: b.at[2 * PAIR], lambda b=buf: b.at[FAR0], lambda b=buf: b.at[FAR1], CROSS)
            for i in BOTH:
                mine = lambda core, i=i: dx1b.at[pl.ds(core * ffn + i * quarter, quarter)]
                net.gather_far(f'd{i}', lambda i=i: wd.at[2 * CROSS, pl.ds(i * quarter, quarter)], lambda m=mine: m(0), lambda m=mine: m(1), PAIR)
            net.exchange('x', x_ref, x, chunk)
            net.multicast('dy', dy_ref, dy, dyp, chunk)
            net.exchange('y', y, y_out, chunk)
            net.exchange('gx', h1, gx_out, chunk)
            for chip in range(n_chips):
                for core in BOTH:
                    if chip + core:
                        slot = 2 * chip + core
                        net.add('bias' + '_far' * (chip == FAR), lambda: bq_ref, lambda n=slot: b_all.at[n], chip, core)
                        net.add('bias' + '_far' * (chip == FAR), lambda: bu_ref, lambda n=slot: u_all.at[n], chip, core)
            for chip in (PAIR, CROSS, FAR):
                net.add('late', lambda n=chip: late.at[n], lambda n=chip: late_in.at[n], chip)
            side = lax.rem(me, 2)
            net.add('mate', lambda: mate, lambda: mate_in, 0, 1)
            net.add('final', lambda: v_own.at[span(side, v_half)], lambda: v_own.at[span(side, v_half)], 0, 1)
            for i in BOTH:
                net.add(f'h{i}', lambda p=pl.ds(i * half, half): h2.at[p], lambda p=pl.ds(i * half, half): h2p.at[p], PAIR)
            net.add('dn_x', lambda: x_dn, lambda: r_dn, CROSS)
            net.add('up_x', lambda: x_up, lambda: r_up, CROSS)
            net.add('at_early', lambda: p_at.at[PAIR], lambda: early_at, PAIR)
            t_half = n_tile // 2
            for i, part in enumerate((pl.ds(0, t_half), pl.ds(t_half, t_half))):
                net.add(f'at_relay{i}', lambda p=part: p_at.at[FAR, p], lambda p=part: got_at.at[p], PAIR)
                net.add(f'at_sum{i}', lambda p=part: sum_at.at[p], lambda p=part: last_at.at[p], CROSS)
                net.add_local(f'at{i}_load', lambda p=part: got_at.at[p], lambda p=part: p_rcv.at[0, p])
                net.add_local(f'at{i}_load', lambda p=part: p_at.at[CROSS, p], lambda p=part: p_rcv.at[1, p])
                net.add_local(f'at{i}_store', lambda p=part: p_rcv.at[1, p], lambda p=part: sum_at.at[p])
            for src, dst in zip(plain, here):
                net.add_local('own', lambda r=src: r, lambda r=dst: r)
            net.add_local('write', lambda: v_own, lambda: g_vec)
            net.add_local('write', lambda: b8.at[0], lambda: g_b)
            for ref, tmp, buf in ((wq_ref, lambda: h2.at[pl.ds(0, n3)], wq), (wu_ref, lambda: x1.at[:, pl.ds(0, ffn)], wu),
                                        (wd_ref, lambda: dx1b.at[pl.ds(0, ffn)], wd)):
                net.add_local('load', lambda r=ref: r, tmp)
                net.add_local('store', tmp, lambda b=buf: b.at[0])
            net.add_local('own', lambda: wo_ref, lambda: wo.at[0])
            net.add_local('own', lambda: bq_ref, lambda: b_all.at[0])
            net.add_local('own', lambda: bu_ref, lambda: u_all.at[0])
            def pass_on(i, stage):
                if stage == 0:
                    net.got(f'at_relay{i}')
                    net.start(f'at{i}_load')
                elif stage == 1:
                    net.done(f'at{i}_load')

                    def body(rows):
                        rows = pl.ds(i * t_half + rows.start, rows.size)
                        p_rcv[1, rows] += p_rcv[0, rows]

                    loop_rows(t_half, 8, body)
                    net.start(f'at{i}_store')
                else:
                    net.done(f'at{i}_store')
                    net.start(f'at_sum{i}')

            def hooks(step, table):
                for at, act in table.items():
                    @pl.when(step == at)
                    def _(act=act):
                        act()

            tile_order = (FAR, PAIR, CROSS, 0)

            def place(i):
                return jnp.where(i == 0, FAR, jnp.where(i == 1, PAIR, jnp.where(i == 2, CROSS, 0)))

            def order(s):
                return 2 * place(lax.div(s, 2)) + 1 - lax.rem(s, 2)

            def to_partner(src, dst, sem):
                return pltpu.make_async_remote_copy(
                    src_ref=p_snd.at[src], dst_ref=p_rcv.at[dst], send_sem=pair_send.at[sem], recv_sem=pair_recv.at[sem],
                    device_id={'tp': net.peer(0, 1)}, device_id_type=pl.DeviceIdType.MESH)

            def keep(i, to):
                return pltpu.make_async_copy(p_rcv.at[i], to, pair_send.at[twice + i])

            def into(i):
                return lambda at, v: p_snd.__setitem__((i,) + at, v)

            def add_sent(i, j):
                def body(rows):
                    p_rcv[j, rows] += p_snd[i, rows]

                loop_rows(n_tile, 16, body)

            def pair_go(s):
                @pl.when(lax.rem(s, 2) == 1)
                def _():
                    to_partner(0, lax.div(s, 2), lax.div(s, 2)).start()

            def pair(s, tile):
                j = lax.div(s, 2)
                odd = lax.rem(s, 2)
                tile(into(odd))

                @pl.when(odd == 1)
                def _():
                    copy = to_partner(0, j, j)
                    copy.wait_send()
                    copy.wait_recv()
                    add_sent(1, j)
                    keep(j, p_at.at[place(j)]).start()

            def stored(i):
                keep(i, p_at.at[tile_order[i]]).wait()

            def pair_begin():
                pl.semaphore_signal(pair_ready, inc=1, device_id={'tp': net.peer(0, 1)}, device_id_type=pl.DeviceIdType.MESH)
                pl.semaphore_wait(pair_ready, 1)

            barrier = pltpu.get_barrier_semaphore()
            for chip in range(n_chips):
                for core in BOTH:
                    if chip + core and chip != FAR:
                        pl.semaphore_signal(barrier, inc=1, device_id={'tp': net.peer(chip, core)}, device_id_type=pl.DeviceIdType.MESH)
            pl.semaphore_wait(barrier, n_chips + 1)
            net.start('qp', 'qc', 'x', 'qm', 'bias', 'own', 'load', 'x_own', 'dy_own')
            net.done('own')
            angle = lax.broadcasted_iota(jnp.int32, (seq, width), 0).astype(F32) * freq_ref[0:1, :]
            cos_t[...] = jnp.cos(angle)
            sin_t[...] = jnp.sin(angle) * freq_ref[1:2, :]
            for b in range(seqs):
                row = mask_ref[pl.ds(me * seqs + b, 1), :].astype(F32)
                ok[b] = jnp.broadcast_to(row, (LANES, seq)).T
            net.done('load')
            net.start('store')
            net.got('qp', 'qc')
            net.start('x_far', 'bias_far', 'qr', 'dy_cross', 'oc', 'op', 'up', 'dy_pair', 'qf', 'qg', 'om')
            net.done('x_own', 'dy_own')
            net.got('bias', 'bias_far')
            for n in range(n_tp):
                b = b_all[n]
                b_att[n] = jnp.concatenate([b[i // heads, i % heads:i % heads + 1, :] for i in range(3 * heads)], axis=1)
                b_ffn[n] = u_all[n]
            net.got('x', 'x_far')

            def ln1(rows):
                x_hat, _ = ln_stats(x[rows, :].astype(F32))
                h1[rows, :] = (x_hat * gain1[...] + bias1[...]).astype(BF16)

            loop_rows(tok, chunk, ln1)
            net.done('store')
            net.got('qm', 'qf', 'qg')

            def arrival(s):
                return s + 2 * lax.div(s, n_chips) - n_chips * lax.div(s, n_chips + 2)

            def qkv_step(ps, w, q_ref, k_ref, v_ref):
                s = ps.index[0]
                hooks(s, {2: lambda: (net.got('op'), net.start('or', 'uc', 'um', 'of')), 4: lambda: (net.got('qr'), net.start('ql')),
                          5: lambda: net.got('ql')})
                n_src = tok // chunk // 2

                @pl.loop(0, 2)
                def _(i):
                    rows = span(i, tok // 2)
                    t = mm(h1[rows, :], w[0], NT) + b_att[arrival(s)]
                    cos, sin = (t_ref[span(i, seq // 2), :].reshape(n_src, 1, p_len, width) for t_ref in (cos_t, sin_t))

                    def rope(v):
                        out = v.reshape(n_src, seqs, p_len, width) * cos + swap_halves(v, hd).reshape(n_src, seqs, p_len, width) * sin
                        return out.astype(BF16)

                    src = span(i, n_src)
                    q_ref[0, src] = rope(t[:, :width] * q_scale)
                    k_ref[0, src] = rope(t[:, width:2 * width])
                    v_ref[0, src] = t[:, 2 * width:].reshape(n_src, seqs, p_len, width).astype(BF16)

            slot3 = lambda rows, cols, f=lambda s: s: pl.BlockSpec((1, rows, cols), lambda s: (f(s), 0, 0))

            def pipe(body, **specs):
                def run(*refs):
                    with jax.named_scope(body.__name__):
                        pltpu.emit_pipeline(body, _explicit_indices=True, **specs)(*refs)

                return run

            pipe(qkv_step, grid=(n_tp,), in_specs=[slot3(n3, dim, arrival)],
                 out_specs=[pl.BlockSpec((1, n_tp, seqs, p_len, width), lambda s: (arrival(s), 0, 0, 0, 0))] * 3)(
                wq, q_hbm, k_hbm, v_hbm)

            srcs = qc // p_len
            lane = lax.broadcasted_iota(jnp.int32, (qc, width), 1)

            def attn_step(ps, q_ref, k_ref, v_ref):
                g, b = ps.index
                hooks(g * seqs + b, {
                    8: lambda: (net.got('dy_cross'), net.start('dy_fwd')), 9: lambda: (net.got('up'), net.start('ur', 'dc', 'dm', 'uf')),
                    14: lambda: (net.got('oc', 'or'), net.start('og', 'ol'))})
                bad = ok[b][:, 0:1] <= 0
                k = k_ref[0, :, 0].reshape(seq, width)
                v_t = v_ref[0, :, 0].reshape(seq, width).T
                for c in range(seq // qc):
                    src = slice(c * srcs, (c + 1) * srcs)
                    cols = slice(c * qc, (c + 1) * qc)
                    q = q_ref[0, src, 0].reshape(qc, width)
                    outs = []
                    for h in range(heads):
                        s = jnp.where(bad, NEG_LARGE, mm(k, jnp.where(lane // hd == h, q, jnp.zeros_like(q)), NT))
                        m = jnp.max(s, axis=0, keepdims=True)
                        e = jnp.exp(s - m)
                        r = 1.0 / col_sum(e)
                        outs.append(mm(v_t[h * hd:(h + 1) * hd], (e * r).astype(BF16), NN))
                        m_st[g, b, h:h + 1, cols] = m
                        l_st[g, b, h:h + 1, cols] = r
                    o4[src, b, :, span(g, width)] = jnp.concatenate(outs, axis=0).T.astype(BF16).reshape(srcs, p_len, width)

            head_blk = pl.BlockSpec((1, n_tp, 1, p_len, width), lambda g, b: (g, 0, b, 0, 0))
            pipe(attn_step, grid=(n_tp, seqs), in_specs=[head_blk] * 3)(q_hbm, k_hbm, v_hbm)

            net.got('om', 'of', 'og', 'ol')

            @pl.loop(0, tok // (2 * chunk))
            def _(i):
                rows = span(i, 2 * chunk)
                o = o4[pl.ds(2 * i, 2)].reshape(2 * chunk, n_tp * width)
                low = (x[rows, :].astype(F32) + (mm(o, wo[...].reshape(n_tp * width, dim), NN) + bias_o[...])).astype(BF16)
                x1[rows, :] = low
                x_hat, _ = ln_stats(low.astype(F32))
                h2[rows, :] = (x_hat * gain2[...] + bias2[...]).astype(BF16)

            net.start('h0', 'h1', 'dp')

            def gelu(pre):
                erf_term = lax.erf(pre * INV_SQRT2)
                phi = 0.5 * (1.0 + erf_term)
                return (pre * phi).astype(BF16), phi + pre * jnp.exp(-0.5 * pre * pre) * INV_SQRT_2PI

            cols = lambda f: pl.BlockSpec((tok, ffn), lambda s: (0, f(s)))
            wu_spec, wd_spec = functools.partial(slot3, dim, ffn), functools.partial(slot3, ffn, dim)

            def mlp_up(n, f, table):
                def up_step(ps, w, act_ref, slope_ref):
                    s = ps.index[0]
                    hooks(s, table)

                    def body(rows):
                        act_ref[rows, :], slope_ref[rows, :] = gelu(mm(h2[rows, :], w[0], NN) + b_ffn[f(s)])

                    loop_rows(tok, half, body)

                pipe(up_step, grid=(n,), in_specs=[wu_spec(f)], out_specs=[cols(f)] * 2)(wu, act_hbm, slope_hbm)

            net.got('um', 'uf')
            mlp_up(n_tp - 2, arrival, {2: lambda: (net.got('uc'), net.start('ug')), 3: lambda: net.got('ug')})
            net.got('dy_pair', 'dy_fwd', 'dm')

            def backward(slot, w_d, w_u, act_ref, slope_ref, add):
                if add:
                    gb[slot] = jnp.zeros_like(gb[0])

                def body(rows):
                    d_pre = mm(dy[rows, :], w_d, NT) * slope_ref[rows, :]
                    low = d_pre.astype(BF16)
                    dpre[rows, :] = low
                    if add:
                        gb[slot] += col_sum(d_pre)
                        acc[rows, :] += mm(act_ref[rows, :], w_d, NN)
                        acc2[rows, :] += mm(low, w_u, NT)

                loop_rows(tok, half, body)

            def pair_gelu(rows, w_u, slot):
                return gelu(mm(h2p[rows, :], w_u, NN) + b_ffn[slot])

            def down_first(f):
                def first(ps, w_u, act_ref):
                    s = ps.index[0]
                    rows = pl.ds(0, half)
                    act_p[rows, :] = pair_gelu(rows, w_u[0], f(s))[0]
                    p_snd[s] = mm(act_ref[...], dy[...], TN) + mm(act_p[rows, :], dyp[rows, :], TN)

                pipe(first, grid=(len(BOTH),), in_specs=[wu_spec(f), cols(f)])(wu, act_hbm)

            def mlp(n, f, add, table, last=None):
                lead = len(BOTH) if last else 0
                f_u = (lambda s: jnp.where(s < lead, last[0](s), f(s - lead))) if last else f
                f_d = lambda s: f(jnp.maximum(s - lead, 0)) if not add else jnp.where(s < lead, 0, f(s - lead))

                def add_other(copy, to, ref):
                    copy.wait_recv()
                    add_sent(1, to)
                    keep(to, ref).start()
                    copy.wait_send()

                def mlp_step(ps, wd_s, wu_s, act_ref, slope_ref):
                    s = ps.index[0]

                    def work(t):
                        backward(f(t), wd_s[0], wu_s[0], act_ref, slope_ref, add)

                    if last:
                        _, at, down, up, begun = last
                        copies = [to_partner(0, at + i, n_tp + at + i) for i in BOTH]

                        @pl.when(s < lead)
                        def _():
                            hooks(s, table)
                            pl.when(s == 1)(lambda: copies[0].start())
                            rows = pl.ds(half, half)
                            act_p[rows, :] = pair_gelu(rows, wu_s[0], f_u(s))[0]
                            p_snd[s] += mm(act_p[rows, :], dyp[rows, :], TN)
                            pl.when(s == 1)(lambda: add_other(copies[0], at, down))

                        @pl.when(s >= lead)
                        def _():
                            t = s - lead
                            pl.when(t == 0)(lambda: begun())
                            pl.when(t == 1)(lambda: copies[1].start())
                            work(t)

                            @pl.when(t < lead)
                            def _():
                                def body(rows):
                                    dpre_p[rows, :] = (mm(dyp[rows, :], wd_s[0], NT) * pair_gelu(rows, wu_s[0], f(t))[1]).astype(BF16)

                                loop_rows(tok, half, body)
                                for i in BOTH:
                                    part = pl.ds(i * half, half)
                                    p_snd[t, pl.ds(0, ffn), part] = mm(h2[:, part], dpre[...], TN) + mm(h2p[:, part], dpre_p[...], TN)

                            pl.when(t == 1)(lambda: add_other(copies[1], at + 1, up))
                            hooks(s, table)
                    else:
                        work(s)
                        hooks(s, table)

                pipe(mlp_step, grid=(n + lead,), in_specs=[wd_spec(f_d), wu_spec(f_u), cols(f_d), cols(f_d)])(wd, wu, act_hbm, slope_hbm)

            acc[...] = jnp.zeros_like(acc)
            acc2[...] = jnp.zeros_like(acc2)
            mlp(1, lambda s: s, True, {})
            net.got('ur')
            net.start('ul')
            net.got('ul')
            mlp_up(2, lambda s: s + FAR0, {})
            net.got('h0')
            cross = lambda s: 2 * CROSS + 1 - s
            down_first(cross)

            def sent_down():
                keep(0, x_dn).wait()
                net.start('dn_x')

            def sent_up():
                keep(1, x_up).wait()
                net.start('up_x')

            mlp(n_chips + 1, lambda t: jnp.where(t < 2, cross(t), t - 1), True, {
                0: lambda: (net.got('dc'), net.start('dg', 'd0r', 'd1r'), net.got('h1', 'dg')),
                3: lambda: (net.got('dp'), net.start('df')), 4: lambda: net.got('df'), 5: sent_up}, (cross, 0, x_dn, x_up, sent_down))

            for slot in (FAR0, FAR1):
                gb[slot] = jnp.zeros_like(gb[slot])

            def far_step(ps, w_u, act_ref, slope_ref):
                part, core = ps.index
                hooks(2 * part + core, {0: lambda: (net.got('d0r'), net.start('d0l')), 1: lambda: net.got('d0l'),
                                        2: lambda: (net.got('d1r'), net.start('d1l')), 3: lambda: net.got('d1l')})
                w_d = dx1b[pl.ds(pl.multiple_of(core * ffn + part * quarter, quarter), quarter), :]

                def body(rows):
                    d_pre = mm(dy[rows, :], w_d, NT) * slope_ref[rows, :]
                    gb[FAR0 + core, :, span(part, quarter)] += col_sum(d_pre)
                    acc[rows, :] += mm(act_ref[rows, :], w_d, NN)
                    acc2[rows, :] += mm(d_pre.astype(BF16), w_u[0], NT)

                loop_rows(tok, half, body)

            narrow = pl.BlockSpec((tok, quarter), lambda part, core: (0, 2 * (FAR0 + core) + part))
            pipe(far_step, grid=(len(BOTH),) * len(BOTH), in_specs=[pl.BlockSpec((1, dim, quarter), lambda part, core: (FAR0 + core, 0, part)), narrow, narrow])(
                wu, act_hbm, slope_hbm)

            def y_rows(rows):
                y[rows, :] = (x1[rows, :].astype(F32) + (acc[rows, :] + bias_d[...])).astype(BF16)

            loop_rows(tok, 2 * chunk, y_rows)
            vec[...] = jnp.zeros_like(vec)
            net.start('y', 'y_far', 'y_own')
            net.sent('d0l', 'd1l')

            @pl.loop(0, tok // (2 * chunk))
            def _(i):
                rows = span(i, 2 * chunk)
                x1_f, dy_f, dh = x1[rows, :].astype(F32), dy[rows, :].astype(F32), acc2[rows, :]
                x_hat, inv_std = ln_stats(x1_f)
                d_x1 = dy_f + ln_grad(dh, x_hat, inv_std, gain2[...])
                acc2[rows, :] = d_x1
                low = d_x1.astype(BF16)
                dx1b[rows, :] = low
                d_o = mm(low, wo[...].reshape(n_tp * width, dim), NT).astype(BF16)
                do4[pl.ds(2 * i, 2)] = d_o.reshape(2, seqs, p_len, n_tp * width)
                for n, t in enumerate((d_x1, dh * x_hat, dh, dy_f)):
                    vec[2 + n:3 + n, :] += col_sum(t)

            pair_begin()

            def bwd_step(ps, q_ref, k_ref, v_ref, w):
                step = ps.index[0]
                g = order(step)
                hooks(step, {2: lambda: (stored(0), net.start('at_relay0', 'at_relay1')),
                             4: lambda: (stored(1), net.start('at_early')), 6: lambda: (stored(2), pass_on(0, 0)), 7: lambda: pass_on(0, 2)})
                pair_go(step)
                b8[g] = jnp.zeros_like(b8[0])
                fold(gb[g], b8.at[g], 3)
                for b in range(seqs):
                    bad = ok[b][:, 0:1] <= 0
                    k = k_ref[0, :, b].reshape(seq, width)
                    v = v_ref[0, :, b].reshape(seq, width)
                    k_t = k.T
                    for c in range(seq // qc):
                        src = slice(c * srcs, (c + 1) * srcs)
                        at = slice(c * qc, (c + 1) * qc)
                        q = q_ref[0, src, b].reshape(qc, width)
                        d_o = do4[src, b, :, span(g, width)].reshape(qc, width)
                        dk = jnp.zeros((seq, width), F32)
                        dv = jnp.zeros((seq, width), F32)
                        dqs = []
                        for h in range(heads):
                            mine = lane // hd == h
                            q_h = jnp.where(mine, q, jnp.zeros_like(q))
                            do_h = jnp.where(mine, d_o, jnp.zeros_like(d_o))
                            s = jnp.where(bad, NEG_LARGE, mm(k, q_h, NT))
                            p = jnp.exp(s - m_st[g, b, h:h + 1, at]) * l_st[g, b, h:h + 1, at]
                            dv += mm(p.astype(BF16), do_h, NN)
                            dp = mm(v, do_h, NT)
                            ds = (p * (dp - col_sum(dp * p))).astype(BF16)
                            dk += mm(ds, q_h, NN)
                            dqs.append(mm(k_t[h * hd:(h + 1) * hd], ds, NN))
                        dq_acc[at, :] = jnp.concatenate(dqs, axis=0).T
                        dk_acc[...] = dk if c == 0 else dk_acc[...] + dk
                        dv_acc[...] = dv if c == 0 else dv_acc[...] + dv
                    cos, sin = cos_t[...], sin_t[...]
                    dq, dk, dv = dq_acc[...], dk_acc[...], dv_acc[...]
                    dq = (dq * cos - swap_halves(dq, hd) * sin) * q_scale
                    dk = dk * cos - swap_halves(dk, hd) * sin
                    for i, t in enumerate((dq, dk, dv)):
                        d4[:, b, :, i * width:(i + 1) * width] = t.astype(BF16).reshape(n_tp, p_len, width)
                        b8[g, i:i + 1, :] += col_sum(t)

                @pl.when(step == 0)
                def _():
                    acc[...] = jnp.zeros_like(acc)

                @pl.loop(0, 2)
                def _(i):
                    acc[span(i, half), :] += mm(d4[pl.ds(n_chips * i, n_chips)].reshape(half, n3), w[0], NN)

                def tile(put):
                    put((pl.ds(0, n3),), mm(d4[...].reshape(tok, n3), h1[...], TN))
                    put((pl.ds(n3, width),), mm(o4[:, :, :, span(g, width)].reshape(tok, width), dx1b[...], TN))

                pair(step, tile)
                hooks(step, {6: lambda: pass_on(0, 1)})

            slot_blk = pl.BlockSpec((1, n_tp, seqs, p_len, width), lambda s: (order(s), 0, 0, 0, 0))
            pipe(bwd_step, grid=(n_tp,), in_specs=[slot_blk] * 3 + [slot3(n3, dim, order)])(
                q_hbm, k_hbm, v_hbm, wq)

            pass_on(1, 0)

            def ln1_bwd(rows):
                x_hat, inv_std = ln_stats(x[rows, :].astype(F32))
                dh = acc[rows, :]
                h1[rows, :] = (acc2[rows, :] + ln_grad(dh, x_hat, inv_std, gain1[...])).astype(BF16)
                vec[0:1, :] += col_sum(dh * x_hat)
                vec[1:2, :] += col_sum(dh)

            loop_rows(tok, 2 * chunk, ln1_bwd)
            stored(3)
            for r in range(6):
                fold(vec[pl.ds(r, 1), :], v_own, r * n_tp)
            mate[0:v_half] = v_own[span(1 - side, v_half), :]
            for n in range(n_chips):
                mate[pl.ds(v_half + n * 8, 8)] = b8[2 * n + 1]
            net.start('mate')
            pass_on(1, 1)
            net.got('mate')
            v_sum = v_own[span(side, v_half), :] + mate_in[0:v_half]
            for n in range(n_chips):
                late[n, 0:v_half] = v_sum
                late[n, v_half:] = b8[2 * n] + mate_in[pl.ds(v_half + n * 8, 8)]
            net.start('late')
            pass_on(1, 2)
            net.start('gx', 'gx_far', 'gx_own')

            net.sent('y', 'y_far')
            net.done('y_own')
            pair_begin()
            mine = lambda s: 1 - s
            down_first(mine)
            mlp(2, mine, False, {}, (mine, 2, p_dn, p_up, lambda: None))
            for i, ref in enumerate((p_dn, p_up)):
                keep(2 + i, ref).wait()

            def total(refs, out, block, at):
                def body(*blocks):
                    v = blocks[1][...]
                    for more in blocks[2:-1]:
                        v += more[...]
                    blocks[-1][...] = v

                pipe(body, grid=(len(BOTH),), in_specs=[pl.BlockSpec(block, at)] * len(refs),
                     out_specs=[pl.BlockSpec(block, lambda i: (i, 0))])(*refs, out)

            by_row, by_col = lambda i: (i, 0), lambda i: (0, i)
            net.got('late')
            late_sum = late[0]
            for n in range(1, n_chips):
                late_sum += late_in[n]
            v_own[span(side, v_half), :] = late_sum[0:v_half]
            b8[0] = late_sum[v_half:]
            net.start('final')
            net.got('dn_x', 'up_x')
            total((p_dn, r_dn), g_down, (t_half, dim), by_row)
            total((p_up, r_up), g_up, (n_tile, half), by_col)
            net.got('at_early', 'at_sum0', 'at_sum1')
            for rows, out, n in ((pl.ds(0, n3), g_q, n3), (pl.ds(n3, width), g_o, width)):
                total((p_at.at[0, rows], early_at.at[rows], last_at.at[rows]), out, (n // 2, dim), by_row)
            for name in net.copies:
                if name not in ('load', 'store', 'own', 'write', 'gx', 'gx_far', 'y', 'y_far', 'd0l', 'd1l') and not name.endswith(('_own', '_load', '_store')):
                    net.sent(name)
            net.got('y', 'y_far', 'final')
            net.start('write')
            net.done('gx_own', 'write')
            net.got('gx', 'gx_far')
            net.sent('gx', 'gx_far')

        big = (tok, dim)
        shapes = lambda *dims, dtype=F32: sds(dims, dtype)
        flat = lambda t: t.reshape(tok, dim)
        inv_freq = ROPE_BASE ** (-2.0 * np.arange(hd // 2) / hd)
        sign = np.repeat([-1.0, 1.0], hd // 2)
        freq = np.stack([np.tile(inv_freq, 2 * heads), np.tile(sign, heads)]).astype(np.float32)
        line = lambda v: v.reshape(1, -1)
        sem = lambda n: pltpu.SemaphoreType.DMA((n,))
        low = functools.partial(shapes, dtype=BF16)
        weights = [low(n_tp, n3, dim), low(n_tp, dim, ffn), low(n_tp, ffn, dim)]
        tiles = [shapes(n_chips, n_tile, dim)] + [shapes(n_tile, dim)] * 10
        out_shape = ([low(*big)] * 2 + [shapes(dim, ffn), shapes(ffn, dim), shapes(n3, dim), shapes(width, dim), shapes(6 * n_tp, LANES), shapes(8, LANES)] + weights
                     + [low(n_tp, n_tp, seqs, p_len, width)] * 3 + [low(tok, n_tp * ffn), shapes(tok, n_tp * ffn)] + tiles)
        plain = [pad_mask] + [line(v) for v in (ln1_gain, ln1_bias, b_out, ln2_gain, b_down, ln2_bias)] + [freq]
        heads4 = low(n_tp, seqs, p_len, n_tp * width)
        stat = shapes(n_tp, seqs, heads, seq)
        tile8 = shapes(n_tp, 8, LANES)
        late = shapes(n_chips, v_half + 8, LANES)
        mate = shapes(v_half + 8 * n_chips, LANES)
        row_ffn = shapes(n_tp, 1, ffn)
        scratch = ([low(*big)] * 9 + [heads4, heads4, low(n_tp, width, dim)] + [shapes(*big)] * 2
                   + [shapes(n_chips, n_tile, dim), shapes(2, n_tile, dim), low(n_tp, seqs, p_len, n3)]
                   + [shapes(seq, width)] * 5 + [shapes(seqs, seq, LANES), stat, stat, shapes(n_tp, 1, n3), row_ffn, row_ffn, row_ffn]
                   + [shapes(n_tp, *b_qkv.shape), tile8, late, late, shapes(8, dim), mate, mate, shapes(6 * n_tp, LANES)]
                   + [low(tok, ffn)] + plain)
        outs = pl.pallas_call(
            kernel, name='layer', out_shape=out_shape, in_specs=[ANY] * 16, out_specs=[ANY] * len(out_shape),
            scratch_shapes=[pltpu.VMEM(v.shape, v.dtype) for v in scratch]
            + [sem(91), sem(91), sem(30), sem(20), sem(12), pltpu.SemaphoreType.REGULAR],
            compiler_params=pltpu.CompilerParams(collective_id=0, has_side_effects=True, vmem_limit_bytes=VMEM_LIMIT),
        )(flat(x_in), flat(grad_y), w_qkv.transpose(0, 2, 3, 1).reshape(n3, dim), b_qkv, w_out.reshape(width, dim),
          w_up, line(b_up), w_down, *plain)

        def finish(*refs):
            it = iter(refs)
            n = len(large)
            src, (v_ref, b_ref), out, (bq_o, bu_o), v_o = (list(itertools.islice(it, k)) for k in (n, 2, n, 2, n))
            for a, b in zip(src, out):
                b[...] = a[...]
            for i in range(3):
                for h in range(heads):
                    bq_o[i, h:h + 1, :] = b_ref[i:i + 1, h * hd:(h + 1) * hd]
            unfold(b_ref, 3, bu_o)
            for r, ref in enumerate(v_o):
                unfold(v_ref, r * n_tp, ref)

        large = [low(*big)] * 2 + [shapes(dim, ffn), shapes(ffn, dim), shapes(n3, dim), shapes(width, dim)]
        small = [shapes(*b_qkv.shape), shapes(1, ffn)] + [shapes(1, dim)] * 6
        moving = [pl.BlockSpec((v.shape[0] // n_chips, v.shape[1]), lambda i: (i, 0)) for v in large]
        fixed = lambda vs: [pl.BlockSpec(v.shape, lambda i, n=len(v.shape): (0,) * n) for v in vs]
        res = pl.pallas_call(
            finish, name='finish', out_shape=large + small, grid=(n_chips,), in_specs=moving + fixed(outs[6:8]),
            out_specs=moving + fixed(small), compiler_params=pltpu.CompilerParams(vmem_limit_bytes=VMEM_LIMIT),
        )(*outs[:8])
        y_out, grad_x, grad_w_up, grad_w_down, gq, go, grad_b_qkv, grad_b_up = res[:8]
        v = [t.reshape(dim) for t in res[8:]]
        return (y_out.reshape(x_in.shape), grad_x.reshape(x_in.shape), v[0], v[1], gq.reshape(3, heads, hd, dim).transpose(0, 3, 1, 2),
                grad_b_qkv, go.reshape(heads, hd, dim), v[2], v[3], v[4], grad_w_up, grad_b_up.reshape(ffn), grad_w_down, v[5])

    return jax.shard_map(device_step, mesh=mesh, in_specs=in_specs, out_specs=out_specs, check_vma=False)
```

```python
import functools
import itertools

import jax
import jax.numpy as jnp
import numpy as np
from jax import lax
from jax.experimental import pallas as pl
from jax.experimental.pallas import tpu as pltpu
from jax.sharding import PartitionSpec as P

LN_EPS = 1e-5
ROPE_BASE = 10000.0
INV_SQRT2 = 0.7071067811865476
INV_SQRT_2PI = 0.3989422804014327
NEG_LARGE = -1e30
F32 = jnp.float32
BF16 = jnp.bfloat16
VMEM_LIMIT = 66_500_000
LANES = 128
NN = (((1,), (0,)), ((), ()))
NT = (((1,), (1,)), ((), ()))
TN = (((0,), (0,)), ((), ()))
PAIR, FAR, CROSS = 1, 2, 3
FAR0 = FAR + FAR
FAR1 = FAR0 + 1
BOTH = range(2)
ANY = pl.BlockSpec(memory_space=pl.ANY)


def mm(a, b, dims):
    return lax.dot_general(a, b, dims, preferred_element_type=F32)


def ln_stats(v):
    centered = v - jnp.mean(v, axis=-1, keepdims=True)
    inv_std = lax.rsqrt(jnp.mean(centered * centered, axis=-1, keepdims=True) + LN_EPS)
    return centered * inv_std, inv_std


def ln_grad(d_out, x_hat, inv_std, gain):
    d_hat = d_out * gain
    return inv_std * (d_hat - jnp.mean(d_hat, axis=-1, keepdims=True) - x_hat * jnp.mean(d_hat * x_hat, axis=-1, keepdims=True))


def col_sum(t):
    return jnp.sum(t, axis=0, keepdims=True)


def swap_halves(t, head_dim):
    half = head_dim // 2
    lane = lax.broadcasted_iota(jnp.int32, t.shape, t.ndim - 1)
    return jnp.where(lane % head_dim < half, pltpu.roll(t, t.shape[-1] - half, t.ndim - 1), pltpu.roll(t, half, t.ndim - 1))


def span(i, n):
    return pl.ds(pl.multiple_of(i * n, n), n)


def fold(row, out, first):
    for i in range(row.shape[-1] // LANES):
        out[pl.ds(first + i, 1), :] = row[:, i * LANES:(i + 1) * LANES]


def unfold(src, first, out):
    for i in range(out.shape[-1] // LANES):
        out[:, pl.ds(i * LANES, LANES)] = src[pl.ds(first + i, 1), :]


def loop_rows(total, n, body):
    @pl.loop(0, total // n)
    def _(i):
        body(span(i, n))


class Net:
    def __init__(self, n_tp, send, recv, local):
        self.n_tp, self.send, self.recv, self.local = n_tp, send, recv, local
        self.copies, self.count, self.n_local = {}, 0, 0

    def peer(self, chip, core=0):
        me = lax.axis_index('tp')
        way = 1 - 2 * lax.rem(lax.div(me, 2), 2)
        at = lax.rem(me + 2 * chip * way + self.n_tp, self.n_tp) if chip else me
        return at + 1 - 2 * lax.rem(at, 2) if core else at

    def add(self, name, src, dst, chip, core=0):
        n = self.count
        self.count += 1

        def make():
            return pltpu.make_async_remote_copy(
                src_ref=src(), dst_ref=dst(), send_sem=self.send.at[n], recv_sem=self.recv.at[n],
                device_id={'tp': self.peer(chip, core)}, device_id_type=pl.DeviceIdType.MESH)

        self.copies.setdefault(name, []).append(make)

    def add_local(self, name, src, dst):
        n = self.n_local
        self.n_local += 1
        self.copies.setdefault(name, []).append(lambda: pltpu.make_async_copy(src(), dst(), self.local.at[n]))

    def start(self, *names):
        for name in names:
            for make in self.copies[name]:
                make().start()

    def got(self, *names):
        for name in names:
            with jax.named_scope('got_' + name):
                for make in self.copies[name]:
                    make().wait_recv()

    def sent(self, *names):
        for name in names:
            for make in self.copies[name]:
                make().wait_send()

    def done(self, *names):
        for name in names:
            with jax.named_scope('done_' + name):
                for make in self.copies[name]:
                    make().wait()

    def gather(self, name, own, buf):
        for stage, chip in (('p', PAIR), ('c', CROSS)):
            self.add(name + stage, lambda: own, lambda c=chip: buf.at[2 * c], chip)
        self.add(name + 'm', lambda: own, lambda: buf.at[1], 0, 1)
        for stage, chip in (('f', PAIR), ('g', CROSS)):
            self.add(name + stage, lambda c=chip: buf.at[2 * c], lambda c=chip: buf.at[2 * c + 1], 0, 1)

    def gather_far(self, name, src, here, other, via):
        self.add(name + 'r', src, here, via)
        self.add(name + 'l', here, other, 0, 1)

    def exchange(self, name, src, dst, rows):
        me = lax.axis_index('tp')
        for core in BOTH:
            for chip in (PAIR, CROSS, FAR, 0):
                if chip + core:
                    self.add(name + '_far' * (chip == FAR), lambda c=chip, k=core: src.at[span(self.peer(c, k), rows)],
                             lambda: dst.at[span(me, rows)], chip, core)
        self.add_local(name + '_own', lambda: src.at[span(me, rows)], lambda: dst.at[span(me, rows)])

    def multicast(self, name, src, dst, pair_dst, rows):
        me = lax.axis_index('tp')
        at = lambda buf: (lambda: buf.at[span(me, rows)])
        other = {0: PAIR, PAIR: 0, CROSS: FAR}
        for chip, stage in ((CROSS, '_cross'), (PAIR, '_pair'), (0, '_pair')):
            for core in BOTH:
                if chip + core:
                    for c, buf in ((chip, dst), (other[chip], pair_dst)):
                        self.add(name + stage, lambda c=c, k=core: src.at[span(self.peer(c, k), rows)], at(buf), chip, core)
        for c, buf in ((0, dst), (PAIR, pair_dst)):
            self.add_local(name + '_own', lambda c=c: src.at[span(self.peer(c), rows)], at(buf))
        came = lambda buf: (lambda: buf.at[span(lax.div(self.peer(CROSS), 2), 2 * rows)])
        self.add(name + '_fwd', came(dst), came(pair_dst), PAIR)
        self.add(name + '_fwd', came(pair_dst), came(dst), PAIR)


def solution(mesh):
    n_tp = mesh.shape['tp']
    n_chips = n_tp // 2
    act_spec = P('dp', 'tp', None)
    rep_vec = P(None)
    part_vec = P('dp')
    in_specs = (act_spec, act_spec, P('dp', None), rep_vec, rep_vec, P(None, None, 'tp', None), P(None, 'tp', None),
                P('tp', None, None), rep_vec, rep_vec, rep_vec, P(None, 'tp'), P('tp'), P('tp', None), rep_vec)
    out_specs = (act_spec, act_spec, part_vec, part_vec, P('dp', None, 'tp', None), P('dp', 'tp', None),
                 P(('dp', 'tp'), None, None), part_vec, part_vec, part_vec, P('dp', 'tp'), P(('dp', 'tp')),
                 P(('dp', 'tp'), None), part_vec)

    def device_step(x_in, grad_y, pad_mask, ln1_gain, ln1_bias, w_qkv, b_qkv, w_out, b_out, ln2_gain, ln2_bias, w_up, b_up, w_down, b_down):
        batch, p_len, dim = x_in.shape
        seq = pad_mask.shape[1]
        _, _, heads, hd = w_qkv.shape
        seqs = batch // n_tp
        ffn = w_up.shape[1]
        width = heads * hd
        n3 = 3 * width
        tok = seqs * seq
        chunk = seqs * p_len
        qc = seq // 2
        q_scale = hd ** -0.5
        sds = jax.ShapeDtypeStruct
        n_tile = n3 + width
        half = dim // 2
        twice = n_tp + n_tp
        quarter = ffn // 2
        v_half = 3 * n_tp

        def kernel(*refs):
            it = iter(refs)
            take = lambda n: [next(it) for _ in range(n)]
            (x_ref, dy_ref, wq_ref, bq_ref, wo_ref, wu_ref, bu_ref, wd_ref), plain = take(8), take(8)
            y_out, gx_out, g_up, g_down, g_q, g_o, g_vec, g_b, wq, wu, wd, q_hbm, k_hbm, v_hbm, act_hbm, slope_hbm = take(16)
            p_at, got_at, sum_at, early_at, last_at, x_dn, x_up, p_dn, p_up, r_dn, r_up = take(11)
            x, h1, dy, x1, h2, dx1b, h2p, dyp, y, o4, do4, wo, acc, acc2, p_rcv, p_snd, d4 = take(17)
            dq_acc, dk_acc, dv_acc, cos_t, sin_t, ok, m_st, l_st, b_att, b_ffn, u_all, gb, b_all, b8, late, late_in, vec, mate, mate_in, v_own = take(20)
            dpre = next(it)
            act_p, dpre_p = (y.at[:, pl.ds(i * ffn, ffn)] for i in BOTH)
            here = take(8)
            send, recv, local, pair_send, pair_recv, pair_ready = take(6)
            net = Net(n_tp, send, recv, local)
            me = lax.axis_index('tp')
            mask_ref, gain1, bias1, bias_o, gain2, bias_d, bias2, freq_ref = here

            net.gather('q', wq_ref, wq)
            net.gather('o', wo_ref, wo)
            net.gather('u', wu_ref, wu)
            net.gather('d', wd_ref, wd)
            for name, buf in (('q', wq), ('o', wo), ('u', wu)):
                net.gather_far(name, lambda b=buf: b.at[2 * PAIR], lambda b=buf: b.at[FAR0], lambda b=buf: b.at[FAR1], CROSS)
            for i in BOTH:
                mine = lambda core, i=i: dx1b.at[pl.ds(core * ffn + i * quarter, quarter)]
                net.gather_far(f'd{i}', lambda i=i: wd.at[2 * CROSS, pl.ds(i * quarter, quarter)], lambda m=mine: m(0), lambda m=mine: m(1), PAIR)
            net.exchange('x', x_ref, x, chunk)
            net.multicast('dy', dy_ref, dy, dyp, chunk)
            net.exchange('y', y, y_out, chunk)
            net.exchange('gx', h1, gx_out, chunk)
            for chip in range(n_chips):
                for core in BOTH:
                    if chip + core:
                        slot = 2 * chip + core
                        net.add('bias' + '_far' * (chip == FAR), lambda: bq_ref, lambda n=slot: b_all.at[n], chip, core)
                        net.add('bias' + '_far' * (chip == FAR), lambda: bu_ref, lambda n=slot: u_all.at[n], chip, core)
            for chip in (PAIR, CROSS, FAR):
                net.add('late', lambda n=chip: late.at[n], lambda n=chip: late_in.at[n], chip)
            side = lax.rem(me, 2)
            net.add('mate', lambda: mate, lambda: mate_in, 0, 1)
            net.add('final', lambda: v_own.at[span(side, v_half)], lambda: v_own.at[span(side, v_half)], 0, 1)
            for i in BOTH:
                net.add(f'h{i}', lambda p=pl.ds(i * half, half): h2.at[p], lambda p=pl.ds(i * half, half): h2p.at[p], PAIR)
            net.add('dn_x', lambda: x_dn, lambda: r_dn, CROSS)
            net.add('up_x', lambda: x_up, lambda: r_up, CROSS)
            net.add('at_early', lambda: p_at.at[PAIR], lambda: early_at, PAIR)
            t_half = n_tile // 2
            for i, part in enumerate((pl.ds(0, t_half), pl.ds(t_half, t_half))):
                net.add(f'at_relay{i}', lambda p=part: p_at.at[FAR, p], lambda p=part: got_at.at[p], PAIR)
                net.add(f'at_sum{i}', lambda p=part: sum_at.at[p], lambda p=part: last_at.at[p], CROSS)
                net.add_local(f'at{i}_load', lambda p=part: got_at.at[p], lambda p=part: p_rcv.at[0, p])
                net.add_local(f'at{i}_load', lambda p=part: p_at.at[CROSS, p], lambda p=part: p_rcv.at[1, p])
                net.add_local(f'at{i}_store', lambda p=part: p_rcv.at[1, p], lambda p=part: sum_at.at[p])
            for src, dst in zip(plain, here):
                net.add_local('own', lambda r=src: r, lambda r=dst: r)
            net.add_local('write', lambda: v_own, lambda: g_vec)
            net.add_local('write', lambda: b8.at[0], lambda: g_b)
            for ref, tmp, buf in ((wq_ref, lambda: h2.at[pl.ds(0, n3)], wq), (wu_ref, lambda: x1.at[:, pl.ds(0, ffn)], wu),
                                        (wd_ref, lambda: dx1b.at[pl.ds(0, ffn)], wd)):
                net.add_local('load', lambda r=ref: r, tmp)
                net.add_local('store', tmp, lambda b=buf: b.at[0])
            net.add_local('own', lambda: wo_ref, lambda: wo.at[0])
            net.add_local('own', lambda: bq_ref, lambda: b_all.at[0])
            net.add_local('own', lambda: bu_ref, lambda: u_all.at[0])
            def pass_on(i, stage):
                if stage == 0:
                    net.got(f'at_relay{i}')
                    net.start(f'at{i}_load')
                elif stage == 1:
                    net.done(f'at{i}_load')

                    def body(rows):
                        rows = pl.ds(i * t_half + rows.start, rows.size)
                        p_rcv[1, rows] += p_rcv[0, rows]

                    loop_rows(t_half, 8, body)
                    net.start(f'at{i}_store')
                else:
                    net.done(f'at{i}_store')
                    net.start(f'at_sum{i}')

            def hooks(step, table):
                for at, act in table.items():
                    @pl.when(step == at)
                    def _(act=act):
                        act()

            tile_order = (FAR, PAIR, CROSS, 0)

            def place(i):
                return jnp.where(i == 0, FAR, jnp.where(i == 1, PAIR, jnp.where(i == 2, CROSS, 0)))

            def order(s):
                return 2 * place(lax.div(s, 2)) + 1 - lax.rem(s, 2)

            def to_partner(src, dst, sem):
                return pltpu.make_async_remote_copy(
                    src_ref=p_snd.at[src], dst_ref=p_rcv.at[dst], send_sem=pair_send.at[sem], recv_sem=pair_recv.at[sem],
                    device_id={'tp': net.peer(0, 1)}, device_id_type=pl.DeviceIdType.MESH)

            def keep(i, to):
                return pltpu.make_async_copy(p_rcv.at[i], to, pair_send.at[twice + i])

            def into(i):
                return lambda at, v: p_snd.__setitem__((i,) + at, v)

            def add_sent(i, j):
                def body(rows):
                    p_rcv[j, rows] += p_snd[i, rows]

                loop_rows(n_tile, 16, body)

            def pair_go(s):
                @pl.when(lax.rem(s, 2) == 1)
                def _():
                    to_partner(0, lax.div(s, 2), lax.div(s, 2)).start()

            def pair(s, tile):
                j = lax.div(s, 2)
                odd = lax.rem(s, 2)
                tile(into(odd))

                @pl.when(odd == 1)
                def _():
                    copy = to_partner(0, j, j)
                    copy.wait_send()
                    copy.wait_recv()
                    add_sent(1, j)
                    keep(j, p_at.at[place(j)]).start()

            def stored(i):
                keep(i, p_at.at[tile_order[i]]).wait()

            def pair_begin():
                pl.semaphore_signal(pair_ready, inc=1, device_id={'tp': net.peer(0, 1)}, device_id_type=pl.DeviceIdType.MESH)
                pl.semaphore_wait(pair_ready, 1)

            barrier = pltpu.get_barrier_semaphore()
            for chip in range(n_chips):
                for core in BOTH:
                    if chip + core and chip != FAR:
                        pl.semaphore_signal(barrier, inc=1, device_id={'tp': net.peer(chip, core)}, device_id_type=pl.DeviceIdType.MESH)
            pl.semaphore_wait(barrier, n_chips + 1)
            net.start('qp', 'qc', 'x', 'qm', 'bias', 'own', 'load', 'x_own', 'dy_own')
            net.done('own')
            angle = lax.broadcasted_iota(jnp.int32, (seq, width), 0).astype(F32) * freq_ref[0:1, :]
            cos_t[...] = jnp.cos(angle)
            sin_t[...] = jnp.sin(angle) * freq_ref[1:2, :]
            for b in range(seqs):
                row = mask_ref[pl.ds(me * seqs + b, 1), :].astype(F32)
                ok[b] = jnp.broadcast_to(row, (LANES, seq)).T
            net.done('load')
            net.start('store')
            net.got('qp', 'qc')
            net.start('x_far', 'bias_far', 'qr', 'dy_cross', 'oc', 'op', 'up', 'dy_pair', 'qf', 'qg', 'om')
            net.done('x_own', 'dy_own')
            net.got('bias', 'bias_far')
            for n in range(n_tp):
                b = b_all[n]
                b_att[n] = jnp.concatenate([b[i // heads, i % heads:i % heads + 1, :] for i in range(3 * heads)], axis=1)
                b_ffn[n] = u_all[n]
            net.got('x', 'x_far')

            def ln1(rows):
                x_hat, _ = ln_stats(x[rows, :].astype(F32))
                h1[rows, :] = (x_hat * gain1[...] + bias1[...]).astype(BF16)

            loop_rows(tok, chunk, ln1)
            net.done('store')
            net.got('qm', 'qf', 'qg')

            def arrival(s):
                return s + 2 * lax.div(s, n_chips) - n_chips * lax.div(s, n_chips + 2)

            def qkv_step(ps, w, q_ref, k_ref, v_ref):
                s = ps.index[0]
                hooks(s, {2: lambda: (net.got('op'), net.start('or', 'uc', 'um', 'of')), 4: lambda: (net.got('qr'), net.start('ql')),
                          5: lambda: net.got('ql')})
                n_src = tok // chunk // 2

                @pl.loop(0, 2)
                def _(i):
                    rows = span(i, tok // 2)
                    t = mm(h1[rows, :], w[0], NT) + b_att[arrival(s)]
                    cos, sin = (t_ref[span(i, seq // 2), :].reshape(n_src, 1, p_len, width) for t_ref in (cos_t, sin_t))

                    def rope(v):
                        out = v.reshape(n_src, seqs, p_len, width) * cos + swap_halves(v, hd).reshape(n_src, seqs, p_len, width) * sin
                        return out.astype(BF16)

                    src = span(i, n_src)
                    q_ref[0, src] = rope(t[:, :width] * q_scale)
                    k_ref[0, src] = rope(t[:, width:2 * width])
                    v_ref[0, src] = t[:, 2 * width:].reshape(n_src, seqs, p_len, width).astype(BF16)

            slot3 = lambda rows, cols, f=lambda s: s: pl.BlockSpec((1, rows, cols), lambda s: (f(s), 0, 0))

            def pipe(body, **specs):
                def run(*refs):
                    with jax.named_scope(body.__name__):
                        pltpu.emit_pipeline(body, _explicit_indices=True, **specs)(*refs)

                return run

            pipe(qkv_step, grid=(n_tp,), in_specs=[slot3(n3, dim, arrival)],
                 out_specs=[pl.BlockSpec((1, n_tp, seqs, p_len, width), lambda s: (arrival(s), 0, 0, 0, 0))] * 3)(
                wq, q_hbm, k_hbm, v_hbm)

            srcs = qc // p_len
            lane = lax.broadcasted_iota(jnp.int32, (qc, width), 1)

            def attn_step(ps, q_ref, k_ref, v_ref):
                g, b = ps.index
                hooks(g * seqs + b, {
                    8: lambda: (net.got('dy_cross'), net.start('dy_fwd')), 9: lambda: (net.got('up'), net.start('ur', 'dc', 'dm', 'uf')),
                    14: lambda: (net.got('oc', 'or'), net.start('og', 'ol'))})
                bad = ok[b][:, 0:1] <= 0
                k = k_ref[0, :, 0].reshape(seq, width)
                v_t = v_ref[0, :, 0].reshape(seq, width).T
                for c in range(seq // qc):
                    src = slice(c * srcs, (c + 1) * srcs)
                    cols = slice(c * qc, (c + 1) * qc)
                    q = q_ref[0, src, 0].reshape(qc, width)
                    outs = []
                    for h in range(heads):
                        s = jnp.where(bad, NEG_LARGE, mm(k, jnp.where(lane // hd == h, q, jnp.zeros_like(q)), NT))
                        m = jnp.max(s, axis=0, keepdims=True)
                        e = jnp.exp(s - m)
                        r = 1.0 / col_sum(e)
                        outs.append(mm(v_t[h * hd:(h + 1) * hd], (e * r).astype(BF16), NN))
                        m_st[g, b, h:h + 1, cols] = m
                        l_st[g, b, h:h + 1, cols] = r
                    o4[src, b, :, span(g, width)] = jnp.concatenate(outs, axis=0).T.astype(BF16).reshape(srcs, p_len, width)

            head_blk = pl.BlockSpec((1, n_tp, 1, p_len, width), lambda g, b: (g, 0, b, 0, 0))
            pipe(attn_step, grid=(n_tp, seqs), in_specs=[head_blk] * 3)(q_hbm, k_hbm, v_hbm)

            net.got('om', 'of', 'og', 'ol')

            @pl.loop(0, tok // (2 * chunk))
            def _(i):
                rows = span(i, 2 * chunk)
                o = o4[pl.ds(2 * i, 2)].reshape(2 * chunk, n_tp * width)
                low = (x[rows, :].astype(F32) + (mm(o, wo[...].reshape(n_tp * width, dim), NN) + bias_o[...])).astype(BF16)
                x1[rows, :] = low
                x_hat, _ = ln_stats(low.astype(F32))
                h2[rows, :] = (x_hat * gain2[...] + bias2[...]).astype(BF16)

            net.start('h0', 'h1', 'dp')

            def gelu(pre):
                erf_term = lax.erf(pre * INV_SQRT2)
                phi = 0.5 * (1.0 + erf_term)
                return (pre * phi).astype(BF16), phi + pre * jnp.exp(-0.5 * pre * pre) * INV_SQRT_2PI

            cols = lambda f: pl.BlockSpec((tok, ffn), lambda s: (0, f(s)))
            wu_spec, wd_spec = functools.partial(slot3, dim, ffn), functools.partial(slot3, ffn, dim)

            def mlp_up(n, f, table):
                def up_step(ps, w, act_ref, slope_ref):
                    s = ps.index[0]
                    hooks(s, table)

                    def body(rows):
                        act_ref[rows, :], slope_ref[rows, :] = gelu(mm(h2[rows, :], w[0], NN) + b_ffn[f(s)])

                    loop_rows(tok, half, body)

                pipe(up_step, grid=(n,), in_specs=[wu_spec(f)], out_specs=[cols(f)] * 2)(wu, act_hbm, slope_hbm)

            net.got('um', 'uf')
            mlp_up(n_tp - 2, arrival, {2: lambda: (net.got('uc'), net.start('ug')), 3: lambda: net.got('ug')})
            net.got('dy_pair', 'dy_fwd', 'dm')

            def backward(slot, w_d, w_u, act_ref, slope_ref, add):
                if add:
                    gb[slot] = jnp.zeros_like(gb[0])

                def body(rows):
                    d_pre = mm(dy[rows, :], w_d, NT) * slope_ref[rows, :]
                    low = d_pre.astype(BF16)
                    dpre[rows, :] = low
                    if add:
                        gb[slot] += col_sum(d_pre)
                        acc[rows, :] += mm(act_ref[rows, :], w_d, NN)
                        acc2[rows, :] += mm(low, w_u, NT)

                loop_rows(tok, half, body)

            def pair_gelu(rows, w_u, slot):
                return gelu(mm(h2p[rows, :], w_u, NN) + b_ffn[slot])

            def down_first(f):
                def first(ps, w_u, act_ref):
                    s = ps.index[0]
                    rows = pl.ds(0, half)
                    act_p[rows, :] = pair_gelu(rows, w_u[0], f(s))[0]
                    p_snd[s] = mm(act_ref[...], dy[...], TN) + mm(act_p[rows, :], dyp[rows, :], TN)

                pipe(first, grid=(len(BOTH),), in_specs=[wu_spec(f), cols(f)])(wu, act_hbm)

            def mlp(n, f, add, table, last=None):
                lead = len(BOTH) if last else 0
                f_u = (lambda s: jnp.where(s < lead, last[0](s), f(s - lead))) if last else f
                f_d = lambda s: f(jnp.maximum(s - lead, 0)) if not add else jnp.where(s < lead, 0, f(s - lead))

                def add_other(copy, to, ref):
                    copy.wait_recv()
                    add_sent(1, to)
                    keep(to, ref).start()
                    copy.wait_send()

                def mlp_step(ps, wd_s, wu_s, act_ref, slope_ref):
                    s = ps.index[0]

                    def work(t):
                        backward(f(t), wd_s[0], wu_s[0], act_ref, slope_ref, add)

                    if last:
                        _, at, down, up, begun = last
                        copies = [to_partner(0, at + i, n_tp + at + i) for i in BOTH]

                        @pl.when(s < lead)
                        def _():
                            hooks(s, table)
                            pl.when(s == 1)(lambda: copies[0].start())
                            rows = pl.ds(half, half)
                            act_p[rows, :] = pair_gelu(rows, wu_s[0], f_u(s))[0]
                            p_snd[s] += mm(act_p[rows, :], dyp[rows, :], TN)
                            pl.when(s == 1)(lambda: add_other(copies[0], at, down))

                        @pl.when(s >= lead)
                        def _():
                            t = s - lead
                            pl.when(t == 0)(lambda: begun())
                            pl.when(t == 1)(lambda: copies[1].start())
                            work(t)

                            @pl.when(t < lead)
                            def _():
                                def body(rows):
                                    dpre_p[rows, :] = (mm(dyp[rows, :], wd_s[0], NT) * pair_gelu(rows, wu_s[0], f(t))[1]).astype(BF16)

                                loop_rows(tok, half, body)
                                for i in BOTH:
                                    part = pl.ds(i * half, half)
                                    p_snd[t, pl.ds(0, ffn), part] = mm(h2[:, part], dpre[...], TN) + mm(h2p[:, part], dpre_p[...], TN)

                            pl.when(t == 1)(lambda: add_other(copies[1], at + 1, up))
                            hooks(s, table)
                    else:
                        work(s)
                        hooks(s, table)

                pipe(mlp_step, grid=(n + lead,), in_specs=[wd_spec(f_d), wu_spec(f_u), cols(f_d), cols(f_d)])(wd, wu, act_hbm, slope_hbm)

            acc[...] = jnp.zeros_like(acc)
            acc2[...] = jnp.zeros_like(acc2)
            mlp(1, lambda s: s, True, {})
            net.got('ur')
            net.start('ul')
            net.got('ul')
            mlp_up(2, lambda s: s + FAR0, {})
            net.got('h0')
            cross = lambda s: 2 * CROSS + 1 - s
            down_first(cross)

            def sent_down():
                keep(0, x_dn).wait()
                net.start('dn_x')

            def sent_up():
                keep(1, x_up).wait()
                net.start('up_x')

            mlp(n_chips + 1, lambda t: jnp.where(t < 2, cross(t), t - 1), True, {
                0: lambda: (net.got('dc'), net.start('dg', 'd0r', 'd1r'), net.got('h1', 'dg')),
                3: lambda: (net.got('dp'), net.start('df')), 4: lambda: net.got('df'), 5: sent_up}, (cross, 0, x_dn, x_up, sent_down))

            for slot in (FAR0, FAR1):
                gb[slot] = jnp.zeros_like(gb[slot])

            def far_step(ps, w_u, act_ref, slope_ref):
                part, core = ps.index
                hooks(2 * part + core, {0: lambda: (net.got('d0r'), net.start('d0l')), 1: lambda: net.got('d0l'),
                                        2: lambda: (net.got('d1r'), net.start('d1l')), 3: lambda: net.got('d1l')})
                w_d = dx1b[pl.ds(pl.multiple_of(core * ffn + part * quarter, quarter), quarter), :]

                def body(rows):
                    d_pre = mm(dy[rows, :], w_d, NT) * slope_ref[rows, :]
                    gb[FAR0 + core, :, span(part, quarter)] += col_sum(d_pre)
                    acc[rows, :] += mm(act_ref[rows, :], w_d, NN)
                    acc2[rows, :] += mm(d_pre.astype(BF16), w_u[0], NT)

                loop_rows(tok, half, body)

            narrow = pl.BlockSpec((tok, quarter), lambda part, core: (0, 2 * (FAR0 + core) + part))
            pipe(far_step, grid=(len(BOTH),) * len(BOTH), in_specs=[pl.BlockSpec((1, dim, quarter), lambda part, core: (FAR0 + core, 0, part)), narrow, narrow])(
                wu, act_hbm, slope_hbm)

            def y_rows(rows):
                y[rows, :] = (x1[rows, :].astype(F32) + (acc[rows, :] + bias_d[...])).astype(BF16)

            loop_rows(tok, 2 * chunk, y_rows)
            vec[...] = jnp.zeros_like(vec)
            net.start('y', 'y_own')
            net.sent('d0l', 'd1l')

            @pl.loop(0, tok // (2 * chunk))
            def _(i):
                rows = span(i, 2 * chunk)
                x1_f, dy_f, dh = x1[rows, :].astype(F32), dy[rows, :].astype(F32), acc2[rows, :]
                x_hat, inv_std = ln_stats(x1_f)
                d_x1 = dy_f + ln_grad(dh, x_hat, inv_std, gain2[...])
                acc2[rows, :] = d_x1
                low = d_x1.astype(BF16)
                dx1b[rows, :] = low
                d_o = mm(low, wo[...].reshape(n_tp * width, dim), NT).astype(BF16)
                do4[pl.ds(2 * i, 2)] = d_o.reshape(2, seqs, p_len, n_tp * width)
                for n, t in enumerate((d_x1, dh * x_hat, dh, dy_f)):
                    vec[2 + n:3 + n, :] += col_sum(t)

            pair_begin()

            def bwd_step(ps, q_ref, k_ref, v_ref, w):
                step = ps.index[0]
                g = order(step)
                hooks(step, {2: lambda: (stored(0), net.start('at_relay0', 'at_relay1')),
                             4: lambda: (stored(1), net.start('at_early', 'y_far')), 6: lambda: (stored(2), pass_on(0, 0)), 7: lambda: pass_on(0, 2)})
                pair_go(step)
                b8[g] = jnp.zeros_like(b8[0])
                fold(gb[g], b8.at[g], 3)
                for b in range(seqs):
                    bad = ok[b][:, 0:1] <= 0
                    k = k_ref[0, :, b].reshape(seq, width)
                    v = v_ref[0, :, b].reshape(seq, width)
                    k_t = k.T
                    for c in range(seq // qc):
                        src = slice(c * srcs, (c + 1) * srcs)
                        at = slice(c * qc, (c + 1) * qc)
                        q = q_ref[0, src, b].reshape(qc, width)
                        d_o = do4[src, b, :, span(g, width)].reshape(qc, width)
                        dk = jnp.zeros((seq, width), F32)
                        dv = jnp.zeros((seq, width), F32)
                        dqs = []
                        for h in range(heads):
                            mine = lane // hd == h
                            q_h = jnp.where(mine, q, jnp.zeros_like(q))
                            do_h = jnp.where(mine, d_o, jnp.zeros_like(d_o))
                            s = jnp.where(bad, NEG_LARGE, mm(k, q_h, NT))
                            p = jnp.exp(s - m_st[g, b, h:h + 1, at]) * l_st[g, b, h:h + 1, at]
                            dv += mm(p.astype(BF16), do_h, NN)
                            dp = mm(v, do_h, NT)
                            ds = (p * (dp - col_sum(dp * p))).astype(BF16)
                            dk += mm(ds, q_h, NN)
                            dqs.append(mm(k_t[h * hd:(h + 1) * hd], ds, NN))
                        dq_acc[at, :] = jnp.concatenate(dqs, axis=0).T
                        dk_acc[...] = dk if c == 0 else dk_acc[...] + dk
                        dv_acc[...] = dv if c == 0 else dv_acc[...] + dv
                    cos, sin = cos_t[...], sin_t[...]
                    dq, dk, dv = dq_acc[...], dk_acc[...], dv_acc[...]
                    dq = (dq * cos - swap_halves(dq, hd) * sin) * q_scale
                    dk = dk * cos - swap_halves(dk, hd) * sin
                    for i, t in enumerate((dq, dk, dv)):
                        d4[:, b, :, i * width:(i + 1) * width] = t.astype(BF16).reshape(n_tp, p_len, width)
                        b8[g, i:i + 1, :] += col_sum(t)

                @pl.when(step == 0)
                def _():
                    acc[...] = jnp.zeros_like(acc)

                @pl.loop(0, 2)
                def _(i):
                    acc[span(i, half), :] += mm(d4[pl.ds(n_chips * i, n_chips)].reshape(half, n3), w[0], NN)

                def tile(put):
                    put((pl.ds(0, n3),), mm(d4[...].reshape(tok, n3), h1[...], TN))
                    put((pl.ds(n3, width),), mm(o4[:, :, :, span(g, width)].reshape(tok, width), dx1b[...], TN))

                pair(step, tile)
                hooks(step, {6: lambda: pass_on(0, 1)})

            slot_blk = pl.BlockSpec((1, n_tp, seqs, p_len, width), lambda s: (order(s), 0, 0, 0, 0))
            pipe(bwd_step, grid=(n_tp,), in_specs=[slot_blk] * 3 + [slot3(n3, dim, order)])(
                q_hbm, k_hbm, v_hbm, wq)

            pass_on(1, 0)

            def ln1_bwd(rows):
                x_hat, inv_std = ln_stats(x[rows, :].astype(F32))
                dh = acc[rows, :]
                h1[rows, :] = (acc2[rows, :] + ln_grad(dh, x_hat, inv_std, gain1[...])).astype(BF16)
                vec[0:1, :] += col_sum(dh * x_hat)
                vec[1:2, :] += col_sum(dh)

            loop_rows(tok, 2 * chunk, ln1_bwd)
            stored(3)
            for r in range(6):
                fold(vec[pl.ds(r, 1), :], v_own, r * n_tp)
            mate[0:v_half] = v_own[span(1 - side, v_half), :]
            for n in range(n_chips):
                mate[pl.ds(v_half + n * 8, 8)] = b8[2 * n + 1]
            net.start('mate')
            pass_on(1, 1)
            net.got('mate')
            v_sum = v_own[span(side, v_half), :] + mate_in[0:v_half]
            for n in range(n_chips):
                late[n, 0:v_half] = v_sum
                late[n, v_half:] = b8[2 * n] + mate_in[pl.ds(v_half + n * 8, 8)]
            net.start('late')
            pass_on(1, 2)
            net.start('gx', 'gx_far', 'gx_own')

            net.sent('y', 'y_far')
            net.done('y_own')
            pair_begin()
            mine = lambda s: 1 - s
            down_first(mine)
            mlp(2, mine, False, {}, (mine, 2, p_dn, p_up, lambda: None))
            for i, ref in enumerate((p_dn, p_up)):
                keep(2 + i, ref).wait()

            def total(refs, out, block, at):
                def body(*blocks):
                    v = blocks[1][...]
                    for more in blocks[2:-1]:
                        v += more[...]
                    blocks[-1][...] = v

                pipe(body, grid=(len(BOTH),), in_specs=[pl.BlockSpec(block, at)] * len(refs),
                     out_specs=[pl.BlockSpec(block, lambda i: (i, 0))])(*refs, out)

            by_row, by_col = lambda i: (i, 0), lambda i: (0, i)
            net.got('late')
            late_sum = late[0]
            for n in range(1, n_chips):
                late_sum += late_in[n]
            v_own[span(side, v_half), :] = late_sum[0:v_half]
            b8[0] = late_sum[v_half:]
            net.start('final')
            net.got('dn_x', 'up_x')
            total((p_dn, r_dn), g_down, (t_half, dim), by_row)
            total((p_up, r_up), g_up, (n_tile, half), by_col)
            net.got('at_early', 'at_sum0', 'at_sum1')
            for rows, out, n in ((pl.ds(0, n3), g_q, n3), (pl.ds(n3, width), g_o, width)):
                total((p_at.at[0, rows], early_at.at[rows], last_at.at[rows]), out, (n // 2, dim), by_row)
            for name in net.copies:
                if name not in ('load', 'store', 'own', 'write', 'gx', 'gx_far', 'y', 'y_far', 'd0l', 'd1l') and not name.endswith(('_own', '_load', '_store')):
                    net.sent(name)
            net.got('y', 'y_far', 'final')
            net.start('write')
            net.done('gx_own', 'write')
            net.got('gx', 'gx_far')
            net.sent('gx', 'gx_far')

        big = (tok, dim)
        shapes = lambda *dims, dtype=F32: sds(dims, dtype)
        flat = lambda t: t.reshape(tok, dim)
        inv_freq = ROPE_BASE ** (-2.0 * np.arange(hd // 2) / hd)
        sign = np.repeat([-1.0, 1.0], hd // 2)
        freq = np.stack([np.tile(inv_freq, 2 * heads), np.tile(sign, heads)]).astype(np.float32)
        line = lambda v: v.reshape(1, -1)
        sem = lambda n: pltpu.SemaphoreType.DMA((n,))
        low = functools.partial(shapes, dtype=BF16)
        weights = [low(n_tp, n3, dim), low(n_tp, dim, ffn), low(n_tp, ffn, dim)]
        tiles = [shapes(n_chips, n_tile, dim)] + [shapes(n_tile, dim)] * 10
        out_shape = ([low(*big)] * 2 + [shapes(dim, ffn), shapes(ffn, dim), shapes(n3, dim), shapes(width, dim), shapes(6 * n_tp, LANES), shapes(8, LANES)] + weights
                     + [low(n_tp, n_tp, seqs, p_len, width)] * 3 + [low(tok, n_tp * ffn), shapes(tok, n_tp * ffn)] + tiles)
        plain = [pad_mask] + [line(v) for v in (ln1_gain, ln1_bias, b_out, ln2_gain, b_down, ln2_bias)] + [freq]
        heads4 = low(n_tp, seqs, p_len, n_tp * width)
        stat = shapes(n_tp, seqs, heads, seq)
        tile8 = shapes(n_tp, 8, LANES)
        late = shapes(n_chips, v_half + 8, LANES)
        mate = shapes(v_half + 8 * n_chips, LANES)
        row_ffn = shapes(n_tp, 1, ffn)
        scratch = ([low(*big)] * 9 + [heads4, heads4, low(n_tp, width, dim)] + [shapes(*big)] * 2
                   + [shapes(n_chips, n_tile, dim), shapes(2, n_tile, dim), low(n_tp, seqs, p_len, n3)]
                   + [shapes(seq, width)] * 5 + [shapes(seqs, seq, LANES), stat, stat, shapes(n_tp, 1, n3), row_ffn, row_ffn, row_ffn]
                   + [shapes(n_tp, *b_qkv.shape), tile8, late, late, shapes(8, dim), mate, mate, shapes(6 * n_tp, LANES)]
                   + [low(tok, ffn)] + plain)
        outs = pl.pallas_call(
            kernel, name='layer', out_shape=out_shape, in_specs=[ANY] * 16, out_specs=[ANY] * len(out_shape),
            scratch_shapes=[pltpu.VMEM(v.shape, v.dtype) for v in scratch]
            + [sem(91), sem(91), sem(30), sem(20), sem(12), pltpu.SemaphoreType.REGULAR],
            compiler_params=pltpu.CompilerParams(collective_id=0, has_side_effects=True, vmem_limit_bytes=VMEM_LIMIT),
        )(flat(x_in), flat(grad_y), w_qkv.transpose(0, 2, 3, 1).reshape(n3, dim), b_qkv, w_out.reshape(width, dim),
          w_up, line(b_up), w_down, *plain)

        def finish(*refs):
            it = iter(refs)
            n = len(large)
            src, (v_ref, b_ref), out, (bq_o, bu_o), v_o = (list(itertools.islice(it, k)) for k in (n, 2, n, 2, n))
            for a, b in zip(src, out):
                b[...] = a[...]
            for i in range(3):
                for h in range(heads):
                    bq_o[i, h:h + 1, :] = b_ref[i:i + 1, h * hd:(h + 1) * hd]
            unfold(b_ref, 3, bu_o)
            for r, ref in enumerate(v_o):
                unfold(v_ref, r * n_tp, ref)

        large = [low(*big)] * 2 + [shapes(dim, ffn), shapes(ffn, dim), shapes(n3, dim), shapes(width, dim)]
        small = [shapes(*b_qkv.shape), shapes(1, ffn)] + [shapes(1, dim)] * 6
        moving = [pl.BlockSpec((v.shape[0] // n_chips, v.shape[1]), lambda i: (i, 0)) for v in large]
        fixed = lambda vs: [pl.BlockSpec(v.shape, lambda i, n=len(v.shape): (0,) * n) for v in vs]
        res = pl.pallas_call(
            finish, name='finish', out_shape=large + small, grid=(n_chips,), in_specs=moving + fixed(outs[6:8]),
            out_specs=moving + fixed(small), compiler_params=pltpu.CompilerParams(vmem_limit_bytes=VMEM_LIMIT),
        )(*outs[:8])
        y_out, grad_x, grad_w_up, grad_w_down, gq, go, grad_b_qkv, grad_b_up = res[:8]
        v = [t.reshape(dim) for t in res[8:]]
        return (y_out.reshape(x_in.shape), grad_x.reshape(x_in.shape), v[0], v[1], gq.reshape(3, heads, hd, dim).transpose(0, 3, 1, 2),
                grad_b_qkv, go.reshape(heads, hd, dim), v[2], v[3], v[4], grad_w_up, grad_b_up.reshape(ffn), grad_w_down, v[5])

    return jax.shard_map(device_step, mesh=mesh, in_specs=in_specs, out_specs=out_specs, check_vma=False)
```

```python
import functools
import itertools

import jax
import jax.numpy as jnp
import numpy as np
from jax import lax
from jax.experimental import pallas as pl
from jax.experimental.pallas import tpu as pltpu
from jax.sharding import PartitionSpec as P

LN_EPS = 1e-5
ROPE_BASE = 10000.0
INV_SQRT2 = 0.7071067811865476
INV_SQRT_2PI = 0.3989422804014327
NEG_LARGE = -1e30
F32 = jnp.float32
BF16 = jnp.bfloat16
VMEM_LIMIT = 66_500_000
LANES = 128
NN = (((1,), (0,)), ((), ()))
NT = (((1,), (1,)), ((), ()))
TN = (((0,), (0,)), ((), ()))
PAIR, FAR, CROSS = 1, 2, 3
FAR0 = FAR + FAR
FAR1 = FAR0 + 1
BOTH = range(2)
ANY = pl.BlockSpec(memory_space=pl.ANY)


def mm(a, b, dims):
    return lax.dot_general(a, b, dims, preferred_element_type=F32)


def ln_stats(v):
    centered = v - jnp.mean(v, axis=-1, keepdims=True)
    inv_std = lax.rsqrt(jnp.mean(centered * centered, axis=-1, keepdims=True) + LN_EPS)
    return centered * inv_std, inv_std


def ln_grad(d_out, x_hat, inv_std, gain):
    d_hat = d_out * gain
    return inv_std * (d_hat - jnp.mean(d_hat, axis=-1, keepdims=True) - x_hat * jnp.mean(d_hat * x_hat, axis=-1, keepdims=True))


def col_sum(t):
    return jnp.sum(t, axis=0, keepdims=True)


def swap_halves(t, head_dim):
    half = head_dim // 2
    lane = lax.broadcasted_iota(jnp.int32, t.shape, t.ndim - 1)
    return jnp.where(lane % head_dim < half, pltpu.roll(t, t.shape[-1] - half, t.ndim - 1), pltpu.roll(t, half, t.ndim - 1))


def span(i, n):
    return pl.ds(pl.multiple_of(i * n, n), n)


def fold(row, out, first):
    for i in range(row.shape[-1] // LANES):
        out[pl.ds(first + i, 1), :] = row[:, i * LANES:(i + 1) * LANES]


def unfold(src, first, out):
    for i in range(out.shape[-1] // LANES):
        out[:, pl.ds(i * LANES, LANES)] = src[pl.ds(first + i, 1), :]


def loop_rows(total, n, body):
    @pl.loop(0, total // n)
    def _(i):
        body(span(i, n))


class Net:
    def __init__(self, n_tp, send, recv, local):
        self.n_tp, self.send, self.recv, self.local = n_tp, send, recv, local
        self.copies, self.count, self.n_local = {}, 0, 0

    def peer(self, chip, core=0):
        me = lax.axis_index('tp')
        way = 1 - 2 * lax.rem(lax.div(me, 2), 2)
        at = lax.rem(me + 2 * chip * way + self.n_tp, self.n_tp) if chip else me
        return at + 1 - 2 * lax.rem(at, 2) if core else at

    def add(self, name, src, dst, chip, core=0):
        n = self.count
        self.count += 1

        def make():
            return pltpu.make_async_remote_copy(
                src_ref=src(), dst_ref=dst(), send_sem=self.send.at[n], recv_sem=self.recv.at[n],
                device_id={'tp': self.peer(chip, core)}, device_id_type=pl.DeviceIdType.MESH)

        self.copies.setdefault(name, []).append(make)

    def add_local(self, name, src, dst):
        n = self.n_local
        self.n_local += 1
        self.copies.setdefault(name, []).append(lambda: pltpu.make_async_copy(src(), dst(), self.local.at[n]))

    def start(self, *names):
        for name in names:
            for make in self.copies[name]:
                make().start()

    def got(self, *names):
        for name in names:
            with jax.named_scope('got_' + name):
                for make in self.copies[name]:
                    make().wait_recv()

    def sent(self, *names):
        for name in names:
            for make in self.copies[name]:
                make().wait_send()

    def done(self, *names):
        for name in names:
            with jax.named_scope('done_' + name):
                for make in self.copies[name]:
                    make().wait()

    def gather(self, name, own, buf):
        for stage, chip in (('p', PAIR), ('c', CROSS)):
            self.add(name + stage, lambda: own, lambda c=chip: buf.at[2 * c], chip)
        self.add(name + 'm', lambda: own, lambda: buf.at[1], 0, 1)
        for stage, chip in (('f', PAIR), ('g', CROSS)):
            self.add(name + stage, lambda c=chip: buf.at[2 * c], lambda c=chip: buf.at[2 * c + 1], 0, 1)

    def gather_far(self, name, src, here, other, via):
        self.add(name + 'r', src, here, via)
        self.add(name + 'l', here, other, 0, 1)

    def exchange(self, name, src, dst, rows):
        me = lax.axis_index('tp')
        for core in BOTH:
            for chip in (PAIR, CROSS, FAR, 0):
                if chip + core:
                    self.add(name + '_far' * (chip == FAR), lambda c=chip, k=core: src.at[span(self.peer(c, k), rows)],
                             lambda: dst.at[span(me, rows)], chip, core)
        self.add_local(name + '_own', lambda: src.at[span(me, rows)], lambda: dst.at[span(me, rows)])

    def multicast(self, name, src, dst, pair_dst, rows):
        me = lax.axis_index('tp')
        at = lambda buf: (lambda: buf.at[span(me, rows)])
        other = {0: PAIR, PAIR: 0, CROSS: FAR}
        for chip, stage in ((CROSS, '_cross'), (PAIR, '_pair'), (0, '_pair')):
            for core in BOTH:
                if chip + core:
                    for c, buf in ((chip, dst), (other[chip], pair_dst)):
                        self.add(name + stage, lambda c=c, k=core: src.at[span(self.peer(c, k), rows)], at(buf), chip, core)
        for c, buf in ((0, dst), (PAIR, pair_dst)):
            self.add_local(name + '_own', lambda c=c: src.at[span(self.peer(c), rows)], at(buf))
        came = lambda buf: (lambda: buf.at[span(lax.div(self.peer(CROSS), 2), 2 * rows)])
        self.add(name + '_fwd', came(dst), came(pair_dst), PAIR)
        self.add(name + '_fwd', came(pair_dst), came(dst), PAIR)


def solution(mesh):
    n_tp = mesh.shape['tp']
    n_chips = n_tp // 2
    act_spec = P('dp', 'tp', None)
    rep_vec = P(None)
    part_vec = P('dp')
    in_specs = (act_spec, act_spec, P('dp', None), rep_vec, rep_vec, P(None, None, 'tp', None), P(None, 'tp', None),
                P('tp', None, None), rep_vec, rep_vec, rep_vec, P(None, 'tp'), P('tp'), P('tp', None), rep_vec)
    out_specs = (act_spec, act_spec, part_vec, part_vec, P('dp', None, 'tp', None), P('dp', 'tp', None),
                 P(('dp', 'tp'), None, None), part_vec, part_vec, part_vec, P('dp', 'tp'), P(('dp', 'tp')),
                 P(('dp', 'tp'), None), part_vec)

    def device_step(x_in, grad_y, pad_mask, ln1_gain, ln1_bias, w_qkv, b_qkv, w_out, b_out, ln2_gain, ln2_bias, w_up, b_up, w_down, b_down):
        batch, p_len, dim = x_in.shape
        seq = pad_mask.shape[1]
        _, _, heads, hd = w_qkv.shape
        seqs = batch // n_tp
        ffn = w_up.shape[1]
        width = heads * hd
        n3 = 3 * width
        tok = seqs * seq
        chunk = seqs * p_len
        qc = seq // 2
        q_scale = hd ** -0.5
        sds = jax.ShapeDtypeStruct
        n_tile = n3 + width
        half = dim // 2
        twice = n_tp + n_tp
        quarter = ffn // 2
        v_half = 3 * n_tp

        def kernel(*refs):
            it = iter(refs)
            take = lambda n: [next(it) for _ in range(n)]
            (x_ref, dy_ref, wq_ref, bq_ref, wo_ref, wu_ref, bu_ref, wd_ref), plain = take(8), take(8)
            y_out, gx_out, g_up, g_down, g_q, g_o, g_vec, g_b, wq, wu, wd, q_hbm, k_hbm, v_hbm, act_hbm, slope_hbm = take(16)
            p_at, got_at, sum_at, early_at, last_at, x_dn, x_up, p_dn, p_up, r_dn, r_up = take(11)
            x, h1, dy, x1, h2, dx1b, h2p, dyp, y, o4, do4, wo, acc, acc2, p_rcv, p_snd = take(16)
            dq_acc, dk_acc, dv_acc, cos_t, sin_t, ok, st, b_att, b_ffn, gb, b_all, b8, late, late_in, vec, mate, mate_in, v_own = take(18)
            dpre = next(it)
            act_p, dpre_p = (y.at[:, pl.ds(i * ffn, ffn)] for i in BOTH)
            here = take(8)
            send, recv, local, pair_send, pair_recv, pair_ready = take(6)
            net = Net(n_tp, send, recv, local)
            me = lax.axis_index('tp')
            mask_ref, gain1, bias1, bias_o, gain2, bias_d, bias2, freq_ref = here

            net.gather('q', wq_ref, wq)
            net.gather('o', wo_ref, wo)
            net.gather('u', wu_ref, wu)
            net.gather('d', wd_ref, wd)
            for name, buf in (('q', wq), ('o', wo), ('u', wu)):
                net.gather_far(name, lambda b=buf: b.at[2 * PAIR], lambda b=buf: b.at[FAR0], lambda b=buf: b.at[FAR1], CROSS)
            for i in BOTH:
                mine = lambda core, i=i: dx1b.at[pl.ds(core * ffn + i * quarter, quarter)]
                net.gather_far(f'd{i}', lambda i=i: wd.at[2 * CROSS, pl.ds(i * quarter, quarter)], lambda m=mine: m(0), lambda m=mine: m(1), PAIR)
            net.exchange('x', x_ref, x, chunk)
            net.multicast('dy', dy_ref, dy, dyp, chunk)
            net.exchange('y', y, y_out, chunk)
            net.exchange('gx', h1, gx_out, chunk)
            for chip in range(n_chips):
                for core in BOTH:
                    if chip + core:
                        slot = 2 * chip + core
                        net.add('bias' + '_far' * (chip == FAR), lambda: bq_ref, lambda n=slot: b_all.at[n], chip, core)
                        net.add('bias' + '_far' * (chip == FAR), lambda: bu_ref, lambda n=slot: b_ffn.at[n], chip, core)
            for chip in (PAIR, CROSS, FAR):
                net.add('late', lambda n=chip: late.at[n], lambda n=chip: late_in.at[n], chip)
            side = lax.rem(me, 2)
            net.add('mate', lambda: mate, lambda: mate_in, 0, 1)
            net.add('final', lambda: v_own.at[span(side, v_half)], lambda: v_own.at[span(side, v_half)], 0, 1)
            for i in BOTH:
                net.add(f'h{i}', lambda p=pl.ds(i * half, half): h2.at[p], lambda p=pl.ds(i * half, half): h2p.at[p], PAIR)
            net.add('dn_x', lambda: x_dn, lambda: r_dn, CROSS)
            net.add('up_x', lambda: x_up, lambda: r_up, CROSS)
            net.add('at_early', lambda: p_at.at[PAIR], lambda: early_at, PAIR)
            t_half = n_tile // 2
            for i, part in enumerate((pl.ds(0, t_half), pl.ds(t_half, t_half))):
                net.add(f'at_relay{i}', lambda p=part: p_at.at[FAR, p], lambda p=part: got_at.at[p], PAIR)
                net.add(f'at_sum{i}', lambda p=part: sum_at.at[p], lambda p=part: last_at.at[p], CROSS)
                net.add_local(f'at{i}_load', lambda p=part: got_at.at[p], lambda p=part: p_rcv.at[0, p])
                net.add_local(f'at{i}_load', lambda p=part: p_at.at[CROSS, p], lambda p=part: p_rcv.at[1, p])
                net.add_local(f'at{i}_store', lambda p=part: p_rcv.at[1, p], lambda p=part: sum_at.at[p])
            for src, dst in zip(plain, here):
                net.add_local('own', lambda r=src: r, lambda r=dst: r)
            net.add_local('write', lambda: v_own, lambda: g_vec)
            net.add_local('write', lambda: b8.at[0], lambda: g_b)
            for ref, tmp, buf in ((wq_ref, lambda: h2.at[pl.ds(0, n3)], wq), (wu_ref, lambda: x1.at[:, pl.ds(0, ffn)], wu),
                                        (wd_ref, lambda: dx1b.at[pl.ds(0, ffn)], wd)):
                net.add_local('load', lambda r=ref: r, tmp)
                net.add_local('store', tmp, lambda b=buf: b.at[0])
            net.add_local('own', lambda: wo_ref, lambda: wo.at[0])
            net.add_local('own', lambda: bq_ref, lambda: b_all.at[0])
            net.add_local('own', lambda: bu_ref, lambda: b_ffn.at[0])
            def pass_on(i, stage):
                if stage == 0:
                    net.got(f'at_relay{i}')
                    net.start(f'at{i}_load')
                elif stage == 1:
                    net.done(f'at{i}_load')

                    def body(rows):
                        rows = pl.ds(i * t_half + rows.start, rows.size)
                        p_rcv[1, rows] += p_rcv[0, rows]

                    loop_rows(t_half, 8, body)
                    net.start(f'at{i}_store')
                else:
                    net.done(f'at{i}_store')
                    net.start(f'at_sum{i}')

            def hooks(step, table):
                for at, act in table.items():
                    @pl.when(step == at)
                    def _(act=act):
                        act()

            tile_order = (FAR, PAIR, CROSS, 0)

            def place(i):
                return jnp.where(i == 0, FAR, jnp.where(i == 1, PAIR, jnp.where(i == 2, CROSS, 0)))

            def order(s):
                return 2 * place(lax.div(s, 2)) + 1 - lax.rem(s, 2)

            def to_partner(src, dst, sem):
                return pltpu.make_async_remote_copy(
                    src_ref=p_snd.at[src], dst_ref=p_rcv.at[dst], send_sem=pair_send.at[sem], recv_sem=pair_recv.at[sem],
                    device_id={'tp': net.peer(0, 1)}, device_id_type=pl.DeviceIdType.MESH)

            def keep(i, to):
                return pltpu.make_async_copy(p_rcv.at[i], to, pair_send.at[twice + i])

            def into(i):
                return lambda at, v: p_snd.__setitem__((i,) + at, v)

            def add_sent(i, j):
                def body(rows):
                    p_rcv[j, rows] += p_snd[i, rows]

                loop_rows(n_tile, 16, body)

            def pair_go(s):
                @pl.when(lax.rem(s, 2) == 1)
                def _():
                    to_partner(0, lax.div(s, 2), lax.div(s, 2)).start()

            def pair(s, tile):
                j = lax.div(s, 2)
                odd = lax.rem(s, 2)
                tile(into(odd))

                @pl.when(odd == 1)
                def _():
                    copy = to_partner(0, j, j)
                    copy.wait_send()
                    copy.wait_recv()
                    add_sent(1, j)
                    keep(j, p_at.at[place(j)]).start()

            def stored(i):
                keep(i, p_at.at[tile_order[i]]).wait()

            def pair_begin():
                pl.semaphore_signal(pair_ready, inc=1, device_id={'tp': net.peer(0, 1)}, device_id_type=pl.DeviceIdType.MESH)
                pl.semaphore_wait(pair_ready, 1)

            barrier = pltpu.get_barrier_semaphore()
            for chip in range(n_chips):
                for core in BOTH:
                    if chip + core and chip != FAR:
                        pl.semaphore_signal(barrier, inc=1, device_id={'tp': net.peer(chip, core)}, device_id_type=pl.DeviceIdType.MESH)
            pl.semaphore_wait(barrier, n_chips + 1)
            net.start('qp', 'qc', 'x', 'qm', 'bias', 'own', 'load', 'x_own', 'dy_own')
            net.done('own')
            angle = lax.broadcasted_iota(jnp.int32, (seq, width), 0).astype(F32) * freq_ref[0:1, :]
            cos_t[...] = jnp.cos(angle)
            sin_t[...] = jnp.sin(angle) * freq_ref[1:2, :]
            for b in range(seqs):
                row = mask_ref[pl.ds(me * seqs + b, 1), :].astype(F32)
                ok[b] = jnp.broadcast_to(row, (LANES, seq)).T.astype(BF16)
            net.done('load')
            net.start('store')
            net.got('qp', 'qc')
            net.start('x_far', 'bias_far', 'qr', 'dy_cross', 'oc', 'op', 'up', 'dy_pair', 'qf', 'qg', 'om')
            net.done('x_own', 'dy_own')
            net.got('bias', 'bias_far')
            for n in range(n_tp):
                b = b_all[n]
                b_att[n] = jnp.concatenate([b[i // heads, i % heads:i % heads + 1, :] for i in range(3 * heads)], axis=1)
            net.got('x', 'x_far')

            def ln1(rows):
                x_hat, _ = ln_stats(x[rows, :].astype(F32))
                h1[rows, :] = (x_hat * gain1[...] + bias1[...]).astype(BF16)

            loop_rows(tok, chunk, ln1)
            net.done('store')
            net.got('qm', 'qf', 'qg')

            def arrival(s):
                return s + 2 * lax.div(s, n_chips) - n_chips * lax.div(s, n_chips + 2)

            def qkv_step(ps, w, q_ref, k_ref, v_ref):
                s = ps.index[0]
                hooks(s, {2: lambda: (net.got('op'), net.start('or', 'uc', 'um', 'of')), 4: lambda: (net.got('qr'), net.start('ql')),
                          5: lambda: net.got('ql')})
                n_src = tok // chunk // 2

                @pl.loop(0, 2)
                def _(i):
                    rows = span(i, tok // 2)
                    t = mm(h1[rows, :], w[0], NT) + b_att[arrival(s)]
                    cos, sin = (t_ref[span(i, seq // 2), :].reshape(n_src, 1, p_len, width) for t_ref in (cos_t, sin_t))

                    def rope(v):
                        out = v.reshape(n_src, seqs, p_len, width) * cos + swap_halves(v, hd).reshape(n_src, seqs, p_len, width) * sin
                        return out.astype(BF16)

                    src = span(i, n_src)
                    q_ref[0, src] = rope(t[:, :width] * q_scale)
                    k_ref[0, src] = rope(t[:, width:2 * width])
                    v_ref[0, src] = t[:, 2 * width:].reshape(n_src, seqs, p_len, width).astype(BF16)

            slot3 = lambda rows, cols, f=lambda s: s: pl.BlockSpec((1, rows, cols), lambda s: (f(s), 0, 0))

            def pipe(body, **specs):
                def run(*refs):
                    with jax.named_scope(body.__name__):
                        pltpu.emit_pipeline(body, _explicit_indices=True, **specs)(*refs)

                return run

            pipe(qkv_step, grid=(n_tp,), in_specs=[slot3(n3, dim, arrival)],
                 out_specs=[pl.BlockSpec((1, n_tp, seqs, p_len, width), lambda s: (arrival(s), 0, 0, 0, 0))] * 3)(
                wq, q_hbm, k_hbm, v_hbm)

            srcs = qc // p_len
            lane = lax.broadcasted_iota(jnp.int32, (qc, width), 1)

            def attn_step(ps, q_ref, k_ref, v_ref):
                g, b = ps.index
                hooks(g * seqs + b, {
                    8: lambda: (net.got('dy_cross'), net.start('dy_fwd')), 9: lambda: (net.got('up'), net.start('ur', 'dc', 'dm', 'uf')),
                    14: lambda: (net.got('oc', 'or'), net.start('og', 'ol'))})
                bad = ok[b][:, 0:1].astype(F32) <= 0
                k = k_ref[0, :, 0].reshape(seq, width)
                v_t = v_ref[0, :, 0].reshape(seq, width).T
                for c in range(seq // qc):
                    src = slice(c * srcs, (c + 1) * srcs)
                    cols = slice(c * qc, (c + 1) * qc)
                    q = q_ref[0, src, 0].reshape(qc, width)
                    outs = []
                    for h in range(heads):
                        s = jnp.where(bad, NEG_LARGE, mm(k, jnp.where(lane // hd == h, q, jnp.zeros_like(q)), NT))
                        m = jnp.max(s, axis=0, keepdims=True)
                        e = jnp.exp(s - m)
                        r = 1.0 / col_sum(e)
                        outs.append(mm(v_t[h * hd:(h + 1) * hd], (e * r).astype(BF16), NN))
                        st[g, b, h:h + 1, cols] = m
                        st[g, b, heads + h:heads + h + 1, cols] = r
                    o4[src, b, :, span(g, width)] = jnp.concatenate(outs, axis=0).T.astype(BF16).reshape(srcs, p_len, width)

            head_blk = pl.BlockSpec((1, n_tp, 1, p_len, width), lambda g, b: (g, 0, b, 0, 0))
            pipe(attn_step, grid=(n_tp, seqs), in_specs=[head_blk] * 3)(q_hbm, k_hbm, v_hbm)

            net.got('om', 'of', 'og', 'ol')

            @pl.loop(0, tok // (2 * chunk))
            def _(i):
                rows = span(i, 2 * chunk)
                o = o4[pl.ds(2 * i, 2)].reshape(2 * chunk, n_tp * width)
                low = (x[rows, :].astype(F32) + (mm(o, wo[...].reshape(n_tp * width, dim), NN) + bias_o[...])).astype(BF16)
                x1[rows, :] = low
                x_hat, _ = ln_stats(low.astype(F32))
                h2[rows, :] = (x_hat * gain2[...] + bias2[...]).astype(BF16)

            net.start('h0', 'h1', 'dp')

            def gelu(pre):
                erf_term = lax.erf(pre * INV_SQRT2)
                phi = 0.5 * (1.0 + erf_term)
                return (pre * phi).astype(BF16), phi + pre * jnp.exp(-0.5 * pre * pre) * INV_SQRT_2PI

            cols = lambda f: pl.BlockSpec((tok, ffn), lambda s: (0, f(s)))
            wu_spec, wd_spec = functools.partial(slot3, dim, ffn), functools.partial(slot3, ffn, dim)

            def mlp_up(n, f, table):
                def up_step(ps, w, act_ref, slope_ref):
                    s = ps.index[0]
                    hooks(s, table)

                    def body(rows):
                        act_ref[rows, :], slope_ref[rows, :] = gelu(mm(h2[rows, :], w[0], NN) + b_ffn[f(s)])

                    loop_rows(tok, half, body)

                pipe(up_step, grid=(n,), in_specs=[wu_spec(f)], out_specs=[cols(f)] * 2)(wu, act_hbm, slope_hbm)

            net.got('um', 'uf')
            mlp_up(n_tp - 2, arrival, {2: lambda: (net.got('uc'), net.start('ug')), 3: lambda: net.got('ug')})
            net.got('dy_pair', 'dy_fwd', 'dm')

            def backward(slot, w_d, w_u, act_ref, slope_ref, add):
                if add:
                    gb[slot] = jnp.zeros_like(gb[0])

                def body(rows):
                    d_pre = mm(dy[rows, :], w_d, NT) * slope_ref[rows, :]
                    low = d_pre.astype(BF16)
                    dpre[rows, :] = low
                    if add:
                        gb[slot] += col_sum(d_pre)
                        acc[rows, :] += mm(act_ref[rows, :], w_d, NN)
                        acc2[rows, :] += mm(low, w_u, NT)

                loop_rows(tok, half, body)

            def pair_gelu(rows, w_u, slot):
                return gelu(mm(h2p[rows, :], w_u, NN) + b_ffn[slot])

            def down_first(f):
                def first(ps, w_u, act_ref):
                    s = ps.index[0]
                    rows = pl.ds(0, half)
                    act_p[rows, :] = pair_gelu(rows, w_u[0], f(s))[0]
                    p_snd[s] = mm(act_ref[...], dy[...], TN) + mm(act_p[rows, :], dyp[rows, :], TN)

                pipe(first, grid=(len(BOTH),), in_specs=[wu_spec(f), cols(f)])(wu, act_hbm)

            def mlp(n, f, add, table, last=None):
                lead = len(BOTH) if last else 0
                f_u = (lambda s: jnp.where(s < lead, last[0](s), f(s - lead))) if last else f
                f_d = lambda s: f(jnp.maximum(s - lead, 0)) if not add else jnp.where(s < lead, 0, f(s - lead))

                def add_other(copy, to, ref):
                    copy.wait_recv()
                    add_sent(1, to)
                    keep(to, ref).start()
                    copy.wait_send()

                def mlp_step(ps, wd_s, wu_s, act_ref, slope_ref):
                    s = ps.index[0]

                    def work(t):
                        backward(f(t), wd_s[0], wu_s[0], act_ref, slope_ref, add)

                    if last:
                        _, at, down, up, begun = last
                        copies = [to_partner(0, at + i, n_tp + at + i) for i in BOTH]

                        @pl.when(s < lead)
                        def _():
                            hooks(s, table)
                            pl.when(s == 1)(lambda: copies[0].start())
                            rows = pl.ds(half, half)
                            act_p[rows, :] = pair_gelu(rows, wu_s[0], f_u(s))[0]
                            p_snd[s] += mm(act_p[rows, :], dyp[rows, :], TN)
                            pl.when(s == 1)(lambda: add_other(copies[0], at, down))

                        @pl.when(s >= lead)
                        def _():
                            t = s - lead
                            pl.when(t == 0)(lambda: begun())
                            pl.when(t == 1)(lambda: copies[1].start())
                            work(t)

                            @pl.when(t < lead)
                            def _():
                                def body(rows):
                                    dpre_p[rows, :] = (mm(dyp[rows, :], wd_s[0], NT) * pair_gelu(rows, wu_s[0], f(t))[1]).astype(BF16)

                                loop_rows(tok, half, body)
                                for i in BOTH:
                                    part = pl.ds(i * half, half)
                                    p_snd[t, pl.ds(0, ffn), part] = mm(h2[:, part], dpre[...], TN) + mm(h2p[:, part], dpre_p[...], TN)

                            pl.when(t == 1)(lambda: add_other(copies[1], at + 1, up))
                            hooks(s, table)
                    else:
                        work(s)
                        hooks(s, table)

                pipe(mlp_step, grid=(n + lead,), in_specs=[wd_spec(f_d), wu_spec(f_u), cols(f_d), cols(f_d)])(wd, wu, act_hbm, slope_hbm)

            acc[...] = jnp.zeros_like(acc)
            acc2[...] = jnp.zeros_like(acc2)
            mlp(1, lambda s: s, True, {})
            net.got('ur')
            net.start('ul')
            net.got('ul')
            mlp_up(2, lambda s: s + FAR0, {})
            net.got('h0')
            cross = lambda s: 2 * CROSS + 1 - s
            down_first(cross)

            def sent_down():
                keep(0, x_dn).wait()
                net.start('dn_x')

            def sent_up():
                keep(1, x_up).wait()
                net.start('up_x')

            mlp(n_chips + 1, lambda t: jnp.where(t < 2, cross(t), t - 1), True, {
                0: lambda: (net.got('dc'), net.start('dg', 'd0r', 'd1r'), net.got('h1', 'dg')),
                3: lambda: (net.got('dp'), net.start('df')), 4: lambda: net.got('df'), 5: sent_up}, (cross, 0, x_dn, x_up, sent_down))

            for slot in (FAR0, FAR1):
                gb[slot] = jnp.zeros_like(gb[slot])

            def far_step(ps, w_u, act_ref, slope_ref):
                part, core = ps.index
                hooks(2 * part + core, {0: lambda: (net.got('d0r'), net.start('d0l')), 1: lambda: net.got('d0l'),
                                        2: lambda: (net.got('d1r'), net.start('d1l')), 3: lambda: net.got('d1l')})
                w_d = dx1b[pl.ds(pl.multiple_of(core * ffn + part * quarter, quarter), quarter), :]

                def body(rows):
                    d_pre = mm(dy[rows, :], w_d, NT) * slope_ref[rows, :]
                    gb[FAR0 + core, :, span(part, quarter)] += col_sum(d_pre)
                    acc[rows, :] += mm(act_ref[rows, :], w_d, NN)
                    acc2[rows, :] += mm(d_pre.astype(BF16), w_u[0], NT)

                loop_rows(tok, half, body)

            narrow = pl.BlockSpec((tok, quarter), lambda part, core: (0, 2 * (FAR0 + core) + part))
            pipe(far_step, grid=(len(BOTH),) * len(BOTH), in_specs=[pl.BlockSpec((1, dim, quarter), lambda part, core: (FAR0 + core, 0, part)), narrow, narrow])(
                wu, act_hbm, slope_hbm)

            def y_rows(rows):
                y[rows, :] = (x1[rows, :].astype(F32) + (acc[rows, :] + bias_d[...])).astype(BF16)

            loop_rows(tok, 2 * chunk, y_rows)
            vec[...] = jnp.zeros_like(vec)
            net.start('y', 'y_far', 'y_own')
            net.sent('d0l', 'd1l')

            @pl.loop(0, tok // (2 * chunk))
            def _(i):
                rows = span(i, 2 * chunk)
                x1_f, dy_f, dh = x1[rows, :].astype(F32), dy[rows, :].astype(F32), acc2[rows, :]
                x_hat, inv_std = ln_stats(x1_f)
                d_x1 = dy_f + ln_grad(dh, x_hat, inv_std, gain2[...])
                acc2[rows, :] = d_x1
                low = d_x1.astype(BF16)
                dx1b[rows, :] = low
                d_o = mm(low, wo[...].reshape(n_tp * width, dim), NT).astype(BF16)
                do4[pl.ds(2 * i, 2)] = d_o.reshape(2, seqs, p_len, n_tp * width)
                for n, t in enumerate((d_x1, dh * x_hat, dh, dy_f)):
                    vec[2 + n:3 + n, :] += col_sum(t)

            pair_begin()

            def bwd_step(ps, q_ref, k_ref, v_ref, w):
                step = ps.index[0]
                g = order(step)
                hooks(step, {2: lambda: (stored(0), net.start('at_relay0', 'at_relay1')),
                             4: lambda: (stored(1), net.start('at_early')), 6: lambda: (stored(2), pass_on(0, 0)), 7: lambda: pass_on(0, 2)})
                pair_go(step)
                b8[g] = jnp.zeros_like(b8[0])
                fold(gb[g], b8.at[g], 3)
                for b in range(seqs):
                    bad = ok[b][:, 0:1].astype(F32) <= 0
                    k = k_ref[0, :, b].reshape(seq, width)
                    v = v_ref[0, :, b].reshape(seq, width)
                    k_t = k.T
                    for c in range(seq // qc):
                        src = slice(c * srcs, (c + 1) * srcs)
                        at = slice(c * qc, (c + 1) * qc)
                        q = q_ref[0, src, b].reshape(qc, width)
                        d_o = do4[src, b, :, span(g, width)].reshape(qc, width)
                        dk = jnp.zeros((seq, width), F32)
                        dv = jnp.zeros((seq, width), F32)
                        dqs = []
                        for h in range(heads):
                            mine = lane // hd == h
                            q_h = jnp.where(mine, q, jnp.zeros_like(q))
                            do_h = jnp.where(mine, d_o, jnp.zeros_like(d_o))
                            s = jnp.where(bad, NEG_LARGE, mm(k, q_h, NT))
                            p = jnp.exp(s - st[g, b, h:h + 1, at]) * st[g, b, heads + h:heads + h + 1, at]
                            dv += mm(p.astype(BF16), do_h, NN)
                            dp = mm(v, do_h, NT)
                            ds = (p * (dp - col_sum(dp * p))).astype(BF16)
                            dk += mm(ds, q_h, NN)
                            dqs.append(mm(k_t[h * hd:(h + 1) * hd], ds, NN))
                        dq_acc[at, :] = jnp.concatenate(dqs, axis=0).T
                        dk_acc[...] = dk if c == 0 else dk_acc[...] + dk
                        dv_acc[...] = dv if c == 0 else dv_acc[...] + dv
                    cos, sin = cos_t[...], sin_t[...]
                    dq, dk, dv = dq_acc[...], dk_acc[...], dv_acc[...]
                    dq = (dq * cos - swap_halves(dq, hd) * sin) * q_scale
                    dk = dk * cos - swap_halves(dk, hd) * sin
                    for i, t in enumerate((dq, dk, dv)):
                        for n in range(n_tp):
                            dpre[pl.ds((n * seqs + b) * p_len, p_len), pl.ds(i * width, width)] = t[n * p_len:(n + 1) * p_len].astype(BF16)
                        b8[g, i:i + 1, :] += col_sum(t)

                @pl.when(step == 0)
                def _():
                    acc[...] = jnp.zeros_like(acc)

                @pl.loop(0, 2)
                def _(i):
                    acc[span(i, half), :] += mm(dpre[span(i, half), pl.ds(0, n3)], w[0], NN)

                def tile(put):
                    put((pl.ds(0, n3),), mm(dpre[:, pl.ds(0, n3)], h1[...], TN))
                    put((pl.ds(n3, width),), mm(o4[:, :, :, span(g, width)].reshape(tok, width), dx1b[...], TN))

                pair(step, tile)
                hooks(step, {6: lambda: pass_on(0, 1)})

            slot_blk = pl.BlockSpec((1, n_tp, seqs, p_len, width), lambda s: (order(s), 0, 0, 0, 0))
            pipe(bwd_step, grid=(n_tp,), in_specs=[slot_blk] * 3 + [slot3(n3, dim, order)])(
                q_hbm, k_hbm, v_hbm, wq)

            pass_on(1, 0)

            def ln1_bwd(rows):
                x_hat, inv_std = ln_stats(x[rows, :].astype(F32))
                dh = acc[rows, :]
                h1[rows, :] = (acc2[rows, :] + ln_grad(dh, x_hat, inv_std, gain1[...])).astype(BF16)
                vec[0:1, :] += col_sum(dh * x_hat)
                vec[1:2, :] += col_sum(dh)

            loop_rows(tok, 2 * chunk, ln1_bwd)
            stored(3)
            for r in range(6):
                fold(vec[pl.ds(r, 1), :], v_own, r * n_tp)
            mate[0:v_half] = v_own[span(1 - side, v_half), :]
            for n in range(n_chips):
                mate[pl.ds(v_half + n * 8, 8)] = b8[2 * n + 1]
            net.start('mate')
            pass_on(1, 1)
            net.got('mate')
            v_sum = v_own[span(side, v_half), :] + mate_in[0:v_half]
            for n in range(n_chips):
                late[n, 0:v_half] = v_sum
                late[n, v_half:] = b8[2 * n] + mate_in[pl.ds(v_half + n * 8, 8)]
            net.start('late')
            pass_on(1, 2)
            net.start('gx', 'gx_far', 'gx_own')

            net.sent('y', 'y_far')
            net.done('y_own')
            pair_begin()
            mine = lambda s: 1 - s
            down_first(mine)
            mlp(2, mine, False, {}, (mine, 2, p_dn, p_up, lambda: None))
            for i, ref in enumerate((p_dn, p_up)):
                keep(2 + i, ref).wait()

            def total(refs, out, block, at):
                def body(*blocks):
                    v = blocks[1][...]
                    for more in blocks[2:-1]:
                        v += more[...]
                    blocks[-1][...] = v

                pipe(body, grid=(len(BOTH),), in_specs=[pl.BlockSpec(block, at)] * len(refs),
                     out_specs=[pl.BlockSpec(block, lambda i: (i, 0))])(*refs, out)

            by_row, by_col = lambda i: (i, 0), lambda i: (0, i)
            net.got('late')
            late_sum = late[0]
            for n in range(1, n_chips):
                late_sum += late_in[n]
            v_own[span(side, v_half), :] = late_sum[0:v_half]
            b8[0] = late_sum[v_half:]
            net.start('final')
            net.got('dn_x', 'up_x')
            total((p_dn, r_dn), g_down, (t_half, dim), by_row)
            total((p_up, r_up), g_up, (n_tile, half), by_col)
            net.got('at_early', 'at_sum0', 'at_sum1')
            for rows, out, n in ((pl.ds(0, n3), g_q, n3), (pl.ds(n3, width), g_o, width)):
                total((p_at.at[0, rows], early_at.at[rows], last_at.at[rows]), out, (n // 2, dim), by_row)
            for name in net.copies:
                if name not in ('load', 'store', 'own', 'write', 'gx', 'gx_far', 'y', 'y_far', 'd0l', 'd1l') and not name.endswith(('_own', '_load', '_store')):
                    net.sent(name)
            net.got('y', 'y_far', 'final')
            net.start('write')
            net.done('gx_own', 'write')
            net.got('gx', 'gx_far')
            net.sent('gx', 'gx_far')

        big = (tok, dim)
        shapes = lambda *dims, dtype=F32: sds(dims, dtype)
        flat = lambda t: t.reshape(tok, dim)
        inv_freq = ROPE_BASE ** (-2.0 * np.arange(hd // 2) / hd)
        sign = np.repeat([-1.0, 1.0], hd // 2)
        freq = np.stack([np.tile(inv_freq, 2 * heads), np.tile(sign, heads)]).astype(np.float32)
        line = lambda v: v.reshape(1, -1)
        sem = lambda n: pltpu.SemaphoreType.DMA((n,))
        low = functools.partial(shapes, dtype=BF16)
        weights = [low(n_tp, n3, dim), low(n_tp, dim, ffn), low(n_tp, ffn, dim)]
        tiles = [shapes(n_chips, n_tile, dim)] + [shapes(n_tile, dim)] * 10
        out_shape = ([low(*big)] * 2 + [shapes(dim, ffn), shapes(ffn, dim), shapes(n3, dim), shapes(width, dim), shapes(6 * n_tp, LANES), shapes(8, LANES)] + weights
                     + [low(n_tp, n_tp, seqs, p_len, width)] * 3 + [low(tok, n_tp * ffn), shapes(tok, n_tp * ffn)] + tiles)
        plain = [pad_mask] + [line(v) for v in (ln1_gain, ln1_bias, b_out, ln2_gain, b_down, ln2_bias)] + [freq]
        heads4 = low(n_tp, seqs, p_len, n_tp * width)
        stat = shapes(n_tp, seqs, heads + heads, seq)
        tile8 = shapes(n_tp, 8, LANES)
        late = shapes(n_chips, v_half + 8, LANES)
        mate = shapes(v_half + 8 * n_chips, LANES)
        row_ffn = shapes(n_tp, 1, ffn)
        scratch = ([low(*big)] * 9 + [heads4, heads4, low(n_tp, width, dim)] + [shapes(*big)] * 2
                   + [shapes(n_chips, n_tile, dim), shapes(2, n_tile, dim)]
                   + [shapes(seq, width)] * 5 + [low(seqs, seq, LANES), stat, shapes(n_tp, 1, n3), row_ffn, row_ffn]
                   + [shapes(n_tp, *b_qkv.shape), tile8, late, late, shapes(8, dim), mate, mate, shapes(6 * n_tp, LANES)]
                   + [low(tok, ffn)] + plain)
        outs = pl.pallas_call(
            kernel, name='layer', out_shape=out_shape, in_specs=[ANY] * 16, out_specs=[ANY] * len(out_shape),
            scratch_shapes=[pltpu.VMEM(v.shape, v.dtype) for v in scratch]
            + [sem(91), sem(91), sem(30), sem(20), sem(12), pltpu.SemaphoreType.REGULAR],
            compiler_params=pltpu.CompilerParams(collective_id=0, has_side_effects=True, vmem_limit_bytes=VMEM_LIMIT),
        )(flat(x_in), flat(grad_y), w_qkv.transpose(0, 2, 3, 1).reshape(n3, dim), b_qkv, w_out.reshape(width, dim),
          w_up, line(b_up), w_down, *plain)

        large = [low(*big)] * 2 + [shapes(dim, ffn), shapes(ffn, dim), shapes(n3, dim), shapes(width, dim)]
        small = [shapes(*b_qkv.shape), shapes(1, ffn)] + [shapes(1, dim)] * len(large)
        given = large + [shapes(*o.shape) for o in outs[6:8]]

        def finish(*refs):
            it = iter(refs)
            src, out, bufs, made, (took, gave) = (list(itertools.islice(it, n)) for n in (
                len(given), len(large + small), len(given), len(small), 2))
            cuts = [(n, pl.ds(i * (r.shape[0] // 2), r.shape[0] // 2)) for i in BOTH for n, r in enumerate(large)]
            whole = [pltpu.make_async_copy(src[n], bufs[n], took.at[n]) for n in range(len(large), len(given))]
            loads = [pltpu.make_async_copy(src[n].at[p], bufs[n].at[p], took.at[len(given) + i]) for i, (n, p) in enumerate(cuts)]
            stores = [pltpu.make_async_copy(bufs[n].at[p], out[n].at[p], gave.at[len(small) + i]) for i, (n, p) in enumerate(cuts)]
            tiny = [pltpu.make_async_copy(b, o, gave.at[i]) for i, (b, o) in enumerate(zip(made, out[len(large):]))]
            for c in whole + loads:
                c.start()
            for c in whole:
                c.wait()
            v_ref, b_ref = bufs[len(large):]
            for i in range(3):
                for h in range(heads):
                    made[0][i, h:h + 1, :] = b_ref[i:i + 1, h * hd:(h + 1) * hd]
            unfold(b_ref, 3, made[1])
            for r, ref in enumerate(made[2:]):
                unfold(v_ref, r * n_tp, ref)
            for c in tiny:
                c.start()
            for load, give in zip(loads, stores):
                load.wait()
                give.start()
            for c in tiny + stores:
                c.wait()

        res = pl.pallas_call(
            finish, name='finish', out_shape=large + small, in_specs=[ANY] * len(given), out_specs=[ANY] * len(large + small),
            scratch_shapes=[pltpu.VMEM(v.shape, v.dtype) for v in given + small] + [sem(20)] * 2,
            compiler_params=pltpu.CompilerParams(vmem_limit_bytes=VMEM_LIMIT),
        )(*outs[:8])
        y_out, grad_x, grad_w_up, grad_w_down, gq, go, grad_b_qkv, grad_b_up = res[:8]
        v = [t.reshape(dim) for t in res[8:]]
        return (y_out.reshape(x_in.shape), grad_x.reshape(x_in.shape), v[0], v[1], gq.reshape(3, heads, hd, dim).transpose(0, 3, 1, 2),
                grad_b_qkv, go.reshape(heads, hd, dim), v[2], v[3], v[4], grad_w_up, grad_b_up.reshape(ffn), grad_w_down, v[5])

    return jax.shard_map(device_step, mesh=mesh, in_specs=in_specs, out_specs=out_specs, check_vma=False)
```

```python
import functools
import itertools

import jax
import jax.numpy as jnp
import numpy as np
from jax import lax
from jax.experimental import pallas as pl
from jax.experimental.pallas import tpu as pltpu
from jax.sharding import PartitionSpec as P

LN_EPS = 1e-5
ROPE_BASE = 10000.0
INV_SQRT2 = 0.7071067811865476
INV_SQRT_2PI = 0.3989422804014327
NEG_LARGE = -1e30
F32 = jnp.float32
BF16 = jnp.bfloat16
VMEM_LIMIT = 66_500_000
LANES = 128
NN = (((1,), (0,)), ((), ()))
NT = (((1,), (1,)), ((), ()))
TN = (((0,), (0,)), ((), ()))
PAIR, FAR, CROSS = 1, 2, 3
FAR0 = FAR + FAR
FAR1 = FAR0 + 1
BOTH = range(2)
ANY = pl.BlockSpec(memory_space=pl.ANY)


def mm(a, b, dims):
    return lax.dot_general(a, b, dims, preferred_element_type=F32)


def ln_stats(v):
    centered = v - jnp.mean(v, axis=-1, keepdims=True)
    inv_std = lax.rsqrt(jnp.mean(centered * centered, axis=-1, keepdims=True) + LN_EPS)
    return centered * inv_std, inv_std


def ln_grad(d_out, x_hat, inv_std, gain):
    d_hat = d_out * gain
    return inv_std * (d_hat - jnp.mean(d_hat, axis=-1, keepdims=True) - x_hat * jnp.mean(d_hat * x_hat, axis=-1, keepdims=True))


def col_sum(t):
    return jnp.sum(t, axis=0, keepdims=True)


def swap_halves(t, head_dim):
    half = head_dim // 2
    lane = lax.broadcasted_iota(jnp.int32, t.shape, t.ndim - 1)
    return jnp.where(lane % head_dim < half, pltpu.roll(t, t.shape[-1] - half, t.ndim - 1), pltpu.roll(t, half, t.ndim - 1))


def span(i, n):
    return pl.ds(pl.multiple_of(i * n, n), n)


def fold(row, out, first):
    for i in range(row.shape[-1] // LANES):
        out[pl.ds(first + i, 1), :] = row[:, i * LANES:(i + 1) * LANES]


def unfold(src, first, out):
    for i in range(out.shape[-1] // LANES):
        out[:, pl.ds(i * LANES, LANES)] = src[pl.ds(first + i, 1), :]


def loop_rows(total, n, body):
    @pl.loop(0, total // n)
    def _(i):
        body(span(i, n))


class Net:
    def __init__(self, n_tp, send, recv, local):
        self.n_tp, self.send, self.recv, self.local = n_tp, send, recv, local
        self.copies, self.count, self.n_local = {}, 0, 0

    def peer(self, chip, core=0):
        me = lax.axis_index('tp')
        way = 1 - 2 * lax.rem(lax.div(me, 2), 2)
        at = lax.rem(me + 2 * chip * way + self.n_tp, self.n_tp) if chip else me
        return at + 1 - 2 * lax.rem(at, 2) if core else at

    def add(self, name, src, dst, chip, core=0):
        n = self.count
        self.count += 1

        def make():
            return pltpu.make_async_remote_copy(
                src_ref=src(), dst_ref=dst(), send_sem=self.send.at[n], recv_sem=self.recv.at[n],
                device_id={'tp': self.peer(chip, core)}, device_id_type=pl.DeviceIdType.MESH)

        self.copies.setdefault(name, []).append(make)

    def add_local(self, name, src, dst):
        n = self.n_local
        self.n_local += 1
        self.copies.setdefault(name, []).append(lambda: pltpu.make_async_copy(src(), dst(), self.local.at[n]))

    def start(self, *names):
        for name in names:
            for make in self.copies[name]:
                make().start()

    def got(self, *names):
        for name in names:
            with jax.named_scope('got_' + name):
                for make in self.copies[name]:
                    make().wait_recv()

    def sent(self, *names):
        for name in names:
            for make in self.copies[name]:
                make().wait_send()

    def done(self, *names):
        for name in names:
            with jax.named_scope('done_' + name):
                for make in self.copies[name]:
                    make().wait()

    def gather(self, name, own, buf):
        for stage, chip in (('p', PAIR), ('c', CROSS)):
            self.add(name + stage, lambda: own, lambda c=chip: buf.at[2 * c], chip)
        self.add(name + 'm', lambda: own, lambda: buf.at[1], 0, 1)
        for stage, chip in (('f', PAIR), ('g', CROSS)):
            self.add(name + stage, lambda c=chip: buf.at[2 * c], lambda c=chip: buf.at[2 * c + 1], 0, 1)

    def gather_far(self, name, src, here, other, via):
        self.add(name + 'r', src, here, via)
        self.add(name + 'l', here, other, 0, 1)

    def exchange(self, name, src, dst, rows, stage=None):
        me = lax.axis_index('tp')
        for core in BOTH:
            for chip in (PAIR, CROSS, FAR, 0):
                if chip == FAR and stage is not None:
                    self.add(name + '_by', lambda k=core: src.at[span(self.peer(FAR, k), rows)], lambda k=core: stage.at[k], PAIR)
                    self.add(name + '_on', lambda k=core: stage.at[k], lambda: dst.at[span(self.peer(PAIR), rows)], CROSS, core)
                elif chip + core:
                    self.add(name, lambda c=chip, k=core: src.at[span(self.peer(c, k), rows)], lambda: dst.at[span(me, rows)], chip, core)
        self.add_local(name + '_own', lambda: src.at[span(me, rows)], lambda: dst.at[span(me, rows)])

    def multicast(self, name, src, dst, pair_dst, rows):
        me = lax.axis_index('tp')
        at = lambda buf: (lambda: buf.at[span(me, rows)])
        other = {0: PAIR, PAIR: 0, CROSS: FAR}
        for chip, stage in ((CROSS, '_cross'), (PAIR, '_pair'), (0, '_pair')):
            for core in BOTH:
                if chip + core:
                    for c, buf in ((chip, dst), (other[chip], pair_dst)):
                        self.add(name + stage, lambda c=c, k=core: src.at[span(self.peer(c, k), rows)], at(buf), chip, core)
        for c, buf in ((0, dst), (PAIR, pair_dst)):
            self.add_local(name + '_own', lambda c=c: src.at[span(self.peer(c), rows)], at(buf))
        came = lambda buf: (lambda: buf.at[span(lax.div(self.peer(CROSS), 2), 2 * rows)])
        self.add(name + '_fwd', came(dst), came(pair_dst), PAIR)
        self.add(name + '_fwd', came(pair_dst), came(dst), PAIR)


def solution(mesh):
    n_tp = mesh.shape['tp']
    n_chips = n_tp // 2
    act_spec = P('dp', 'tp', None)
    rep_vec = P(None)
    part_vec = P('dp')
    in_specs = (act_spec, act_spec, P('dp', None), rep_vec, rep_vec, P(None, None, 'tp', None), P(None, 'tp', None),
                P('tp', None, None), rep_vec, rep_vec, rep_vec, P(None, 'tp'), P('tp'), P('tp', None), rep_vec)
    out_specs = (act_spec, act_spec, part_vec, part_vec, P('dp', None, 'tp', None), P('dp', 'tp', None),
                 P(('dp', 'tp'), None, None), part_vec, part_vec, part_vec, P('dp', 'tp'), P(('dp', 'tp')),
                 P(('dp', 'tp'), None), part_vec)

    def device_step(x_in, grad_y, pad_mask, ln1_gain, ln1_bias, w_qkv, b_qkv, w_out, b_out, ln2_gain, ln2_bias, w_up, b_up, w_down, b_down):
        batch, p_len, dim = x_in.shape
        seq = pad_mask.shape[1]
        _, _, heads, hd = w_qkv.shape
        seqs = batch // n_tp
        ffn = w_up.shape[1]
        width = heads * hd
        n3 = 3 * width
        tok = seqs * seq
        chunk = seqs * p_len
        qc = seq // 2
        q_scale = hd ** -0.5
        sds = jax.ShapeDtypeStruct
        n_tile = n3 + width
        half = dim // 2
        twice = n_tp + n_tp
        quarter = ffn // 2
        v_half = 3 * n_tp

        def kernel(*refs):
            it = iter(refs)
            take = lambda n: [next(it) for _ in range(n)]
            (x_ref, dy_ref, wq_ref, bq_ref, wo_ref, wu_ref, bu_ref, wd_ref), plain = take(8), take(8)
            y_out, gx_out, g_up, g_down, g_q, g_o, g_vec, g_b, wq, wu, wd, q_hbm, k_hbm, v_hbm, act_hbm, slope_hbm, stage = take(17)
            p_at, got_at, sum_at, early_at, last_at, x_dn, x_up, p_dn, p_up, r_dn, r_up = take(11)
            x, h1, dy, x1, h2, dx1b, h2p, dyp, y, o4, do4, wo, acc, acc2, p_rcv, p_snd, d4 = take(17)
            dq_acc, dk_acc, dv_acc, cos_t, sin_t, ok, m_st, l_st, b_att, b_ffn, u_all, gb, b_all, b8, late, late_in, vec, mate, mate_in, v_own = take(20)
            dpre = next(it)
            act_p, dpre_p = (y.at[:, pl.ds(i * ffn, ffn)] for i in BOTH)
            here = take(8)
            send, recv, local, pair_send, pair_recv, pair_ready = take(6)
            net = Net(n_tp, send, recv, local)
            me = lax.axis_index('tp')
            mask_ref, gain1, bias1, bias_o, gain2, bias_d, bias2, freq_ref = here

            net.gather('q', wq_ref, wq)
            net.gather('o', wo_ref, wo)
            net.gather('u', wu_ref, wu)
            net.gather('d', wd_ref, wd)
            for name, buf in (('q', wq), ('o', wo), ('u', wu)):
                net.gather_far(name, lambda b=buf: b.at[2 * PAIR], lambda b=buf: b.at[FAR0], lambda b=buf: b.at[FAR1], CROSS)
            for i in BOTH:
                mine = lambda core, i=i: dx1b.at[pl.ds(core * ffn + i * quarter, quarter)]
                net.gather_far(f'd{i}', lambda i=i: wd.at[2 * CROSS, pl.ds(i * quarter, quarter)], lambda m=mine: m(0), lambda m=mine: m(1), PAIR)
            net.exchange('x', x_ref, x, chunk)
            net.multicast('dy', dy_ref, dy, dyp, chunk)
            net.exchange('y', y, y_out, chunk, stage)
            net.exchange('gx', h1, gx_out, chunk)
            for chip in range(n_chips):
                for core in BOTH:
                    if chip + core:
                        slot = 2 * chip + core
                        net.add('bias', lambda: bq_ref, lambda n=slot: b_all.at[n], chip, core)
                        net.add('bias', lambda: bu_ref, lambda n=slot: u_all.at[n], chip, core)
            for chip in (PAIR, CROSS, FAR):
                net.add('late', lambda n=chip: late.at[n], lambda n=chip: late_in.at[n], chip)
            side = lax.rem(me, 2)
            net.add('mate', lambda: mate, lambda: mate_in, 0, 1)
            net.add('final', lambda: v_own.at[span(side, v_half)], lambda: v_own.at[span(side, v_half)], 0, 1)
            for i in BOTH:
                net.add(f'h{i}', lambda p=pl.ds(i * half, half): h2.at[p], lambda p=pl.ds(i * half, half): h2p.at[p], PAIR)
            net.add('dn_x', lambda: x_dn, lambda: r_dn, CROSS)
            net.add('up_x', lambda: x_up, lambda: r_up, CROSS)
            net.add('at_early', lambda: p_at.at[PAIR], lambda: early_at, PAIR)
            t_half = n_tile // 2
            for i, part in enumerate((pl.ds(0, t_half), pl.ds(t_half, t_half))):
                net.add(f'at_relay{i}', lambda p=part: p_at.at[FAR, p], lambda p=part: got_at.at[p], PAIR)
                net.add(f'at_sum{i}', lambda p=part: sum_at.at[p], lambda p=part: last_at.at[p], CROSS)
                net.add_local(f'at{i}_load', lambda p=part: got_at.at[p], lambda p=part: p_rcv.at[0, p])
                net.add_local(f'at{i}_load', lambda p=part: p_at.at[CROSS, p], lambda p=part: p_rcv.at[1, p])
                net.add_local(f'at{i}_store', lambda p=part: p_rcv.at[1, p], lambda p=part: sum_at.at[p])
            for src, dst in zip(plain, here):
                net.add_local('own', lambda r=src: r, lambda r=dst: r)
            net.add_local('write', lambda: v_own, lambda: g_vec)
            net.add_local('write', lambda: b8.at[0], lambda: g_b)
            for ref, tmp, buf in ((wq_ref, lambda: h2.at[pl.ds(0, n3)], wq), (wu_ref, lambda: x1.at[:, pl.ds(0, ffn)], wu),
                                        (wd_ref, lambda: dx1b.at[pl.ds(0, ffn)], wd)):
                net.add_local('load', lambda r=ref: r, tmp)
                net.add_local('store', tmp, lambda b=buf: b.at[0])
            net.add_local('own', lambda: wo_ref, lambda: wo.at[0])
            net.add_local('own', lambda: bq_ref, lambda: b_all.at[0])
            net.add_local('own', lambda: bu_ref, lambda: u_all.at[0])
            def pass_on(i, stage):
                if stage == 0:
                    net.got(f'at_relay{i}')
                    net.start(f'at{i}_load')
                elif stage == 1:
                    net.done(f'at{i}_load')

                    def body(rows):
                        rows = pl.ds(i * t_half + rows.start, rows.size)
                        p_rcv[1, rows] += p_rcv[0, rows]

                    loop_rows(t_half, 8, body)
                    net.start(f'at{i}_store')
                else:
                    net.done(f'at{i}_store')
                    net.start(f'at_sum{i}')

            def hooks(step, table):
                for at, act in table.items():
                    @pl.when(step == at)
                    def _(act=act):
                        act()

            tile_order = (FAR, PAIR, CROSS, 0)

            def place(i):
                return jnp.where(i == 0, FAR, jnp.where(i == 1, PAIR, jnp.where(i == 2, CROSS, 0)))

            def order(s):
                return 2 * place(lax.div(s, 2)) + 1 - lax.rem(s, 2)

            def to_partner(src, dst, sem):
                return pltpu.make_async_remote_copy(
                    src_ref=p_snd.at[src], dst_ref=p_rcv.at[dst], send_sem=pair_send.at[sem], recv_sem=pair_recv.at[sem],
                    device_id={'tp': net.peer(0, 1)}, device_id_type=pl.DeviceIdType.MESH)

            def keep(i, to):
                return pltpu.make_async_copy(p_rcv.at[i], to, pair_send.at[twice + i])

            def into(i):
                return lambda at, v: p_snd.__setitem__((i,) + at, v)

            def add_sent(i, j):
                def body(rows):
                    p_rcv[j, rows] += p_snd[i, rows]

                loop_rows(n_tile, 16, body)

            def pair_go(s):
                @pl.when(lax.rem(s, 2) == 1)
                def _():
                    to_partner(0, lax.div(s, 2), lax.div(s, 2)).start()

            def pair(s, tile):
                j = lax.div(s, 2)
                odd = lax.rem(s, 2)
                tile(into(odd))

                @pl.when(odd == 1)
                def _():
                    copy = to_partner(0, j, j)
                    copy.wait_send()
                    copy.wait_recv()
                    add_sent(1, j)
                    keep(j, p_at.at[place(j)]).start()

            def stored(i):
                keep(i, p_at.at[tile_order[i]]).wait()

            def pair_begin():
                pl.semaphore_signal(pair_ready, inc=1, device_id={'tp': net.peer(0, 1)}, device_id_type=pl.DeviceIdType.MESH)
                pl.semaphore_wait(pair_ready, 1)

            barrier = pltpu.get_barrier_semaphore()
            for chip in range(n_chips):
                for core in BOTH:
                    if chip + core:
                        pl.semaphore_signal(barrier, inc=1, device_id={'tp': net.peer(chip, core)}, device_id_type=pl.DeviceIdType.MESH)
            pl.semaphore_wait(barrier, n_tp - 1)
            net.start('qp', 'qc', 'x', 'qm', 'bias', 'own', 'load', 'x_own', 'dy_own')
            net.done('own')
            angle = lax.broadcasted_iota(jnp.int32, (seq, width), 0).astype(F32) * freq_ref[0:1, :]
            cos_t[...] = jnp.cos(angle)
            sin_t[...] = jnp.sin(angle) * freq_ref[1:2, :]
            for b in range(seqs):
                row = mask_ref[pl.ds(me * seqs + b, 1), :].astype(F32)
                ok[b] = jnp.broadcast_to(row, (LANES, seq)).T
            net.done('load')
            net.start('store')
            net.got('qp', 'qc')
            net.start('qr', 'dy_cross', 'oc', 'op', 'up', 'dy_pair', 'qf', 'qg', 'om')
            net.done('x_own', 'dy_own')
            net.got('bias')
            for n in range(n_tp):
                b = b_all[n]
                b_att[n] = jnp.concatenate([b[i // heads, i % heads:i % heads + 1, :] for i in range(3 * heads)], axis=1)
                b_ffn[n] = u_all[n]
            net.got('x')

            def ln1(rows):
                x_hat, _ = ln_stats(x[rows, :].astype(F32))
                h1[rows, :] = (x_hat * gain1[...] + bias1[...]).astype(BF16)

            loop_rows(tok, chunk, ln1)
            net.done('store')
            net.got('qm', 'qf', 'qg')

            def arrival(s):
                return s + 2 * lax.div(s, n_chips) - n_chips * lax.div(s, n_chips + 2)

            def qkv_step(ps, w, q_ref, k_ref, v_ref):
                s = ps.index[0]
                hooks(s, {2: lambda: (net.got('op'), net.start('or', 'uc', 'um', 'of')), 4: lambda: (net.got('qr'), net.start('ql')),
                          5: lambda: net.got('ql')})
                n_src = tok // chunk // 2

                @pl.loop(0, 2)
                def _(i):
                    rows = span(i, tok // 2)
                    t = mm(h1[rows, :], w[0], NT) + b_att[arrival(s)]
                    cos, sin = (t_ref[span(i, seq // 2), :].reshape(n_src, 1, p_len, width) for t_ref in (cos_t, sin_t))

                    def rope(v):
                        out = v.reshape(n_src, seqs, p_len, width) * cos + swap_halves(v, hd).reshape(n_src, seqs, p_len, width) * sin
                        return out.astype(BF16)

                    src = span(i, n_src)
                    q_ref[0, src] = rope(t[:, :width] * q_scale)
                    k_ref[0, src] = rope(t[:, width:2 * width])
                    v_ref[0, src] = t[:, 2 * width:].reshape(n_src, seqs, p_len, width).astype(BF16)

            slot3 = lambda rows, cols, f=lambda s: s: pl.BlockSpec((1, rows, cols), lambda s: (f(s), 0, 0))

            def pipe(body, **specs):
                def run(*refs):
                    with jax.named_scope(body.__name__):
                        pltpu.emit_pipeline(body, _explicit_indices=True, **specs)(*refs)

                return run

            pipe(qkv_step, grid=(n_tp,), in_specs=[slot3(n3, dim, arrival)],
                 out_specs=[pl.BlockSpec((1, n_tp, seqs, p_len, width), lambda s: (arrival(s), 0, 0, 0, 0))] * 3)(
                wq, q_hbm, k_hbm, v_hbm)

            srcs = qc // p_len
            lane = lax.broadcasted_iota(jnp.int32, (qc, width), 1)

            def attn_step(ps, q_ref, k_ref, v_ref):
                g, b = ps.index
                hooks(g * seqs + b, {
                    8: lambda: (net.got('dy_cross'), net.start('dy_fwd')), 9: lambda: (net.got('up'), net.start('ur', 'dc', 'dm', 'uf')),
                    14: lambda: (net.got('oc', 'or'), net.start('og', 'ol'))})
                bad = ok[b][:, 0:1] <= 0
                k = k_ref[0, :, 0].reshape(seq, width)
                v_t = v_ref[0, :, 0].reshape(seq, width).T
                for c in range(seq // qc):
                    src = slice(c * srcs, (c + 1) * srcs)
                    cols = slice(c * qc, (c + 1) * qc)
                    q = q_ref[0, src, 0].reshape(qc, width)
                    outs = []
                    for h in range(heads):
                        s = jnp.where(bad, NEG_LARGE, mm(k, jnp.where(lane // hd == h, q, jnp.zeros_like(q)), NT))
                        m = jnp.max(s, axis=0, keepdims=True)
                        e = jnp.exp(s - m)
                        r = 1.0 / col_sum(e)
                        outs.append(mm(v_t[h * hd:(h + 1) * hd], (e * r).astype(BF16), NN))
                        m_st[g, b, h:h + 1, cols] = m
                        l_st[g, b, h:h + 1, cols] = r
                    o4[src, b, :, span(g, width)] = jnp.concatenate(outs, axis=0).T.astype(BF16).reshape(srcs, p_len, width)

            head_blk = pl.BlockSpec((1, n_tp, 1, p_len, width), lambda g, b: (g, 0, b, 0, 0))
            pipe(attn_step, grid=(n_tp, seqs), in_specs=[head_blk] * 3)(q_hbm, k_hbm, v_hbm)

            net.got('om', 'of', 'og', 'ol')

            @pl.loop(0, tok // (2 * chunk))
            def _(i):
                rows = span(i, 2 * chunk)
                o = o4[pl.ds(2 * i, 2)].reshape(2 * chunk, n_tp * width)
                low = (x[rows, :].astype(F32) + (mm(o, wo[...].reshape(n_tp * width, dim), NN) + bias_o[...])).astype(BF16)
                x1[rows, :] = low
                x_hat, _ = ln_stats(low.astype(F32))
                h2[rows, :] = (x_hat * gain2[...] + bias2[...]).astype(BF16)

            net.start('h0', 'h1', 'dp')

            def gelu(pre):
                erf_term = lax.erf(pre * INV_SQRT2)
                phi = 0.5 * (1.0 + erf_term)
                return (pre * phi).astype(BF16), phi + pre * jnp.exp(-0.5 * pre * pre) * INV_SQRT_2PI

            cols = lambda f: pl.BlockSpec((tok, ffn), lambda s: (0, f(s)))
            wu_spec, wd_spec = functools.partial(slot3, dim, ffn), functools.partial(slot3, ffn, dim)

            def mlp_up(n, f, table):
                def up_step(ps, w, act_ref, slope_ref):
                    s = ps.index[0]
                    hooks(s, table)

                    def body(rows):
                        act_ref[rows, :], slope_ref[rows, :] = gelu(mm(h2[rows, :], w[0], NN) + b_ffn[f(s)])

                    loop_rows(tok, half, body)

                pipe(up_step, grid=(n,), in_specs=[wu_spec(f)], out_specs=[cols(f)] * 2)(wu, act_hbm, slope_hbm)

            net.got('um', 'uf')
            mlp_up(n_tp - 2, arrival, {2: lambda: (net.got('uc'), net.start('ug')), 3: lambda: net.got('ug')})
            net.got('dy_pair', 'dy_fwd', 'dm')

            def backward(slot, w_d, w_u, act_ref, slope_ref, add):
                if add:
                    gb[slot] = jnp.zeros_like(gb[0])

                def body(rows):
                    d_pre = mm(dy[rows, :], w_d, NT) * slope_ref[rows, :]
                    low = d_pre.astype(BF16)
                    dpre[rows, :] = low
                    if add:
                        gb[slot] += col_sum(d_pre)
                        acc[rows, :] += mm(act_ref[rows, :], w_d, NN)
                        acc2[rows, :] += mm(low, w_u, NT)

                loop_rows(tok, half, body)

            def pair_gelu(rows, w_u, slot):
                return gelu(mm(h2p[rows, :], w_u, NN) + b_ffn[slot])

            def grads(chip, at, x_ref, between):
                f = lambda s: 2 * chip + 1 - s
                copy = to_partner(0, at, n_tp + at)

                def first(ps, w_u, act_ref):
                    s = ps.index[0]
                    rows = pl.ds(0, half)
                    act_p[rows, :] = pair_gelu(rows, w_u[0], f(s))[0]
                    p_snd[s] = mm(act_ref[...], dy[...], TN) + mm(act_p[rows, :], dyp[rows, :], TN)

                def second(ps, w_u):
                    s = ps.index[0]
                    pl.when(s == 1)(lambda: copy.start())
                    rows = pl.ds(half, half)
                    act_p[rows, :] = pair_gelu(rows, w_u[0], f(s))[0]
                    p_snd[s] += mm(act_p[rows, :], dyp[rows, :], TN)

                    @pl.when(s == 1)
                    def _():
                        copy.wait_recv()
                        add_sent(1, at)
                        keep(at, x_ref).start()
                        copy.wait_send()

                pipe(first, grid=(len(BOTH),), in_specs=[wu_spec(f), cols(f)])(wu, act_hbm)
                between()
                pipe(second, grid=(len(BOTH),), in_specs=[wu_spec(f)])(wu)
                keep(at, x_ref).wait()

            def mlp(n, f, add, table, last=None):
                def mlp_step(ps, wd_s, wu_s, act_ref, slope_ref):
                    s = ps.index[0]
                    backward(f(s), wd_s[0], wu_s[0], act_ref, slope_ref, add)
                    if last:
                        at, ref, send = last
                        copy = to_partner(0, at + 1, n_tp + at + 1)
                        pl.when(s == 1)(lambda: copy.start())

                        @pl.when(s < 2)
                        def _():
                            def body(rows):
                                dpre_p[rows, :] = (mm(dyp[rows, :], wd_s[0], NT) * pair_gelu(rows, wu_s[0], f(s))[1]).astype(BF16)

                            loop_rows(tok, half, body)
                            for i in BOTH:
                                part = pl.ds(i * half, half)
                                p_snd[s, pl.ds(0, ffn), part] = mm(h2[:, part], dpre[...], TN) + mm(h2p[:, part], dpre_p[...], TN)

                        @pl.when(s == 1)
                        def _():
                            copy.wait_recv()
                            add_sent(1, at + 1)
                            keep(at + 1, ref).start()
                            copy.wait_send()

                    hooks(s, table)

                pipe(mlp_step, grid=(n,), in_specs=[wd_spec(f), wu_spec(f), cols(f), cols(f)])(wd, wu, act_hbm, slope_hbm)

            acc[...] = jnp.zeros_like(acc)
            acc2[...] = jnp.zeros_like(acc2)
            mlp(2, lambda s: s, True, {})
            net.got('ur')
            net.start('ul')
            net.got('ul')
            mlp_up(2, lambda s: s + FAR0, {})
            net.got('h0')
            grads(CROSS, 0, x_dn, lambda: (net.got('dc'), net.start('dg', 'd0r', 'd1r'), net.got('h1')))
            net.start('dn_x')
            net.got('dg')

            def sent_up():
                keep(1, x_up).wait()
                net.start('up_x')

            slots = lambda s: jnp.where(s < 2, 2 * CROSS + 1 - s, s)
            mlp(n_chips, slots, True, {0: lambda: (net.got('dp'), net.start('df')), 1: lambda: net.got('df'), 2: sent_up}, (0, x_up, 'up_x'))

            for slot in (FAR0, FAR1):
                gb[slot] = jnp.zeros_like(gb[slot])

            def far_step(ps, w_u, act_ref, slope_ref):
                part, core = ps.index
                hooks(2 * part + core, {0: lambda: (net.got('d0r'), net.start('d0l')), 1: lambda: net.got('d0l'),
                                        2: lambda: (net.got('d1r'), net.start('d1l')), 3: lambda: net.got('d1l')})
                w_d = dx1b[pl.ds(pl.multiple_of(core * ffn + part * quarter, quarter), quarter), :]

                def body(rows):
                    d_pre = mm(dy[rows, :], w_d, NT) * slope_ref[rows, :]
                    gb[FAR0 + core, :, span(part, quarter)] += col_sum(d_pre)
                    acc[rows, :] += mm(act_ref[rows, :], w_d, NN)
                    acc2[rows, :] += mm(d_pre.astype(BF16), w_u[0], NT)

                loop_rows(tok, half, body)

            narrow = pl.BlockSpec((tok, quarter), lambda part, core: (0, 2 * (FAR0 + core) + part))
            pipe(far_step, grid=(len(BOTH),) * len(BOTH), in_specs=[pl.BlockSpec((1, dim, quarter), lambda part, core: (FAR0 + core, 0, part)), narrow, narrow])(
                wu, act_hbm, slope_hbm)

            def y_rows(rows):
                y[rows, :] = (x1[rows, :].astype(F32) + (acc[rows, :] + bias_d[...])).astype(BF16)

            loop_rows(tok, 2 * chunk, y_rows)
            vec[...] = jnp.zeros_like(vec)
            net.start('y', 'y_by', 'y_own')
            net.sent('d0l', 'd1l')

            @pl.loop(0, tok // (2 * chunk))
            def _(i):
                rows = span(i, 2 * chunk)
                x1_f, dy_f, dh = x1[rows, :].astype(F32), dy[rows, :].astype(F32), acc2[rows, :]
                x_hat, inv_std = ln_stats(x1_f)
                d_x1 = dy_f + ln_grad(dh, x_hat, inv_std, gain2[...])
                acc2[rows, :] = d_x1
                low = d_x1.astype(BF16)
                dx1b[rows, :] = low
                d_o = mm(low, wo[...].reshape(n_tp * width, dim), NT).astype(BF16)
                do4[pl.ds(2 * i, 2)] = d_o.reshape(2, seqs, p_len, n_tp * width)
                for n, t in enumerate((d_x1, dh * x_hat, dh, dy_f)):
                    vec[2 + n:3 + n, :] += col_sum(t)

            pair_begin()

            def bwd_step(ps, q_ref, k_ref, v_ref, w):
                step = ps.index[0]
                g = order(step)
                hooks(step, {2: lambda: (stored(0), net.start('at_relay0', 'at_relay1')),
                             3: lambda: (net.got('y_by'), net.start('y_on')), 4: lambda: (stored(1), net.start('at_early')), 6: lambda: (stored(2), pass_on(0, 0)), 7: lambda: pass_on(0, 2)})
                pair_go(step)
                b8[g] = jnp.zeros_like(b8[0])
                fold(gb[g], b8.at[g], 3)
                for b in range(seqs):
                    bad = ok[b][:, 0:1] <= 0
                    k = k_ref[0, :, b].reshape(seq, width)
                    v = v_ref[0, :, b].reshape(seq, width)
                    k_t = k.T
                    for c in range(seq // qc):
                        src = slice(c * srcs, (c + 1) * srcs)
                        at = slice(c * qc, (c + 1) * qc)
                        q = q_ref[0, src, b].reshape(qc, width)
                        d_o = do4[src, b, :, span(g, width)].reshape(qc, width)
                        dk = jnp.zeros((seq, width), F32)
                        dv = jnp.zeros((seq, width), F32)
                        dqs = []
                        for h in range(heads):
                            mine = lane // hd == h
                            q_h = jnp.where(mine, q, jnp.zeros_like(q))
                            do_h = jnp.where(mine, d_o, jnp.zeros_like(d_o))
                            s = jnp.where(bad, NEG_LARGE, mm(k, q_h, NT))
                            p = jnp.exp(s - m_st[g, b, h:h + 1, at]) * l_st[g, b, h:h + 1, at]
                            dv += mm(p.astype(BF16), do_h, NN)
                            dp = mm(v, do_h, NT)
                            ds = (p * (dp - col_sum(dp * p))).astype(BF16)
                            dk += mm(ds, q_h, NN)
                            dqs.append(mm(k_t[h * hd:(h + 1) * hd], ds, NN))
                        dq_acc[at, :] = jnp.concatenate(dqs, axis=0).T
                        dk_acc[...] = dk if c == 0 else dk_acc[...] + dk
                        dv_acc[...] = dv if c == 0 else dv_acc[...] + dv
                    cos, sin = cos_t[...], sin_t[...]
                    dq, dk, dv = dq_acc[...], dk_acc[...], dv_acc[...]
                    dq = (dq * cos - swap_halves(dq, hd) * sin) * q_scale
                    dk = dk * cos - swap_halves(dk, hd) * sin
                    for i, t in enumerate((dq, dk, dv)):
                        d4[:, b, :, i * width:(i + 1) * width] = t.astype(BF16).reshape(n_tp, p_len, width)
                        b8[g, i:i + 1, :] += col_sum(t)

                @pl.when(step == 0)
                def _():
                    acc[...] = jnp.zeros_like(acc)

                @pl.loop(0, 2)
                def _(i):
                    acc[span(i, half), :] += mm(d4[pl.ds(n_chips * i, n_chips)].reshape(half, n3), w[0], NN)

                def tile(put):
                    put((pl.ds(0, n3),), mm(d4[...].reshape(tok, n3), h1[...], TN))
                    put((pl.ds(n3, width),), mm(o4[:, :, :, span(g, width)].reshape(tok, width), dx1b[...], TN))

                pair(step, tile)
                hooks(step, {6: lambda: pass_on(0, 1)})

            slot_blk = pl.BlockSpec((1, n_tp, seqs, p_len, width), lambda s: (order(s), 0, 0, 0, 0))
            pipe(bwd_step, grid=(n_tp,), in_specs=[slot_blk] * 3 + [slot3(n3, dim, order)])(
                q_hbm, k_hbm, v_hbm, wq)

            pass_on(1, 0)

            def ln1_bwd(rows):
                x_hat, inv_std = ln_stats(x[rows, :].astype(F32))
                dh = acc[rows, :]
                h1[rows, :] = (acc2[rows, :] + ln_grad(dh, x_hat, inv_std, gain1[...])).astype(BF16)
                vec[0:1, :] += col_sum(dh * x_hat)
                vec[1:2, :] += col_sum(dh)

            loop_rows(tok, 2 * chunk, ln1_bwd)
            stored(3)
            for r in range(6):
                fold(vec[pl.ds(r, 1), :], v_own, r * n_tp)
            mate[0:v_half] = v_own[span(1 - side, v_half), :]
            for n in range(n_chips):
                mate[pl.ds(v_half + n * 8, 8)] = b8[2 * n + 1]
            net.start('mate')
            pass_on(1, 1)
            net.got('mate')
            v_sum = v_own[span(side, v_half), :] + mate_in[0:v_half]
            for n in range(n_chips):
                late[n, 0:v_half] = v_sum
                late[n, v_half:] = b8[2 * n] + mate_in[pl.ds(v_half + n * 8, 8)]
            net.start('late')
            pass_on(1, 2)
            net.start('gx', 'gx_own')

            net.sent('y', 'y_by')
            net.done('y_own')
            pair_begin()
            grads(0, 2, p_dn, lambda: None)
            mlp(2, lambda s: 1 - s, False, {}, (2, p_up, None))
            keep(3, p_up).wait()

            def total(refs, out, block, at):
                def body(*blocks):
                    v = blocks[1][...]
                    for more in blocks[2:-1]:
                        v += more[...]
                    blocks[-1][...] = v

                pipe(body, grid=(len(BOTH),), in_specs=[pl.BlockSpec(block, at)] * len(refs),
                     out_specs=[pl.BlockSpec(block, lambda i: (i, 0))])(*refs, out)

            by_row, by_col = lambda i: (i, 0), lambda i: (0, i)
            net.got('late')
            late_sum = late[0]
            for n in range(1, n_chips):
                late_sum += late_in[n]
            v_own[span(side, v_half), :] = late_sum[0:v_half]
            b8[0] = late_sum[v_half:]
            net.start('final')
            net.got('dn_x', 'up_x')
            total((p_dn, r_dn), g_down, (t_half, dim), by_row)
            total((p_up, r_up), g_up, (n_tile, half), by_col)
            net.got('at_early', 'at_sum0', 'at_sum1')
            for rows, out, n in ((pl.ds(0, n3), g_q, n3), (pl.ds(n3, width), g_o, width)):
                total((p_at.at[0, rows], early_at.at[rows], last_at.at[rows]), out, (n // 2, dim), by_row)
            for name in net.copies:
                if name not in ('load', 'store', 'own', 'write', 'gx', 'y', 'y_by', 'd0l', 'd1l') and not name.endswith(('_own', '_load', '_store')):
                    net.sent(name)
            net.got('y', 'y_on', 'final')
            net.start('write')
            net.done('gx_own', 'write')
            net.got('gx')
            net.sent('gx')

        big = (tok, dim)
        shapes = lambda *dims, dtype=F32: sds(dims, dtype)
        flat = lambda t: t.reshape(tok, dim)
        inv_freq = ROPE_BASE ** (-2.0 * np.arange(hd // 2) / hd)
        sign = np.repeat([-1.0, 1.0], hd // 2)
        freq = np.stack([np.tile(inv_freq, 2 * heads), np.tile(sign, heads)]).astype(np.float32)
        line = lambda v: v.reshape(1, -1)
        sem = lambda n: pltpu.SemaphoreType.DMA((n,))
        low = functools.partial(shapes, dtype=BF16)
        weights = [low(n_tp, n3, dim), low(n_tp, dim, ffn), low(n_tp, ffn, dim)]
        tiles = [shapes(n_chips, n_tile, dim)] + [shapes(n_tile, dim)] * 10
        out_shape = ([low(*big)] * 2 + [shapes(dim, ffn), shapes(ffn, dim), shapes(n3, dim), shapes(width, dim), shapes(6 * n_tp, LANES), shapes(8, LANES)] + weights
                     + [low(n_tp, n_tp, seqs, p_len, width)] * 3 + [low(tok, n_tp * ffn), shapes(tok, n_tp * ffn), low(2, chunk, dim)] + tiles)
        plain = [pad_mask] + [line(v) for v in (ln1_gain, ln1_bias, b_out, ln2_gain, b_down, ln2_bias)] + [freq]
        heads4 = low(n_tp, seqs, p_len, n_tp * width)
        stat = shapes(n_tp, seqs, heads, seq)
        tile8 = shapes(n_tp, 8, LANES)
        late = shapes(n_chips, v_half + 8, LANES)
        mate = shapes(v_half + 8 * n_chips, LANES)
        row_ffn = shapes(n_tp, 1, ffn)
        scratch = ([low(*big)] * 9 + [heads4, heads4, low(n_tp, width, dim)] + [shapes(*big)] * 2
                   + [shapes(n_chips, n_tile, dim), shapes(2, n_tile, dim), low(n_tp, seqs, p_len, n3)]
                   + [shapes(seq, width)] * 5 + [shapes(seqs, seq, LANES), stat, stat, shapes(n_tp, 1, n3), row_ffn, row_ffn, row_ffn]
                   + [shapes(n_tp, *b_qkv.shape), tile8, late, late, shapes(8, dim), mate, mate, shapes(6 * n_tp, LANES)]
                   + [low(tok, ffn)] + plain)
        outs = pl.pallas_call(
            kernel, name='layer', out_shape=out_shape, in_specs=[ANY] * 16, out_specs=[ANY] * len(out_shape),
            scratch_shapes=[pltpu.VMEM(v.shape, v.dtype) for v in scratch]
            + [sem(93), sem(93), sem(30), sem(20), sem(12), pltpu.SemaphoreType.REGULAR],
            compiler_params=pltpu.CompilerParams(collective_id=0, has_side_effects=True, vmem_limit_bytes=VMEM_LIMIT),
        )(flat(x_in), flat(grad_y), w_qkv.transpose(0, 2, 3, 1).reshape(n3, dim), b_qkv, w_out.reshape(width, dim),
          w_up, line(b_up), w_down, *plain)

        def finish(*refs):
            it = iter(refs)
            n = len(large)
            src, (v_ref, b_ref), out, (bq_o, bu_o), v_o = (list(itertools.islice(it, k)) for k in (n, 2, n, 2, n))
            for a, b in zip(src, out):
                b[...] = a[...]
            for i in range(3):
                for h in range(heads):
                    bq_o[i, h:h + 1, :] = b_ref[i:i + 1, h * hd:(h + 1) * hd]
            unfold(b_ref, 3, bu_o)
            for r, ref in enumerate(v_o):
                unfold(v_ref, r * n_tp, ref)

        large = [low(*big)] * 2 + [shapes(dim, ffn), shapes(ffn, dim), shapes(n3, dim), shapes(width, dim)]
        small = [shapes(*b_qkv.shape), shapes(1, ffn)] + [shapes(1, dim)] * 6
        moving = [pl.BlockSpec((v.shape[0] // n_chips, v.shape[1]), lambda i: (i, 0)) for v in large]
        fixed = lambda vs: [pl.BlockSpec(v.shape, lambda i, n=len(v.shape): (0,) * n) for v in vs]
        res = pl.pallas_call(
            finish, name='finish', out_shape=large + small, grid=(n_chips,), in_specs=moving + fixed(outs[6:8]),
            out_specs=moving + fixed(small), compiler_params=pltpu.CompilerParams(vmem_limit_bytes=VMEM_LIMIT),
        )(*outs[:8])
        y_out, grad_x, grad_w_up, grad_w_down, gq, go, grad_b_qkv, grad_b_up = res[:8]
        v = [t.reshape(dim) for t in res[8:]]
        return (y_out.reshape(x_in.shape), grad_x.reshape(x_in.shape), v[0], v[1], gq.reshape(3, heads, hd, dim).transpose(0, 3, 1, 2),
                grad_b_qkv, go.reshape(heads, hd, dim), v[2], v[3], v[4], grad_w_up, grad_b_up.reshape(ffn), grad_w_down, v[5])

    return jax.shard_map(device_step, mesh=mesh, in_specs=in_specs, out_specs=out_specs, check_vma=False)
```

```python
import functools

import jax
import jax.numpy as jnp
import numpy as np
from jax import lax
from jax.experimental import pallas as pl
from jax.experimental.pallas import tpu as pltpu
from jax.sharding import PartitionSpec as P

LN_EPS = 1e-5
ROPE_BASE = 10000.0
INV_SQRT2 = 0.7071067811865476
INV_SQRT_2PI = 0.3989422804014327
NEG_LARGE = -1e30
F32 = jnp.float32
BF16 = jnp.bfloat16
VMEM_LIMIT = 66_500_000
LANES = 128
NN = (((1,), (0,)), ((), ()))
NT = (((1,), (1,)), ((), ()))
TN = (((0,), (0,)), ((), ()))
PAIR, FAR, CROSS = 1, 2, 3
FAR0 = FAR + FAR
FAR1 = FAR0 + 1
BOTH = range(2)
ANY = pl.BlockSpec(memory_space=pl.ANY)


def mm(a, b, dims):
    return lax.dot_general(a, b, dims, preferred_element_type=F32)


def ln_stats(v):
    centered = v - jnp.mean(v, axis=-1, keepdims=True)
    inv_std = lax.rsqrt(jnp.mean(centered * centered, axis=-1, keepdims=True) + LN_EPS)
    return centered * inv_std, inv_std


def ln_grad(d_out, x_hat, inv_std, gain):
    d_hat = d_out * gain
    return inv_std * (d_hat - jnp.mean(d_hat, axis=-1, keepdims=True) - x_hat * jnp.mean(d_hat * x_hat, axis=-1, keepdims=True))


def col_sum(t):
    return jnp.sum(t, axis=0, keepdims=True)


def swap_halves(t, head_dim):
    half = head_dim // 2
    lane = lax.broadcasted_iota(jnp.int32, t.shape, t.ndim - 1)
    return jnp.where(lane % head_dim < half, pltpu.roll(t, t.shape[-1] - half, t.ndim - 1), pltpu.roll(t, half, t.ndim - 1))


def span(i, n):
    return pl.ds(pl.multiple_of(i * n, n), n)


def fold(row, out, first):
    for i in range(row.shape[-1] // LANES):
        out[pl.ds(first + i, 1), :] = row[:, i * LANES:(i + 1) * LANES]


def unfold(src, first, out):
    for i in range(out.shape[-1] // LANES):
        out[:, pl.ds(i * LANES, LANES)] = src[pl.ds(first + i, 1), :]


def loop_rows(total, n, body):
    @pl.loop(0, total // n)
    def _(i):
        body(span(i, n))


class Net:
    def __init__(self, n_tp, send, recv, local):
        self.n_tp, self.send, self.recv, self.local = n_tp, send, recv, local
        self.copies, self.count, self.n_local = {}, 0, 0

    def peer(self, chip, core=0):
        me = lax.axis_index('tp')
        way = 1 - 2 * lax.rem(lax.div(me, 2), 2)
        at = lax.rem(me + 2 * chip * way + self.n_tp, self.n_tp) if chip else me
        return at + 1 - 2 * lax.rem(at, 2) if core else at

    def add(self, name, src, dst, chip, core=0):
        n = self.count
        self.count += 1

        def make():
            return pltpu.make_async_remote_copy(
                src_ref=src(), dst_ref=dst(), send_sem=self.send.at[n], recv_sem=self.recv.at[n],
                device_id={'tp': self.peer(chip, core)}, device_id_type=pl.DeviceIdType.MESH)

        self.copies.setdefault(name, []).append(make)

    def add_local(self, name, src, dst):
        n = self.n_local
        self.n_local += 1
        self.copies.setdefault(name, []).append(lambda: pltpu.make_async_copy(src(), dst(), self.local.at[n]))

    def start(self, *names):
        for name in names:
            for make in self.copies[name]:
                make().start()

    def got(self, *names):
        for name in names:
            with jax.named_scope('got_' + name):
                for make in self.copies[name]:
                    make().wait_recv()

    def sent(self, *names):
        for name in names:
            for make in self.copies[name]:
                make().wait_send()

    def done(self, *names):
        for name in names:
            with jax.named_scope('done_' + name):
                for make in self.copies[name]:
                    make().wait()

    def gather(self, name, own, buf):
        for stage, chip in (('p', PAIR), ('c', CROSS)):
            self.add(name + stage, lambda: own, lambda c=chip: buf.at[2 * c], chip)
        self.add(name + 'm', lambda: own, lambda: buf.at[1], 0, 1)
        for stage, chip in (('f', PAIR), ('g', CROSS)):
            self.add(name + stage, lambda c=chip: buf.at[2 * c], lambda c=chip: buf.at[2 * c + 1], 0, 1)

    def gather_far(self, name, src, here, other, via):
        self.add(name + 'r', src, here, via)
        self.add(name + 'l', here, other, 0, 1)

    def exchange(self, name, src, dst, rows):
        me = lax.axis_index('tp')
        for core in BOTH:
            for chip in (PAIR, CROSS, FAR, 0):
                if chip + core:
                    self.add(name, lambda c=chip, k=core: src.at[span(self.peer(c, k), rows)], lambda: dst.at[span(me, rows)], chip, core)
        self.add_local(name + '_own', lambda: src.at[span(me, rows)], lambda: dst.at[span(me, rows)])

    def multicast(self, name, src, dst, pair_dst, rows):
        me = lax.axis_index('tp')
        at = lambda buf: (lambda: buf.at[span(me, rows)])
        other = {0: PAIR, PAIR: 0, CROSS: FAR}
        for chip, stage in ((CROSS, '_cross'), (PAIR, '_pair'), (0, '_pair')):
            for core in BOTH:
                if chip + core:
                    for c, buf in ((chip, dst), (other[chip], pair_dst)):
                        self.add(name + stage, lambda c=c, k=core: src.at[span(self.peer(c, k), rows)], at(buf), chip, core)
        for c, buf in ((0, dst), (PAIR, pair_dst)):
            self.add_local(name + '_own', lambda c=c: src.at[span(self.peer(c), rows)], at(buf))
        came = lambda buf: (lambda: buf.at[span(lax.div(self.peer(CROSS), 2), 2 * rows)])
        self.add(name + '_fwd', came(dst), came(pair_dst), PAIR)
        self.add(name + '_fwd', came(pair_dst), came(dst), PAIR)


def solution(mesh):
    n_tp = mesh.shape['tp']
    n_chips = n_tp // 2
    act_spec = P('dp', 'tp', None)
    rep_vec = P(None)
    part_vec = P('dp')
    in_specs = (act_spec, act_spec, P('dp', None), rep_vec, rep_vec, P(None, None, 'tp', None), P(None, 'tp', None),
                P('tp', None, None), rep_vec, rep_vec, rep_vec, P(None, 'tp'), P('tp'), P('tp', None), rep_vec)
    out_specs = (act_spec, act_spec, part_vec, part_vec, P('dp', None, 'tp', None), P('dp', 'tp', None),
                 P(('dp', 'tp'), None, None), part_vec, part_vec, part_vec, P('dp', 'tp'), P(('dp', 'tp')),
                 P(('dp', 'tp'), None), part_vec)

    def device_step(x_in, grad_y, pad_mask, ln1_gain, ln1_bias, w_qkv, b_qkv, w_out, b_out, ln2_gain, ln2_bias, w_up, b_up, w_down, b_down):
        batch, p_len, dim = x_in.shape
        seq = pad_mask.shape[1]
        _, _, heads, hd = w_qkv.shape
        seqs = batch // n_tp
        ffn = w_up.shape[1]
        width = heads * hd
        n3 = 3 * width
        tok = seqs * seq
        chunk = seqs * p_len
        qc = seq // 2
        q_scale = hd ** -0.5
        sds = jax.ShapeDtypeStruct
        n_tile = n3 + width
        half = dim // 2
        twice = n_tp + n_tp
        quarter = ffn // 2
        v_half = 3 * n_tp

        def kernel(*refs):
            it = iter(refs)
            take = lambda n: [next(it) for _ in range(n)]
            (x_ref, dy_ref, wq_ref, bq_ref, wo_ref, wu_ref, bu_ref, wd_ref), plain = take(8), take(8)
            y_out, gx_out, g_up, g_down, g_q, g_o, g_vec, g_b, wq, wu, wd, q_hbm, k_hbm, v_hbm, act_hbm, slope_hbm = take(16)
            p_at, got_at, sum_at, early_at, last_at, x_dn, x_up, p_dn, p_up, r_dn, r_up = take(11)
            x, h1, dy, x1, h2, dx1b, h2p, dyp, y, o4, do4, wo, acc, acc2, p_rcv, p_snd, d4 = take(17)
            dq_acc, dk_acc, dv_acc, cos_t, sin_t, ok, m_st, l_st, b_att, b_ffn, u_all, gb, b_all, b8, late, late_in, vec, mate, mate_in, v_own = take(20)
            dpre = next(it)
            act_p, dpre_p = (y.at[:, pl.ds(i * ffn, ffn)] for i in BOTH)
            here = take(8)
            send, recv, local, pair_send, pair_recv, pair_ready = take(6)
            net = Net(n_tp, send, recv, local)
            me = lax.axis_index('tp')
            mask_ref, gain1, bias1, bias_o, gain2, bias_d, bias2, freq_ref = here

            net.gather('q', wq_ref, wq)
            net.gather('o', wo_ref, wo)
            net.gather('u', wu_ref, wu)
            net.gather('d', wd_ref, wd)
            for name, buf in (('q', wq), ('o', wo), ('u', wu)):
                net.gather_far(name, lambda b=buf: b.at[2 * PAIR], lambda b=buf: b.at[FAR0], lambda b=buf: b.at[FAR1], CROSS)
            for i in BOTH:
                mine = lambda core, i=i: dx1b.at[pl.ds(core * ffn + i * quarter, quarter)]
                net.gather_far(f'd{i}', lambda i=i: wd.at[2 * CROSS, pl.ds(i * quarter, quarter)], lambda m=mine: m(0), lambda m=mine: m(1), PAIR)
            net.exchange('x', x_ref, x, chunk)
            net.multicast('dy', dy_ref, dy, dyp, chunk)
            net.exchange('y', y, y_out, chunk)
            net.exchange('gx', h1, gx_out, chunk)
            for chip in range(n_chips):
                for core in BOTH:
                    if chip + core:
                        slot = 2 * chip + core
                        net.add('bias', lambda: bq_ref, lambda n=slot: b_all.at[n], chip, core)
                        net.add('bias', lambda: bu_ref, lambda n=slot: u_all.at[n], chip, core)
            for chip in (PAIR, CROSS, FAR):
                net.add('late', lambda n=chip: late.at[n], lambda n=chip: late_in.at[n], chip)
            side = lax.rem(me, 2)
            net.add('mate', lambda: mate, lambda: mate_in, 0, 1)
            net.add('final', lambda: v_own.at[span(side, v_half)], lambda: v_own.at[span(side, v_half)], 0, 1)
            for i in BOTH:
                net.add(f'h{i}', lambda p=pl.ds(i * half, half): h2.at[p], lambda p=pl.ds(i * half, half): h2p.at[p], PAIR)
            net.add('dn_x', lambda: x_dn, lambda: r_dn, CROSS)
            net.add('up_x', lambda: x_up, lambda: r_up, CROSS)
            net.add('at_early', lambda: p_at.at[PAIR], lambda: early_at, PAIR)
            t_half = n_tile // 2
            for i, part in enumerate((pl.ds(0, t_half), pl.ds(t_half, t_half))):
                net.add(f'at_relay{i}', lambda p=part: p_at.at[FAR, p], lambda p=part: got_at.at[p], PAIR)
                net.add(f'at_sum{i}', lambda p=part: sum_at.at[p], lambda p=part: last_at.at[p], CROSS)
                net.add_local(f'at{i}_load', lambda p=part: got_at.at[p], lambda p=part: p_rcv.at[0, p])
                net.add_local(f'at{i}_load', lambda p=part: p_at.at[CROSS, p], lambda p=part: p_rcv.at[1, p])
                net.add_local(f'at{i}_store', lambda p=part: p_rcv.at[1, p], lambda p=part: sum_at.at[p])
            for src, dst in zip(plain, here):
                net.add_local('own', lambda r=src: r, lambda r=dst: r)
            net.add_local('write', lambda: v_own, lambda: g_vec)
            net.add_local('write', lambda: b8.at[0], lambda: g_b)
            for ref, tmp, buf in ((wq_ref, lambda: h2.at[pl.ds(0, n3)], wq), (wu_ref, lambda: x1.at[:, pl.ds(0, ffn)], wu),
                                        (wd_ref, lambda: dx1b.at[pl.ds(0, ffn)], wd)):
                net.add_local('load', lambda r=ref: r, tmp)
                net.add_local('store', tmp, lambda b=buf: b.at[0])
            net.add_local('own', lambda: wo_ref, lambda: wo.at[0])
            net.add_local('own', lambda: bq_ref, lambda: b_all.at[0])
            net.add_local('own', lambda: bu_ref, lambda: u_all.at[0])
            def pass_on(i, stage):
                if stage == 0:
                    net.got(f'at_relay{i}')
                    net.start(f'at{i}_load')
                elif stage == 1:
                    net.done(f'at{i}_load')

                    def body(rows):
                        rows = pl.ds(i * t_half + rows.start, rows.size)
                        p_rcv[1, rows] += p_rcv[0, rows]

                    loop_rows(t_half, 8, body)
                    net.start(f'at{i}_store')
                else:
                    net.done(f'at{i}_store')
                    net.start(f'at_sum{i}')

            def hooks(step, table):
                for at, act in table.items():
                    @pl.when(step == at)
                    def _(act=act):
                        act()

            tile_order = (FAR, PAIR, CROSS, 0)

            def place(i):
                return jnp.where(i == 0, FAR, jnp.where(i == 1, PAIR, jnp.where(i == 2, CROSS, 0)))

            def order(s):
                return 2 * place(lax.div(s, 2)) + 1 - lax.rem(s, 2)

            def to_partner(src, dst, sem):
                return pltpu.make_async_remote_copy(
                    src_ref=p_snd.at[src], dst_ref=p_rcv.at[dst], send_sem=pair_send.at[sem], recv_sem=pair_recv.at[sem],
                    device_id={'tp': net.peer(0, 1)}, device_id_type=pl.DeviceIdType.MESH)

            def keep(i, to):
                return pltpu.make_async_copy(p_rcv.at[i], to, pair_send.at[twice + i])

            def into(i):
                return lambda at, v: p_snd.__setitem__((i,) + at, v)

            def add_sent(i, j):
                def body(rows):
                    p_rcv[j, rows] += p_snd[i, rows]

                loop_rows(n_tile, 16, body)

            def pair_go(s):
                @pl.when(lax.rem(s, 2) == 1)
                def _():
                    to_partner(0, lax.div(s, 2), lax.div(s, 2)).start()

            def pair(s, tile):
                j = lax.div(s, 2)
                odd = lax.rem(s, 2)
                tile(into(odd))

                @pl.when(odd == 1)
                def _():
                    copy = to_partner(0, j, j)
                    copy.wait_send()
                    copy.wait_recv()
                    add_sent(1, j)
                    keep(j, p_at.at[place(j)]).start()

            def stored(i):
                keep(i, p_at.at[tile_order[i]]).wait()

            def pair_begin():
                pl.semaphore_signal(pair_ready, inc=1, device_id={'tp': net.peer(0, 1)}, device_id_type=pl.DeviceIdType.MESH)
                pl.semaphore_wait(pair_ready, 1)

            barrier = pltpu.get_barrier_semaphore()
            for chip in range(n_chips):
                for core in BOTH:
                    if chip + core:
                        pl.semaphore_signal(barrier, inc=1, device_id={'tp': net.peer(chip, core)}, device_id_type=pl.DeviceIdType.MESH)
            pl.semaphore_wait(barrier, n_tp - 1)
            net.start('qp', 'qc', 'x', 'qm', 'bias', 'own', 'load', 'x_own', 'dy_own')
            net.done('own')
            angle = lax.broadcasted_iota(jnp.int32, (seq, width), 0).astype(F32) * freq_ref[0:1, :]
            cos_t[...] = jnp.cos(angle)
            sin_t[...] = jnp.sin(angle) * freq_ref[1:2, :]
            for b in range(seqs):
                row = mask_ref[pl.ds(me * seqs + b, 1), :].astype(F32)
                ok[b] = jnp.broadcast_to(row, (LANES, seq)).T
            net.done('load')
            net.start('store')
            net.got('qp', 'qc')
            net.start('qr', 'dy_cross', 'oc', 'op', 'up', 'dy_pair', 'qf', 'qg', 'om')
            net.done('x_own', 'dy_own')
            net.got('bias')
            for n in range(n_tp):
                b = b_all[n]
                b_att[n] = jnp.concatenate([b[i // heads, i % heads:i % heads + 1, :] for i in range(3 * heads)], axis=1)
                b_ffn[n] = u_all[n]
            net.got('x')

            def ln1(rows):
                x_hat, _ = ln_stats(x[rows, :].astype(F32))
                h1[rows, :] = (x_hat * gain1[...] + bias1[...]).astype(BF16)

            loop_rows(tok, chunk, ln1)
            net.done('store')
            net.got('qm', 'qf', 'qg')

            def arrival(s):
                return s + 2 * lax.div(s, n_chips) - n_chips * lax.div(s, n_chips + 2)

            def qkv_step(ps, w, q_ref, k_ref, v_ref):
                s = ps.index[0]
                hooks(s, {2: lambda: (net.got('op'), net.start('or', 'uc', 'um', 'of')), 4: lambda: (net.got('qr'), net.start('ql')),
                          5: lambda: net.got('ql')})
                n_src = tok // chunk // 2

                @pl.loop(0, 2)
                def _(i):
                    rows = span(i, tok // 2)
                    t = mm(h1[rows, :], w[0], NT) + b_att[arrival(s)]
                    cos, sin = (t_ref[span(i, seq // 2), :].reshape(n_src, 1, p_len, width) for t_ref in (cos_t, sin_t))

                    def rope(v):
                        out = v.reshape(n_src, seqs, p_len, width) * cos + swap_halves(v, hd).reshape(n_src, seqs, p_len, width) * sin
                        return out.astype(BF16)

                    src = span(i, n_src)
                    q_ref[0, src] = rope(t[:, :width] * q_scale)
                    k_ref[0, src] = rope(t[:, width:2 * width])
                    v_ref[0, src] = t[:, 2 * width:].reshape(n_src, seqs, p_len, width).astype(BF16)

            slot3 = lambda rows, cols, f=lambda s: s: pl.BlockSpec((1, rows, cols), lambda s: (f(s), 0, 0))

            def pipe(body, **specs):
                def run(*refs):
                    with jax.named_scope(body.__name__):
                        pltpu.emit_pipeline(body, _explicit_indices=True, **specs)(*refs)

                return run

            pipe(qkv_step, grid=(n_tp,), in_specs=[slot3(n3, dim, arrival)],
                 out_specs=[pl.BlockSpec((1, n_tp, seqs, p_len, width), lambda s: (arrival(s), 0, 0, 0, 0))] * 3)(
                wq, q_hbm, k_hbm, v_hbm)

            srcs = qc // p_len
            lane = lax.broadcasted_iota(jnp.int32, (qc, width), 1)

            def attn_step(ps, q_ref, k_ref, v_ref):
                g, b = ps.index
                hooks(g * seqs + b, {
                    8: lambda: (net.got('dy_cross'), net.start('dy_fwd')), 9: lambda: (net.got('up'), net.start('ur', 'dc', 'dm', 'uf')),
                    14: lambda: (net.got('oc', 'or'), net.start('og', 'ol'))})
                bad = ok[b][:, 0:1] <= 0
                k = k_ref[0, :, 0].reshape(seq, width)
                v_t = v_ref[0, :, 0].reshape(seq, width).T
                for c in range(seq // qc):
                    src = slice(c * srcs, (c + 1) * srcs)
                    cols = slice(c * qc, (c + 1) * qc)
                    q = q_ref[0, src, 0].reshape(qc, width)
                    outs = []
                    for h in range(heads):
                        s = jnp.where(bad, NEG_LARGE, mm(k, jnp.where(lane // hd == h, q, jnp.zeros_like(q)), NT))
                        m = jnp.max(s, axis=0, keepdims=True)
                        e = jnp.exp(s - m)
                        r = 1.0 / col_sum(e)
                        outs.append(mm(v_t[h * hd:(h + 1) * hd], (e * r).astype(BF16), NN))
                        m_st[g, b, h:h + 1, cols] = m
                        l_st[g, b, h:h + 1, cols] = r
                    o4[src, b, :, span(g, width)] = jnp.concatenate(outs, axis=0).T.astype(BF16).reshape(srcs, p_len, width)

            head_blk = pl.BlockSpec((1, n_tp, 1, p_len, width), lambda g, b: (g, 0, b, 0, 0))
            pipe(attn_step, grid=(n_tp, seqs), in_specs=[head_blk] * 3)(q_hbm, k_hbm, v_hbm)

            net.got('om', 'of', 'og', 'ol')

            @pl.loop(0, tok // (2 * chunk))
            def _(i):
                rows = span(i, 2 * chunk)
                o = o4[pl.ds(2 * i, 2)].reshape(2 * chunk, n_tp * width)
                low = (x[rows, :].astype(F32) + (mm(o, wo[...].reshape(n_tp * width, dim), NN) + bias_o[...])).astype(BF16)
                x1[rows, :] = low
                x_hat, _ = ln_stats(low.astype(F32))
                h2[rows, :] = (x_hat * gain2[...] + bias2[...]).astype(BF16)

            net.start('h0', 'h1', 'dp')

            def gelu(pre):
                erf_term = lax.erf(pre * INV_SQRT2)
                phi = 0.5 * (1.0 + erf_term)
                return (pre * phi).astype(BF16), phi + pre * jnp.exp(-0.5 * pre * pre) * INV_SQRT_2PI

            cols = lambda f: pl.BlockSpec((tok, ffn), lambda s: (0, f(s)))
            wu_spec, wd_spec = functools.partial(slot3, dim, ffn), functools.partial(slot3, ffn, dim)

            def mlp_up(n, f, table):
                def up_step(ps, w, act_ref, slope_ref):
                    s = ps.index[0]
                    hooks(s, table)

                    def body(rows):
                        act_ref[rows, :], slope_ref[rows, :] = gelu(mm(h2[rows, :], w[0], NN) + b_ffn[f(s)])

                    loop_rows(tok, half, body)

                pipe(up_step, grid=(n,), in_specs=[wu_spec(f)], out_specs=[cols(f)] * 2)(wu, act_hbm, slope_hbm)

            net.got('um', 'uf')
            mlp_up(n_tp - 2, arrival, {2: lambda: (net.got('uc'), net.start('ug')), 3: lambda: net.got('ug')})
            net.got('dy_pair', 'dy_fwd', 'dm')

            def backward(slot, w_d, w_u, act_ref, slope_ref, add):
                if add:
                    gb[slot] = jnp.zeros_like(gb[0])

                def body(rows):
                    d_pre = mm(dy[rows, :], w_d, NT) * slope_ref[rows, :]
                    low = d_pre.astype(BF16)
                    dpre[rows, :] = low
                    if add:
                        gb[slot] += col_sum(d_pre)
                        acc[rows, :] += mm(act_ref[rows, :], w_d, NN)
                        acc2[rows, :] += mm(low, w_u, NT)

                loop_rows(tok, half, body)

            def pair_gelu(rows, w_u, slot):
                return gelu(mm(h2p[rows, :], w_u, NN) + b_ffn[slot])

            def grads(chip, at, x_ref, between, arrive):
                f = lambda s: 2 * chip + 1 - s
                copy = to_partner(0, at, n_tp + at)

                def first(ps, w_u, act_ref):
                    s = ps.index[0]
                    rows = pl.ds(0, half)
                    act_p[rows, :] = pair_gelu(rows, w_u[0], f(s))[0]
                    p_snd[s] = mm(act_ref[...], dy[...], TN) + mm(act_p[rows, :], dyp[rows, :], TN)

                def second(ps, w_u):
                    s = ps.index[0]
                    pl.when(s == 0)(lambda: arrive())
                    pl.when(s == 1)(lambda: copy.start())
                    rows = pl.ds(half, half)
                    act_p[rows, :] = pair_gelu(rows, w_u[0], f(s))[0]
                    p_snd[s] += mm(act_p[rows, :], dyp[rows, :], TN)

                    @pl.when(s == 1)
                    def _():
                        copy.wait_recv()
                        add_sent(1, at)
                        keep(at, x_ref).start()
                        copy.wait_send()

                pipe(first, grid=(len(BOTH),), in_specs=[wu_spec(f), cols(f)])(wu, act_hbm)
                between()
                pipe(second, grid=(len(BOTH),), in_specs=[wu_spec(f)])(wu)
                keep(at, x_ref).wait()

            def mlp(n, f, add, table, last=None):
                def mlp_step(ps, wd_s, wu_s, act_ref, slope_ref):
                    s = ps.index[0]
                    backward(f(s), wd_s[0], wu_s[0], act_ref, slope_ref, add)
                    if last:
                        at, ref, send = last
                        copy = to_partner(0, at + 1, n_tp + at + 1)
                        pl.when(s == 1)(lambda: copy.start())

                        @pl.when(s < 2)
                        def _():
                            def body(rows):
                                dpre_p[rows, :] = (mm(dyp[rows, :], wd_s[0], NT) * pair_gelu(rows, wu_s[0], f(s))[1]).astype(BF16)

                            loop_rows(tok, half, body)
                            for i in BOTH:
                                part = pl.ds(i * half, half)
                                p_snd[s, pl.ds(0, ffn), part] = mm(h2[:, part], dpre[...], TN) + mm(h2p[:, part], dpre_p[...], TN)

                        @pl.when(s == 1)
                        def _():
                            copy.wait_recv()
                            add_sent(1, at + 1)
                            keep(at + 1, ref).start()
                            copy.wait_send()

                    hooks(s, table)

                pipe(mlp_step, grid=(n,), in_specs=[wd_spec(f), wu_spec(f), cols(f), cols(f)])(wd, wu, act_hbm, slope_hbm)

            acc[...] = jnp.zeros_like(acc)
            acc2[...] = jnp.zeros_like(acc2)
            mlp(2, lambda s: s, True, {})
            net.got('ur')
            net.start('ul')
            net.got('ul')
            mlp_up(2, lambda s: s + FAR0, {})
            net.got('h0')
            grads(CROSS, 0, x_dn, lambda: (net.got('dc'), net.start('dg', 'd0r', 'd1r')), lambda: net.got('h1'))
            net.start('dn_x')
            net.got('dg')

            def sent_up():
                keep(1, x_up).wait()
                net.start('up_x')

            slots = lambda s: jnp.where(s < 2, 2 * CROSS + 1 - s, s)
            mlp(n_chips, slots, True, {0: lambda: (net.got('dp'), net.start('df')), 1: lambda: net.got('df'), 2: sent_up}, (0, x_up, 'up_x'))

            for slot in (FAR0, FAR1):
                gb[slot] = jnp.zeros_like(gb[slot])

            def far_step(ps, w_u, act_ref, slope_ref):
                part, core = ps.index
                hooks(2 * part + core, {0: lambda: (net.got('d0r'), net.start('d0l')), 1: lambda: net.got('d0l'),
                                        2: lambda: (net.got('d1r'), net.start('d1l')), 3: lambda: net.got('d1l')})
                w_d = dx1b[pl.ds(pl.multiple_of(core * ffn + part * quarter, quarter), quarter), :]

                def body(rows):
                    d_pre = mm(dy[rows, :], w_d, NT) * slope_ref[rows, :]
                    gb[FAR0 + core, :, span(part, quarter)] += col_sum(d_pre)
                    acc[rows, :] += mm(act_ref[rows, :], w_d, NN)
                    acc2[rows, :] += mm(d_pre.astype(BF16), w_u[0], NT)

                loop_rows(tok, half, body)

            narrow = pl.BlockSpec((tok, quarter), lambda part, core: (0, 2 * (FAR0 + core) + part))
            pipe(far_step, grid=(len(BOTH),) * len(BOTH), in_specs=[pl.BlockSpec((1, dim, quarter), lambda part, core: (FAR0 + core, 0, part)), narrow, narrow])(
                wu, act_hbm, slope_hbm)

            def y_rows(rows):
                y[rows, :] = (x1[rows, :].astype(F32) + (acc[rows, :] + bias_d[...])).astype(BF16)

            loop_rows(tok, 2 * chunk, y_rows)
            vec[...] = jnp.zeros_like(vec)
            net.start('y', 'y_own')
            net.sent('d0l', 'd1l')

            @pl.loop(0, tok // (2 * chunk))
            def _(i):
                rows = span(i, 2 * chunk)
                x1_f, dy_f, dh = x1[rows, :].astype(F32), dy[rows, :].astype(F32), acc2[rows, :]
                x_hat, inv_std = ln_stats(x1_f)
                d_x1 = dy_f + ln_grad(dh, x_hat, inv_std, gain2[...])
                acc2[rows, :] = d_x1
                low = d_x1.astype(BF16)
                dx1b[rows, :] = low
                d_o = mm(low, wo[...].reshape(n_tp * width, dim), NT).astype(BF16)
                do4[pl.ds(2 * i, 2)] = d_o.reshape(2, seqs, p_len, n_tp * width)
                for n, t in enumerate((d_x1, dh * x_hat, dh, dy_f)):
                    vec[2 + n:3 + n, :] += col_sum(t)

            pair_begin()

            def bwd_step(ps, q_ref, k_ref, v_ref, w):
                step = ps.index[0]
                g = order(step)
                hooks(step, {2: lambda: (stored(0), net.start('at_relay0', 'at_relay1')),
                             4: lambda: (stored(1), net.start('at_early')), 6: lambda: (stored(2), pass_on(0, 0)), 7: lambda: pass_on(0, 2)})
                pair_go(step)
                b8[g] = jnp.zeros_like(b8[0])
                fold(gb[g], b8.at[g], 3)
                for b in range(seqs):
                    bad = ok[b][:, 0:1] <= 0
                    k = k_ref[0, :, b].reshape(seq, width)
                    v = v_ref[0, :, b].reshape(seq, width)
                    k_t = k.T
                    for c in range(seq // qc):
                        src = slice(c * srcs, (c + 1) * srcs)
                        at = slice(c * qc, (c + 1) * qc)
                        q = q_ref[0, src, b].reshape(qc, width)
                        d_o = do4[src, b, :, span(g, width)].reshape(qc, width)
                        dk = jnp.zeros((seq, width), F32)
                        dv = jnp.zeros((seq, width), F32)
                        dqs = []
                        for h in range(heads):
                            mine = lane // hd == h
                            q_h = jnp.where(mine, q, jnp.zeros_like(q))
                            do_h = jnp.where(mine, d_o, jnp.zeros_like(d_o))
                            s = jnp.where(bad, NEG_LARGE, mm(k, q_h, NT))
                            p = jnp.exp(s - m_st[g, b, h:h + 1, at]) * l_st[g, b, h:h + 1, at]
                            dv += mm(p.astype(BF16), do_h, NN)
                            dp = mm(v, do_h, NT)
                            ds = (p * (dp - col_sum(dp * p))).astype(BF16)
                            dk += mm(ds, q_h, NN)
                            dqs.append(mm(k_t[h * hd:(h + 1) * hd], ds, NN))
                        dq_acc[at, :] = jnp.concatenate(dqs, axis=0).T
                        dk_acc[...] = dk if c == 0 else dk_acc[...] + dk
                        dv_acc[...] = dv if c == 0 else dv_acc[...] + dv
                    cos, sin = cos_t[...], sin_t[...]
                    dq, dk, dv = dq_acc[...], dk_acc[...], dv_acc[...]
                    dq = (dq * cos - swap_halves(dq, hd) * sin) * q_scale
                    dk = dk * cos - swap_halves(dk, hd) * sin
                    for i, t in enumerate((dq, dk, dv)):
                        d4[:, b, :, i * width:(i + 1) * width] = t.astype(BF16).reshape(n_tp, p_len, width)
                        b8[g, i:i + 1, :] += col_sum(t)

                @pl.when(step == 0)
                def _():
                    acc[...] = jnp.zeros_like(acc)

                @pl.loop(0, 2)
                def _(i):
                    acc[span(i, half), :] += mm(d4[pl.ds(n_chips * i, n_chips)].reshape(half, n3), w[0], NN)

                def tile(put):
                    put((pl.ds(0, n3),), mm(d4[...].reshape(tok, n3), h1[...], TN))
                    put((pl.ds(n3, width),), mm(o4[:, :, :, span(g, width)].reshape(tok, width), dx1b[...], TN))

                pair(step, tile)
                hooks(step, {6: lambda: pass_on(0, 1)})

            slot_blk = pl.BlockSpec((1, n_tp, seqs, p_len, width), lambda s: (order(s), 0, 0, 0, 0))
            pipe(bwd_step, grid=(n_tp,), in_specs=[slot_blk] * 3 + [slot3(n3, dim, order)])(
                q_hbm, k_hbm, v_hbm, wq)

            pass_on(1, 0)

            def ln1_bwd(rows):
                x_hat, inv_std = ln_stats(x[rows, :].astype(F32))
                dh = acc[rows, :]
                h1[rows, :] = (acc2[rows, :] + ln_grad(dh, x_hat, inv_std, gain1[...])).astype(BF16)
                vec[0:1, :] += col_sum(dh * x_hat)
                vec[1:2, :] += col_sum(dh)

            loop_rows(tok, 2 * chunk, ln1_bwd)
            stored(3)
            for r in range(6):
                fold(vec[pl.ds(r, 1), :], v_own, r * n_tp)
            mate[0:v_half] = v_own[span(1 - side, v_half), :]
            for n in range(n_chips):
                mate[pl.ds(v_half + n * 8, 8)] = b8[2 * n + 1]
            net.start('mate')
            pass_on(1, 1)
            net.got('mate')
            v_sum = v_own[span(side, v_half), :] + mate_in[0:v_half]
            for n in range(n_chips):
                late[n, 0:v_half] = v_sum
                late[n, v_half:] = b8[2 * n] + mate_in[pl.ds(v_half + n * 8, 8)]
            net.start('late')
            pass_on(1, 2)
            net.start('gx', 'gx_own')

            net.sent('y')
            net.done('y_own')
            pair_begin()
            grads(0, 2, p_dn, lambda: None, lambda: None)
            mlp(2, lambda s: 1 - s, False, {}, (2, p_up, None))
            keep(3, p_up).wait()

            def total(refs, out, block, at):
                def body(*blocks):
                    v = blocks[1][...]
                    for more in blocks[2:-1]:
                        v += more[...]
                    blocks[-1][...] = v

                pipe(body, grid=(len(BOTH),), in_specs=[pl.BlockSpec(block, at)] * len(refs),
                     out_specs=[pl.BlockSpec(block, lambda i: (i, 0))])(*refs, out)

            by_row, by_col = lambda i: (i, 0), lambda i: (0, i)
            net.got('late')
            late_sum = late[0]
            for n in range(1, n_chips):
                late_sum += late_in[n]
            v_own[span(side, v_half), :] = late_sum[0:v_half]
            b8[0] = late_sum[v_half:]
            net.start('final')
            net.got('dn_x', 'up_x')
            total((p_dn, r_dn), g_down, (t_half, dim), by_row)
            total((p_up, r_up), g_up, (n_tile, half), by_col)
            net.got('at_early', 'at_sum0', 'at_sum1')
            for rows, out, n in ((pl.ds(0, n3), g_q, n3), (pl.ds(n3, width), g_o, width)):
                total((p_at.at[0, rows], early_at.at[rows], last_at.at[rows]), out, (n // 2, dim), by_row)
            for name in net.copies:
                if name not in ('load', 'store', 'own', 'write', 'gx', 'y', 'd0l', 'd1l') and not name.endswith(('_own', '_load', '_store')):
                    net.sent(name)
            net.got('y', 'final')
            net.start('write')
            net.done('gx_own', 'write')
            net.got('gx')
            net.sent('gx')

        big = (tok, dim)
        shapes = lambda *dims, dtype=F32: sds(dims, dtype)
        flat = lambda t: t.reshape(tok, dim)
        inv_freq = ROPE_BASE ** (-2.0 * np.arange(hd // 2) / hd)
        sign = np.repeat([-1.0, 1.0], hd // 2)
        freq = np.stack([np.tile(inv_freq, 2 * heads), np.tile(sign, heads)]).astype(np.float32)
        line = lambda v: v.reshape(1, -1)
        sem = lambda n: pltpu.SemaphoreType.DMA((n,))
        low = functools.partial(shapes, dtype=BF16)
        weights = [low(n_tp, n3, dim), low(n_tp, dim, ffn), low(n_tp, ffn, dim)]
        tiles = [shapes(n_chips, n_tile, dim)] + [shapes(n_tile, dim)] * 10
        out_shape = ([low(*big)] * 2 + [shapes(dim, ffn), shapes(ffn, dim), shapes(n3, dim), shapes(width, dim), shapes(6 * n_tp, LANES), shapes(8, LANES)] + weights
                     + [low(n_tp, n_tp, seqs, p_len, width)] * 3 + [low(tok, n_tp * ffn), shapes(tok, n_tp * ffn)] + tiles)
        plain = [pad_mask] + [line(v) for v in (ln1_gain, ln1_bias, b_out, ln2_gain, b_down, ln2_bias)] + [freq]
        heads4 = low(n_tp, seqs, p_len, n_tp * width)
        stat = shapes(n_tp, seqs, heads, seq)
        tile8 = shapes(n_tp, 8, LANES)
        late = shapes(n_chips, v_half + 8, LANES)
        mate = shapes(v_half + 8 * n_chips, LANES)
        row_ffn = shapes(n_tp, 1, ffn)
        scratch = ([low(*big)] * 9 + [heads4, heads4, low(n_tp, width, dim)] + [shapes(*big)] * 2
                   + [shapes(n_chips, n_tile, dim), shapes(2, n_tile, dim), low(n_tp, seqs, p_len, n3)]
                   + [shapes(seq, width)] * 5 + [shapes(seqs, seq, LANES), stat, stat, shapes(n_tp, 1, n3), row_ffn, row_ffn, row_ffn]
                   + [shapes(n_tp, *b_qkv.shape), tile8, late, late, shapes(8, dim), mate, mate, shapes(6 * n_tp, LANES)]
                   + [low(tok, ffn)] + plain)
        outs = pl.pallas_call(
            kernel, name='layer', out_shape=out_shape, in_specs=[ANY] * 16, out_specs=[ANY] * len(out_shape),
            scratch_shapes=[pltpu.VMEM(v.shape, v.dtype) for v in scratch]
            + [sem(91), sem(91), sem(30), sem(20), sem(12), pltpu.SemaphoreType.REGULAR],
            compiler_params=pltpu.CompilerParams(collective_id=0, has_side_effects=True, vmem_limit_bytes=VMEM_LIMIT),
        )(flat(x_in), flat(grad_y), w_qkv.transpose(0, 2, 3, 1).reshape(n3, dim), b_qkv, w_out.reshape(width, dim),
          w_up, line(b_up), w_down, *plain)

        def finish(*refs):
            src, (v_ref, b_ref), out, (bq_o, bu_o), v_o = refs[:6], refs[6:8], refs[8:14], refs[14:16], refs[16:]
            for a, b in zip(src, out):
                b[...] = a[...]
            for i in range(3):
                for h in range(heads):
                    bq_o[i, h:h + 1, :] = b_ref[i:i + 1, h * hd:(h + 1) * hd]
            unfold(b_ref, 3, bu_o)
            for r, ref in enumerate(v_o):
                unfold(v_ref, r * n_tp, ref)

        large = [low(*big)] * 2 + [shapes(dim, ffn), shapes(ffn, dim), shapes(n3, dim), shapes(width, dim)]
        small = [shapes(*b_qkv.shape), shapes(1, ffn)] + [shapes(1, dim)] * 6
        moving = [pl.BlockSpec((v.shape[0] // n_chips, v.shape[1]), lambda i: (i, 0)) for v in large]
        fixed = lambda vs: [pl.BlockSpec(v.shape, lambda i, n=len(v.shape): (0,) * n) for v in vs]
        res = pl.pallas_call(
            finish, name='finish', out_shape=large + small, grid=(n_chips,), in_specs=moving + fixed(outs[6:8]),
            out_specs=moving + fixed(small), compiler_params=pltpu.CompilerParams(vmem_limit_bytes=VMEM_LIMIT),
        )(*outs[:8])
        y_out, grad_x, grad_w_up, grad_w_down, gq, go, grad_b_qkv, grad_b_up = res[:8]
        v = [t.reshape(dim) for t in res[8:]]
        return (y_out.reshape(x_in.shape), grad_x.reshape(x_in.shape), v[0], v[1], gq.reshape(3, heads, hd, dim).transpose(0, 3, 1, 2),
                grad_b_qkv, go.reshape(heads, hd, dim), v[2], v[3], v[4], grad_w_up, grad_b_up.reshape(ffn), grad_w_down, v[5])

    return jax.shard_map(device_step, mesh=mesh, in_specs=in_specs, out_specs=out_specs, check_vma=False)
```

```python
import functools

import jax
import jax.numpy as jnp
import numpy as np
from jax import lax
from jax.experimental import pallas as pl
from jax.experimental.pallas import tpu as pltpu
from jax.sharding import PartitionSpec as P

LN_EPS = 1e-5
ROPE_BASE = 10000.0
INV_SQRT2 = 0.7071067811865476
INV_SQRT_2PI = 0.3989422804014327
NEG_LARGE = -1e30
F32 = jnp.float32
BF16 = jnp.bfloat16
VMEM_LIMIT = 66_500_000
LANES = 128
NN = (((1,), (0,)), ((), ()))
NT = (((1,), (1,)), ((), ()))
TN = (((0,), (0,)), ((), ()))
PAIR, FAR, CROSS = 1, 2, 3
FAR0 = FAR + FAR
FAR1 = FAR0 + 1
BOTH = range(2)
ANY = pl.BlockSpec(memory_space=pl.ANY)


def mm(a, b, dims):
    return lax.dot_general(a, b, dims, preferred_element_type=F32)


def ln_stats(v):
    centered = v - jnp.mean(v, axis=-1, keepdims=True)
    inv_std = lax.rsqrt(jnp.mean(centered * centered, axis=-1, keepdims=True) + LN_EPS)
    return centered * inv_std, inv_std


def ln_grad(d_out, x_hat, inv_std, gain):
    d_hat = d_out * gain
    return inv_std * (d_hat - jnp.mean(d_hat, axis=-1, keepdims=True) - x_hat * jnp.mean(d_hat * x_hat, axis=-1, keepdims=True))


def col_sum(t):
    return jnp.sum(t, axis=0, keepdims=True)


def swap_halves(t, head_dim):
    half = head_dim // 2
    lane = lax.broadcasted_iota(jnp.int32, t.shape, t.ndim - 1)
    return jnp.where(lane % head_dim < half, pltpu.roll(t, t.shape[-1] - half, t.ndim - 1), pltpu.roll(t, half, t.ndim - 1))


def span(i, n):
    return pl.ds(pl.multiple_of(i * n, n), n)


def fold(row, out, first):
    for i in range(row.shape[-1] // LANES):
        out[pl.ds(first + i, 1), :] = row[:, i * LANES:(i + 1) * LANES]


def unfold(src, first, out):
    for i in range(out.shape[-1] // LANES):
        out[:, pl.ds(i * LANES, LANES)] = src[pl.ds(first + i, 1), :]


def loop_rows(total, n, body):
    @pl.loop(0, total // n)
    def _(i):
        body(span(i, n))


class Net:
    def __init__(self, n_tp, send, recv, local):
        self.n_tp, self.send, self.recv, self.local = n_tp, send, recv, local
        self.copies, self.count, self.n_local = {}, 0, 0

    def peer(self, chip, core=0):
        me = lax.axis_index('tp')
        way = 1 - 2 * lax.rem(lax.div(me, 2), 2)
        at = lax.rem(me + 2 * chip * way + self.n_tp, self.n_tp) if chip else me
        return at + 1 - 2 * lax.rem(at, 2) if core else at

    def add(self, name, src, dst, chip, core=0):
        n = self.count
        self.count += 1

        def make():
            return pltpu.make_async_remote_copy(
                src_ref=src(), dst_ref=dst(), send_sem=self.send.at[n], recv_sem=self.recv.at[n],
                device_id={'tp': self.peer(chip, core)}, device_id_type=pl.DeviceIdType.MESH)

        self.copies.setdefault(name, []).append(make)

    def add_local(self, name, src, dst):
        n = self.n_local
        self.n_local += 1
        self.copies.setdefault(name, []).append(lambda: pltpu.make_async_copy(src(), dst(), self.local.at[n]))

    def start(self, *names):
        for name in names:
            for make in self.copies[name]:
                make().start()

    def got(self, *names):
        for name in names:
            with jax.named_scope('got_' + name):
                for make in self.copies[name]:
                    make().wait_recv()

    def sent(self, *names):
        for name in names:
            for make in self.copies[name]:
                make().wait_send()

    def done(self, *names):
        for name in names:
            with jax.named_scope('done_' + name):
                for make in self.copies[name]:
                    make().wait()

    def gather(self, name, own, buf):
        for stage, chip in (('p', PAIR), ('c', CROSS)):
            self.add(name + stage, lambda: own, lambda c=chip: buf.at[2 * c], chip)
        self.add(name + 'm', lambda: own, lambda: buf.at[1], 0, 1)
        for stage, chip in (('f', PAIR), ('g', CROSS)):
            self.add(name + stage, lambda c=chip: buf.at[2 * c], lambda c=chip: buf.at[2 * c + 1], 0, 1)

    def gather_far(self, name, src, here, other, via):
        self.add(name + 'r', src, here, via)
        self.add(name + 'l', here, other, 0, 1)

    def exchange(self, name, src, dst, rows):
        me = lax.axis_index('tp')
        for core in BOTH:
            for chip in (PAIR, CROSS, FAR, 0):
                if chip + core:
                    self.add(name, lambda c=chip, k=core: src.at[span(self.peer(c, k), rows)], lambda: dst.at[span(me, rows)], chip, core)
        self.add_local(name + '_own', lambda: src.at[span(me, rows)], lambda: dst.at[span(me, rows)])

    def multicast(self, name, src, dst, pair_dst, rows):
        me = lax.axis_index('tp')
        at = lambda buf: (lambda: buf.at[span(me, rows)])
        other = {0: PAIR, PAIR: 0, CROSS: FAR}
        for chip, stage in ((CROSS, '_cross'), (PAIR, '_pair'), (0, '_pair')):
            for core in BOTH:
                if chip + core:
                    for c, buf in ((chip, dst), (other[chip], pair_dst)):
                        self.add(name + stage, lambda c=c, k=core: src.at[span(self.peer(c, k), rows)], at(buf), chip, core)
        for c, buf in ((0, dst), (PAIR, pair_dst)):
            self.add_local(name + '_own', lambda c=c: src.at[span(self.peer(c), rows)], at(buf))
        came = lambda buf: (lambda: buf.at[span(lax.div(self.peer(CROSS), 2), 2 * rows)])
        self.add(name + '_fwd', came(dst), came(pair_dst), PAIR)
        self.add(name + '_fwd', came(pair_dst), came(dst), PAIR)


def solution(mesh):
    n_tp = mesh.shape['tp']
    n_chips = n_tp // 2
    act_spec = P('dp', 'tp', None)
    rep_vec = P(None)
    part_vec = P('dp')
    in_specs = (act_spec, act_spec, P('dp', None), rep_vec, rep_vec, P(None, None, 'tp', None), P(None, 'tp', None),
                P('tp', None, None), rep_vec, rep_vec, rep_vec, P(None, 'tp'), P('tp'), P('tp', None), rep_vec)
    out_specs = (act_spec, act_spec, part_vec, part_vec, P('dp', None, 'tp', None), P('dp', 'tp', None),
                 P(('dp', 'tp'), None, None), part_vec, part_vec, part_vec, P('dp', 'tp'), P(('dp', 'tp')),
                 P(('dp', 'tp'), None), part_vec)

    def device_step(x_in, grad_y, pad_mask, ln1_gain, ln1_bias, w_qkv, b_qkv, w_out, b_out, ln2_gain, ln2_bias, w_up, b_up, w_down, b_down):
        batch, p_len, dim = x_in.shape
        seq = pad_mask.shape[1]
        _, _, heads, hd = w_qkv.shape
        seqs = batch // n_tp
        ffn = w_up.shape[1]
        width = heads * hd
        n3 = 3 * width
        tok = seqs * seq
        chunk = seqs * p_len
        qc = seq // 2
        q_scale = hd ** -0.5
        sds = jax.ShapeDtypeStruct
        n_tile = n3 + width
        half = dim // 2
        twice = n_tp + n_tp
        quarter = ffn // 2
        v_half = 3 * n_tp

        def kernel(*refs):
            it = iter(refs)
            take = lambda n: [next(it) for _ in range(n)]
            (x_ref, dy_ref, wq_ref, bq_ref, wo_ref, wu_ref, bu_ref, wd_ref), plain = take(8), take(8)
            y_out, gx_out, g_up, g_down, g_q, g_o, g_vec, g_b, wq, wu, wd, q_hbm, k_hbm, v_hbm, act_hbm, slope_hbm = take(16)
            p_at, got_at, sum_at, early_at, last_at, x_dn, x_up, p_dn, p_up, r_dn, r_up = take(11)
            x, h1, dy, x1, h2, dx1b, h2p, dyp, y, o4, do4, wo, acc, acc2, p_rcv, p_snd, d4 = take(17)
            dq_acc, dk_acc, dv_acc, cos_t, sin_t, ok, m_st, l_st, b_att, b_ffn, u_all, gb, b_all, b8, late, late_in, vec, mate, mate_in, v_own = take(20)
            dpre = next(it)
            act_p, dpre_p = (y.at[:, pl.ds(i * ffn, ffn)] for i in BOTH)
            here = take(8)
            send, recv, local, pair_send, pair_recv, pair_ready = take(6)
            net = Net(n_tp, send, recv, local)
            me = lax.axis_index('tp')
            mask_ref, gain1, bias1, bias_o, gain2, bias_d, bias2, freq_ref = here

            net.gather('q', wq_ref, wq)
            net.gather('o', wo_ref, wo)
            net.gather('u', wu_ref, wu)
            net.gather('d', wd_ref, wd)
            for name, buf in (('q', wq), ('o', wo), ('u', wu)):
                net.gather_far(name, lambda b=buf: b.at[2 * PAIR], lambda b=buf: b.at[FAR0], lambda b=buf: b.at[FAR1], CROSS)
            for i in BOTH:
                mine = lambda core, i=i: dx1b.at[pl.ds(core * ffn + i * quarter, quarter)]
                net.gather_far(f'd{i}', lambda i=i: wd.at[2 * CROSS, pl.ds(i * quarter, quarter)], lambda m=mine: m(0), lambda m=mine: m(1), PAIR)
            net.exchange('x', x_ref, x, chunk)
            net.multicast('dy', dy_ref, dy, dyp, chunk)
            net.exchange('y', y, y_out, chunk)
            net.exchange('gx', h1, gx_out, chunk)
            for chip in range(n_chips):
                for core in BOTH:
                    if chip + core:
                        slot = 2 * chip + core
                        net.add('bias', lambda: bq_ref, lambda n=slot: b_all.at[n], chip, core)
                        net.add('bias', lambda: bu_ref, lambda n=slot: u_all.at[n], chip, core)
            for chip in (PAIR, CROSS, FAR):
                net.add('late', lambda n=chip: late.at[n], lambda n=chip: late_in.at[n], chip)
            side = lax.rem(me, 2)
            net.add('mate', lambda: mate, lambda: mate_in, 0, 1)
            net.add('final', lambda: v_own.at[span(side, v_half)], lambda: v_own.at[span(side, v_half)], 0, 1)
            for i in BOTH:
                net.add(f'h{i}', lambda p=pl.ds(i * half, half): h2.at[p], lambda p=pl.ds(i * half, half): h2p.at[p], PAIR)
            net.add('dn_x', lambda: x_dn, lambda: r_dn, CROSS)
            net.add('up_x', lambda: x_up, lambda: r_up, CROSS)
            net.add('at_early', lambda: p_at.at[PAIR], lambda: early_at, PAIR)
            t_half = n_tile // 2
            for i, part in enumerate((pl.ds(0, t_half), pl.ds(t_half, t_half))):
                net.add(f'at_relay{i}', lambda p=part: p_at.at[FAR, p], lambda p=part: got_at.at[p], PAIR)
                net.add(f'at_sum{i}', lambda p=part: sum_at.at[p], lambda p=part: last_at.at[p], CROSS)
                net.add_local(f'at{i}_load', lambda p=part: got_at.at[p], lambda p=part: p_rcv.at[0, p])
                net.add_local(f'at{i}_load', lambda p=part: p_at.at[CROSS, p], lambda p=part: p_rcv.at[1, p])
                net.add_local(f'at{i}_store', lambda p=part: p_rcv.at[1, p], lambda p=part: sum_at.at[p])
            for src, dst in zip(plain, here):
                net.add_local('own', lambda r=src: r, lambda r=dst: r)
            net.add_local('write', lambda: v_own, lambda: g_vec)
            net.add_local('write', lambda: b8.at[0], lambda: g_b)
            for ref, tmp, buf in ((wq_ref, lambda: h2.at[pl.ds(0, n3)], wq), (wu_ref, lambda: x1.at[:, pl.ds(0, ffn)], wu),
                                        (wd_ref, lambda: dx1b.at[pl.ds(0, ffn)], wd)):
                net.add_local('load', lambda r=ref: r, tmp)
                net.add_local('store', tmp, lambda b=buf: b.at[0])
            net.add_local('own', lambda: wo_ref, lambda: wo.at[0])
            net.add_local('own', lambda: bq_ref, lambda: b_all.at[0])
            net.add_local('own', lambda: bu_ref, lambda: u_all.at[0])
            def pass_on(i, stage):
                if stage == 0:
                    net.got(f'at_relay{i}')
                    net.start(f'at{i}_load')
                elif stage == 1:
                    net.done(f'at{i}_load')

                    def body(rows):
                        rows = pl.ds(i * t_half + rows.start, rows.size)
                        p_rcv[1, rows] += p_rcv[0, rows]

                    loop_rows(t_half, 8, body)
                    net.start(f'at{i}_store')
                else:
                    net.done(f'at{i}_store')
                    net.start(f'at_sum{i}')

            def hooks(step, table):
                for at, act in table.items():
                    @pl.when(step == at)
                    def _(act=act):
                        act()

            tile_order = (FAR, PAIR, CROSS, 0)

            def place(i):
                return jnp.where(i == 0, FAR, jnp.where(i == 1, PAIR, jnp.where(i == 2, CROSS, 0)))

            def order(s):
                return 2 * place(lax.div(s, 2)) + 1 - lax.rem(s, 2)

            def to_partner(src, dst, sem):
                return pltpu.make_async_remote_copy(
                    src_ref=p_snd.at[src], dst_ref=p_rcv.at[dst], send_sem=pair_send.at[sem], recv_sem=pair_recv.at[sem],
                    device_id={'tp': net.peer(0, 1)}, device_id_type=pl.DeviceIdType.MESH)

            def keep(i, to):
                return pltpu.make_async_copy(p_rcv.at[i], to, pair_send.at[twice + i])

            def into(i):
                return lambda at, v: p_snd.__setitem__((i,) + at, v)

            def add_sent(i, j):
                def body(rows):
                    p_rcv[j, rows] += p_snd[i, rows]

                loop_rows(n_tile, 16, body)

            def pair_go(s):
                @pl.when(lax.rem(s, 2) == 1)
                def _():
                    to_partner(0, lax.div(s, 2), lax.div(s, 2)).start()

            def pair(s, tile):
                j = lax.div(s, 2)
                odd = lax.rem(s, 2)
                tile(into(odd))

                @pl.when(odd == 1)
                def _():
                    copy = to_partner(0, j, j)
                    copy.wait_send()
                    copy.wait_recv()
                    add_sent(1, j)
                    keep(j, p_at.at[place(j)]).start()

            def stored(i):
                keep(i, p_at.at[tile_order[i]]).wait()

            def pair_begin():
                pl.semaphore_signal(pair_ready, inc=1, device_id={'tp': net.peer(0, 1)}, device_id_type=pl.DeviceIdType.MESH)
                pl.semaphore_wait(pair_ready, 1)

            barrier = pltpu.get_barrier_semaphore()
            for chip in range(n_chips):
                for core in BOTH:
                    if chip + core:
                        pl.semaphore_signal(barrier, inc=1, device_id={'tp': net.peer(chip, core)}, device_id_type=pl.DeviceIdType.MESH)
            pl.semaphore_wait(barrier, n_tp - 1)
            net.start('qp', 'qc', 'x', 'qm', 'bias', 'own', 'load', 'x_own', 'dy_own')
            net.done('own')
            angle = lax.broadcasted_iota(jnp.int32, (seq, width), 0).astype(F32) * freq_ref[0:1, :]
            cos_t[...] = jnp.cos(angle)
            sin_t[...] = jnp.sin(angle) * freq_ref[1:2, :]
            for b in range(seqs):
                row = mask_ref[pl.ds(me * seqs + b, 1), :].astype(F32)
                ok[b] = jnp.broadcast_to(row, (LANES, seq)).T
            net.done('load')
            net.start('store')
            net.got('qp', 'qc')
            net.start('qr', 'dy_cross', 'oc', 'op', 'up', 'dy_pair', 'qf', 'qg', 'om')
            net.done('x_own', 'dy_own')
            net.got('bias')
            for n in range(n_tp):
                b = b_all[n]
                b_att[n] = jnp.concatenate([b[i // heads, i % heads:i % heads + 1, :] for i in range(3 * heads)], axis=1)
                b_ffn[n] = u_all[n]
            net.got('x')

            def ln1(rows):
                x_hat, _ = ln_stats(x[rows, :].astype(F32))
                h1[rows, :] = (x_hat * gain1[...] + bias1[...]).astype(BF16)

            loop_rows(tok, chunk, ln1)
            net.done('store')
            net.got('qm', 'qf', 'qg')

            def arrival(s):
                return s + 2 * lax.div(s, n_chips) - n_chips * lax.div(s, n_chips + 2)

            def qkv_step(ps, w, q_ref, k_ref, v_ref):
                s = ps.index[0]
                hooks(s, {2: lambda: (net.got('op'), net.start('or', 'uc', 'um', 'of')), 4: lambda: (net.got('qr'), net.start('ql')),
                          5: lambda: net.got('ql')})
                n_src = tok // chunk // 2

                @pl.loop(0, 2)
                def _(i):
                    rows = span(i, tok // 2)
                    t = mm(h1[rows, :], w[0], NT) + b_att[arrival(s)]
                    cos, sin = (t_ref[span(i, seq // 2), :].reshape(n_src, 1, p_len, width) for t_ref in (cos_t, sin_t))

                    def rope(v):
                        out = v.reshape(n_src, seqs, p_len, width) * cos + swap_halves(v, hd).reshape(n_src, seqs, p_len, width) * sin
                        return out.astype(BF16)

                    src = span(i, n_src)
                    q_ref[0, src] = rope(t[:, :width] * q_scale)
                    k_ref[0, src] = rope(t[:, width:2 * width])
                    v_ref[0, src] = t[:, 2 * width:].reshape(n_src, seqs, p_len, width).astype(BF16)

            slot3 = lambda rows, cols, f=lambda s: s: pl.BlockSpec((1, rows, cols), lambda s: (f(s), 0, 0))

            def pipe(body, **specs):
                def run(*refs):
                    with jax.named_scope(body.__name__):
                        pltpu.emit_pipeline(body, _explicit_indices=True, **specs)(*refs)

                return run

            pipe(qkv_step, grid=(n_tp,), in_specs=[slot3(n3, dim, arrival)],
                 out_specs=[pl.BlockSpec((1, n_tp, seqs, p_len, width), lambda s: (arrival(s), 0, 0, 0, 0))] * 3)(
                wq, q_hbm, k_hbm, v_hbm)

            srcs = qc // p_len
            lane = lax.broadcasted_iota(jnp.int32, (qc, width), 1)

            def attn_step(ps, q_ref, k_ref, v_ref):
                g, b = ps.index
                hooks(g * seqs + b, {
                    8: lambda: (net.got('dy_cross'), net.start('dy_fwd')), 9: lambda: (net.got('up'), net.start('ur', 'dc', 'dm', 'uf')),
                    14: lambda: (net.got('oc', 'or'), net.start('og', 'ol'))})
                bad = ok[b][:, 0:1] <= 0
                k = k_ref[0, :, 0].reshape(seq, width)
                v_t = v_ref[0, :, 0].reshape(seq, width).T
                for c in range(seq // qc):
                    src = slice(c * srcs, (c + 1) * srcs)
                    cols = slice(c * qc, (c + 1) * qc)
                    q = q_ref[0, src, 0].reshape(qc, width)
                    outs = []
                    for h in range(heads):
                        s = jnp.where(bad, NEG_LARGE, mm(k, jnp.where(lane // hd == h, q, jnp.zeros_like(q)), NT))
                        m = jnp.max(s, axis=0, keepdims=True)
                        e = jnp.exp(s - m)
                        r = 1.0 / col_sum(e)
                        outs.append(mm(v_t[h * hd:(h + 1) * hd], (e * r).astype(BF16), NN))
                        m_st[g, b, h:h + 1, cols] = m
                        l_st[g, b, h:h + 1, cols] = r
                    o4[src, b, :, span(g, width)] = jnp.concatenate(outs, axis=0).T.astype(BF16).reshape(srcs, p_len, width)

            head_blk = pl.BlockSpec((1, n_tp, 1, p_len, width), lambda g, b: (g, 0, b, 0, 0))
            pipe(attn_step, grid=(n_tp, seqs), in_specs=[head_blk] * 3)(q_hbm, k_hbm, v_hbm)

            net.got('om', 'of', 'og', 'ol')

            @pl.loop(0, tok // (2 * chunk))
            def _(i):
                rows = span(i, 2 * chunk)
                o = o4[pl.ds(2 * i, 2)].reshape(2 * chunk, n_tp * width)
                low = (x[rows, :].astype(F32) + (mm(o, wo[...].reshape(n_tp * width, dim), NN) + bias_o[...])).astype(BF16)
                x1[rows, :] = low
                x_hat, _ = ln_stats(low.astype(F32))
                h2[rows, :] = (x_hat * gain2[...] + bias2[...]).astype(BF16)

            net.start('h0', 'h1', 'dp')

            def gelu(pre):
                erf_term = lax.erf(pre * INV_SQRT2)
                phi = 0.5 * (1.0 + erf_term)
                return (pre * phi).astype(BF16), phi + pre * jnp.exp(-0.5 * pre * pre) * INV_SQRT_2PI

            cols = lambda f: pl.BlockSpec((tok, ffn), lambda s: (0, f(s)))
            wu_spec, wd_spec = functools.partial(slot3, dim, ffn), functools.partial(slot3, ffn, dim)

            def mlp_up(n, f, table):
                def up_step(ps, w, act_ref, slope_ref):
                    s = ps.index[0]
                    hooks(s, table)

                    def body(rows):
                        act_ref[rows, :], slope_ref[rows, :] = gelu(mm(h2[rows, :], w[0], NN) + b_ffn[f(s)])

                    loop_rows(tok, half, body)

                pipe(up_step, grid=(n,), in_specs=[wu_spec(f)], out_specs=[cols(f)] * 2)(wu, act_hbm, slope_hbm)

            net.got('um', 'uf')
            mlp_up(n_tp - 2, arrival, {2: lambda: (net.got('uc'), net.start('ug')), 3: lambda: net.got('ug')})
            net.got('dy_pair', 'dy_fwd', 'dm')

            def backward(slot, w_d, w_u, act_ref, slope_ref, add):
                if add:
                    gb[slot] = jnp.zeros_like(gb[0])

                def body(rows):
                    d_pre = mm(dy[rows, :], w_d, NT) * slope_ref[rows, :]
                    low = d_pre.astype(BF16)
                    dpre[rows, :] = low
                    if add:
                        gb[slot] += col_sum(d_pre)
                        acc[rows, :] += mm(act_ref[rows, :], w_d, NN)
                        acc2[rows, :] += mm(low, w_u, NT)

                loop_rows(tok, half, body)

            def pair_gelu(rows, w_u, slot):
                return gelu(mm(h2p[rows, :], w_u, NN) + b_ffn[slot])

            def grads(chip, at, x_ref, between, arrive):
                f = lambda s: 2 * chip + 1 - s
                copy = to_partner(0, at, n_tp + at)

                def first(ps, w_u, act_ref):
                    s = ps.index[0]
                    rows = pl.ds(0, half)
                    act_p[rows, :] = pair_gelu(rows, w_u[0], f(s))[0]
                    p_snd[s] = mm(act_ref[...], dy[...], TN) + mm(act_p[rows, :], dyp[rows, :], TN)

                def second(ps, w_u):
                    s = ps.index[0]
                    pl.when(s == 0)(lambda: arrive())
                    pl.when(s == 1)(lambda: copy.start())
                    rows = pl.ds(half, half)
                    act_p[rows, :] = pair_gelu(rows, w_u[0], f(s))[0]
                    p_snd[s] += mm(act_p[rows, :], dyp[rows, :], TN)

                    @pl.when(s == 1)
                    def _():
                        copy.wait_recv()
                        add_sent(1, at)
                        keep(at, x_ref).start()
                        copy.wait_send()

                pipe(first, grid=(len(BOTH),), in_specs=[wu_spec(f), cols(f)])(wu, act_hbm)
                between()
                pipe(second, grid=(len(BOTH),), in_specs=[wu_spec(f)])(wu)
                keep(at, x_ref).wait()

            def mlp(n, f, add, table, last=None):
                def mlp_step(ps, wd_s, wu_s, act_ref, slope_ref):
                    s = ps.index[0]
                    backward(f(s), wd_s[0], wu_s[0], act_ref, slope_ref, add)
                    if last:
                        at, ref, send = last
                        copy = to_partner(0, at + 1, n_tp + at + 1)
                        pl.when(s == 1)(lambda: copy.start())

                        @pl.when(s < 2)
                        def _():
                            def body(rows):
                                dpre_p[rows, :] = (mm(dyp[rows, :], wd_s[0], NT) * pair_gelu(rows, wu_s[0], f(s))[1]).astype(BF16)

                            loop_rows(tok, half, body)
                            for i in BOTH:
                                part = pl.ds(i * half, half)
                                p_snd[s, pl.ds(0, ffn), part] = mm(h2[:, part], dpre[...], TN) + mm(h2p[:, part], dpre_p[...], TN)

                        @pl.when(s == 1)
                        def _():
                            copy.wait_recv()
                            add_sent(1, at + 1)
                            keep(at + 1, ref).start()
                            copy.wait_send()

                    hooks(s, table)

                pipe(mlp_step, grid=(n,), in_specs=[wd_spec(f), wu_spec(f), cols(f), cols(f)])(wd, wu, act_hbm, slope_hbm)

            acc[...] = jnp.zeros_like(acc)
            acc2[...] = jnp.zeros_like(acc2)
            mlp(2, lambda s: s, True, {})
            net.got('ur')
            net.start('ul')
            net.got('ul')
            mlp_up(2, lambda s: s + FAR0, {})
            net.got('h0')
            grads(CROSS, 0, x_dn, lambda: (net.got('dc'), net.start('dg', 'd0r', 'd1r')), lambda: net.got('h1'))
            net.start('dn_x')
            net.got('dg')

            def sent_up():
                keep(1, x_up).wait()
                net.start('up_x')

            slots = lambda s: jnp.where(s < 2, 2 * CROSS + 1 - s, s)
            mlp(n_chips, slots, True, {0: lambda: (net.got('dp'), net.start('df')), 1: lambda: net.got('df'), 2: sent_up}, (0, x_up, 'up_x'))

            for slot in (FAR0, FAR1):
                gb[slot] = jnp.zeros_like(gb[slot])

            def y_rows(rows):
                y[rows, :] = (x1[rows, :].astype(F32) + (acc[rows, :] + bias_d[...])).astype(BF16)

            def far_step(ps, w_u, act_ref, slope_ref):
                part, core = ps.index
                hooks(2 * part + core, {0: lambda: (net.got('d0r'), net.start('d0l')), 1: lambda: net.got('d0l'),
                                        2: lambda: (net.got('d1r'), net.start('d1l')), 3: lambda: net.got('d1l')})
                w_d = dx1b[pl.ds(pl.multiple_of(core * ffn + part * quarter, quarter), quarter), :]

                def forward(rows):
                    acc[rows, :] += mm(act_ref[rows, :], w_d, NN)

                loop_rows(tok, half, forward)

                @pl.when(part + core == FAR)
                def _():
                    loop_rows(tok, chunk, y_rows)
                    net.start('y', 'y_own')

                def body(rows):
                    d_pre = mm(dy[rows, :], w_d, NT) * slope_ref[rows, :]
                    gb[FAR0 + core, :, span(part, quarter)] += col_sum(d_pre)
                    acc2[rows, :] += mm(d_pre.astype(BF16), w_u[0], NT)

                loop_rows(tok, half, body)

            narrow = pl.BlockSpec((tok, quarter), lambda part, core: (0, 2 * (FAR0 + core) + part))
            pipe(far_step, grid=(len(BOTH),) * len(BOTH), in_specs=[pl.BlockSpec((1, dim, quarter), lambda part, core: (FAR0 + core, 0, part)), narrow, narrow])(
                wu, act_hbm, slope_hbm)

            vec[...] = jnp.zeros_like(vec)
            net.sent('d0l', 'd1l')

            @pl.loop(0, tok // (2 * chunk))
            def _(i):
                rows = span(i, 2 * chunk)
                x1_f, dy_f, dh = x1[rows, :].astype(F32), dy[rows, :].astype(F32), acc2[rows, :]
                x_hat, inv_std = ln_stats(x1_f)
                d_x1 = dy_f + ln_grad(dh, x_hat, inv_std, gain2[...])
                acc2[rows, :] = d_x1
                low = d_x1.astype(BF16)
                dx1b[rows, :] = low
                d_o = mm(low, wo[...].reshape(n_tp * width, dim), NT).astype(BF16)
                do4[pl.ds(2 * i, 2)] = d_o.reshape(2, seqs, p_len, n_tp * width)
                for n, t in enumerate((d_x1, dh * x_hat, dh, dy_f)):
                    vec[2 + n:3 + n, :] += col_sum(t)

            pair_begin()

            def bwd_step(ps, q_ref, k_ref, v_ref, w):
                step = ps.index[0]
                g = order(step)
                hooks(step, {2: lambda: (stored(0), net.start('at_relay0', 'at_relay1')),
                             4: lambda: (stored(1), net.start('at_early')), 6: lambda: (stored(2), pass_on(0, 0)), 7: lambda: pass_on(0, 2)})
                pair_go(step)
                b8[g] = jnp.zeros_like(b8[0])
                fold(gb[g], b8.at[g], 3)
                for b in range(seqs):
                    bad = ok[b][:, 0:1] <= 0
                    k = k_ref[0, :, b].reshape(seq, width)
                    v = v_ref[0, :, b].reshape(seq, width)
                    k_t = k.T
                    for c in range(seq // qc):
                        src = slice(c * srcs, (c + 1) * srcs)
                        at = slice(c * qc, (c + 1) * qc)
                        q = q_ref[0, src, b].reshape(qc, width)
                        d_o = do4[src, b, :, span(g, width)].reshape(qc, width)
                        dk = jnp.zeros((seq, width), F32)
                        dv = jnp.zeros((seq, width), F32)
                        dqs = []
                        for h in range(heads):
                            mine = lane // hd == h
                            q_h = jnp.where(mine, q, jnp.zeros_like(q))
                            do_h = jnp.where(mine, d_o, jnp.zeros_like(d_o))
                            s = jnp.where(bad, NEG_LARGE, mm(k, q_h, NT))
                            p = jnp.exp(s - m_st[g, b, h:h + 1, at]) * l_st[g, b, h:h + 1, at]
                            dv += mm(p.astype(BF16), do_h, NN)
                            dp = mm(v, do_h, NT)
                            ds = (p * (dp - col_sum(dp * p))).astype(BF16)
                            dk += mm(ds, q_h, NN)
                            dqs.append(mm(k_t[h * hd:(h + 1) * hd], ds, NN))
                        dq_acc[at, :] = jnp.concatenate(dqs, axis=0).T
                        dk_acc[...] = dk if c == 0 else dk_acc[...] + dk
                        dv_acc[...] = dv if c == 0 else dv_acc[...] + dv
                    cos, sin = cos_t[...], sin_t[...]
                    dq, dk, dv = dq_acc[...], dk_acc[...], dv_acc[...]
                    dq = (dq * cos - swap_halves(dq, hd) * sin) * q_scale
                    dk = dk * cos - swap_halves(dk, hd) * sin
                    for i, t in enumerate((dq, dk, dv)):
                        d4[:, b, :, i * width:(i + 1) * width] = t.astype(BF16).reshape(n_tp, p_len, width)
                        b8[g, i:i + 1, :] += col_sum(t)

                @pl.when(step == 0)
                def _():
                    acc[...] = jnp.zeros_like(acc)

                @pl.loop(0, 2)
                def _(i):
                    acc[span(i, half), :] += mm(d4[pl.ds(n_chips * i, n_chips)].reshape(half, n3), w[0], NN)

                def tile(put):
                    put((pl.ds(0, n3),), mm(d4[...].reshape(tok, n3), h1[...], TN))
                    put((pl.ds(n3, width),), mm(o4[:, :, :, span(g, width)].reshape(tok, width), dx1b[...], TN))

                pair(step, tile)
                hooks(step, {6: lambda: pass_on(0, 1)})

            slot_blk = pl.BlockSpec((1, n_tp, seqs, p_len, width), lambda s: (order(s), 0, 0, 0, 0))
            pipe(bwd_step, grid=(n_tp,), in_specs=[slot_blk] * 3 + [slot3(n3, dim, order)])(
                q_hbm, k_hbm, v_hbm, wq)

            pass_on(1, 0)

            def ln1_bwd(rows):
                x_hat, inv_std = ln_stats(x[rows, :].astype(F32))
                dh = acc[rows, :]
                h1[rows, :] = (acc2[rows, :] + ln_grad(dh, x_hat, inv_std, gain1[...])).astype(BF16)
                vec[0:1, :] += col_sum(dh * x_hat)
                vec[1:2, :] += col_sum(dh)

            loop_rows(tok, 2 * chunk, ln1_bwd)
            stored(3)
            for r in range(6):
                fold(vec[pl.ds(r, 1), :], v_own, r * n_tp)
            mate[0:v_half] = v_own[span(1 - side, v_half), :]
            for n in range(n_chips):
                mate[pl.ds(v_half + n * 8, 8)] = b8[2 * n + 1]
            net.start('mate')
            pass_on(1, 1)
            net.got('mate')
            v_sum = v_own[span(side, v_half), :] + mate_in[0:v_half]
            for n in range(n_chips):
                late[n, 0:v_half] = v_sum
                late[n, v_half:] = b8[2 * n] + mate_in[pl.ds(v_half + n * 8, 8)]
            net.start('late')
            pass_on(1, 2)
            net.start('gx', 'gx_own')

            net.sent('y')
            net.done('y_own')
            pair_begin()
            grads(0, 2, p_dn, lambda: None, lambda: None)
            mlp(2, lambda s: 1 - s, False, {}, (2, p_up, None))
            keep(3, p_up).wait()

            def total(refs, out, block, at):
                def body(*blocks):
                    v = blocks[1][...]
                    for more in blocks[2:-1]:
                        v += more[...]
                    blocks[-1][...] = v

                pipe(body, grid=(len(BOTH),), in_specs=[pl.BlockSpec(block, at)] * len(refs),
                     out_specs=[pl.BlockSpec(block, lambda i: (i, 0))])(*refs, out)

            by_row, by_col = lambda i: (i, 0), lambda i: (0, i)
            net.got('late')
            late_sum = late[0]
            for n in range(1, n_chips):
                late_sum += late_in[n]
            v_own[span(side, v_half), :] = late_sum[0:v_half]
            b8[0] = late_sum[v_half:]
            net.start('final')
            net.got('dn_x', 'up_x')
            total((p_dn, r_dn), g_down, (t_half, dim), by_row)
            total((p_up, r_up), g_up, (n_tile, half), by_col)
            net.got('at_early', 'at_sum0', 'at_sum1')
            for rows, out, n in ((pl.ds(0, n3), g_q, n3), (pl.ds(n3, width), g_o, width)):
                total((p_at.at[0, rows], early_at.at[rows], last_at.at[rows]), out, (n // 2, dim), by_row)
            for name in net.copies:
                if name not in ('load', 'store', 'own', 'write', 'gx', 'y', 'd0l', 'd1l') and not name.endswith(('_own', '_load', '_store')):
                    net.sent(name)
            net.got('y', 'final')
            net.start('write')
            net.done('gx_own', 'write')
            net.got('gx')
            net.sent('gx')

        big = (tok, dim)
        shapes = lambda *dims, dtype=F32: sds(dims, dtype)
        flat = lambda t: t.reshape(tok, dim)
        inv_freq = ROPE_BASE ** (-2.0 * np.arange(hd // 2) / hd)
        sign = np.repeat([-1.0, 1.0], hd // 2)
        freq = np.stack([np.tile(inv_freq, 2 * heads), np.tile(sign, heads)]).astype(np.float32)
        line = lambda v: v.reshape(1, -1)
        sem = lambda n: pltpu.SemaphoreType.DMA((n,))
        low = functools.partial(shapes, dtype=BF16)
        weights = [low(n_tp, n3, dim), low(n_tp, dim, ffn), low(n_tp, ffn, dim)]
        tiles = [shapes(n_chips, n_tile, dim)] + [shapes(n_tile, dim)] * 10
        out_shape = ([low(*big)] * 2 + [shapes(dim, ffn), shapes(ffn, dim), shapes(n3, dim), shapes(width, dim), shapes(6 * n_tp, LANES), shapes(8, LANES)] + weights
                     + [low(n_tp, n_tp, seqs, p_len, width)] * 3 + [low(tok, n_tp * ffn), shapes(tok, n_tp * ffn)] + tiles)
        plain = [pad_mask] + [line(v) for v in (ln1_gain, ln1_bias, b_out, ln2_gain, b_down, ln2_bias)] + [freq]
        heads4 = low(n_tp, seqs, p_len, n_tp * width)
        stat = shapes(n_tp, seqs, heads, seq)
        tile8 = shapes(n_tp, 8, LANES)
        late = shapes(n_chips, v_half + 8, LANES)
        mate = shapes(v_half + 8 * n_chips, LANES)
        row_ffn = shapes(n_tp, 1, ffn)
        scratch = ([low(*big)] * 9 + [heads4, heads4, low(n_tp, width, dim)] + [shapes(*big)] * 2
                   + [shapes(n_chips, n_tile, dim), shapes(2, n_tile, dim), low(n_tp, seqs, p_len, n3)]
                   + [shapes(seq, width)] * 5 + [shapes(seqs, seq, LANES), stat, stat, shapes(n_tp, 1, n3), row_ffn, row_ffn, row_ffn]
                   + [shapes(n_tp, *b_qkv.shape), tile8, late, late, shapes(8, dim), mate, mate, shapes(6 * n_tp, LANES)]
                   + [low(tok, ffn)] + plain)
        outs = pl.pallas_call(
            kernel, name='layer', out_shape=out_shape, in_specs=[ANY] * 16, out_specs=[ANY] * len(out_shape),
            scratch_shapes=[pltpu.VMEM(v.shape, v.dtype) for v in scratch]
            + [sem(91), sem(91), sem(30), sem(20), sem(12), pltpu.SemaphoreType.REGULAR],
            compiler_params=pltpu.CompilerParams(collective_id=0, has_side_effects=True, vmem_limit_bytes=VMEM_LIMIT),
        )(flat(x_in), flat(grad_y), w_qkv.transpose(0, 2, 3, 1).reshape(n3, dim), b_qkv, w_out.reshape(width, dim),
          w_up, line(b_up), w_down, *plain)

        def finish(*refs):
            src, (v_ref, b_ref), out, (bq_o, bu_o), v_o = refs[:6], refs[6:8], refs[8:14], refs[14:16], refs[16:]
            for a, b in zip(src, out):
                b[...] = a[...]
            for i in range(3):
                for h in range(heads):
                    bq_o[i, h:h + 1, :] = b_ref[i:i + 1, h * hd:(h + 1) * hd]
            unfold(b_ref, 3, bu_o)
            for r, ref in enumerate(v_o):
                unfold(v_ref, r * n_tp, ref)

        large = [low(*big)] * 2 + [shapes(dim, ffn), shapes(ffn, dim), shapes(n3, dim), shapes(width, dim)]
        small = [shapes(*b_qkv.shape), shapes(1, ffn)] + [shapes(1, dim)] * 6
        moving = [pl.BlockSpec((v.shape[0] // n_chips, v.shape[1]), lambda i: (i, 0)) for v in large]
        fixed = lambda vs: [pl.BlockSpec(v.shape, lambda i, n=len(v.shape): (0,) * n) for v in vs]
        res = pl.pallas_call(
            finish, name='finish', out_shape=large + small, grid=(n_chips,), in_specs=moving + fixed(outs[6:8]),
            out_specs=moving + fixed(small), compiler_params=pltpu.CompilerParams(vmem_limit_bytes=VMEM_LIMIT),
        )(*outs[:8])
        y_out, grad_x, grad_w_up, grad_w_down, gq, go, grad_b_qkv, grad_b_up = res[:8]
        v = [t.reshape(dim) for t in res[8:]]
        return (y_out.reshape(x_in.shape), grad_x.reshape(x_in.shape), v[0], v[1], gq.reshape(3, heads, hd, dim).transpose(0, 3, 1, 2),
                grad_b_qkv, go.reshape(heads, hd, dim), v[2], v[3], v[4], grad_w_up, grad_b_up.reshape(ffn), grad_w_down, v[5])

    return jax.shard_map(device_step, mesh=mesh, in_specs=in_specs, out_specs=out_specs, check_vma=False)
```
